32 devices in a mesh: dp: 8 (over z, core), fsdp: 4 (over y, x).
Axes of the slice: x: 2, y: 2, z: 4, core: 2. Of those that a mesh axis runs over, the one named last changes fastest.
Arguments:
- tokens: bfloat16 [32, 1024, 768], P(('dp', 'fsdp')), may hold values from -8 to 8
- hidden_token_indicator: int32 [32, 1024], P(('dp', 'fsdp')), may hold values 0 or 1
- lengths: int32 [32], P(('dp', 'fsdp')), may hold values from 256 to 1024, as said below
- time_ids: int32 [32], P(('dp', 'fsdp')), may hold values from 0 to 999
- cotangent: bfloat16 [32, 1024, 768], P(('dp', 'fsdp')), may hold values from -6 to 6
- gain_one: bfloat16 [768], P('fsdp'), may hold values from 0.5 to 1.5
- w_qkv: bfloat16 [768, 2304], P('fsdp'), may hold values from -0.21875 to 0.21875
- w_out: bfloat16 [768, 768], P('fsdp'), may hold values from -0.875 to 0.875
- gain_two: bfloat16 [768], P('fsdp'), may hold values from 0.5 to 1.5
- w_fc1: bfloat16 [768, 3072], P('fsdp'), may hold values from -0.21875 to 0.21875
- b_fc1: bfloat16 [3072], P('fsdp'), may hold values from -3 to 3
- w_fc2: bfloat16 [3072, 768], P('fsdp'), may hold values from -0.109375 to 0.109375
- b_fc2: bfloat16 [768], P('fsdp'), may hold values from -3 to 3
- w_ada: bfloat16 [4608, 128], P('fsdp'), may hold values from -0.5 to 0.5
- b_ada: bfloat16 [4608], P('fsdp'), may hold values from -3 to 3
- mask_embed: bfloat16 [768], P('fsdp'), may hold values from -5 to 5
- time_table: float32 [1000, 128], replicated, may hold values from -5 to 5
Outputs:
- output: bfloat16 [32, 1024, 768], P(('dp', 'fsdp'))
- input_grad: bfloat16 [32, 1024, 768], P(('dp', 'fsdp'))
- gain_one_grad: float32 [768], P('fsdp')
- w_qkv_grad: float32 [768, 2304], P('fsdp')
- w_out_grad: float32 [768, 768], P('fsdp')
- gain_two_grad: float32 [768], P('fsdp')
- w_fc1_grad: float32 [768, 3072], P('fsdp')
- b_fc1_grad: float32 [3072], P('fsdp')
- w_fc2_grad: float32 [3072, 768], P('fsdp')
- b_fc2_grad: float32 [768], P('fsdp')
- w_ada_grad: float32 [4608, 128], P('fsdp')
- b_ada_grad: float32 [4608], P('fsdp')
- mask_embed_grad: float32 [768], P('fsdp')
- time_table_grad: float32 [1000, 128], replicated
- rms_stats: float32 [3], replicated
The draws below stay inside these ranges and needn't reach their ends.
Inputs may be any that keep to these rules, and one draw needn't show every extreme that they name: `lengths`: the valid tokens of a sequence are its leading positions; in every draw some sequence has all 1024 valid.
All inputs are finite; a program needn't handle non-finite values. No bound on the sum of `hidden_token_indicator` on one device may be relied on, other than what follows from the above.
Results may differ from the reference program's by a relative error of at most 0.02.
Values may be sent and summed in bfloat16 or wider, within the bound.
A program may use at most 192 MiB of HBM per device.

```python
import jax
import jax.numpy as jnp
from jax import lax

D = 768
HD = 64
FF = 3072
COND = 128
NT = 1000
SEQ = 1024
SEQS = 32


def draw_lengths(key, part):
    key_short, key_long, key_pick, key_full = jax.random.split(key, 4)
    short_len = jax.random.randint(key_short, (SEQS,), SEQ // 4, SEQ // 2 + 1)
    long_len = jax.random.randint(key_long, (SEQS,), SEQ // 2, SEQ + 1)
    chooser = jax.random.randint(key_pick, (SEQS,), 0, 2)
    picked = jnp.where(chooser == 1, long_len, short_len)
    full_index = jax.random.randint(key_full, (), 0, SEQS)
    picked = jnp.where(jnp.arange(SEQS) == full_index, SEQ, picked)
    return picked.astype(jnp.int32)


def draw_tokens(key, part):
    key_base = jax.random.fold_in(key, 0)
    ladder = 0.5 * 4.0 ** (jnp.arange(SEQS, dtype=jnp.float32) / max(SEQS - 1, 1))
    values = jnp.clip(jax.random.normal(key_base, (SEQS, SEQ, D), jnp.float32), -4.0, 4.0)
    return (values * ladder[:, None, None]).astype(jnp.bfloat16)


def plant(result, key, smallest, largest):
    index_at = [jax.random.randint(jax.random.fold_in(key, axis), (), 0, length) for axis, length in enumerate(result.shape)]
    widest = result.shape.index(max(result.shape))
    neighbour = index_at[:widest] + [(index_at[widest] + 1) % result.shape[widest]] + index_at[widest + 1:]
    return result.at[tuple(index_at)].set(smallest).at[tuple(neighbour)].set(largest)


def levels(stream_key, extent, pieces, least, high):
    factor_of, own = 1.0, jax.random.fold_in(stream_key, 6)
    for dim, shards_of in pieces:
        draws = jnp.exp(jax.random.uniform(jax.random.fold_in(own, dim), (shards_of,), jnp.float32, least / len(pieces), high / len(pieces)))
        factor_of = factor_of * jnp.repeat(draws, extent[dim] // shards_of).reshape([-1 if axis == dim else 1 for axis in range(len(extent))])
    return factor_of


def normal_values(own_key, extent, deviation, reach, cuts=(), kind=jnp.bfloat16):
    drawn = jax.random.normal(own_key, extent, jnp.float32) * deviation
    if len(cuts) > 0:
        drawn = levels(own_key, extent, cuts, -0.22, 0.18) * drawn
    return jnp.clip(drawn, min=-reach, max=reach).astype(kind)


def setup_inputs(seed: int = 0) -> dict:
    streams_of = jax.random.split(jax.random.key(seed), 18)
    return {
        "tokens": draw_tokens(jax.random.fold_in(streams_of[17], 71), 0),
        "hidden_token_indicator": plant((jax.random.randint(streams_of[1], (SEQS, SEQ), 0, 3) < 1).astype(jnp.int32), jax.random.fold_in(streams_of[1], 1), 0, 1),
        "lengths": draw_lengths(jax.random.fold_in(streams_of[17], 71), 0),
        "time_ids": plant(jax.random.randint(streams_of[3], (SEQS,), 0, NT), jax.random.fold_in(streams_of[3], 1), 0, NT - 1).astype(jnp.int32),
        "cotangent": normal_values(streams_of[4], (SEQS, SEQ, D), 1.0, 6.0, ((0, 32),)),
        "gain_one": jnp.clip(1.0 + 0.1 * jax.random.normal(streams_of[5], (D,), jnp.float32), 0.5, 1.5).astype(jnp.bfloat16),
        "w_qkv": normal_values(streams_of[6], (D, 3 * D), D ** -0.5, 0.21875, ((0, 4),)),
        "w_out": normal_values(streams_of[7], (D, D), (D // 16) ** -0.5, 0.875, ((0, 4),)),
        "gain_two": jnp.clip(1.0 + 0.1 * jax.random.normal(streams_of[8], (D,), jnp.float32), 0.5, 1.5).astype(jnp.bfloat16),
        "w_fc1": normal_values(streams_of[9], (D, FF), D ** -0.5, 0.21875, ((0, 4),)),
        "b_fc1": normal_values(streams_of[10], (FF,), 0.5, 3.0, ((0, 4),)),
        "w_fc2": normal_values(streams_of[11], (FF, D), FF ** -0.5, 0.109375, ((0, 4),)),
        "b_fc2": normal_values(streams_of[12], (D,), 0.5, 3.0, ((0, 4),)),
        "w_ada": normal_values(streams_of[13], (6 * D, COND), COND ** -0.5, 0.5, ((0, 4),)),
        "b_ada": normal_values(streams_of[14], (6 * D,), 0.5, 3.0, ((0, 4),)),
        "mask_embed": normal_values(streams_of[15], (D,), 1.0, 5.0, ((0, 4),)),
        "time_table": normal_values(streams_of[16], (NT, COND), 1.0, 5.0, (), jnp.float32),
    }


@jax.custom_vjp
def low(v):
    return lax.optimization_barrier(v.astype(jnp.bfloat16)).astype(jnp.float32)

@jax.custom_vjp
def low_back(v):
    return v

def low_keep(v):
    return (low(v), None)

def low_pass(kept, grad):
    return (grad,)

def back_keep(v):
    return (v, None)

def back_low(kept, grad):
    return (low(grad),)
low.defvjp(low_keep, low_pass)
low_back.defvjp(back_keep, back_low)
eps = 1e-05
highest = lax.Precision.HIGHEST

def layer_norm(values):
    centred = values - lax.optimization_barrier(jnp.mean(values, axis=-1, keepdims=True))
    return centred * lax.rsqrt(lax.optimization_barrier(jnp.mean(centred * centred, axis=-1, keepdims=True)) + eps)

def modulated(values, gain_vec, scale_vec, shift_vec):
    return layer_norm(values) * gain_vec * (1.0 + scale_vec) + shift_vec

def gelu_tanh(values):
    return jax.nn.gelu(values, approximate=True)

def rotary_tables(length, head_width):
    midpoint_span = head_width // 2
    position = jnp.arange(length, dtype=jnp.float32)
    reciprocal_factor = 1.0 / 10000.0 ** (jnp.arange(midpoint_span, dtype=jnp.float32) * 2.0 / head_width)
    angles = position[:, None] * reciprocal_factor[None, :]
    angles = jnp.concatenate([angles, angles], axis=-1)
    return (jnp.cos(angles)[:, None, :], jnp.sin(angles)[:, None, :])

def rotary(values, cosine_table, sine_table):
    midpoint_span = values.shape[-1] // 2
    turned = jnp.concatenate([-values[..., midpoint_span:], values[..., :midpoint_span]], axis=-1)
    return values * cosine_table + turned * sine_table

def dense_map(left, right):
    return jnp.einsum('gsi,ij->gsj', left, right, precision=highest)

def attention_heads(queries, keys_rot, values_in, key_valid):
    score_scale = HD ** (-0.5)

    def one_head(argument_bundle):
        query_per_head, lookup_vectors_each_branch, value_per_head = argument_bundle
        raw_scores = jnp.einsum('gqd,gkd->gqk', query_per_head, lookup_vectors_each_branch, precision=highest) * score_scale
        scores = low_back(jnp.where(key_valid, raw_scores, -1e+30))
        total_log = jax.nn.logsumexp(scores, axis=-1, keepdims=True)
        attention_weights = low(jnp.exp(scores - total_log))
        return jnp.einsum('gqk,gkd->gqd', attention_weights, value_per_head, precision=highest)
    return lax.map(jax.checkpoint(one_head), (queries, keys_rot, values_in))

def layer_forward(params, tokens_in, mask_rows, seq_lengths, step_ids):
    gain_one, w_qkv, w_out, gain_two, w_fc1, b_fc1, w_fc2, b_fc2, w_ada, b_ada, mask_embed, time_table = params
    partition_list, length, model_width = tokens_in.shape
    head_count = model_width // HD
    hidden0 = jnp.where(mask_rows[..., None] == 1, mask_embed, tokens_in)
    cond_vec = jax.nn.silu(time_table[step_ids])
    modulation = jnp.dot(cond_vec, w_ada.T, precision=highest) + b_ada
    shift_a, scale_a, gate_a, shift_m, scale_m, gate_m = jnp.split(modulation[:, None, :], 6, axis=-1)
    norm_one = low(modulated(hidden0, gain_one, scale_a, shift_a))
    projected = low_back(dense_map(norm_one, w_qkv))
    cosine_table, sine_table = rotary_tables(length, HD)

    def head_major(values):
        return values.reshape(partition_list, length, head_count, HD)
    queries = low(rotary(head_major(projected[..., :model_width]), cosine_table, sine_table))
    keys_rot = low(rotary(head_major(projected[..., model_width:2 * model_width]), cosine_table, sine_table))
    values_in = low(head_major(projected[..., 2 * model_width:]))
    key_valid = jnp.arange(length)[None, None, :] < seq_lengths[:, None, None]
    stacked = attention_heads(queries.transpose(2, 0, 1, 3), keys_rot.transpose(2, 0, 1, 3), values_in.transpose(2, 0, 1, 3), key_valid)
    attended = stacked.transpose(1, 2, 0, 3).reshape(partition_list, length, model_width)
    attended = low_back(low(attended))
    attn_proj = low_back(dense_map(attended, w_out))
    branch_a = gate_a * attn_proj
    hidden1 = hidden0 + branch_a
    norm_two = low(modulated(hidden1, gain_two, scale_m, shift_m))
    hidden_pre = low_back(dense_map(norm_two, w_fc1) + b_fc1)
    active = low(gelu_tanh(hidden_pre))
    mlp_proj = low_back(dense_map(active, w_fc2) + b_fc2)
    branch_m = gate_m * mlp_proj
    return (hidden1 + branch_m, branch_a, branch_m)

def reference(tokens, hidden_token_indicator, lengths, time_ids, cotangent, gain_one, w_qkv, w_out, gain_two, w_fc1, b_fc1, w_fc2, b_fc2, w_ada, b_ada, mask_embed, time_table):
    group_size = 4 if SEQS % 4 == 0 else 1
    group_count = SEQS // group_size
    params = tuple((weight_in.astype(jnp.float32) for weight_in in (gain_one, w_qkv, w_out, gain_two, w_fc1, b_fc1, w_fc2, b_fc2, w_ada, b_ada, mask_embed, time_table)))

    def regroup(source):
        return source.reshape((group_count, group_size) + source.shape[1:])

    def step_group(carried, group_batch):
        grad_sums, stat_sums = carried
        tok_group, flag_group, len_group, time_group, cot_group = group_batch

        def closed(param_set, incoming_symbol_ids):
            return layer_forward(param_set, incoming_symbol_ids, flag_group, len_group, time_group)
        outputs, pullback = jax.vjp(closed, params, tok_group.astype(jnp.float32))
        block_out, branch_a, branch_m = outputs
        grad_params, grad_tokens = pullback((cot_group.astype(jnp.float32), jnp.zeros_like(branch_a), jnp.zeros_like(branch_m)))
        valid_rows = (jnp.arange(SEQ)[None, :] < len_group[:, None]).astype(jnp.float32)[..., None]
        partial_sums = jnp.stack([jnp.sum(valid_rows * block_out * block_out), jnp.sum(valid_rows * branch_a * branch_a), jnp.sum(valid_rows * branch_m * branch_m)])
        grad_sums = jax.tree.map(lambda running, added: running + added, grad_sums, grad_params)
        return ((grad_sums, stat_sums + partial_sums), (block_out.astype(jnp.bfloat16), grad_tokens.astype(jnp.bfloat16)))
    initial = (tuple((jnp.zeros_like(weight_in) for weight_in in params)), jnp.zeros((3,), jnp.float32))
    (grad_sums, stat_sums), (out_rows, grad_rows) = lax.scan(step_group, initial, (regroup(tokens), regroup(hidden_token_indicator), regroup(lengths), regroup(time_ids), regroup(cotangent)))
    valid_count = jnp.sum(lengths).astype(jnp.float32)
    rms_stats = jnp.sqrt(stat_sums / (valid_count * D))
    return (out_rows.reshape(tokens.shape), grad_rows.reshape(tokens.shape), grad_sums[0], grad_sums[1], grad_sums[2], grad_sums[3], grad_sums[4], grad_sums[5], grad_sums[6], grad_sums[7], grad_sums[8], grad_sums[9], grad_sums[10], grad_sums[11], rms_stats)
```

```python
import functools, math
import jax, jax.numpy as jnp
from jax import lax
from jax.experimental import pallas as pl
from jax.experimental.pallas import tpu as pltpu

HD = 64
EPS = 1e-5
LOG2E = math.log2(math.e)
QSCALE = LOG2E * HD ** -0.5
f32, bf16 = jnp.float32, jnp.bfloat16
NT = (((1,), (1,)), ((), ()))
NN = (((1,), (0,)), ((), ()))
TN = (((0,), (0,)), ((), ()))

def dot(a, b, dims=NN):
    return lax.dot_general(a, b, dims, preferred_element_type=f32)

def norm_parts(x):
    mean = jnp.mean(x, axis=-1, keepdims=True)
    cen = x - mean
    rs = lax.rsqrt(jnp.mean(cen * cen, axis=-1, keepdims=True) + EPS)
    return cen * rs, rs

def swap_halves(u):
    lane = lax.broadcasted_iota(jnp.int32, u.shape, 1)
    return jnp.where(lane % HD < HD // 2, pltpu.roll(u, 96, 1), pltpu.roll(u, 32, 1))

def pre_kernel(tok_ref, flag_ref, vec_ref, w_ref, cos_ref, sin_ref, n1_ref, qkv_ref):
    emb, gain, scale, shift = (vec_ref[i:i + 1, :] for i in range(4))
    h0 = jnp.where(flag_ref[...] == 1, emb, tok_ref[...].astype(f32))
    n, _ = norm_parts(h0)
    n1 = (n * gain * (1.0 + scale) + shift).astype(bf16)
    n1_ref[...] = n1
    d = n1.shape[1]
    cos, sin = cos_ref[...], sin_ref[...]
    for part in range(3):
        y = dot(n1, w_ref[:, part * d:(part + 1) * d])
        for c in range(d // 128):
            lo = part * d + c * 128
            u = y[:, c * 128:(c + 1) * 128]
            if part < 2:
                u = u * cos + swap_halves(u) * sin
                if part == 0:
                    u = u * QSCALE
            qkv_ref[:, lo:lo + 128] = u.astype(bf16)

def pre_call(tok, flag, vecs, w, cos, sin, rows=256):
    s, d = tok.shape
    return pl.pallas_call(
        pre_kernel, grid=(s // rows,),
        in_specs=[pl.BlockSpec((rows, d), lambda i: (i, 0)), pl.BlockSpec((rows, 1), lambda i: (i, 0)),
                  pl.BlockSpec((8, d), lambda i: (0, 0)), pl.BlockSpec((d, 3 * d), lambda i: (0, 0)),
                  pl.BlockSpec((rows, 128), lambda i: (i, 0)), pl.BlockSpec((rows, 128), lambda i: (i, 0))],
        out_specs=[pl.BlockSpec((rows, d), lambda i: (i, 0)), pl.BlockSpec((rows, 3 * d), lambda i: (i, 0))],
        out_shape=[jax.ShapeDtypeStruct((s, d), bf16), jax.ShapeDtypeStruct((s, 3 * d), bf16)],
        cost_estimate=pl.CostEstimate(flops=2 * s * d * 3 * d, bytes_accessed=12 * s * d, transcendentals=0),
        name="pre")(tok, flag, vecs, w, cos, sin)

def attn_fwd_kernel(len_ref, q_ref, k_ref, v_ref, o_ref, lse_ref, *, rows):
    p = pl.program_id(0)
    s = q_ref.shape[0]
    length = len_ref[0]
    lane = lax.broadcasted_iota(jnp.int32, (s, 128), 1)
    pos = lax.broadcasted_iota(jnp.int32, (s, 128), 0)
    lane_q = lax.broadcasted_iota(jnp.int32, (rows, 128), 1)
    k = k_ref[...].astype(f32)
    v = v_ref[...].astype(f32)
    kx, vx = [], []
    for h in (0, 1):
        extra = HD * (1 - h)
        mine = (lane >= HD) if h else (lane < HD)
        bias = jnp.where(pos >= length, -1e30, 0.0)
        kx.append(jnp.where(mine, k, jnp.where(lane == extra, bias, 0.0)).astype(bf16))
        vx.append(jnp.where(mine, v, jnp.where(lane == extra, 1.0, 0.0)).astype(bf16))
    for b in range(s // rows):
        q = q_ref[b * rows:(b + 1) * rows, :].astype(f32)
        outs, lses = [], []
        for h in (0, 1):
            extra = HD * (1 - h)
            mine = (lane_q >= HD) if h else (lane_q < HD)
            qx = jnp.where(mine, q, jnp.where(lane_q == extra, 1.0, 0.0)).astype(bf16)
            sc = dot(qx, kx[h], NT)
            m = jnp.max(sc, axis=1, keepdims=True)
            pr = jnp.exp2(sc - m).astype(bf16)
            o = dot(pr, vx[h])
            tot = o[:, extra:extra + 1]
            outs.append(o * (1.0 / tot))
            lses.append(m + jnp.log(tot) * LOG2E)
        o_ref[b * rows:(b + 1) * rows, :] = jnp.where(lane_q < HD, outs[0], outs[1]).astype(bf16)
        old = jnp.where(p == 0, 0.0, lse_ref[b * rows:(b + 1) * rows, :])
        lse_ref[b * rows:(b + 1) * rows, :] = jnp.where(
            lane_q == 2 * p, lses[0], jnp.where(lane_q == 2 * p + 1, lses[1], old))

def attn_fwd_call(length, qkv, rows=256):
    s, d3 = qkv.shape
    d = d3 // 3
    np_ = d // 128
    return pl.pallas_call(
        functools.partial(attn_fwd_kernel, rows=rows), grid=(np_,),
        in_specs=[pl.BlockSpec(memory_space=pltpu.SMEM),
                  pl.BlockSpec((s, 128), lambda i: (0, i)),
                  pl.BlockSpec((s, 128), lambda i: (0, np_ + i)),
                  pl.BlockSpec((s, 128), lambda i: (0, 2 * np_ + i))],
        out_specs=[pl.BlockSpec((s, 128), lambda i: (0, i)), pl.BlockSpec((s, 128), lambda i: (0, 0))],
        out_shape=[jax.ShapeDtypeStruct((s, d), bf16), jax.ShapeDtypeStruct((s, 128), f32)],
        cost_estimate=pl.CostEstimate(flops=8 * s * s * d, bytes_accessed=8 * s * d, transcendentals=s * s * 12),
        name="attn_fwd")(length, qkv, qkv, qkv)

def split3(x):
    hi = x.astype(bf16).astype(f32)
    r = x - hi
    mid = r.astype(bf16).astype(f32)
    return hi, mid, r - mid

def attn_bwd_kernel(len_ref, q_ref, k_ref, v_ref, o_ref, g_ref, lse_ref, cos_ref, sin_ref,
                    dq_ref, dk_ref, dv_ref, dqs, *, rows):
    p = pl.program_id(0)
    s = q_ref.shape[0]
    length = len_ref[0]
    lane = lax.broadcasted_iota(jnp.int32, (s, 128), 1)
    pos = lax.broadcasted_iota(jnp.int32, (s, 128), 0)
    lane_q = lax.broadcasted_iota(jnp.int32, (rows, 128), 1)
    k = k_ref[...].astype(f32)
    v = v_ref[...].astype(f32)
    bias = jnp.where(pos >= length, -1e30, 0.0)
    dks, dvs = [], []
    for h in (0, 1):
        e = HD * (1 - h)
        mine = (lane >= HD) if h else (lane < HD)
        mine_q = (lane_q >= HD) if h else (lane_q < HD)
        ones = jnp.where((lane >= e) & (lane < e + 3), 1.0, 0.0)
        kx = jnp.where(mine, k, jnp.where(lane == e + 3, bias, ones)).astype(bf16)
        vx = jnp.where(mine, v, ones).astype(bf16)
        kt = jnp.where(mine, k, 0.0).T.astype(bf16)
        dk = jnp.zeros((s, 128), f32)
        dv = jnp.zeros((s, 128), f32)
        for b in range(s // rows):
            sl = slice(b * rows, (b + 1) * rows)
            qb = q_ref[sl, :]
            gb = g_ref[sl, :]
            q = qb.astype(f32)
            g = gb.astype(f32)
            lse = jnp.sum(jnp.where(lane_q == 2 * p + h, lse_ref[sl, :], 0.0), axis=1, keepdims=True)
            dd = jnp.sum(jnp.where(mine_q, g * o_ref[sl, :].astype(f32), 0.0), axis=1, keepdims=True)
            l0, l1, l2 = split3(-lse)
            d0, d1, d2 = split3(-dd)
            qx = jnp.where(mine_q, q, jnp.where(lane_q == e, l0, jnp.where(lane_q == e + 1, l1, jnp.where(
                lane_q == e + 2, l2, jnp.where(lane_q == e + 3, 1.0, 0.0))))).astype(bf16)
            gx = jnp.where(mine_q, g, jnp.where(lane_q == e, d0, jnp.where(lane_q == e + 1, d1, jnp.where(
                lane_q == e + 2, d2, 0.0)))).astype(bf16)
            pt = jnp.exp2(dot(kx, qx, NT))
            dst = (pt * dot(vx, gx, NT)).astype(bf16)
            dv = dv + dot(pt.astype(bf16), gb)
            dk = dk + dot(dst, qb)
            dqt = dot(kt, dst)
            if h == 0:
                dqs[:, sl] = dqt
            else:
                dqs[:, sl] = dqs[:, sl] + dqt
        dks.append(dk)
        dvs.append(dv)
    cos, sin = cos_ref[...], sin_ref[...]
    dq = dqs[...].T * (HD ** -0.5)
    dk = jnp.where(lane < HD, dks[0], dks[1]) * (1.0 / LOG2E)
    dq_ref[...] = (dq * cos - swap_halves(dq) * sin).astype(bf16)
    dk_ref[...] = (dk * cos - swap_halves(dk) * sin).astype(bf16)
    dv_ref[...] = jnp.where(lane < HD, dvs[0], dvs[1]).astype(bf16)

def attn_bwd_call(length, qkv, att, gatt, lse, cos, sin, rows=256):
    s, d3 = qkv.shape
    d = d3 // 3
    np_ = d // 128
    col = pl.BlockSpec((s, 128), lambda i: (0, i))
    const = pl.BlockSpec((s, 128), lambda i: (0, 0))
    return pl.pallas_call(
        functools.partial(attn_bwd_kernel, rows=rows), grid=(np_,),
        in_specs=[pl.BlockSpec(memory_space=pltpu.SMEM), col,
                  pl.BlockSpec((s, 128), lambda i: (0, np_ + i)),
                  pl.BlockSpec((s, 128), lambda i: (0, 2 * np_ + i)), col, col, const, const, const],
        out_specs=[col, col, col],
        out_shape=[jax.ShapeDtypeStruct((s, d), bf16)] * 3,
        scratch_shapes=[pltpu.VMEM((128, s), f32)],
        cost_estimate=pl.CostEstimate(flops=20 * s * s * d, bytes_accessed=16 * s * d, transcendentals=s * s * 12),
        name="attn_bwd")(length, qkv, qkv, qkv, att, gatt, lse, cos, sin)

def gelu_both(v):
    a, b = 0.7978845608028654, 0.044715
    v2 = v * v
    t = jnp.tanh(a * v * (1.0 + b * v2))
    half = 0.5 + 0.5 * t
    return v * half, half + (0.5 * a) * v * (1.0 - t * t) * (1.0 + 3.0 * b * v2)

def colsum(x):
    return jnp.sum(x, axis=0, keepdims=True)

def mid_kernel(len_ref, att_ref, tok_ref, flag_ref, cot_ref, vec_ref, b1_ref, wo_ref, w1_ref, w2_ref,
               out_ref, gh1_ref, gatt_ref, n2_ref, act_ref, gm_ref, gpre_ref, gap_ref, sum_ref, sb1_ref,
               gp_s, *, cut):
    i = pl.program_id(0)
    rows, d = att_ref.shape
    ff = w1_ref.shape[1]
    emb, gain, scale, shift, gate_a, gate_m, b2 = (vec_ref[r:r + 1, :] for r in range(7))
    h0 = jnp.where(flag_ref[...] == 1, emb, tok_ref[...].astype(f32))
    ap = dot(att_ref[...], wo_ref[...])
    br_a = gate_a * ap
    h1 = h0 + br_a
    n, rs = norm_parts(h1)
    n2 = (n * gain * (1.0 + scale) + shift).astype(bf16)
    n2_ref[...] = n2
    mp = jnp.zeros((rows, d), f32) + b2
    for j in range(ff // cut):
        sl = slice(j * cut, (j + 1) * cut)
        act, gp = gelu_both(dot(n2, w1_ref[:, sl]) + b1_ref[:, sl])
        act = act.astype(bf16)
        act_ref[:, sl] = act
        gp_s[:, sl] = gp
        mp = mp + dot(act, w2_ref[sl, :])
    br_m = gate_m * mp
    bo = h1 + br_m
    out_ref[...] = bo.astype(bf16)
    pos = lax.broadcasted_iota(jnp.int32, (rows, 1), 0) + i * rows
    valid = jnp.where(pos < len_ref[0], 1.0, 0.0)
    cot = cot_ref[...].astype(f32)
    gm = (gate_m * cot).astype(bf16)
    gm_ref[...] = gm
    gn2 = jnp.zeros((rows, d), f32)
    sb1 = []
    for j in range(ff // cut):
        sl = slice(j * cut, (j + 1) * cut)
        gpre = (dot(gm, w2_ref[sl, :], NT) * gp_s[:, sl]).astype(bf16)
        gpre_ref[:, sl] = gpre
        sb1.append(colsum(gpre.astype(f32)))
        gn2 = gn2 + dot(gpre, w1_ref[:, sl], NT)
    e = gn2 * (gain * (1.0 + scale))
    gh1 = cot + rs * (e - jnp.mean(e, axis=1, keepdims=True) - n * jnp.mean(e * n, axis=1, keepdims=True))
    gh1_ref[...] = gh1
    gap = (gate_a * gh1).astype(bf16)
    gap_ref[...] = gap
    gatt_ref[...] = dot(gap, wo_ref[...], NT).astype(bf16)
    new = jnp.concatenate([
        colsum(cot * mp), colsum(gm.astype(f32)), colsum(gn2 * n), colsum(gn2), colsum(gh1 * ap),
        colsum(valid * bo * bo), colsum(valid * br_a * br_a), colsum(valid * br_m * br_m)], axis=0)
    sb1 = jnp.concatenate(sb1, axis=1)
    @pl.when(i == 0)
    def _():
        sum_ref[...] = new
        sb1_ref[...] = sb1
    @pl.when(i > 0)
    def _():
        sum_ref[...] += new
        sb1_ref[...] += sb1

def mid_call(length, att, tok, flag, cot, vec, b1, wo, w1, w2, rows=256, cut=768):
    s, d = tok.shape
    ff = w1.shape[1]
    row = lambda c: pl.BlockSpec((rows, c), lambda i: (i, 0))
    whole = lambda a: pl.BlockSpec(a.shape, lambda i: (0, 0))
    sd = jax.ShapeDtypeStruct
    return pl.pallas_call(
        functools.partial(mid_kernel, cut=cut), grid=(s // rows,),
        in_specs=[pl.BlockSpec(memory_space=pltpu.SMEM), row(d), row(d), row(1), row(d), whole(vec), whole(b1),
                  whole(wo), whole(w1), whole(w2)],
        out_specs=[row(d), row(d), row(d), row(d), row(ff), row(d), row(ff), row(d),
                   pl.BlockSpec((8, d), lambda i: (0, 0)), pl.BlockSpec((1, ff), lambda i: (0, 0))],
        out_shape=[sd((s, d), bf16), sd((s, d), f32), sd((s, d), bf16), sd((s, d), bf16), sd((s, ff), bf16),
                   sd((s, d), bf16), sd((s, ff), bf16), sd((s, d), bf16), sd((8, d), f32), sd((1, ff), f32)],
        scratch_shapes=[pltpu.VMEM((rows, ff), f32)],
        compiler_params=pltpu.CompilerParams(vmem_limit_bytes=60000 * 1024),
        cost_estimate=pl.CostEstimate(flops=2 * s * d * (2 * d + 4 * ff), bytes_accessed=30 * s * d,
                                      transcendentals=s * ff),
        name="mid")(length, att, tok, flag, cot, vec, b1, wo, w1, w2)

def post_kernel(dq_ref, dk_ref, dv_ref, tok_ref, flag_ref, gh1_ref, vec_ref, w_ref, ig_ref, sum_ref):
    i = pl.program_id(0)
    d = tok_ref.shape[1]
    emb, gain, scale = (vec_ref[r:r + 1, :] for r in range(3))
    masked = flag_ref[...] == 1
    h0 = jnp.where(masked, emb, tok_ref[...].astype(f32))
    n, rs = norm_parts(h0)
    gn1 = dot(dq_ref[...], w_ref[:, :d], NT) + dot(dk_ref[...], w_ref[:, d:2 * d], NT) + dot(
        dv_ref[...], w_ref[:, 2 * d:], NT)
    e = gn1 * (gain * (1.0 + scale))
    gh0 = gh1_ref[...] + rs * (e - jnp.mean(e, axis=1, keepdims=True) - n * jnp.mean(e * n, axis=1, keepdims=True))
    ig_ref[...] = jnp.where(masked, 0.0, gh0).astype(bf16)
    zero = jnp.zeros((5, d), f32)
    new = jnp.concatenate([colsum(gn1 * n), colsum(gn1), colsum(jnp.where(masked, gh0, 0.0)), zero], axis=0)
    @pl.when(i == 0)
    def _():
        sum_ref[...] = new
    @pl.when(i > 0)
    def _():
        sum_ref[...] += new

def post_call(dq, dk, dv, tok, flag, gh1, vec, w, rows=256):
    s, d = tok.shape
    row = lambda c: pl.BlockSpec((rows, c), lambda i: (i, 0))
    whole = lambda a: pl.BlockSpec(a.shape, lambda i: (0, 0))
    sd = jax.ShapeDtypeStruct
    return pl.pallas_call(
        post_kernel, grid=(s // rows,),
        in_specs=[row(d), row(d), row(d), row(d), row(1), row(d), whole(vec), whole(w)],
        out_specs=[row(d), pl.BlockSpec((8, d), lambda i: (0, 0))],
        out_shape=[sd((s, d), bf16), sd((8, d), f32)],
        cost_estimate=pl.CostEstimate(flops=6 * s * d * d, bytes_accessed=16 * s * d, transcendentals=0),
        name="post")(dq, dk, dv, tok, flag, gh1, vec, w)

def wgrad_kernel(a_ref, b_ref, o_ref):
    o_ref[...] = dot(a_ref[...], b_ref[...], TN).astype(bf16)

def wgrad_call(a, b, cols=768, bcols=768):
    s, m = a.shape
    n = b.shape[1]
    return pl.pallas_call(
        wgrad_kernel, grid=(m // cols, n // bcols),
        in_specs=[pl.BlockSpec((s, cols), lambda i, j: (0, i)), pl.BlockSpec((s, bcols), lambda i, j: (0, j))],
        out_specs=pl.BlockSpec((cols, bcols), lambda i, j: (i, j)),
        out_shape=jax.ShapeDtypeStruct((m, n), bf16),
        cost_estimate=pl.CostEstimate(flops=2 * s * m * n, bytes_accessed=2 * (s * (m + n) + m * n),
                                      transcendentals=0),
        name="wgrad")(a, b)
from jax.sharding import PartitionSpec as P

highest = lax.Precision.HIGHEST


def rotary_tables(length):
    half = HD // 2
    rate = 1.0 / 10000.0 ** (jnp.arange(half, dtype=f32) * 2.0 / HD)
    angle = jnp.arange(length, dtype=f32)[:, None] * rate[None, :]
    angle = jnp.concatenate([angle] * (128 // half), axis=-1)
    sign = jnp.where(jnp.arange(128) % HD < half, -1.0, 1.0)
    return jnp.cos(angle), jnp.sin(angle) * sign


def per_device(shape, tokens, hidden_token_indicator, lengths, time_ids, cotangent, gain_one, w_qkv, w_out, gain_two,
               w_fc1, b_fc1, w_fc2, b_fc2, w_ada, b_ada, mask_embed, time_table):
    groups = shape["fsdp"]
    s, d = tokens.shape[1:]
    ff = b_fc1.shape[0] * groups
    gather = lambda w: lax.all_gather(w, "fsdp", axis=0, tiled=True)
    tok, cot = tokens[0], cotangent[0]
    flag = hidden_token_indicator.reshape(s, 1)
    sizes = [v.shape[0] for v in (gain_one, gain_two, b_fc2, mask_embed, b_fc1, b_ada)]
    packed = gather(jnp.concatenate([gain_one, gain_two, b_fc2, mask_embed, b_fc1, b_ada])[None])
    cuts = [sum(sizes[:i]) for i in range(len(sizes) + 1)]
    gain1, gain2, b2, emb, b1, bada = (
        packed[:, cuts[i]:cuts[i + 1]].reshape(1, -1).astype(f32) for i in range(len(sizes)))
    ada_all, qkv_all, out_all, fc1_all, fc2_all = (gather(w) for w in (w_ada, w_qkv, w_out, w_fc1, w_fc2))
    cond_pre = lax.dynamic_slice_in_dim(time_table, time_ids[0], 1, axis=0)
    cond = jax.nn.silu(cond_pre)
    modulation = jnp.dot(cond, ada_all.astype(f32).T, precision=highest) + bada
    shift_a, scale_a, gate_a, shift_m, scale_m, gate_m = (modulation[:, i * d:(i + 1) * d] for i in range(6))
    cos, sin = rotary_tables(s)
    zero = jnp.zeros((1, d), f32)
    vec_pre = jnp.concatenate([emb, gain1, scale_a, shift_a] + [zero] * 4, axis=0)
    vec_mid = jnp.concatenate([emb, gain2, scale_m, shift_m, gate_a, gate_m, b2, zero], axis=0)
    n1, qkv = pre_call(tok, flag, vec_pre, qkv_all, cos, sin)
    att, lse = attn_fwd_call(lengths, qkv)
    out, gh1, gatt, n2, act, gm, gpre, gap, sums, gb1 = mid_call(
        lengths, att, tok, flag, cot, vec_mid, b1, out_all, fc1_all, fc2_all)
    g_fc2 = wgrad_call(act, gm)
    g_fc1 = wgrad_call(n2, gpre)
    g_out = wgrad_call(att, gap)
    dq, dk, dv = attn_bwd_call(lengths, qkv, att, gatt, lse, cos, sin)
    g_qkv = jnp.concatenate([wgrad_call(n1, x) for x in (dq, dk, dv)], axis=1)
    igrad, sums1 = post_call(dq, dk, dv, tok, flag, gh1, vec_pre, qkv_all)
    ggm, gb2, a2, s2, gga, st0, st1, st2 = (sums[i:i + 1] for i in range(8))
    a1, s1, gemb = (sums1[i:i + 1] for i in range(3))
    gmod = jnp.concatenate([s1, a1 * gain1, gga, s2, a2 * gain2, ggm], axis=1)
    small = jnp.concatenate([(1.0 + scale_a) * a1, (1.0 + scale_m) * a2, gb2, gemb, gb1, gmod], axis=1)
    stats = jnp.concatenate([jnp.sum(st0).reshape(1, 1), jnp.sum(st1).reshape(1, 1), jnp.sum(st2).reshape(1, 1),
                             lengths.astype(f32).reshape(1, 1), time_ids.astype(f32).reshape(1, 1)], axis=1)
    row = jnp.concatenate([small, cond_pre, stats, jnp.zeros((1, 123), f32)], axis=1)
    rows = lax.all_gather(row, ("dp", "fsdp"), axis=0, tiled=True)
    width = small.shape[1]
    conds, tail = rows[:, width:width + cond.shape[1]], rows[:, width + cond.shape[1]:]
    gmods = rows[:, width - gmod.shape[1]:width]
    silu_c, pull = jax.vjp(jax.nn.silu, conds)
    grad_cond = pull(jnp.dot(gmods, ada_all.astype(f32), precision=highest))[0]
    hot = (jnp.arange(time_table.shape[0])[:, None] == tail[:, 4].astype(jnp.int32)[None, :]).astype(f32)
    table = jnp.dot(hot, grad_cond, precision=highest)
    totals = jnp.sum(tail[:, :4], axis=0)
    rms = jnp.sqrt(totals[:3] / (totals[3] * d))
    me = lax.axis_index("fsdp")
    parts, base = [], 0
    for size in sizes:
        parts.append(jnp.sum(lax.dynamic_slice_in_dim(rows, base + me * size, size, axis=1), axis=0))
        base += size * groups
    g1, g2, gb2, gemb, gb1, gbada = parts
    n_ada = w_ada.shape[0]
    mods = lax.dynamic_slice_in_dim(rows, width - gmod.shape[1] + me * n_ada, n_ada, axis=1)
    g_ada = lax.dot_general(mods, silu_c, (((0,), (0,)), ((), ())), precision=highest)

    def reduce(g):
        part = lax.psum_scatter(g, "fsdp", scatter_dimension=0, tiled=True)
        return lax.psum(part, "dp").astype(f32)

    return (out[None], igrad[None], g1, reduce(g_qkv), reduce(g_out), g2, reduce(g_fc1), gb1, reduce(g_fc2), gb2,
            g_ada, gbada, gemb, table, rms)


def solution(mesh):
    both = ("dp", "fsdp")
    f1, f2 = P("fsdp"), P("fsdp", None)
    placed = (P(both, None, None), P(both, None), P(both), P(both), P(both, None, None), f1, f2, f2, f1, f2, f1, f2, f1,
              f2, f1, f1, P())
    outs = (P(both, None, None), P(both, None, None), f1, f2, f2, f1, f2, f1, f2, f1, f2, f1, f1, P(), P())
    return jax.shard_map(functools.partial(per_device, dict(mesh.shape)), mesh=mesh, in_specs=placed, out_specs=outs,
                         check_vma=False)
```

```python
import functools, math
import jax, jax.numpy as jnp
from jax import lax
from jax.experimental import pallas as pl
from jax.experimental.pallas import tpu as pltpu

HD = 64
EPS = 1e-5
LOG2E = math.log2(math.e)
QSCALE = LOG2E * HD ** -0.5
f32, bf16 = jnp.float32, jnp.bfloat16
NT = (((1,), (1,)), ((), ()))
NN = (((1,), (0,)), ((), ()))
TN = (((0,), (0,)), ((), ()))

def dot(a, b, dims=NN):
    return lax.dot_general(a, b, dims, preferred_element_type=f32)

def norm_parts(x):
    mean = jnp.mean(x, axis=-1, keepdims=True)
    cen = x - mean
    rs = lax.rsqrt(jnp.mean(cen * cen, axis=-1, keepdims=True) + EPS)
    return cen * rs, rs

def swap_halves(u):
    lane = lax.broadcasted_iota(jnp.int32, u.shape, 1)
    return jnp.where(lane % HD < HD // 2, pltpu.roll(u, 96, 1), pltpu.roll(u, 32, 1))

def pre_kernel(tok_ref, flag_ref, vec_ref, w_ref, cos_ref, sin_ref, n1_ref, qkv_ref):
    emb, gain, scale, shift = (vec_ref[i:i + 1, :] for i in range(4))
    h0 = jnp.where(flag_ref[...] == 1, emb, tok_ref[...].astype(f32))
    n, _ = norm_parts(h0)
    n1 = (n * gain * (1.0 + scale) + shift).astype(bf16)
    n1_ref[...] = n1
    d = n1.shape[1]
    cos, sin = cos_ref[...], sin_ref[...]
    for part in range(3):
        y = dot(n1, w_ref[:, part * d:(part + 1) * d])
        for c in range(d // 128):
            lo = part * d + c * 128
            u = y[:, c * 128:(c + 1) * 128]
            if part < 2:
                u = u * cos + swap_halves(u) * sin
                if part == 0:
                    u = u * QSCALE
            qkv_ref[:, lo:lo + 128] = u.astype(bf16)

def pre_call(tok, flag, vecs, w, cos, sin, rows=256):
    s, d = tok.shape
    return pl.pallas_call(
        pre_kernel, grid=(s // rows,),
        in_specs=[pl.BlockSpec((rows, d), lambda i: (i, 0)), pl.BlockSpec((rows, 1), lambda i: (i, 0)),
                  pl.BlockSpec((8, d), lambda i: (0, 0)), pl.BlockSpec((d, 3 * d), lambda i: (0, 0)),
                  pl.BlockSpec((rows, 128), lambda i: (i, 0)), pl.BlockSpec((rows, 128), lambda i: (i, 0))],
        out_specs=[pl.BlockSpec((rows, d), lambda i: (i, 0)), pl.BlockSpec((rows, 3 * d), lambda i: (i, 0))],
        out_shape=[jax.ShapeDtypeStruct((s, d), bf16), jax.ShapeDtypeStruct((s, 3 * d), bf16)],
        cost_estimate=pl.CostEstimate(flops=2 * s * d * 3 * d, bytes_accessed=12 * s * d, transcendentals=0),
        name="pre")(tok, flag, vecs, w, cos, sin)

def attn_fwd_kernel(len_ref, q_ref, k_ref, v_ref, o_ref, lse_ref, *, rows):
    p = pl.program_id(0)
    s = q_ref.shape[0]
    length = len_ref[0]
    lane = lax.broadcasted_iota(jnp.int32, (s, 128), 1)
    pos = lax.broadcasted_iota(jnp.int32, (s, 128), 0)
    lane_q = lax.broadcasted_iota(jnp.int32, (rows, 128), 1)
    k = k_ref[...].astype(f32)
    v = v_ref[...].astype(f32)
    kx, vx = [], []
    for h in (0, 1):
        extra = HD * (1 - h)
        mine = (lane >= HD) if h else (lane < HD)
        bias = jnp.where(pos >= length, -1e30, 0.0)
        kx.append(jnp.where(mine, k, jnp.where(lane == extra, bias, 0.0)).astype(bf16))
        vx.append(jnp.where(mine, v, jnp.where(lane == extra, 1.0, 0.0)).astype(bf16))
    for b in range(s // rows):
        q = q_ref[b * rows:(b + 1) * rows, :].astype(f32)
        outs, lses = [], []
        for h in (0, 1):
            extra = HD * (1 - h)
            mine = (lane_q >= HD) if h else (lane_q < HD)
            qx = jnp.where(mine, q, jnp.where(lane_q == extra, 1.0, 0.0)).astype(bf16)
            sc = dot(qx, kx[h], NT)
            m = jnp.max(sc, axis=1, keepdims=True)
            pr = jnp.exp2(sc - m).astype(bf16)
            o = dot(pr, vx[h])
            tot = o[:, extra:extra + 1]
            outs.append(o * (1.0 / tot))
            lses.append(m + jnp.log(tot) * LOG2E)
        o_ref[b * rows:(b + 1) * rows, :] = jnp.where(lane_q < HD, outs[0], outs[1]).astype(bf16)
        old = jnp.where(p == 0, 0.0, lse_ref[b * rows:(b + 1) * rows, :])
        lse_ref[b * rows:(b + 1) * rows, :] = jnp.where(
            lane_q == 2 * p, lses[0], jnp.where(lane_q == 2 * p + 1, lses[1], old))

def attn_fwd_call(length, qkv, rows=256):
    s, d3 = qkv.shape
    d = d3 // 3
    np_ = d // 128
    return pl.pallas_call(
        functools.partial(attn_fwd_kernel, rows=rows), grid=(np_,),
        in_specs=[pl.BlockSpec(memory_space=pltpu.SMEM),
                  pl.BlockSpec((s, 128), lambda i: (0, i)),
                  pl.BlockSpec((s, 128), lambda i: (0, np_ + i)),
                  pl.BlockSpec((s, 128), lambda i: (0, 2 * np_ + i))],
        out_specs=[pl.BlockSpec((s, 128), lambda i: (0, i)), pl.BlockSpec((s, 128), lambda i: (0, 0))],
        out_shape=[jax.ShapeDtypeStruct((s, d), bf16), jax.ShapeDtypeStruct((s, 128), f32)],
        cost_estimate=pl.CostEstimate(flops=8 * s * s * d, bytes_accessed=8 * s * d, transcendentals=s * s * 12),
        name="attn_fwd")(length, qkv, qkv, qkv)

def split3(x):
    hi = x.astype(bf16).astype(f32)
    r = x - hi
    mid = r.astype(bf16).astype(f32)
    return hi, mid, r - mid

def attn_bwd_kernel(len_ref, q_ref, k_ref, v_ref, o_ref, g_ref, lse_ref, cos_ref, sin_ref,
                    dq_ref, dk_ref, dv_ref, dqs, *, rows):
    p = pl.program_id(0)
    s = q_ref.shape[0]
    length = len_ref[0]
    lane = lax.broadcasted_iota(jnp.int32, (s, 128), 1)
    pos = lax.broadcasted_iota(jnp.int32, (s, 128), 0)
    lane_q = lax.broadcasted_iota(jnp.int32, (rows, 128), 1)
    k = k_ref[...].astype(f32)
    v = v_ref[...].astype(f32)
    bias = jnp.where(pos >= length, -1e30, 0.0)
    dks, dvs = [], []
    for h in (0, 1):
        e = HD * (1 - h)
        mine = (lane >= HD) if h else (lane < HD)
        mine_q = (lane_q >= HD) if h else (lane_q < HD)
        ones = jnp.where((lane >= e) & (lane < e + 3), 1.0, 0.0)
        kx = jnp.where(mine, k, jnp.where(lane == e + 3, bias, ones)).astype(bf16)
        vx = jnp.where(mine, v, ones).astype(bf16)
        kt = jnp.where(mine, k, 0.0).T.astype(bf16)
        dk = jnp.zeros((s, 128), f32)
        dv = jnp.zeros((s, 128), f32)
        for b in range(s // rows):
            sl = slice(b * rows, (b + 1) * rows)
            qb = q_ref[sl, :]
            gb = g_ref[sl, :]
            q = qb.astype(f32)
            g = gb.astype(f32)
            lse = jnp.sum(jnp.where(lane_q == 2 * p + h, lse_ref[sl, :], 0.0), axis=1, keepdims=True)
            dd = jnp.sum(jnp.where(mine_q, g * o_ref[sl, :].astype(f32), 0.0), axis=1, keepdims=True)
            l0, l1, l2 = split3(-lse)
            d0, d1, d2 = split3(-dd)
            qx = jnp.where(mine_q, q, jnp.where(lane_q == e, l0, jnp.where(lane_q == e + 1, l1, jnp.where(
                lane_q == e + 2, l2, jnp.where(lane_q == e + 3, 1.0, 0.0))))).astype(bf16)
            gx = jnp.where(mine_q, g, jnp.where(lane_q == e, d0, jnp.where(lane_q == e + 1, d1, jnp.where(
                lane_q == e + 2, d2, 0.0)))).astype(bf16)
            pt = jnp.exp2(dot(kx, qx, NT))
            dst = (pt * dot(vx, gx, NT)).astype(bf16)
            dv = dv + dot(pt.astype(bf16), gb)
            dk = dk + dot(dst, qb)
            dqt = dot(kt, dst)
            if h == 0:
                dqs[:, sl] = dqt
            else:
                dqs[:, sl] = dqs[:, sl] + dqt
        dks.append(dk)
        dvs.append(dv)
    cos, sin = cos_ref[...], sin_ref[...]
    dq = dqs[...].T * (HD ** -0.5)
    dk = jnp.where(lane < HD, dks[0], dks[1]) * (1.0 / LOG2E)
    dq_ref[...] = (dq * cos - swap_halves(dq) * sin).astype(bf16)
    dk_ref[...] = (dk * cos - swap_halves(dk) * sin).astype(bf16)
    dv_ref[...] = jnp.where(lane < HD, dvs[0], dvs[1]).astype(bf16)

def attn_bwd_call(length, qkv, att, gatt, lse, cos, sin, rows=256):
    s, d3 = qkv.shape
    d = d3 // 3
    np_ = d // 128
    col = pl.BlockSpec((s, 128), lambda i: (0, i))
    const = pl.BlockSpec((s, 128), lambda i: (0, 0))
    return pl.pallas_call(
        functools.partial(attn_bwd_kernel, rows=rows), grid=(np_,),
        in_specs=[pl.BlockSpec(memory_space=pltpu.SMEM), col,
                  pl.BlockSpec((s, 128), lambda i: (0, np_ + i)),
                  pl.BlockSpec((s, 128), lambda i: (0, 2 * np_ + i)), col, col, const, const, const],
        out_specs=[col, col, col],
        out_shape=[jax.ShapeDtypeStruct((s, d), bf16)] * 3,
        scratch_shapes=[pltpu.VMEM((128, s), f32)],
        cost_estimate=pl.CostEstimate(flops=20 * s * s * d, bytes_accessed=16 * s * d, transcendentals=s * s * 12),
        name="attn_bwd")(length, qkv, qkv, qkv, att, gatt, lse, cos, sin)

def gelu_both(v):
    a, b = 0.7978845608028654, 0.044715
    v2 = v * v
    t = jnp.tanh(a * v * (1.0 + b * v2))
    half = 0.5 + 0.5 * t
    return v * half, half + (0.5 * a) * v * (1.0 - t * t) * (1.0 + 3.0 * b * v2)

def colsum(x):
    return jnp.sum(x, axis=0, keepdims=True)

def mid_kernel(len_ref, att_ref, tok_ref, flag_ref, cot_ref, vec_ref, b1_ref, wo_ref, w1_ref, w2_ref,
               out_ref, gh1_ref, gatt_ref, n2_ref, act_ref, gm_ref, gpre_ref, gap_ref, sum_ref, sb1_ref,
               gp_s, *, cut):
    i = pl.program_id(0)
    rows, d = att_ref.shape
    ff = w1_ref.shape[1]
    emb, gain, scale, shift, gate_a, gate_m, b2 = (vec_ref[r:r + 1, :] for r in range(7))
    h0 = jnp.where(flag_ref[...] == 1, emb, tok_ref[...].astype(f32))
    ap = dot(att_ref[...], wo_ref[...])
    br_a = gate_a * ap
    h1 = h0 + br_a
    n, rs = norm_parts(h1)
    n2 = (n * gain * (1.0 + scale) + shift).astype(bf16)
    n2_ref[...] = n2
    mp = jnp.zeros((rows, d), f32) + b2
    for j in range(ff // cut):
        sl = slice(j * cut, (j + 1) * cut)
        act, gp = gelu_both(dot(n2, w1_ref[:, sl]) + b1_ref[:, sl])
        act = act.astype(bf16)
        act_ref[:, sl] = act
        gp_s[:, sl] = gp
        mp = mp + dot(act, w2_ref[sl, :])
    br_m = gate_m * mp
    bo = h1 + br_m
    out_ref[...] = bo.astype(bf16)
    pos = lax.broadcasted_iota(jnp.int32, (rows, 1), 0) + i * rows
    valid = jnp.where(pos < len_ref[0], 1.0, 0.0)
    cot = cot_ref[...].astype(f32)
    gm = (gate_m * cot).astype(bf16)
    gm_ref[...] = gm
    gn2 = jnp.zeros((rows, d), f32)
    sb1 = []
    for j in range(ff // cut):
        sl = slice(j * cut, (j + 1) * cut)
        gpre = (dot(gm, w2_ref[sl, :], NT) * gp_s[:, sl]).astype(bf16)
        gpre_ref[:, sl] = gpre
        sb1.append(colsum(gpre.astype(f32)))
        gn2 = gn2 + dot(gpre, w1_ref[:, sl], NT)
    e = gn2 * (gain * (1.0 + scale))
    gh1 = cot + rs * (e - jnp.mean(e, axis=1, keepdims=True) - n * jnp.mean(e * n, axis=1, keepdims=True))
    gh1_ref[...] = gh1
    gap = (gate_a * gh1).astype(bf16)
    gap_ref[...] = gap
    gatt_ref[...] = dot(gap, wo_ref[...], NT).astype(bf16)
    new = jnp.concatenate([
        colsum(cot * mp), colsum(gm.astype(f32)), colsum(gn2 * n), colsum(gn2), colsum(gh1 * ap),
        colsum(valid * bo * bo), colsum(valid * br_a * br_a), colsum(valid * br_m * br_m)], axis=0)
    sb1 = jnp.concatenate(sb1, axis=1)
    @pl.when(i == 0)
    def _():
        sum_ref[...] = new
        sb1_ref[...] = sb1
    @pl.when(i > 0)
    def _():
        sum_ref[...] += new
        sb1_ref[...] += sb1

def mid_call(length, att, tok, flag, cot, vec, b1, wo, w1, w2, rows=256, cut=768):
    s, d = tok.shape
    ff = w1.shape[1]
    row = lambda c: pl.BlockSpec((rows, c), lambda i: (i, 0))
    whole = lambda a: pl.BlockSpec(a.shape, lambda i: (0, 0))
    sd = jax.ShapeDtypeStruct
    return pl.pallas_call(
        functools.partial(mid_kernel, cut=cut), grid=(s // rows,),
        in_specs=[pl.BlockSpec(memory_space=pltpu.SMEM), row(d), row(d), row(1), row(d), whole(vec), whole(b1),
                  whole(wo), whole(w1), whole(w2)],
        out_specs=[row(d), row(d), row(d), row(d), row(ff), row(d), row(ff), row(d),
                   pl.BlockSpec((8, d), lambda i: (0, 0)), pl.BlockSpec((1, ff), lambda i: (0, 0))],
        out_shape=[sd((s, d), bf16), sd((s, d), f32), sd((s, d), bf16), sd((s, d), bf16), sd((s, ff), bf16),
                   sd((s, d), bf16), sd((s, ff), bf16), sd((s, d), bf16), sd((8, d), f32), sd((1, ff), f32)],
        scratch_shapes=[pltpu.VMEM((rows, ff), f32)],
        compiler_params=pltpu.CompilerParams(vmem_limit_bytes=60000 * 1024),
        cost_estimate=pl.CostEstimate(flops=2 * s * d * (2 * d + 4 * ff), bytes_accessed=30 * s * d,
                                      transcendentals=s * ff),
        name="mid")(length, att, tok, flag, cot, vec, b1, wo, w1, w2)

def post_kernel(dq_ref, dk_ref, dv_ref, tok_ref, flag_ref, gh1_ref, vec_ref, w_ref, ig_ref, sum_ref):
    i = pl.program_id(0)
    d = tok_ref.shape[1]
    emb, gain, scale = (vec_ref[r:r + 1, :] for r in range(3))
    masked = flag_ref[...] == 1
    h0 = jnp.where(masked, emb, tok_ref[...].astype(f32))
    n, rs = norm_parts(h0)
    gn1 = dot(dq_ref[...], w_ref[:, :d], NT) + dot(dk_ref[...], w_ref[:, d:2 * d], NT) + dot(
        dv_ref[...], w_ref[:, 2 * d:], NT)
    e = gn1 * (gain * (1.0 + scale))
    gh0 = gh1_ref[...] + rs * (e - jnp.mean(e, axis=1, keepdims=True) - n * jnp.mean(e * n, axis=1, keepdims=True))
    ig_ref[...] = jnp.where(masked, 0.0, gh0).astype(bf16)
    zero = jnp.zeros((5, d), f32)
    new = jnp.concatenate([colsum(gn1 * n), colsum(gn1), colsum(jnp.where(masked, gh0, 0.0)), zero], axis=0)
    @pl.when(i == 0)
    def _():
        sum_ref[...] = new
    @pl.when(i > 0)
    def _():
        sum_ref[...] += new

def post_call(dq, dk, dv, tok, flag, gh1, vec, w, rows=256):
    s, d = tok.shape
    row = lambda c: pl.BlockSpec((rows, c), lambda i: (i, 0))
    whole = lambda a: pl.BlockSpec(a.shape, lambda i: (0, 0))
    sd = jax.ShapeDtypeStruct
    return pl.pallas_call(
        post_kernel, grid=(s // rows,),
        in_specs=[row(d), row(d), row(d), row(d), row(1), row(d), whole(vec), whole(w)],
        out_specs=[row(d), pl.BlockSpec((8, d), lambda i: (0, 0))],
        out_shape=[sd((s, d), bf16), sd((8, d), f32)],
        cost_estimate=pl.CostEstimate(flops=6 * s * d * d, bytes_accessed=16 * s * d, transcendentals=0),
        name="post")(dq, dk, dv, tok, flag, gh1, vec, w)

def wgrad_kernel(a_ref, b_ref, o_ref):
    o_ref[...] = dot(a_ref[...], b_ref[...], TN).astype(bf16)

def wgrad_call(a, b, cols=768, bcols=768):
    s, m = a.shape
    n = b.shape[1]
    return pl.pallas_call(
        wgrad_kernel, grid=(m // cols, n // bcols),
        in_specs=[pl.BlockSpec((s, cols), lambda i, j: (0, i)), pl.BlockSpec((s, bcols), lambda i, j: (0, j))],
        out_specs=pl.BlockSpec((cols, bcols), lambda i, j: (i, j)),
        out_shape=jax.ShapeDtypeStruct((m, n), bf16),
        cost_estimate=pl.CostEstimate(flops=2 * s * m * n, bytes_accessed=2 * (s * (m + n) + m * n),
                                      transcendentals=0),
        name="wgrad")(a, b)

MESH = pl.DeviceIdType.MESH


def flip(i, b):
    return i + 2 ** b * (1 - 2 * ((i // 2 ** b) % 2))


def xor(i, mask):
    b = 0
    while mask >> b:
        if (mask >> b) & 1:
            i = flip(i, b)
        b += 1
    return i


def subsets(bits):
    masks = [0]
    for b in bits:
        masks = masks + [m | (1 << b) for m in masks]
    return masks


def log2(n):
    return n.bit_length() - 1


class Place:
    def __init__(self, shape):
        self.groups, self.lines = shape["fsdp"], shape["dp"]
        self.bits = log2(self.groups)
        self.orders = [list(range(self.bits)), list(range(self.bits))[::-1]]
        self.me = lax.axis_index("fsdp")
        self.dp = lax.axis_index("dp")
        self.core = self.dp % 2
        self.partner = flip(self.dp, 0)


def remote(src, dst, ssem, rsem, where):
    return pltpu.make_async_remote_copy(src_ref=src, dst_ref=dst, send_sem=ssem, recv_sem=rsem, device_id=where,
                                        device_id_type=MESH)


class Gather:
    def __init__(self, place, ins, outs, sems):
        self.p, self.ins, self.outs = place, ins, outs
        self.ss, self.rs, self.fs, self.fr, self.os, self.orr = sems

    @staticmethod
    def scratch(count, groups):
        a = pltpu.SemaphoreType.DMA((count, 2, groups - 1))
        b = pltpu.SemaphoreType.DMA((count,))
        return [a, a, a, a, b, b]

    def send(self, w, color, t, mask):
        p = self.p
        order = p.orders[color]
        e = 2 ** t - 1 + subsets(order[:t]).index(mask)
        piece = p.core * 2 + color
        blk = xor(p.me, mask)
        src = self.ins[w].at[piece] if mask == 0 else self.outs[w].at[blk, piece]
        return remote(src, self.outs[w].at[blk, piece], self.ss.at[w, color, e], self.rs.at[w, color, e],
                      (p.dp, flip(p.me, order[t])))

    def arrival(self, w, color, t, mask):
        p = self.p
        order = p.orders[color]
        e = 2 ** t - 1 + subsets(order[:t]).index(mask)
        got = self.outs[w].at[xor(p.me, mask | (1 << order[t])), p.core * 2 + color]
        return e, got

    def landed(self, w, color, e, got):
        return remote(got, got, self.ss.at[w, color, e], self.rs.at[w, color, e], (self.p.partner, self.p.me))

    def forward(self, w, color, e, got):
        return remote(got, got, self.fs.at[w, color, e], self.fr.at[w, color, e], (self.p.partner, self.p.me))

    def own(self, w):
        p = self.p
        return remote(self.ins[w], self.outs[w].at[p.me], self.os.at[w], self.orr.at[w], (p.partner, p.me))

    def start(self, w):
        for t in range(self.p.bits):
            for color in (0, 1):
                self.send(w, color, t, 0).start()
        self.own(w).start()

    def after(self, w, t):
        for color in (0, 1):
            order = self.p.orders[color]
            for mask in subsets(order[:t]):
                e, got = self.arrival(w, color, t, mask)
                self.landed(w, color, e, got).wait_recv()
                for later in range(t + 1, self.p.bits):
                    self.send(w, color, later, mask | (1 << order[t])).start()
                self.forward(w, color, e, got).start()

    def finish(self, w):
        p = self.p
        for color in (0, 1):
            order = p.orders[color]
            for t in range(p.bits):
                for mask in subsets(order[:t]):
                    e, got = self.arrival(w, color, t, mask)
                    other = self.outs[w].at[xor(p.me, mask | (1 << order[t])), (1 - p.core) * 2 + color]
                    self.forward(w, color, e, other).wait_recv()
                    self.forward(w, color, e, got).wait_send()
                    self.send(w, color, t, mask).wait_send()
        self.own(w).wait()


class Direct:
    def __init__(self, place, src, out, sems):
        self.p, self.src, self.out = place, src, out
        self.ss, self.rs = sems

    @staticmethod
    def scratch(groups):
        return [pltpu.SemaphoreType.DMA((groups,))] * 2

    def copy(self, m, arrived):
        p = self.p
        where = (p.partner, p.me) if m == 0 else (p.dp, xor(p.me, m))
        slot = xor(p.me, m) if arrived else p.me
        return remote(self.src, self.out.at[slot], self.ss.at[m], self.rs.at[m], where)

    def start(self):
        for m in range(self.p.groups):
            self.copy(m, False).start()

    def finish(self):
        for m in range(self.p.groups):
            self.copy(m, True).wait_recv()
            self.copy(m, False).wait_send()


def greet(devices):
    barrier = pltpu.get_barrier_semaphore()
    for where in devices:
        pl.semaphore_signal(barrier, inc=1, device_id=where, device_id_type=MESH)
    pl.semaphore_wait(barrier, len(devices))


def gather_peers(p, everyone):
    masks = range(1, p.groups) if everyone else [1 << b for b in range(p.bits)]
    return [(p.partner, p.me)] + [(p.dp, xor(p.me, m)) for m in masks]


def quarter(w):
    return w.reshape(4, w.shape[0] // 4, w.shape[1])


def gather_shape(w, groups):
    return jax.ShapeDtypeStruct((groups, 4, w.shape[0] // 4, w.shape[1]), w.dtype)


ANY = pl.BlockSpec(memory_space=pl.ANY)


def head_kernel(shape, count, *refs):
    ins, small, outs, small_out = refs[:count], refs[count], refs[count + 1:2 * count + 1], refs[2 * count + 1]
    sems = refs[2 * count + 2:]
    p = Place(shape)
    g = Gather(p, ins, outs, sems[:6])
    s = Direct(p, small, small_out, sems[6:])
    greet(gather_peers(p, True))
    s.start()
    for w in range(count):
        g.start(w)
    for t in range(p.bits):
        for w in range(count):
            g.after(w, t)
    for w in range(count):
        g.finish(w)
    s.finish()


def head_call(shape, small, ws):
    groups = shape["fsdp"]
    outs = [gather_shape(w, groups) for w in ws] + [jax.ShapeDtypeStruct((groups,) + small.shape, small.dtype)]
    res = pl.pallas_call(
        functools.partial(head_kernel, shape, len(ws)), in_specs=[ANY] * (len(ws) + 1), out_specs=[ANY] * len(outs),
        out_shape=outs, scratch_shapes=Gather.scratch(len(ws), groups) + Direct.scratch(groups),
        compiler_params=pltpu.CompilerParams(collective_id=1, has_side_effects=True), name="head",
    )(*[quarter(w) for w in ws], small)
    return [r.reshape(-1, r.shape[-1]) for r in res[:-1]], res[-1]


class Reduce:
    def __init__(self, place, counts, kinds, srcs, outs, scratch):
        self.p, self.counts, self.kinds, self.srcs, self.outs = place, counts, kinds, srcs, outs
        (self.own, self.cb, self.xb, self.zb, self.mb, self.u2, self.fin,
         self.load, self.cs, self.cr, self.xs, self.xr, self.zs, self.zr, self.ms, self.mr, self.fs, self.fr,
         self.ps, self.pr, self.st) = scratch
        p = place
        self.total = sum(counts)
        self.n = p.lines // 2
        self.zi = p.dp // 2
        left = self.zi // (self.n // 2)
        self.e = self.zi * (1 - left) + (self.n - 1 - self.zi) * left
        step = 2 * (1 - 2 * left)
        self.inner = (p.dp + step, p.me)
        self.outer = (p.dp - step, p.me)
        self.last = self.n // 2 - 1
        self.stages = ([self.begin, self.core_add] + [functools.partial(self.group_add, t) for t in range(p.bits)]
                       + [functools.partial(self.climb, j) for j in range(1, self.last + 1)] + [self.middle]
                       + [functools.partial(self.descend, j) for j in range(self.last - 1, -1, -1)])
        self.ticks = self.total + len(self.stages) - 1

    @staticmethod
    def scratch(total, groups, rows, cols):
        sem = pltpu.SemaphoreType.DMA
        vm = lambda *lead: pltpu.VMEM((total,) + lead + (rows // 2, cols), bf16)
        one = sem((total,))
        line = pltpu.VMEM((total, rows, cols), bf16)
        return [vm(groups, 2), vm(groups, 2), vm(2, groups - 1), line, line, line, line,
                one, one, one, sem((total, 2, groups - 1)), sem((total, 2, groups - 1)),
                one, one, one, one, one, one, one, one, one]

    def greet(self):
        p = self.p
        barrier = pltpu.get_barrier_semaphore()
        for where in [(p.partner, p.me)] + [(p.dp, flip(p.me, b)) for b in range(p.bits)] + [self.inner]:
            pl.semaphore_signal(barrier, inc=1, device_id=where, device_id_type=MESH)
        @pl.when(self.e > 0)
        def _():
            pl.semaphore_signal(barrier, inc=1, device_id=self.outer, device_id_type=MESH)
        half = self.n // 2
        pl.semaphore_wait(barrier, 2 + p.bits + (self.e + half - 1) // half)

    def source(self, k, fn):
        base = 0
        for i, count in enumerate(self.counts):
            @pl.when((k >= base) & (k < base + count))
            def _(i=i, base=base):
                fn(i, k - base)
            base += count

    def target(self, i, j, core):
        rows, cols = self.fin.shape[1:]
        out = self.outs[i]
        if self.kinds[i] == "cols":
            return out.at[:, pl.ds(pl.multiple_of((2 * j + core) * cols, cols), cols)]
        return out.at[pl.ds(pl.multiple_of(j * rows, rows), rows), pl.ds(pl.multiple_of(core * cols, cols), cols)]

    def load_copy(self, k, src):
        return pltpu.make_async_copy(src.at[self.p.core], self.own.at[k], self.load.at[k])

    def core_copy(self, k, src):
        p = self.p
        return remote(src.at[1 - p.core], self.cb.at[k], self.cs.at[k], self.cr.at[k], (p.partner, p.me))

    def begin(self, k):
        def go(i, j):
            self.core_copy(k, self.srcs[i].at[j]).start()
            self.load_copy(k, self.srcs[i].at[j]).start()
        self.source(k, go)

    def slot(self, order, t, mask):
        base = sum(self.p.groups >> (u + 1) for u in range(t))
        return base + subsets(order[t + 1:]).index(mask)

    def group_copy(self, k, color, t, mask):
        p = self.p
        order = p.orders[color]
        i = self.slot(order, t, mask)
        return remote(self.own.at[k, xor(p.me, (1 << order[t]) | mask), color], self.xb.at[k, color, i],
                      self.xs.at[k, color, i], self.xr.at[k, color, i], (p.dp, flip(p.me, order[t])))

    def group_send(self, k, t):
        for color in (0, 1):
            for mask in subsets(self.p.orders[color][t + 1:]):
                self.group_copy(k, color, t, mask).start()

    def core_add(self, k):
        self.load_copy(k, self.srcs[0].at[0]).wait()
        self.core_copy(k, self.srcs[0].at[0]).wait_recv()
        for f in range(self.p.groups):
            for color in (0, 1):
                self.own[k, f, color] = (self.own[k, f, color].astype(f32) + self.cb[k, f, color].astype(f32)).astype(bf16)
        self.group_send(k, 0)

    def group_add(self, t, k):
        p = self.p
        for color in (0, 1):
            order = p.orders[color]
            for mask in subsets(order[t + 1:]):
                self.group_copy(k, color, t, mask).wait_recv()
                blk, i = xor(p.me, mask), self.slot(order, t, mask)
                total = self.own[k, blk, color].astype(f32) + self.xb[k, color, i].astype(f32)
                if t == p.bits - 1:
                    self.u2[k, self.part(color)] = total.astype(bf16)
                else:
                    self.own[k, blk, color] = total.astype(bf16)
        if t < p.bits - 1:
            self.group_send(k, t + 1)
        else:
            @pl.when(self.e == 0)
            def _():
                (self.climb_copy(k) if self.last > 0 else self.middle_copy(k)).start()

    def part(self, color):
        half = self.u2.shape[1] // 2
        return slice(color * half, (color + 1) * half)

    def climb_copy(self, k):
        return remote(self.u2.at[k], self.zb.at[k], self.zs.at[k], self.zr.at[k], self.inner)

    def middle_copy(self, k):
        return remote(self.u2.at[k], self.mb.at[k], self.ms.at[k], self.mr.at[k], self.inner)

    def climb(self, j, k):
        @pl.when(self.e == j)
        def _():
            self.climb_copy(k).wait_recv()
            for color in (0, 1):
                total = self.u2[k, self.part(color)].astype(f32) + self.zb[k, self.part(color)].astype(f32)
                self.u2[k, self.part(color)] = total.astype(bf16)
            (self.middle_copy(k) if j == self.last else self.climb_copy(k)).start()

    def share_copy(self, k):
        return remote(self.fin.at[k], self.fin.at[k], self.fs.at[k], self.fr.at[k], self.outer)

    def share_wait(self, k):
        return remote(self.fin.at[k], self.fin.at[k], self.fs.at[k], self.fr.at[k], self.inner)

    def pass_copy(self, k, dst):
        p = self.p
        return remote(self.fin.at[k], dst, self.ps.at[k], self.pr.at[k], (p.partner, p.me))

    def store_copy(self, k, dst):
        return pltpu.make_async_copy(self.fin.at[k], dst, self.st.at[k])

    def done(self, k):
        def go(i, j):
            self.pass_copy(k, self.target(i, j, self.p.core)).start()
            self.store_copy(k, self.target(i, j, self.p.core)).start()
        self.source(k, go)

    def middle(self, k):
        @pl.when(self.e == self.last)
        def _():
            self.middle_copy(k).wait_recv()
            for color in (0, 1):
                total = self.u2[k, self.part(color)].astype(f32) + self.mb[k, self.part(color)].astype(f32)
                self.fin[k, self.part(color)] = total.astype(bf16)
            if self.last > 0:
                self.share_copy(k).start()
            self.done(k)

    def descend(self, j, k):
        @pl.when(self.e == j)
        def _():
            self.share_wait(k).wait_recv()
            if j > 0:
                self.share_copy(k).start()
            self.done(k)

    def tick(self, t):
        for s in range(len(self.stages) - 1, -1, -1):
            k = t - s
            @pl.when((k >= 0) & (k < self.total))
            def _(s=s, k=k):
                self.stages[s](k)

    def drain(self):
        p = self.p
        @pl.loop(0, self.total)
        def _(k):
            self.core_copy(k, self.srcs[0].at[0]).wait_send()
            for color in (0, 1):
                for t in range(p.bits):
                    for mask in subsets(p.orders[color][t + 1:]):
                        self.group_copy(k, color, t, mask).wait_send()
            @pl.when(self.e == self.last)
            def _():
                self.middle_copy(k).wait_send()
            @pl.when(self.e < self.last)
            def _():
                self.climb_copy(k).wait_send()
            @pl.when(self.e > 0)
            def _():
                self.share_copy(k).wait_send()
            def go(i, j):
                self.pass_copy(k, self.target(i, j, 1 - p.core)).wait()
                self.store_copy(k, self.target(i, j, p.core)).wait()
            self.source(k, go)


def reduce_kernel(shape, counts, kinds, *refs):
    n = len(counts)
    r = Reduce(Place(shape), counts, kinds, refs[:n], refs[n:2 * n], refs[2 * n:])
    r.greet()
    @pl.loop(0, r.ticks)
    def _(t):
        r.tick(t)
    r.drain()


def reduced_shapes(grads, kinds):
    rows, cols = 2 * grads[0].shape[-2], 2 * grads[0].shape[-1]
    return [jax.ShapeDtypeStruct((rows, g.shape[0] * cols) if kind == "cols" else (g.shape[0] * rows, cols), bf16)
            for g, kind in zip(grads, kinds)]


def reduce_call(shape, grads, kinds, ident):
    groups = shape["fsdp"]
    counts = [g.shape[0] for g in grads]
    rows, cols = 2 * grads[0].shape[-2], grads[0].shape[-1]
    return pl.pallas_call(
        functools.partial(reduce_kernel, shape, counts, kinds), in_specs=[ANY] * len(grads),
        out_specs=[ANY] * len(grads), out_shape=reduced_shapes(grads, kinds),
        scratch_shapes=Reduce.scratch(sum(counts), groups, rows, cols),
        compiler_params=pltpu.CompilerParams(collective_id=ident, has_side_effects=True, vmem_limit_bytes=64000 * 1024),
        name="reduce")(*grads)


def wgrad_cols_kernel(a_ref, b_ref, o_ref):
    y = dot(a_ref[...], b_ref[...], TN).astype(bf16)
    _, _, g, _, r, c = o_ref.shape
    for half in (0, 1):
        o_ref[0, half] = y[:, half * c:(half + 1) * c].reshape(g, 2, r, c)


def wgrad_cols(a, b, groups):
    s, m = a.shape
    n = b.shape[1]
    r, c = m // groups // 2, m // 2
    return pl.pallas_call(
        wgrad_cols_kernel, grid=(n // m,),
        in_specs=[pl.BlockSpec((s, m), lambda i: (0, 0)), pl.BlockSpec((s, m), lambda i: (0, i))],
        out_specs=pl.BlockSpec((1, 2, groups, 2, r, c), lambda i: (i, 0, 0, 0, 0, 0)),
        out_shape=jax.ShapeDtypeStruct((n // m, 2, groups, 2, r, c), bf16),
        cost_estimate=pl.CostEstimate(flops=2 * s * m * n, bytes_accessed=2 * (s * (m + n) + m * n),
                                      transcendentals=0), name="wgrad_cols")(a, b)


def wgrad_rows_kernel(a_ref, b_ref, o_ref):
    y = dot(a_ref[...], b_ref[...], TN).astype(bf16)
    q, _, _, _, r, c = o_ref.shape
    for half in (0, 1):
        o_ref[:, half, 0] = y[:, half * c:(half + 1) * c].reshape(q, 2, r, c)


def wgrad_rows(a, b, groups):
    s, m = a.shape
    n = b.shape[1]
    q, r, c = m // n, n // groups // 2, n // 2
    return pl.pallas_call(
        wgrad_rows_kernel, grid=(groups,),
        in_specs=[pl.BlockSpec((s, m // groups), lambda i: (0, i)), pl.BlockSpec((s, n), lambda i: (0, 0))],
        out_specs=pl.BlockSpec((q, 2, 1, 2, r, c), lambda i: (0, 0, i, 0, 0, 0)),
        out_shape=jax.ShapeDtypeStruct((q, 2, groups, 2, r, c), bf16),
        cost_estimate=pl.CostEstimate(flops=2 * s * m * n, bytes_accessed=2 * (s * (m + n) + m * n),
                                      transcendentals=0), name="wgrad_rows")(a, b)


def body_kernel(shape, count, *refs):
    ins, outs, sems = refs[:count], refs[count:2 * count], refs[2 * count:]
    p = Place(shape)
    g = Gather(p, ins, outs, sems)
    greet(gather_peers(p, False))
    for w in range(count):
        g.start(w)
    for t in range(p.bits):
        for w in range(count):
            g.after(w, t)
    for w in range(count):
        g.finish(w)


def body_call(shape, ws):
    groups = shape["fsdp"]
    res = pl.pallas_call(
        functools.partial(body_kernel, shape, len(ws)), in_specs=[ANY] * len(ws), out_specs=[ANY] * len(ws),
        out_shape=[gather_shape(w, groups) for w in ws], scratch_shapes=Gather.scratch(len(ws), groups),
        compiler_params=pltpu.CompilerParams(collective_id=2, has_side_effects=True), name="body",
    )(*[quarter(w) for w in ws])
    return [r.reshape(-1, r.shape[-1]) for r in res]
from jax.sharding import PartitionSpec as P

highest = lax.Precision.HIGHEST


def rotary_tables(length):
    half = HD // 2
    rate = 1.0 / 10000.0 ** (jnp.arange(half, dtype=f32) * 2.0 / HD)
    angle = jnp.arange(length, dtype=f32)[:, None] * rate[None, :]
    angle = jnp.concatenate([angle] * (128 // half), axis=-1)
    sign = jnp.where(jnp.arange(128) % HD < half, -1.0, 1.0)
    return jnp.cos(angle), jnp.sin(angle) * sign


def per_device(shape, tokens, hidden_token_indicator, lengths, time_ids, cotangent, gain_one, w_qkv, w_out, gain_two,
               w_fc1, b_fc1, w_fc2, b_fc2, w_ada, b_ada, mask_embed, time_table):
    groups = shape["fsdp"]
    s, d = tokens.shape[1:]
    ff = b_fc1.shape[0] * groups
    tok, cot = tokens[0], cotangent[0]
    flag = hidden_token_indicator.reshape(s, 1)
    sizes = [v.shape[0] for v in (gain_one, gain_two, b_fc2, mask_embed, b_fc1, b_ada)]
    small = jnp.concatenate([gain_one, gain_two, b_fc2, mask_embed, b_fc1, b_ada])[None]
    (ada_all, qkv_all), packed = head_call(shape, small, [w_ada, w_qkv])
    packed = packed[:, 0]
    out_all, fc1_all, fc2_all = body_call(shape, [w_out, w_fc1, w_fc2])
    cuts = [sum(sizes[:i]) for i in range(len(sizes) + 1)]
    gain1, gain2, b2, emb, b1, bada = (
        packed[:, cuts[i]:cuts[i + 1]].reshape(1, -1).astype(f32) for i in range(len(sizes)))
    cond_pre = lax.dynamic_slice_in_dim(time_table, time_ids[0], 1, axis=0)
    cond = jax.nn.silu(cond_pre)
    modulation = jnp.dot(cond, ada_all.astype(f32).T, precision=highest) + bada
    shift_a, scale_a, gate_a, shift_m, scale_m, gate_m = (modulation[:, i * d:(i + 1) * d] for i in range(6))
    cos, sin = rotary_tables(s)
    zero = jnp.zeros((1, d), f32)
    vec_pre = jnp.concatenate([emb, gain1, scale_a, shift_a] + [zero] * 4, axis=0)
    vec_mid = jnp.concatenate([emb, gain2, scale_m, shift_m, gate_a, gate_m, b2, zero], axis=0)
    n1, qkv = pre_call(tok, flag, vec_pre, qkv_all, cos, sin)
    att, lse = attn_fwd_call(lengths, qkv)
    out, gh1, gatt, n2, act, gm, gpre, gap, sums, gb1 = mid_call(
        lengths, att, tok, flag, cot, vec_mid, b1, out_all, fc1_all, fc2_all)
    g_fc2 = wgrad_rows(act, gm, groups)
    g_fc1 = wgrad_cols(n2, gpre, groups)
    g_out = wgrad_cols(att, gap, groups)
    dq, dk, dv = attn_bwd_call(lengths, qkv, att, gatt, lse, cos, sin)
    g_qkv = [wgrad_cols(n1, x, groups) for x in (dq, dk, dv)]
    r_fc2, r_fc1, r_out = reduce_call(shape, [g_fc2, g_fc1, g_out], ["rows", "cols", "cols"], 3)
    r_qkv = reduce_call(shape, g_qkv, ["cols"] * 3, 4)
    igrad, sums1 = post_call(dq, dk, dv, tok, flag, gh1, vec_pre, qkv_all)
    ggm, gb2, a2, s2, gga, st0, st1, st2 = (sums[i:i + 1] for i in range(8))
    a1, s1, gemb = (sums1[i:i + 1] for i in range(3))
    gmod = jnp.concatenate([s1, a1 * gain1, gga, s2, a2 * gain2, ggm], axis=1)
    small = jnp.concatenate([(1.0 + scale_a) * a1, (1.0 + scale_m) * a2, gb2, gemb, gb1, gmod], axis=1)
    stats = jnp.concatenate([jnp.sum(st0).reshape(1, 1), jnp.sum(st1).reshape(1, 1), jnp.sum(st2).reshape(1, 1),
                             lengths.astype(f32).reshape(1, 1), time_ids.astype(f32).reshape(1, 1)], axis=1)
    row = jnp.concatenate([small, cond_pre, stats, jnp.zeros((1, 123), f32)], axis=1)
    rows = lax.all_gather(row, ("dp", "fsdp"), axis=0, tiled=True)
    width = small.shape[1]
    conds, tail = rows[:, width:width + cond.shape[1]], rows[:, width + cond.shape[1]:]
    gmods = rows[:, width - gmod.shape[1]:width]
    silu_c, pull = jax.vjp(jax.nn.silu, conds)
    grad_cond = pull(jnp.dot(gmods, ada_all.astype(f32), precision=highest))[0]
    hot = (jnp.arange(time_table.shape[0])[:, None] == tail[:, 4].astype(jnp.int32)[None, :]).astype(f32)
    table = jnp.dot(hot, grad_cond, precision=highest)
    totals = jnp.sum(tail[:, :4], axis=0)
    rms = jnp.sqrt(totals[:3] / (totals[3] * d))
    me = lax.axis_index("fsdp")
    parts, base = [], 0
    for size in sizes:
        parts.append(jnp.sum(lax.dynamic_slice_in_dim(rows, base + me * size, size, axis=1), axis=0))
        base += size * groups
    g1, g2, gb2, gemb, gb1, gbada = parts
    n_ada = w_ada.shape[0]
    mods = lax.dynamic_slice_in_dim(rows, width - gmod.shape[1] + me * n_ada, n_ada, axis=1)
    g_ada = lax.dot_general(mods, silu_c, (((0,), (0,)), ((), ())), precision=highest)

    return (out[None], igrad[None], g1, jnp.concatenate(r_qkv, axis=1).astype(f32), r_out.astype(f32), g2, r_fc1.astype(f32), gb1,
            r_fc2.astype(f32), gb2,
            g_ada, gbada, gemb, table, rms)


def solution(mesh):
    both = ("dp", "fsdp")
    f1, f2 = P("fsdp"), P("fsdp", None)
    placed = (P(both, None, None), P(both, None), P(both), P(both), P(both, None, None), f1, f2, f2, f1, f2, f1, f2, f1,
              f2, f1, f1, P())
    outs = (P(both, None, None), P(both, None, None), f1, f2, f2, f1, f2, f1, f2, f1, f2, f1, f1, P(), P())
    return jax.shard_map(functools.partial(per_device, dict(mesh.shape)), mesh=mesh, in_specs=placed, out_specs=outs,
                         check_vma=False)
```

```python
import functools, math
import jax, jax.numpy as jnp
from jax import lax
from jax.experimental import pallas as pl
from jax.experimental.pallas import tpu as pltpu

HD = 64
EPS = 1e-5
LOG2E = math.log2(math.e)
QSCALE = LOG2E * HD ** -0.5
f32, bf16 = jnp.float32, jnp.bfloat16
NT = (((1,), (1,)), ((), ()))
NN = (((1,), (0,)), ((), ()))
TN = (((0,), (0,)), ((), ()))

def dot(a, b, dims=NN):
    return lax.dot_general(a, b, dims, preferred_element_type=f32)

def norm_parts(x):
    mean = jnp.mean(x, axis=-1, keepdims=True)
    cen = x - mean
    rs = lax.rsqrt(jnp.mean(cen * cen, axis=-1, keepdims=True) + EPS)
    return cen * rs, rs

def swap_halves(u):
    lane = lax.broadcasted_iota(jnp.int32, u.shape, 1)
    return jnp.where(lane % HD < HD // 2, pltpu.roll(u, 96, 1), pltpu.roll(u, 32, 1))

def pre_kernel(tok_ref, flag_ref, vec_ref, w_ref, cos_ref, sin_ref, n1_ref, qkv_ref):
    emb, gain, scale, shift = (vec_ref[i:i + 1, :] for i in range(4))
    h0 = jnp.where(flag_ref[...] == 1, emb, tok_ref[...].astype(f32))
    n, _ = norm_parts(h0)
    n1 = (n * gain * (1.0 + scale) + shift).astype(bf16)
    n1_ref[...] = n1
    d = n1.shape[1]
    cos, sin = cos_ref[...], sin_ref[...]
    for part in range(3):
        y = dot(n1, w_ref[:, part * d:(part + 1) * d])
        for c in range(d // 128):
            lo = part * d + c * 128
            u = y[:, c * 128:(c + 1) * 128]
            if part < 2:
                u = u * cos + swap_halves(u) * sin
                if part == 0:
                    u = u * QSCALE
            qkv_ref[:, lo:lo + 128] = u.astype(bf16)

def pre_call(tok, flag, vecs, w, cos, sin, rows=256):
    s, d = tok.shape
    return pl.pallas_call(
        pre_kernel, grid=(s // rows,),
        in_specs=[pl.BlockSpec((rows, d), lambda i: (i, 0)), pl.BlockSpec((rows, 1), lambda i: (i, 0)),
                  pl.BlockSpec((8, d), lambda i: (0, 0)), pl.BlockSpec((d, 3 * d), lambda i: (0, 0)),
                  pl.BlockSpec((rows, 128), lambda i: (i, 0)), pl.BlockSpec((rows, 128), lambda i: (i, 0))],
        out_specs=[pl.BlockSpec((rows, d), lambda i: (i, 0)), pl.BlockSpec((rows, 3 * d), lambda i: (i, 0))],
        out_shape=[jax.ShapeDtypeStruct((s, d), bf16), jax.ShapeDtypeStruct((s, 3 * d), bf16)],
        cost_estimate=pl.CostEstimate(flops=2 * s * d * 3 * d, bytes_accessed=12 * s * d, transcendentals=0),
        name="pre")(tok, flag, vecs, w, cos, sin)

def attn_fwd_body(len_ref, q_ref, k_ref, v_ref, o_ref, lse_ref, rows):
    p = pl.program_id(0)
    s = q_ref.shape[0]
    length = len_ref[0]
    lane = lax.broadcasted_iota(jnp.int32, (s, 128), 1)
    pos = lax.broadcasted_iota(jnp.int32, (s, 128), 0)
    lane_q = lax.broadcasted_iota(jnp.int32, (rows, 128), 1)
    k = k_ref[...].astype(f32)
    v = v_ref[...].astype(f32)
    kx, vx = [], []
    for h in (0, 1):
        extra = HD * (1 - h)
        mine = (lane >= HD) if h else (lane < HD)
        bias = jnp.where(pos >= length, -1e30, 0.0)
        kx.append(jnp.where(mine, k, jnp.where(lane == extra, bias, 0.0)).astype(bf16))
        vx.append(jnp.where(mine, v, jnp.where(lane == extra, 1.0, 0.0)).astype(bf16))
    for b in range(s // rows):
        q = q_ref[b * rows:(b + 1) * rows, :].astype(f32)
        outs, lses = [], []
        for h in (0, 1):
            extra = HD * (1 - h)
            mine = (lane_q >= HD) if h else (lane_q < HD)
            qx = jnp.where(mine, q, jnp.where(lane_q == extra, 1.0, 0.0)).astype(bf16)
            sc = dot(qx, kx[h], NT)
            m = jnp.max(sc, axis=1, keepdims=True)
            pr = jnp.exp2(sc - m).astype(bf16)
            o = dot(pr, vx[h])
            tot = o[:, extra:extra + 1]
            outs.append(o * (1.0 / tot))
            lses.append(m + jnp.log(tot) * LOG2E)
        o_ref[b * rows:(b + 1) * rows, :] = jnp.where(lane_q < HD, outs[0], outs[1]).astype(bf16)
        old = jnp.where(p == 0, 0.0, lse_ref[b * rows:(b + 1) * rows, :])
        lse_ref[b * rows:(b + 1) * rows, :] = jnp.where(
            lane_q == 2 * p, lses[0], jnp.where(lane_q == 2 * p + 1, lses[1], old))

def split3(x):
    hi = x.astype(bf16).astype(f32)
    r = x - hi
    mid = r.astype(bf16).astype(f32)
    return hi, mid, r - mid

def attn_bwd_body(len_ref, q_ref, k_ref, v_ref, o_ref, g_ref, lse_ref, cos_ref, sin_ref,
                  dq_ref, dk_ref, dv_ref, dqs, dks, dvs, rows):
    p, h = pl.program_id(0), pl.program_id(1)
    s = q_ref.shape[0]
    length = len_ref[0]
    lane = lax.broadcasted_iota(jnp.int32, (s, 128), 1)
    pos = lax.broadcasted_iota(jnp.int32, (s, 128), 0)
    lane_q = lax.broadcasted_iota(jnp.int32, (rows, 128), 1)
    e = HD * (1 - h)
    mine, mine_q = lane // HD == h, lane_q // HD == h
    k = k_ref[...].astype(f32)
    v = v_ref[...].astype(f32)
    ones = jnp.where((lane >= e) & (lane < e + 3), 1.0, 0.0)
    bias = jnp.where(pos >= length, -1e30, 0.0)
    kx = jnp.where(mine, k, jnp.where(lane == e + 3, bias, ones)).astype(bf16)
    vx = jnp.where(mine, v, ones).astype(bf16)
    kt = jnp.where(mine, k, 0.0).T.astype(bf16)
    dk = jnp.zeros((s, 128), f32)
    dv = jnp.zeros((s, 128), f32)
    for b in range(s // rows):
        sl = slice(b * rows, (b + 1) * rows)
        qb = q_ref[sl, :]
        gb = g_ref[sl, :]
        q = qb.astype(f32)
        g = gb.astype(f32)
        lse = jnp.sum(jnp.where(lane_q == 2 * p + h, lse_ref[sl, :], 0.0), axis=1, keepdims=True)
        dd = jnp.sum(jnp.where(mine_q, g * o_ref[sl, :].astype(f32), 0.0), axis=1, keepdims=True)
        l0, l1, l2 = split3(-lse)
        d0, d1, d2 = split3(-dd)
        qx = jnp.where(mine_q, q, jnp.where(lane_q == e, l0, jnp.where(lane_q == e + 1, l1, jnp.where(
            lane_q == e + 2, l2, jnp.where(lane_q == e + 3, 1.0, 0.0))))).astype(bf16)
        gx = jnp.where(mine_q, g, jnp.where(lane_q == e, d0, jnp.where(lane_q == e + 1, d1, jnp.where(
            lane_q == e + 2, d2, 0.0)))).astype(bf16)
        pt = jnp.exp2(dot(kx, qx, NT))
        dst = (pt * dot(vx, gx, NT)).astype(bf16)
        dv = dv + dot(pt.astype(bf16), gb)
        dk = dk + dot(dst, qb)
        dqt = dot(kt, dst)
        dqs[:, sl] = jnp.where(h == 0, dqt, dqs[:, sl] + dqt)
    @pl.when(h == 0)
    def _():
        dks[...] = dk
        dvs[...] = dv
    @pl.when(h == 1)
    def _():
        cos, sin = cos_ref[...], sin_ref[...]
        dq = dqs[...].T * (HD ** -0.5)
        dkk = jnp.where(lane < HD, dks[...], dk) * (1.0 / LOG2E)
        dq_ref[...] = (dq * cos - swap_halves(dq) * sin).astype(bf16)
        dk_ref[...] = (dkk * cos - swap_halves(dkk) * sin).astype(bf16)
        dv_ref[...] = jnp.where(lane < HD, dvs[...], dv).astype(bf16)


def gelu_both(v):
    a, b = 0.7978845608028654, 0.044715
    v2 = v * v
    t = jnp.tanh(a * v * (1.0 + b * v2))
    half = 0.5 + 0.5 * t
    return v * half, half + (0.5 * a) * v * (1.0 - t * t) * (1.0 + 3.0 * b * v2)

def colsum(x):
    return jnp.sum(x, axis=0, keepdims=True)

def mid_kernel(len_ref, att_ref, tok_ref, flag_ref, cot_ref, vec_ref, b1_ref, wo_ref, w1_ref, w2_ref,
               out_ref, gh1_ref, gatt_ref, n2_ref, act_ref, gm_ref, gpre_ref, gap_ref, sum_ref, sb1_ref,
               gp_s, *, cut):
    i = pl.program_id(0)
    rows, d = att_ref.shape
    ff = w1_ref.shape[1]
    emb, gain, scale, shift, gate_a, gate_m, b2 = (vec_ref[r:r + 1, :] for r in range(7))
    h0 = jnp.where(flag_ref[...] == 1, emb, tok_ref[...].astype(f32))
    ap = dot(att_ref[...], wo_ref[...])
    br_a = gate_a * ap
    h1 = h0 + br_a
    n, rs = norm_parts(h1)
    n2 = (n * gain * (1.0 + scale) + shift).astype(bf16)
    n2_ref[...] = n2
    mp = jnp.zeros((rows, d), f32) + b2
    for j in range(ff // cut):
        sl = slice(j * cut, (j + 1) * cut)
        act, gp = gelu_both(dot(n2, w1_ref[:, sl]) + b1_ref[:, sl])
        act = act.astype(bf16)
        act_ref[:, sl] = act
        gp_s[:, sl] = gp
        mp = mp + dot(act, w2_ref[sl, :])
    br_m = gate_m * mp
    bo = h1 + br_m
    out_ref[...] = bo.astype(bf16)
    pos = lax.broadcasted_iota(jnp.int32, (rows, 1), 0) + i * rows
    valid = jnp.where(pos < len_ref[0], 1.0, 0.0)
    cot = cot_ref[...].astype(f32)
    gm = (gate_m * cot).astype(bf16)
    gm_ref[...] = gm
    gn2 = jnp.zeros((rows, d), f32)
    sb1 = []
    for j in range(ff // cut):
        sl = slice(j * cut, (j + 1) * cut)
        gpre = (dot(gm, w2_ref[sl, :], NT) * gp_s[:, sl]).astype(bf16)
        gpre_ref[:, sl] = gpre
        sb1.append(colsum(gpre.astype(f32)))
        gn2 = gn2 + dot(gpre, w1_ref[:, sl], NT)
    e = gn2 * (gain * (1.0 + scale))
    gh1 = cot + rs * (e - jnp.mean(e, axis=1, keepdims=True) - n * jnp.mean(e * n, axis=1, keepdims=True))
    gh1_ref[...] = gh1
    gap = (gate_a * gh1).astype(bf16)
    gap_ref[...] = gap
    gatt_ref[...] = dot(gap, wo_ref[...], NT).astype(bf16)
    new = jnp.concatenate([
        colsum(cot * mp), colsum(gm.astype(f32)), colsum(gn2 * n), colsum(gn2), colsum(gh1 * ap),
        colsum(valid * bo * bo), colsum(valid * br_a * br_a), colsum(valid * br_m * br_m)], axis=0)
    sb1 = jnp.concatenate(sb1, axis=1)
    @pl.when(i == 0)
    def _():
        sum_ref[...] = new
        sb1_ref[...] = sb1
    @pl.when(i > 0)
    def _():
        sum_ref[...] += new
        sb1_ref[...] += sb1

def mid_call(length, att, tok, flag, cot, vec, b1, wo, w1, w2, rows=256, cut=768):
    s, d = tok.shape
    ff = w1.shape[1]
    row = lambda c: pl.BlockSpec((rows, c), lambda i: (i, 0))
    whole = lambda a: pl.BlockSpec(a.shape, lambda i: (0, 0))
    sd = jax.ShapeDtypeStruct
    return pl.pallas_call(
        functools.partial(mid_kernel, cut=cut), grid=(s // rows,),
        in_specs=[pl.BlockSpec(memory_space=pltpu.SMEM), row(d), row(d), row(1), row(d), whole(vec), whole(b1),
                  whole(wo), whole(w1), whole(w2)],
        out_specs=[row(d), row(d), row(d), row(d), row(ff), row(d), row(ff), row(d),
                   pl.BlockSpec((8, d), lambda i: (0, 0)), pl.BlockSpec((1, ff), lambda i: (0, 0))],
        out_shape=[sd((s, d), bf16), sd((s, d), f32), sd((s, d), bf16), sd((s, d), bf16), sd((s, ff), bf16),
                   sd((s, d), bf16), sd((s, ff), bf16), sd((s, d), bf16), sd((8, d), f32), sd((1, ff), f32)],
        scratch_shapes=[pltpu.VMEM((rows, ff), f32)],
        compiler_params=pltpu.CompilerParams(vmem_limit_bytes=60000 * 1024),
        cost_estimate=pl.CostEstimate(flops=2 * s * d * (2 * d + 4 * ff), bytes_accessed=30 * s * d,
                                      transcendentals=s * ff),
        name="mid")(length, att, tok, flag, cot, vec, b1, wo, w1, w2)

def post_body(dq_ref, dk_ref, dv_ref, tok_ref, flag_ref, gh1_ref, vec_ref, w_ref, ig_ref, sum_ref):
    i = pl.program_id(0)
    d = tok_ref.shape[1]
    emb, gain, scale = (vec_ref[r:r + 1, :] for r in range(3))
    masked = flag_ref[...] == 1
    h0 = jnp.where(masked, emb, tok_ref[...].astype(f32))
    n, rs = norm_parts(h0)
    gn1 = dot(dq_ref[...], w_ref[:, :d], NT) + dot(dk_ref[...], w_ref[:, d:2 * d], NT) + dot(
        dv_ref[...], w_ref[:, 2 * d:], NT)
    e = gn1 * (gain * (1.0 + scale))
    gh0 = gh1_ref[...] + rs * (e - jnp.mean(e, axis=1, keepdims=True) - n * jnp.mean(e * n, axis=1, keepdims=True))
    ig_ref[...] = jnp.where(masked, 0.0, gh0).astype(bf16)
    zero = jnp.zeros((5, d), f32)
    new = jnp.concatenate([colsum(gn1 * n), colsum(gn1), colsum(jnp.where(masked, gh0, 0.0)), zero], axis=0)
    @pl.when(i == 0)
    def _():
        sum_ref[...] = new
    @pl.when(i > 0)
    def _():
        sum_ref[...] += new


MESH = pl.DeviceIdType.MESH


def flip(i, b):
    return i + 2 ** b * (1 - 2 * ((i // 2 ** b) % 2))


def xor(i, mask):
    b = 0
    while mask >> b:
        if (mask >> b) & 1:
            i = flip(i, b)
        b += 1
    return i


def subsets(bits):
    masks = [0]
    for b in bits:
        masks = masks + [m | (1 << b) for m in masks]
    return masks


def log2(n):
    return n.bit_length() - 1


class Place:
    def __init__(self, shape):
        self.groups, self.lines = shape["fsdp"], shape["dp"]
        self.bits = log2(self.groups)
        self.orders = [list(range(self.bits)), list(range(self.bits))[::-1]]
        self.me = lax.axis_index("fsdp")
        self.dp = lax.axis_index("dp")
        self.core = self.dp % 2
        self.partner = flip(self.dp, 0)


def remote(src, dst, ssem, rsem, where):
    return pltpu.make_async_remote_copy(src_ref=src, dst_ref=dst, send_sem=ssem, recv_sem=rsem, device_id=where,
                                        device_id_type=MESH)


class Gather:
    def __init__(self, place, ins, outs, sems):
        self.p, self.ins, self.outs = place, ins, outs
        self.ss, self.rs, self.fs, self.fr, self.os, self.orr = sems

    @staticmethod
    def scratch(count, groups):
        a = pltpu.SemaphoreType.DMA((count, 2, groups - 1))
        b = pltpu.SemaphoreType.DMA((count,))
        return [a, a, a, a, b, b]

    def send(self, w, color, t, mask):
        p = self.p
        order = p.orders[color]
        e = 2 ** t - 1 + subsets(order[:t]).index(mask)
        piece = p.core * 2 + color
        blk = xor(p.me, mask)
        src = self.ins[w].at[piece] if mask == 0 else self.outs[w].at[blk, piece]
        return remote(src, self.outs[w].at[blk, piece], self.ss.at[w, color, e], self.rs.at[w, color, e],
                      (p.dp, flip(p.me, order[t])))

    def arrival(self, w, color, t, mask):
        p = self.p
        order = p.orders[color]
        e = 2 ** t - 1 + subsets(order[:t]).index(mask)
        got = self.outs[w].at[xor(p.me, mask | (1 << order[t])), p.core * 2 + color]
        return e, got

    def landed(self, w, color, e, got):
        return remote(got, got, self.ss.at[w, color, e], self.rs.at[w, color, e], (self.p.partner, self.p.me))

    def forward(self, w, color, e, got):
        return remote(got, got, self.fs.at[w, color, e], self.fr.at[w, color, e], (self.p.partner, self.p.me))

    def own(self, w):
        p = self.p
        return remote(self.ins[w], self.outs[w].at[p.me], self.os.at[w], self.orr.at[w], (p.partner, p.me))

    def start(self, w):
        for t in range(self.p.bits):
            for color in (0, 1):
                self.send(w, color, t, 0).start()
        self.own(w).start()

    def after(self, w, t):
        for color in (0, 1):
            order = self.p.orders[color]
            for mask in subsets(order[:t]):
                e, got = self.arrival(w, color, t, mask)
                self.landed(w, color, e, got).wait_recv()
                for later in range(t + 1, self.p.bits):
                    self.send(w, color, later, mask | (1 << order[t])).start()
                self.forward(w, color, e, got).start()

    def finish(self, w):
        p = self.p
        for color in (0, 1):
            order = p.orders[color]
            for t in range(p.bits):
                for mask in subsets(order[:t]):
                    e, got = self.arrival(w, color, t, mask)
                    other = self.outs[w].at[xor(p.me, mask | (1 << order[t])), (1 - p.core) * 2 + color]
                    self.forward(w, color, e, other).wait_recv()
                    self.forward(w, color, e, got).wait_send()
                    self.send(w, color, t, mask).wait_send()
        self.own(w).wait()


class Direct:
    def __init__(self, place, src, out, sems):
        self.p, self.src, self.out = place, src, out
        self.ss, self.rs = sems

    @staticmethod
    def scratch(groups):
        return [pltpu.SemaphoreType.DMA((groups,))] * 2

    def copy(self, m, arrived):
        p = self.p
        where = (p.partner, p.me) if m == 0 else (p.dp, xor(p.me, m))
        slot = xor(p.me, m) if arrived else p.me
        return remote(self.src, self.out.at[slot], self.ss.at[m], self.rs.at[m], where)

    def start(self):
        for m in range(self.p.groups):
            self.copy(m, False).start()

    def finish(self):
        for m in range(self.p.groups):
            self.copy(m, True).wait_recv()
            self.copy(m, False).wait_send()


def greet(devices):
    barrier = pltpu.get_barrier_semaphore()
    for where in devices:
        pl.semaphore_signal(barrier, inc=1, device_id=where, device_id_type=MESH)
    pl.semaphore_wait(barrier, len(devices))


def gather_peers(p, everyone):
    masks = range(1, p.groups) if everyone else [1 << b for b in range(p.bits)]
    return [(p.partner, p.me)] + [(p.dp, xor(p.me, m)) for m in masks]


def quarter(w):
    return w.reshape(4, w.shape[0] // 4, w.shape[1])


def gather_shape(w, groups):
    return jax.ShapeDtypeStruct((groups, 4, w.shape[0] // 4, w.shape[1]), w.dtype)


ANY = pl.BlockSpec(memory_space=pl.ANY)


def head_kernel(shape, count, *refs):
    ins, small, outs, small_out = refs[:count], refs[count], refs[count + 1:2 * count + 1], refs[2 * count + 1]
    sems = refs[2 * count + 2:]
    p = Place(shape)
    g = Gather(p, ins, outs, sems[:6])
    s = Direct(p, small, small_out, sems[6:])
    greet(gather_peers(p, True))
    s.start()
    for w in range(count):
        g.start(w)
    for t in range(p.bits):
        for w in range(count):
            g.after(w, t)
    for w in range(count):
        g.finish(w)
    s.finish()


def head_call(shape, small, ws):
    groups = shape["fsdp"]
    outs = [gather_shape(w, groups) for w in ws] + [jax.ShapeDtypeStruct((groups,) + small.shape, small.dtype)]
    res = pl.pallas_call(
        functools.partial(head_kernel, shape, len(ws)), in_specs=[ANY] * (len(ws) + 1), out_specs=[ANY] * len(outs),
        out_shape=outs, scratch_shapes=Gather.scratch(len(ws), groups) + Direct.scratch(groups),
        compiler_params=pltpu.CompilerParams(collective_id=1, has_side_effects=True), name="head",
    )(*[quarter(w) for w in ws], small)
    return [r.reshape(-1, r.shape[-1]) for r in res[:-1]], res[-1]


class Reduce:
    def __init__(self, place, counts, kinds, srcs, outs, scratch, lag=(1, 2)):
        self.p, self.counts, self.kinds, self.srcs, self.outs = place, counts, kinds, srcs, outs
        (self.own, self.cb, self.xb, self.zb, self.mb, self.u2, self.fin,
         self.load, self.cs, self.cr, self.xs, self.xr, self.zs, self.zr, self.ms, self.mr, self.fs, self.fr,
         self.ps, self.pr, self.st) = scratch
        p = place
        self.total = sum(counts)
        self.n = p.lines // 2
        self.zi = p.dp // 2
        left = self.zi // (self.n // 2)
        self.e = self.zi * (1 - left) + (self.n - 1 - self.zi) * left
        step = 2 * (1 - 2 * left)
        self.inner = (p.dp + step, p.me)
        self.outer = (p.dp - step, p.me)
        self.last = self.n // 2 - 1
        self.stages = ([self.begin, self.core_add] + [functools.partial(self.group_add, t) for t in range(p.bits)]
                       + [functools.partial(self.climb, j) for j in range(1, self.last + 1)] + [self.middle]
                       + [functools.partial(self.descend, j) for j in range(self.last - 1, -1, -1)])
        self.lags = [0, lag[0]] + [lag[0] + lag[1] * (i + 1) for i in range(len(self.stages) - 2)]
        self.ticks = self.total + self.lags[-1]

    @staticmethod
    def scratch(total, groups, rows, cols):
        sem = pltpu.SemaphoreType.DMA
        vm = lambda *lead: pltpu.VMEM((total,) + lead + (rows // 2, cols), bf16)
        one = sem((total,))
        line = pltpu.VMEM((total, rows, cols), bf16)
        return [vm(groups, 2), vm(groups, 2), vm(2, groups - 1), line, line, line, line,
                one, one, one, sem((total, 2, groups - 1)), sem((total, 2, groups - 1)),
                one, one, one, one, one, one, one, one, one]

    def greet(self):
        p = self.p
        barrier = pltpu.get_barrier_semaphore()
        for where in [(p.partner, p.me)] + [(p.dp, flip(p.me, b)) for b in range(p.bits)] + [self.inner]:
            pl.semaphore_signal(barrier, inc=1, device_id=where, device_id_type=MESH)
        @pl.when(self.e > 0)
        def _():
            pl.semaphore_signal(barrier, inc=1, device_id=self.outer, device_id_type=MESH)
        half = self.n // 2
        pl.semaphore_wait(barrier, 2 + p.bits + (self.e + half - 1) // half)

    def source(self, k, fn):
        base = 0
        for i, count in enumerate(self.counts):
            @pl.when((k >= base) & (k < base + count))
            def _(i=i, base=base):
                fn(i, k - base)
            base += count

    def target(self, i, j, core):
        rows, cols = self.fin.shape[1:]
        out = self.outs[i]
        if self.kinds[i] == "cols":
            return out.at[:, pl.ds(pl.multiple_of((2 * j + core) * cols, cols), cols)]
        return out.at[pl.ds(pl.multiple_of(j * rows, rows), rows), pl.ds(pl.multiple_of(core * cols, cols), cols)]

    def load_copy(self, k, src):
        return pltpu.make_async_copy(src.at[self.p.core], self.own.at[k], self.load.at[k])

    def core_copy(self, k, src):
        p = self.p
        return remote(src.at[1 - p.core], self.cb.at[k], self.cs.at[k], self.cr.at[k], (p.partner, p.me))

    def begin(self, k):
        def go(i, j):
            self.core_copy(k, self.srcs[i].at[j]).start()
            self.load_copy(k, self.srcs[i].at[j]).start()
        self.source(k, go)

    def slot(self, order, t, mask):
        base = sum(self.p.groups >> (u + 1) for u in range(t))
        return base + subsets(order[t + 1:]).index(mask)

    def group_copy(self, k, color, t, mask):
        p = self.p
        order = p.orders[color]
        i = self.slot(order, t, mask)
        return remote(self.own.at[k, xor(p.me, (1 << order[t]) | mask), color], self.xb.at[k, color, i],
                      self.xs.at[k, color, i], self.xr.at[k, color, i], (p.dp, flip(p.me, order[t])))

    def group_send(self, k, t):
        for color in (0, 1):
            for mask in subsets(self.p.orders[color][t + 1:]):
                self.group_copy(k, color, t, mask).start()

    def core_add(self, k):
        self.load_copy(k, self.srcs[0].at[0]).wait()
        self.core_copy(k, self.srcs[0].at[0]).wait_recv()
        for f in range(self.p.groups):
            for color in (0, 1):
                self.own[k, f, color] = (self.own[k, f, color].astype(f32) + self.cb[k, f, color].astype(f32)).astype(bf16)
        self.group_send(k, 0)

    def group_add(self, t, k):
        p = self.p
        for color in (0, 1):
            order = p.orders[color]
            for mask in subsets(order[t + 1:]):
                self.group_copy(k, color, t, mask).wait_recv()
                blk, i = xor(p.me, mask), self.slot(order, t, mask)
                total = self.own[k, blk, color].astype(f32) + self.xb[k, color, i].astype(f32)
                if t == p.bits - 1:
                    self.u2[k, self.part(color)] = total.astype(bf16)
                else:
                    self.own[k, blk, color] = total.astype(bf16)
        if t < p.bits - 1:
            self.group_send(k, t + 1)
        else:
            @pl.when(self.e == 0)
            def _():
                (self.climb_copy(k) if self.last > 0 else self.middle_copy(k)).start()

    def part(self, color):
        half = self.u2.shape[1] // 2
        return slice(color * half, (color + 1) * half)

    def climb_copy(self, k):
        return remote(self.u2.at[k], self.zb.at[k], self.zs.at[k], self.zr.at[k], self.inner)

    def middle_copy(self, k):
        return remote(self.u2.at[k], self.mb.at[k], self.ms.at[k], self.mr.at[k], self.inner)

    def climb(self, j, k):
        @pl.when(self.e == j)
        def _():
            self.climb_copy(k).wait_recv()
            for color in (0, 1):
                total = self.u2[k, self.part(color)].astype(f32) + self.zb[k, self.part(color)].astype(f32)
                self.u2[k, self.part(color)] = total.astype(bf16)
            (self.middle_copy(k) if j == self.last else self.climb_copy(k)).start()

    def share_copy(self, k):
        return remote(self.fin.at[k], self.fin.at[k], self.fs.at[k], self.fr.at[k], self.outer)

    def share_wait(self, k):
        return remote(self.fin.at[k], self.fin.at[k], self.fs.at[k], self.fr.at[k], self.inner)

    def pass_copy(self, k, dst):
        p = self.p
        return remote(self.fin.at[k], dst, self.ps.at[k], self.pr.at[k], (p.partner, p.me))

    def store_copy(self, k, dst):
        return pltpu.make_async_copy(self.fin.at[k], dst, self.st.at[k])

    def done(self, k):
        def go(i, j):
            self.pass_copy(k, self.target(i, j, self.p.core)).start()
            self.store_copy(k, self.target(i, j, self.p.core)).start()
        self.source(k, go)

    def middle(self, k):
        @pl.when(self.e == self.last)
        def _():
            self.middle_copy(k).wait_recv()
            for color in (0, 1):
                total = self.u2[k, self.part(color)].astype(f32) + self.mb[k, self.part(color)].astype(f32)
                self.fin[k, self.part(color)] = total.astype(bf16)
            if self.last > 0:
                self.share_copy(k).start()
            self.done(k)

    def descend(self, j, k):
        @pl.when(self.e == j)
        def _():
            self.share_wait(k).wait_recv()
            if j > 0:
                self.share_copy(k).start()
            self.done(k)

    def tick(self, t):
        for s in range(len(self.stages) - 1, -1, -1):
            k = t - self.lags[s]
            @pl.when((k >= 0) & (k < self.total))
            def _(s=s, k=k):
                self.stages[s](k)

    def opening(self, step):
        @pl.when(step == 0)
        def _():
            self.greet()
        self.tick(step)

    def closing(self, step, steps):
        @pl.when(step == steps - 1)
        def _():
            @pl.loop(steps, max(self.ticks, steps))
            def _(t):
                self.tick(t)
            self.drain()

    def drain(self):
        p = self.p
        @pl.loop(0, self.total)
        def _(k):
            self.core_copy(k, self.srcs[0].at[0]).wait_send()
            for color in (0, 1):
                for t in range(p.bits):
                    for mask in subsets(p.orders[color][t + 1:]):
                        self.group_copy(k, color, t, mask).wait_send()
            @pl.when(self.e == self.last)
            def _():
                self.middle_copy(k).wait_send()
            @pl.when(self.e < self.last)
            def _():
                self.climb_copy(k).wait_send()
            @pl.when(self.e > 0)
            def _():
                self.share_copy(k).wait_send()
            def go(i, j):
                self.pass_copy(k, self.target(i, j, 1 - p.core)).wait()
                self.store_copy(k, self.target(i, j, p.core)).wait()
            self.source(k, go)


def reduced_shapes(grads, kinds):
    rows, cols = 2 * grads[0].shape[-2], 2 * grads[0].shape[-1]
    return [jax.ShapeDtypeStruct((rows, g.shape[0] * cols) if kind == "cols" else (g.shape[0] * rows, cols), bf16)
            for g, kind in zip(grads, kinds)]


def wgrad_cols_kernel(a_ref, b_ref, o_ref):
    y = dot(a_ref[...], b_ref[...], TN).astype(bf16)
    _, _, g, _, r, c = o_ref.shape
    for half in (0, 1):
        o_ref[0, half] = y[:, half * c:(half + 1) * c].reshape(g, 2, r, c)


def wgrad_cols(a, b, groups):
    s, m = a.shape
    n = b.shape[1]
    r, c = m // groups // 2, m // 2
    return pl.pallas_call(
        wgrad_cols_kernel, grid=(n // m,),
        in_specs=[pl.BlockSpec((s, m), lambda i: (0, 0)), pl.BlockSpec((s, m), lambda i: (0, i))],
        out_specs=pl.BlockSpec((1, 2, groups, 2, r, c), lambda i: (i, 0, 0, 0, 0, 0)),
        out_shape=jax.ShapeDtypeStruct((n // m, 2, groups, 2, r, c), bf16),
        cost_estimate=pl.CostEstimate(flops=2 * s * m * n, bytes_accessed=2 * (s * (m + n) + m * n),
                                      transcendentals=0), name="wgrad_cols")(a, b)


def wgrad_rows_kernel(a_ref, b_ref, o_ref):
    y = dot(a_ref[...], b_ref[...], TN).astype(bf16)
    q, _, _, _, r, c = o_ref.shape
    for half in (0, 1):
        o_ref[:, half, 0] = y[:, half * c:(half + 1) * c].reshape(q, 2, r, c)


def wgrad_rows(a, b, groups):
    s, m = a.shape
    n = b.shape[1]
    q, r, c = m // n, n // groups // 2, n // 2
    return pl.pallas_call(
        wgrad_rows_kernel, grid=(groups,),
        in_specs=[pl.BlockSpec((s, m // groups), lambda i: (0, i)), pl.BlockSpec((s, n), lambda i: (0, 0))],
        out_specs=pl.BlockSpec((q, 2, 1, 2, r, c), lambda i: (0, 0, i, 0, 0, 0)),
        out_shape=jax.ShapeDtypeStruct((q, 2, groups, 2, r, c), bf16),
        cost_estimate=pl.CostEstimate(flops=2 * s * m * n, bytes_accessed=2 * (s * (m + n) + m * n),
                                      transcendentals=0), name="wgrad_rows")(a, b)


def attn_fwd_kernel(shape, count, rows, *refs):
    len_ref, q_ref, k_ref, v_ref = refs[:4]
    ins = refs[4:4 + count]
    o_ref, lse_ref = refs[4 + count:6 + count]
    outs = refs[6 + count:6 + 2 * count]
    step, steps = pl.program_id(0), pl.num_programs(0)
    p = Place(shape)
    g = Gather(p, ins, outs, refs[6 + 2 * count:])
    @pl.when(step == 0)
    def _():
        greet(gather_peers(p, False))
        for w in range(count):
            g.start(w)
    for w, at in ((0, 2), (1, 4)):
        @pl.when(step == at)
        def _(w=w):
            g.after(w, 0)
    attn_fwd_body(len_ref, q_ref, k_ref, v_ref, o_ref, lse_ref, rows)
    @pl.when(step == steps - 1)
    def _():
        for w in range(2, count):
            g.after(w, 0)
        for t in range(1, p.bits):
            for w in range(count):
                g.after(w, t)
        for w in range(count):
            g.finish(w)


def attn_fwd_call(shape, length, qkv, ws, rows=256):
    groups = shape["fsdp"]
    s, d3 = qkv.shape
    d = d3 // 3
    np_ = d // 128
    sd = jax.ShapeDtypeStruct
    res = pl.pallas_call(
        functools.partial(attn_fwd_kernel, shape, len(ws), rows), grid=(np_,),
        in_specs=[pl.BlockSpec(memory_space=pltpu.SMEM), pl.BlockSpec((s, 128), lambda i: (0, i)),
                  pl.BlockSpec((s, 128), lambda i: (0, np_ + i)),
                  pl.BlockSpec((s, 128), lambda i: (0, 2 * np_ + i))] + [ANY] * len(ws),
        out_specs=[pl.BlockSpec((s, 128), lambda i: (0, i)), pl.BlockSpec((s, 128), lambda i: (0, 0))]
        + [ANY] * len(ws),
        out_shape=[sd((s, d), bf16), sd((s, 128), f32)] + [gather_shape(w, groups) for w in ws],
        scratch_shapes=Gather.scratch(len(ws), groups),
        compiler_params=pltpu.CompilerParams(collective_id=2, has_side_effects=True),
        cost_estimate=pl.CostEstimate(flops=8 * s * s * d, bytes_accessed=8 * s * d, transcendentals=s * s * 12),
        name="attn_fwd")(length, qkv, qkv, qkv, *[quarter(w) for w in ws])
    return res[0], res[1], [r.reshape(-1, r.shape[-1]) for r in res[2:]]


def attn_bwd_kernel(shape, counts, kinds, pairs, rows, *refs):
    n = len(counts)
    ins, srcs, grads, outs = refs[:9], refs[9:9 + n], refs[9 + n:12 + n], refs[12 + n:12 + 2 * n]
    work, scratch = refs[12 + 2 * n:15 + 2 * n], refs[15 + 2 * n:]
    step = pl.program_id(0) * 2 + pl.program_id(1)
    r = Reduce(Place(shape), counts, kinds, srcs, outs, scratch)
    r.opening(step)
    attn_bwd_body(*ins, *grads, *work, rows)
    r.closing(step, 2 * pairs)


def attn_bwd_call(shape, length, qkv, att, gatt, lse, cos, sin, grads, kinds, rows=256):
    groups = shape["fsdp"]
    s, d3 = qkv.shape
    d = d3 // 3
    np_ = d // 128
    counts = [g.shape[0] for g in grads]
    r, c = 2 * grads[0].shape[-2], grads[0].shape[-1]
    col = pl.BlockSpec((s, 128), lambda i, h: (0, i))
    const = pl.BlockSpec((s, 128), lambda i, h: (0, 0))
    res = pl.pallas_call(
        functools.partial(attn_bwd_kernel, shape, counts, kinds, np_, rows), grid=(np_, 2),
        in_specs=[pl.BlockSpec(memory_space=pltpu.SMEM), col,
                  pl.BlockSpec((s, 128), lambda i, h: (0, np_ + i)),
                  pl.BlockSpec((s, 128), lambda i, h: (0, 2 * np_ + i)), col, col, const, const, const]
        + [ANY] * len(grads),
        out_specs=[col, col, col] + [ANY] * len(grads),
        out_shape=[jax.ShapeDtypeStruct((s, d), bf16)] * 3 + reduced_shapes(grads, kinds),
        scratch_shapes=[pltpu.VMEM((128, s), f32), pltpu.VMEM((s, 128), f32), pltpu.VMEM((s, 128), f32)]
        + Reduce.scratch(sum(counts), groups, r, c),
        compiler_params=pltpu.CompilerParams(collective_id=3, has_side_effects=True, vmem_limit_bytes=64000 * 1024),
        cost_estimate=pl.CostEstimate(flops=20 * s * s * d, bytes_accessed=16 * s * d, transcendentals=s * s * 12),
        name="attn_bwd")(length, qkv, qkv, qkv, att, gatt, lse, cos, sin, *grads)
    return res[:3], res[3:]


def post_kernel(shape, counts, kinds, steps, *refs):
    n = len(counts)
    ins, srcs, outs, reduced = refs[:8], refs[8:8 + n], refs[8 + n:10 + n], refs[10 + n:10 + 2 * n]
    r = Reduce(Place(shape), counts, kinds, srcs, reduced, refs[10 + 2 * n:])
    step = pl.program_id(0)
    r.opening(step)
    post_body(*ins, *outs)
    r.closing(step, steps)


def post_call(shape, dq, dk, dv, tok, flag, gh1, vec, w, grads, kinds, rows=128):
    s, d = tok.shape
    row = lambda c: pl.BlockSpec((rows, c), lambda i: (i, 0))
    whole = lambda a: pl.BlockSpec(a.shape, lambda i: (0, 0))
    sd = jax.ShapeDtypeStruct
    counts = [g.shape[0] for g in grads]
    r, c = 2 * grads[0].shape[-2], grads[0].shape[-1]
    res = pl.pallas_call(
        functools.partial(post_kernel, shape, counts, kinds, s // rows), grid=(s // rows,),
        in_specs=[row(d), row(d), row(d), row(d), row(1), row(d), whole(vec), whole(w)] + [ANY] * len(grads),
        out_specs=[row(d), pl.BlockSpec((8, d), lambda i: (0, 0))] + [ANY] * len(grads),
        out_shape=[sd((s, d), bf16), sd((8, d), f32)] + reduced_shapes(grads, kinds),
        scratch_shapes=Reduce.scratch(sum(counts), shape["fsdp"], r, c),
        compiler_params=pltpu.CompilerParams(collective_id=4, has_side_effects=True, vmem_limit_bytes=64000 * 1024),
        cost_estimate=pl.CostEstimate(flops=6 * s * d * d, bytes_accessed=16 * s * d, transcendentals=0),
        name="post")(dq, dk, dv, tok, flag, gh1, vec, w, *grads)
    return res[0], res[1], res[2:]
from jax.sharding import PartitionSpec as P

highest = lax.Precision.HIGHEST


def rotary_tables(length):
    half = HD // 2
    rate = 1.0 / 10000.0 ** (jnp.arange(half, dtype=f32) * 2.0 / HD)
    angle = jnp.arange(length, dtype=f32)[:, None] * rate[None, :]
    angle = jnp.concatenate([angle] * (128 // half), axis=-1)
    sign = jnp.where(jnp.arange(128) % HD < half, -1.0, 1.0)
    return jnp.cos(angle), jnp.sin(angle) * sign


def per_device(shape, tokens, hidden_token_indicator, lengths, time_ids, cotangent, gain_one, w_qkv, w_out, gain_two,
               w_fc1, b_fc1, w_fc2, b_fc2, w_ada, b_ada, mask_embed, time_table):
    groups = shape["fsdp"]
    s, d = tokens.shape[1:]
    ff = b_fc1.shape[0] * groups
    tok, cot = tokens[0], cotangent[0]
    flag = hidden_token_indicator.reshape(s, 1)
    sizes = [v.shape[0] for v in (gain_one, gain_two, b_fc2, mask_embed, b_fc1, b_ada)]
    small = jnp.concatenate([gain_one, gain_two, b_fc2, mask_embed, b_fc1, b_ada])[None]
    (ada_all, qkv_all), packed = head_call(shape, small, [w_ada, w_qkv])
    packed = packed[:, 0]
    cuts = [sum(sizes[:i]) for i in range(len(sizes) + 1)]
    gain1, gain2, b2, emb, b1, bada = (
        packed[:, cuts[i]:cuts[i + 1]].reshape(1, -1).astype(f32) for i in range(len(sizes)))
    cond_pre = lax.dynamic_slice_in_dim(time_table, time_ids[0], 1, axis=0)
    cond = jax.nn.silu(cond_pre)
    modulation = jnp.dot(cond, ada_all.astype(f32).T, precision=highest) + bada
    shift_a, scale_a, gate_a, shift_m, scale_m, gate_m = (modulation[:, i * d:(i + 1) * d] for i in range(6))
    cos, sin = rotary_tables(s)
    zero = jnp.zeros((1, d), f32)
    vec_pre = jnp.concatenate([emb, gain1, scale_a, shift_a] + [zero] * 4, axis=0)
    vec_mid = jnp.concatenate([emb, gain2, scale_m, shift_m, gate_a, gate_m, b2, zero], axis=0)
    n1, qkv = pre_call(tok, flag, vec_pre, qkv_all, cos, sin)
    att, lse, (out_all, fc1_all, fc2_all) = attn_fwd_call(shape, lengths, qkv, [w_out, w_fc1, w_fc2])
    out, gh1, gatt, n2, act, gm, gpre, gap, sums, gb1 = mid_call(
        lengths, att, tok, flag, cot, vec_mid, b1, out_all, fc1_all, fc2_all)
    g_fc2 = wgrad_rows(act, gm, groups)
    g_fc1 = wgrad_cols(n2, gpre, groups)
    g_out = wgrad_cols(att, gap, groups)
    (dq, dk, dv), (r_fc2, r_fc1, r_out) = attn_bwd_call(
        shape, lengths, qkv, att, gatt, lse, cos, sin, [g_fc2, g_fc1, g_out], ["rows", "cols", "cols"])
    g_qkv = [wgrad_cols(n1, x, groups) for x in (dq, dk, dv)]
    igrad, sums1, r_qkv = post_call(shape, dq, dk, dv, tok, flag, gh1, vec_pre, qkv_all, g_qkv, ["cols"] * 3)
    ggm, gb2, a2, s2, gga, st0, st1, st2 = (sums[i:i + 1] for i in range(8))
    a1, s1, gemb = (sums1[i:i + 1] for i in range(3))
    gmod = jnp.concatenate([s1, a1 * gain1, gga, s2, a2 * gain2, ggm], axis=1)
    small = jnp.concatenate([(1.0 + scale_a) * a1, (1.0 + scale_m) * a2, gb2, gemb, gb1, gmod], axis=1)
    stats = jnp.concatenate([jnp.sum(st0).reshape(1, 1), jnp.sum(st1).reshape(1, 1), jnp.sum(st2).reshape(1, 1),
                             lengths.astype(f32).reshape(1, 1), time_ids.astype(f32).reshape(1, 1)], axis=1)
    row = jnp.concatenate([small, cond_pre, stats, jnp.zeros((1, 123), f32)], axis=1)
    rows = lax.all_gather(row, ("dp", "fsdp"), axis=0, tiled=True)
    width = small.shape[1]
    conds, tail = rows[:, width:width + cond.shape[1]], rows[:, width + cond.shape[1]:]
    gmods = rows[:, width - gmod.shape[1]:width]
    silu_c, pull = jax.vjp(jax.nn.silu, conds)
    grad_cond = pull(jnp.dot(gmods, ada_all.astype(f32), precision=highest))[0]
    hot = (jnp.arange(time_table.shape[0])[:, None] == tail[:, 4].astype(jnp.int32)[None, :]).astype(f32)
    table = jnp.dot(hot, grad_cond, precision=highest)
    totals = jnp.sum(tail[:, :4], axis=0)
    rms = jnp.sqrt(totals[:3] / (totals[3] * d))
    me = lax.axis_index("fsdp")
    parts, base = [], 0
    for size in sizes:
        parts.append(jnp.sum(lax.dynamic_slice_in_dim(rows, base + me * size, size, axis=1), axis=0))
        base += size * groups
    g1, g2, gb2, gemb, gb1, gbada = parts
    n_ada = w_ada.shape[0]
    mods = lax.dynamic_slice_in_dim(rows, width - gmod.shape[1] + me * n_ada, n_ada, axis=1)
    g_ada = lax.dot_general(mods, silu_c, (((0,), (0,)), ((), ())), precision=highest)

    return (out[None], igrad[None], g1, jnp.concatenate(r_qkv, axis=1).astype(f32), r_out.astype(f32), g2, r_fc1.astype(f32), gb1,
            r_fc2.astype(f32), gb2,
            g_ada, gbada, gemb, table, rms)


def solution(mesh):
    both = ("dp", "fsdp")
    f1, f2 = P("fsdp"), P("fsdp", None)
    placed = (P(both, None, None), P(both, None), P(both), P(both), P(both, None, None), f1, f2, f2, f1, f2, f1, f2, f1,
              f2, f1, f1, P())
    outs = (P(both, None, None), P(both, None, None), f1, f2, f2, f1, f2, f1, f2, f1, f2, f1, f1, P(), P())
    return jax.shard_map(functools.partial(per_device, dict(mesh.shape)), mesh=mesh, in_specs=placed, out_specs=outs,
                         check_vma=False)
```

```python
import functools, math
import jax, jax.numpy as jnp
from jax import lax
from jax.experimental import pallas as pl
from jax.experimental.pallas import tpu as pltpu

HD = 64
EPS = 1e-5
LOG2E = math.log2(math.e)
QSCALE = LOG2E * HD ** -0.5
f32, bf16 = jnp.float32, jnp.bfloat16
NT = (((1,), (1,)), ((), ()))
NN = (((1,), (0,)), ((), ()))
TN = (((0,), (0,)), ((), ()))

def dot(a, b, dims=NN):
    return lax.dot_general(a, b, dims, preferred_element_type=f32)

def norm_parts(x):
    mean = jnp.mean(x, axis=-1, keepdims=True)
    cen = x - mean
    rs = lax.rsqrt(jnp.mean(cen * cen, axis=-1, keepdims=True) + EPS)
    return cen * rs, rs

def swap_halves(u):
    lane = lax.broadcasted_iota(jnp.int32, u.shape, 1)
    return jnp.where(lane % HD < HD // 2, pltpu.roll(u, 96, 1), pltpu.roll(u, 32, 1))

def pre_kernel(tok_ref, flag_ref, vec_ref, w_ref, cos_ref, sin_ref, n1_ref, qkv_ref):
    emb, gain, scale, shift = (vec_ref[i:i + 1, :] for i in range(4))
    h0 = jnp.where(flag_ref[...] == 1, emb, tok_ref[...].astype(f32))
    n, _ = norm_parts(h0)
    n1 = (n * gain * (1.0 + scale) + shift).astype(bf16)
    n1_ref[...] = n1
    d = n1.shape[1]
    cos, sin = cos_ref[...], sin_ref[...]
    for part in range(3):
        y = dot(n1, w_ref[:, part * d:(part + 1) * d])
        for c in range(d // 128):
            lo = part * d + c * 128
            u = y[:, c * 128:(c + 1) * 128]
            if part < 2:
                u = u * cos + swap_halves(u) * sin
                if part == 0:
                    u = u * QSCALE
            qkv_ref[:, lo:lo + 128] = u.astype(bf16)

def pre_call(tok, flag, vecs, w, cos, sin, rows=256):
    s, d = tok.shape
    return pl.pallas_call(
        pre_kernel, grid=(s // rows,),
        in_specs=[pl.BlockSpec((rows, d), lambda i: (i, 0)), pl.BlockSpec((rows, 1), lambda i: (i, 0)),
                  pl.BlockSpec((8, d), lambda i: (0, 0)), pl.BlockSpec((d, 3 * d), lambda i: (0, 0)),
                  pl.BlockSpec((rows, 128), lambda i: (i, 0)), pl.BlockSpec((rows, 128), lambda i: (i, 0))],
        out_specs=[pl.BlockSpec((rows, d), lambda i: (i, 0)), pl.BlockSpec((rows, 3 * d), lambda i: (i, 0))],
        out_shape=[jax.ShapeDtypeStruct((s, d), bf16), jax.ShapeDtypeStruct((s, 3 * d), bf16)],
        cost_estimate=pl.CostEstimate(flops=2 * s * d * 3 * d, bytes_accessed=12 * s * d, transcendentals=0),
        name="pre")(tok, flag, vecs, w, cos, sin)

def attn_fwd_body(len_ref, q_ref, k_ref, v_ref, o_ref, lse_ref, rows):
    p = pl.program_id(0)
    s = q_ref.shape[0]
    length = len_ref[0]
    lane = lax.broadcasted_iota(jnp.int32, (s, 128), 1)
    pos = lax.broadcasted_iota(jnp.int32, (s, 128), 0)
    lane_q = lax.broadcasted_iota(jnp.int32, (rows, 128), 1)
    k = k_ref[...].astype(f32)
    v = v_ref[...].astype(f32)
    kx, vx = [], []
    for h in (0, 1):
        extra = HD * (1 - h)
        mine = (lane >= HD) if h else (lane < HD)
        bias = jnp.where(pos >= length, -1e30, 0.0)
        kx.append(jnp.where(mine, k, jnp.where(lane == extra, bias, 0.0)).astype(bf16))
        vx.append(jnp.where(mine, v, jnp.where(lane == extra, 1.0, 0.0)).astype(bf16))
    for b in range(s // rows):
        q = q_ref[b * rows:(b + 1) * rows, :].astype(f32)
        outs, lses = [], []
        for h in (0, 1):
            extra = HD * (1 - h)
            mine = (lane_q >= HD) if h else (lane_q < HD)
            qx = jnp.where(mine, q, jnp.where(lane_q == extra, 1.0, 0.0)).astype(bf16)
            sc = dot(qx, kx[h], NT)
            m = jnp.max(sc, axis=1, keepdims=True)
            pr = jnp.exp2(sc - m).astype(bf16)
            o = dot(pr, vx[h])
            tot = o[:, extra:extra + 1]
            outs.append(o * (1.0 / tot))
            lses.append(m + jnp.log(tot) * LOG2E)
        o_ref[b * rows:(b + 1) * rows, :] = jnp.where(lane_q < HD, outs[0], outs[1]).astype(bf16)
        old = jnp.where(p == 0, 0.0, lse_ref[b * rows:(b + 1) * rows, :])
        lse_ref[b * rows:(b + 1) * rows, :] = jnp.where(
            lane_q == 2 * p, lses[0], jnp.where(lane_q == 2 * p + 1, lses[1], old))

def split3(x):
    hi = x.astype(bf16).astype(f32)
    r = x - hi
    mid = r.astype(bf16).astype(f32)
    return hi, mid, r - mid

def attn_bwd_body(len_ref, q_ref, k_ref, v_ref, o_ref, g_ref, lse_ref, cos_ref, sin_ref,
                  dq_ref, dk_ref, dv_ref, dqs, dks, dvs, rows):
    p, h = pl.program_id(0), pl.program_id(1)
    s = q_ref.shape[0]
    length = len_ref[0]
    lane = lax.broadcasted_iota(jnp.int32, (s, 128), 1)
    pos = lax.broadcasted_iota(jnp.int32, (s, 128), 0)
    lane_q = lax.broadcasted_iota(jnp.int32, (rows, 128), 1)
    e = HD * (1 - h)
    mine, mine_q = lane // HD == h, lane_q // HD == h
    k = k_ref[...].astype(f32)
    v = v_ref[...].astype(f32)
    ones = jnp.where((lane >= e) & (lane < e + 3), 1.0, 0.0)
    bias = jnp.where(pos >= length, -1e30, 0.0)
    kx = jnp.where(mine, k, jnp.where(lane == e + 3, bias, ones)).astype(bf16)
    vx = jnp.where(mine, v, ones).astype(bf16)
    kt = jnp.where(mine, k, 0.0).T.astype(bf16)
    dk = jnp.zeros((s, 128), f32)
    dv = jnp.zeros((s, 128), f32)
    for b in range(s // rows):
        sl = slice(b * rows, (b + 1) * rows)
        qb = q_ref[sl, :]
        gb = g_ref[sl, :]
        q = qb.astype(f32)
        g = gb.astype(f32)
        lse = jnp.sum(jnp.where(lane_q == 2 * p + h, lse_ref[sl, :], 0.0), axis=1, keepdims=True)
        dd = jnp.sum(jnp.where(mine_q, g * o_ref[sl, :].astype(f32), 0.0), axis=1, keepdims=True)
        l0, l1, l2 = split3(-lse)
        d0, d1, d2 = split3(-dd)
        qx = jnp.where(mine_q, q, jnp.where(lane_q == e, l0, jnp.where(lane_q == e + 1, l1, jnp.where(
            lane_q == e + 2, l2, jnp.where(lane_q == e + 3, 1.0, 0.0))))).astype(bf16)
        gx = jnp.where(mine_q, g, jnp.where(lane_q == e, d0, jnp.where(lane_q == e + 1, d1, jnp.where(
            lane_q == e + 2, d2, 0.0)))).astype(bf16)
        pt = jnp.exp2(dot(kx, qx, NT))
        dst = (pt * dot(vx, gx, NT)).astype(bf16)
        dv = dv + dot(pt.astype(bf16), gb)
        dk = dk + dot(dst, qb)
        dqt = dot(kt, dst)
        dqs[:, sl] = jnp.where(h == 0, dqt, dqs[:, sl] + dqt)
    @pl.when(h == 0)
    def _():
        dks[...] = dk
        dvs[...] = dv
    @pl.when(h == 1)
    def _():
        cos, sin = cos_ref[...], sin_ref[...]
        dq = dqs[...].T * (HD ** -0.5)
        dkk = jnp.where(lane < HD, dks[...], dk) * (1.0 / LOG2E)
        dq_ref[...] = (dq * cos - swap_halves(dq) * sin).astype(bf16)
        dk_ref[...] = (dkk * cos - swap_halves(dkk) * sin).astype(bf16)
        dv_ref[...] = jnp.where(lane < HD, dvs[...], dv).astype(bf16)


def gelu_both(v):
    a, b = 0.7978845608028654, 0.044715
    v2 = v * v
    t = jnp.tanh(a * v * (1.0 + b * v2))
    half = 0.5 + 0.5 * t
    return v * half, half + (0.5 * a) * v * (1.0 - t * t) * (1.0 + 3.0 * b * v2)

def colsum(x):
    return jnp.sum(x, axis=0, keepdims=True)

def mid_kernel(len_ref, att_ref, tok_ref, flag_ref, cot_ref, vec_ref, b1_ref, wo_ref, w1_ref, w2_ref,
               out_ref, gh1_ref, gatt_ref, n2_ref, act_ref, gm_ref, gpre_ref, gap_ref, sum_ref, sb1_ref,
               gp_s, *, cut):
    i = pl.program_id(0)
    rows, d = att_ref.shape
    ff = w1_ref.shape[1]
    emb, gain, scale, shift, gate_a, gate_m, b2 = (vec_ref[r:r + 1, :] for r in range(7))
    h0 = jnp.where(flag_ref[...] == 1, emb, tok_ref[...].astype(f32))
    ap = dot(att_ref[...], wo_ref[...])
    br_a = gate_a * ap
    h1 = h0 + br_a
    n, rs = norm_parts(h1)
    n2 = (n * gain * (1.0 + scale) + shift).astype(bf16)
    n2_ref[...] = n2
    mp = jnp.zeros((rows, d), f32) + b2
    for j in range(ff // cut):
        sl = slice(j * cut, (j + 1) * cut)
        act, gp = gelu_both(dot(n2, w1_ref[:, sl]) + b1_ref[:, sl])
        act = act.astype(bf16)
        act_ref[:, sl] = act
        gp_s[:, sl] = gp
        mp = mp + dot(act, w2_ref[sl, :])
    br_m = gate_m * mp
    bo = h1 + br_m
    out_ref[...] = bo.astype(bf16)
    pos = lax.broadcasted_iota(jnp.int32, (rows, 1), 0) + i * rows
    valid = jnp.where(pos < len_ref[0], 1.0, 0.0)
    cot = cot_ref[...].astype(f32)
    gm = (gate_m * cot).astype(bf16)
    gm_ref[...] = gm
    gn2 = jnp.zeros((rows, d), f32)
    sb1 = []
    for j in range(ff // cut):
        sl = slice(j * cut, (j + 1) * cut)
        gpre = (dot(gm, w2_ref[sl, :], NT) * gp_s[:, sl]).astype(bf16)
        gpre_ref[:, sl] = gpre
        sb1.append(colsum(gpre.astype(f32)))
        gn2 = gn2 + dot(gpre, w1_ref[:, sl], NT)
    e = gn2 * (gain * (1.0 + scale))
    gh1 = cot + rs * (e - jnp.mean(e, axis=1, keepdims=True) - n * jnp.mean(e * n, axis=1, keepdims=True))
    gh1_ref[...] = gh1
    gap = (gate_a * gh1).astype(bf16)
    gap_ref[...] = gap
    gatt_ref[...] = dot(gap, wo_ref[...], NT).astype(bf16)
    new = jnp.concatenate([
        colsum(cot * mp), colsum(gm.astype(f32)), colsum(gn2 * n), colsum(gn2), colsum(gh1 * ap),
        colsum(valid * bo * bo), colsum(valid * br_a * br_a), colsum(valid * br_m * br_m)], axis=0)
    sb1 = jnp.concatenate(sb1, axis=1)
    @pl.when(i == 0)
    def _():
        sum_ref[...] = new
        sb1_ref[...] = sb1
    @pl.when(i > 0)
    def _():
        sum_ref[...] += new
        sb1_ref[...] += sb1

def mid_call(length, att, tok, flag, cot, vec, b1, wo, w1, w2, rows=256, cut=768):
    s, d = tok.shape
    ff = w1.shape[1]
    row = lambda c: pl.BlockSpec((rows, c), lambda i: (i, 0))
    whole = lambda a: pl.BlockSpec(a.shape, lambda i: (0, 0))
    sd = jax.ShapeDtypeStruct
    return pl.pallas_call(
        functools.partial(mid_kernel, cut=cut), grid=(s // rows,),
        in_specs=[pl.BlockSpec(memory_space=pltpu.SMEM), row(d), row(d), row(1), row(d), whole(vec), whole(b1),
                  whole(wo), whole(w1), whole(w2)],
        out_specs=[row(d), row(d), row(d), row(d), row(ff), row(d), row(ff), row(d),
                   pl.BlockSpec((8, d), lambda i: (0, 0)), pl.BlockSpec((1, ff), lambda i: (0, 0))],
        out_shape=[sd((s, d), bf16), sd((s, d), f32), sd((s, d), bf16), sd((s, d), bf16), sd((s, ff), bf16),
                   sd((s, d), bf16), sd((s, ff), bf16), sd((s, d), bf16), sd((8, d), f32), sd((1, ff), f32)],
        scratch_shapes=[pltpu.VMEM((rows, ff), f32)],
        compiler_params=pltpu.CompilerParams(vmem_limit_bytes=60000 * 1024),
        cost_estimate=pl.CostEstimate(flops=2 * s * d * (2 * d + 4 * ff), bytes_accessed=30 * s * d,
                                      transcendentals=s * ff),
        name="mid")(length, att, tok, flag, cot, vec, b1, wo, w1, w2)

def post_body(dq_ref, dk_ref, dv_ref, tok_ref, flag_ref, gh1_ref, vec_ref, w_ref, ig_ref, sum_ref):
    i = pl.program_id(0)
    d = tok_ref.shape[1]
    emb, gain, scale = (vec_ref[r:r + 1, :] for r in range(3))
    masked = flag_ref[...] == 1
    h0 = jnp.where(masked, emb, tok_ref[...].astype(f32))
    n, rs = norm_parts(h0)
    gn1 = dot(dq_ref[...], w_ref[:, :d], NT) + dot(dk_ref[...], w_ref[:, d:2 * d], NT) + dot(
        dv_ref[...], w_ref[:, 2 * d:], NT)
    e = gn1 * (gain * (1.0 + scale))
    gh0 = gh1_ref[...] + rs * (e - jnp.mean(e, axis=1, keepdims=True) - n * jnp.mean(e * n, axis=1, keepdims=True))
    ig_ref[...] = jnp.where(masked, 0.0, gh0).astype(bf16)
    zero = jnp.zeros((5, d), f32)
    new = jnp.concatenate([colsum(gn1 * n), colsum(gn1), colsum(jnp.where(masked, gh0, 0.0)), zero], axis=0)
    @pl.when(i == 0)
    def _():
        sum_ref[...] = new
    @pl.when(i > 0)
    def _():
        sum_ref[...] += new


MESH = pl.DeviceIdType.MESH


def flip(i, b):
    return i + 2 ** b * (1 - 2 * ((i // 2 ** b) % 2))


def xor(i, mask):
    b = 0
    while mask >> b:
        if (mask >> b) & 1:
            i = flip(i, b)
        b += 1
    return i


def subsets(bits):
    masks = [0]
    for b in bits:
        masks = masks + [m | (1 << b) for m in masks]
    return masks


def log2(n):
    return n.bit_length() - 1


class Place:
    def __init__(self, shape):
        self.groups, self.lines = shape["fsdp"], shape["dp"]
        self.bits = log2(self.groups)
        self.orders = [list(range(self.bits)), list(range(self.bits))[::-1]]
        self.me = lax.axis_index("fsdp")
        self.dp = lax.axis_index("dp")
        self.core = self.dp % 2
        self.partner = flip(self.dp, 0)


def remote(src, dst, ssem, rsem, where):
    return pltpu.make_async_remote_copy(src_ref=src, dst_ref=dst, send_sem=ssem, recv_sem=rsem, device_id=where,
                                        device_id_type=MESH)


class Gather:
    def __init__(self, place, ins, outs, sems):
        self.p, self.ins, self.outs = place, ins, outs
        self.ss, self.rs, self.fs, self.fr, self.os, self.orr = sems

    @staticmethod
    def scratch(count, groups):
        a = pltpu.SemaphoreType.DMA((count, 2, groups - 1))
        b = pltpu.SemaphoreType.DMA((count,))
        return [a, a, a, a, b, b]

    def send(self, w, color, t, mask):
        p = self.p
        order = p.orders[color]
        e = 2 ** t - 1 + subsets(order[:t]).index(mask)
        piece = p.core * 2 + color
        blk = xor(p.me, mask)
        src = self.ins[w].at[piece] if mask == 0 else self.outs[w].at[blk, piece]
        return remote(src, self.outs[w].at[blk, piece], self.ss.at[w, color, e], self.rs.at[w, color, e],
                      (p.dp, flip(p.me, order[t])))

    def arrival(self, w, color, t, mask):
        p = self.p
        order = p.orders[color]
        e = 2 ** t - 1 + subsets(order[:t]).index(mask)
        got = self.outs[w].at[xor(p.me, mask | (1 << order[t])), p.core * 2 + color]
        return e, got

    def landed(self, w, color, e, got):
        return remote(got, got, self.ss.at[w, color, e], self.rs.at[w, color, e], (self.p.partner, self.p.me))

    def forward(self, w, color, e, got):
        return remote(got, got, self.fs.at[w, color, e], self.fr.at[w, color, e], (self.p.partner, self.p.me))

    def own(self, w):
        p = self.p
        return remote(self.ins[w], self.outs[w].at[p.me], self.os.at[w], self.orr.at[w], (p.partner, p.me))

    def start(self, w):
        for t in range(self.p.bits):
            for color in (0, 1):
                self.send(w, color, t, 0).start()
        self.own(w).start()

    def after(self, w, t):
        for color in (0, 1):
            order = self.p.orders[color]
            for mask in subsets(order[:t]):
                e, got = self.arrival(w, color, t, mask)
                self.landed(w, color, e, got).wait_recv()
                for later in range(t + 1, self.p.bits):
                    self.send(w, color, later, mask | (1 << order[t])).start()
                self.forward(w, color, e, got).start()

    def finish(self, w):
        p = self.p
        for color in (0, 1):
            order = p.orders[color]
            for t in range(p.bits):
                for mask in subsets(order[:t]):
                    e, got = self.arrival(w, color, t, mask)
                    other = self.outs[w].at[xor(p.me, mask | (1 << order[t])), (1 - p.core) * 2 + color]
                    self.forward(w, color, e, other).wait_recv()
                    self.forward(w, color, e, got).wait_send()
                    self.send(w, color, t, mask).wait_send()
        self.own(w).wait()


class Direct:
    def __init__(self, place, src, out, sems):
        self.p, self.src, self.out = place, src, out
        self.ss, self.rs = sems

    @staticmethod
    def scratch(groups):
        return [pltpu.SemaphoreType.DMA((groups,))] * 2

    def copy(self, m, arrived):
        p = self.p
        where = (p.partner, p.me) if m == 0 else (p.dp, xor(p.me, m))
        slot = xor(p.me, m) if arrived else p.me
        return remote(self.src, self.out.at[slot], self.ss.at[m], self.rs.at[m], where)

    def start(self):
        for m in range(self.p.groups):
            self.copy(m, False).start()

    def finish(self):
        for m in range(self.p.groups):
            self.copy(m, True).wait_recv()
            self.copy(m, False).wait_send()


def greet(devices):
    barrier = pltpu.get_barrier_semaphore()
    for where in devices:
        pl.semaphore_signal(barrier, inc=1, device_id=where, device_id_type=MESH)
    pl.semaphore_wait(barrier, len(devices))


def gather_peers(p, everyone):
    masks = range(1, p.groups) if everyone else [1 << b for b in range(p.bits)]
    return [(p.partner, p.me)] + [(p.dp, xor(p.me, m)) for m in masks]


def quarter(w):
    return w.reshape(4, w.shape[0] // 4, w.shape[1])


def gather_shape(w, groups):
    return jax.ShapeDtypeStruct((groups, 4, w.shape[0] // 4, w.shape[1]), w.dtype)


ANY = pl.BlockSpec(memory_space=pl.ANY)


def head_kernel(shape, count, *refs):
    ins, small, outs, small_out = refs[:count], refs[count], refs[count + 1:2 * count + 1], refs[2 * count + 1]
    sems = refs[2 * count + 2:]
    p = Place(shape)
    g = Gather(p, ins, outs, sems[:6])
    s = Direct(p, small, small_out, sems[6:])
    greet(gather_peers(p, True))
    s.start()
    for w in range(count):
        g.start(w)
    for t in range(p.bits):
        for w in range(count):
            g.after(w, t)
    for w in range(count):
        g.finish(w)
    s.finish()


def head_call(shape, small, ws):
    groups = shape["fsdp"]
    outs = [gather_shape(w, groups) for w in ws] + [jax.ShapeDtypeStruct((groups,) + small.shape, small.dtype)]
    res = pl.pallas_call(
        functools.partial(head_kernel, shape, len(ws)), in_specs=[ANY] * (len(ws) + 1), out_specs=[ANY] * len(outs),
        out_shape=outs, scratch_shapes=Gather.scratch(len(ws), groups) + Direct.scratch(groups),
        compiler_params=pltpu.CompilerParams(collective_id=1, has_side_effects=True), name="head",
    )(*[quarter(w) for w in ws], small)
    return [r.reshape(-1, r.shape[-1]) for r in res[:-1]], res[-1]


class Reduce:
    def __init__(self, place, counts, kinds, srcs, outs, scratch, lag=(1, 2)):
        self.p, self.counts, self.kinds, self.srcs, self.outs = place, counts, kinds, srcs, outs
        (self.own, self.cb, self.xb, self.zb, self.mb, self.u2, self.fin,
         self.load, self.cs, self.cr, self.xs, self.xr, self.zs, self.zr, self.ms, self.mr, self.fs, self.fr,
         self.ps, self.pr, self.st) = scratch
        p = place
        self.total = sum(counts)
        self.n = p.lines // 2
        self.zi = p.dp // 2
        left = self.zi // (self.n // 2)
        self.e = self.zi * (1 - left) + (self.n - 1 - self.zi) * left
        step = 2 * (1 - 2 * left)
        self.inner = (p.dp + step, p.me)
        self.outer = (p.dp - step, p.me)
        self.last = self.n // 2 - 1
        self.stages = ([self.begin, self.core_add] + [functools.partial(self.group_add, t) for t in range(p.bits)]
                       + [functools.partial(self.climb, j) for j in range(1, self.last + 1)] + [self.middle]
                       + [functools.partial(self.descend, j) for j in range(self.last - 1, -1, -1)])
        self.lags = [0, lag[0]] + [lag[0] + lag[1] * (i + 1) for i in range(len(self.stages) - 2)]
        self.ticks = self.total + self.lags[-1]

    @staticmethod
    def scratch(total, groups, rows, cols):
        sem = pltpu.SemaphoreType.DMA
        vm = lambda *lead: pltpu.VMEM((total,) + lead + (rows // 2, cols), bf16)
        one = sem((total,))
        line = pltpu.VMEM((total, rows, cols), bf16)
        return [vm(groups, 2), vm(groups, 2), vm(2, groups - 1), line, line, line, line,
                one, one, one, sem((total, 2, groups - 1)), sem((total, 2, groups - 1)),
                one, one, one, one, one, one, one, one, one]

    def greet(self):
        p = self.p
        barrier = pltpu.get_barrier_semaphore()
        for where in [(p.partner, p.me)] + [(p.dp, flip(p.me, b)) for b in range(p.bits)] + [self.inner]:
            pl.semaphore_signal(barrier, inc=1, device_id=where, device_id_type=MESH)
        @pl.when(self.e > 0)
        def _():
            pl.semaphore_signal(barrier, inc=1, device_id=self.outer, device_id_type=MESH)
        half = self.n // 2
        pl.semaphore_wait(barrier, 2 + p.bits + (self.e + half - 1) // half)

    def source(self, k, fn):
        base = 0
        for i, count in enumerate(self.counts):
            @pl.when((k >= base) & (k < base + count))
            def _(i=i, base=base):
                fn(i, k - base)
            base += count

    def target(self, i, j, core):
        rows, cols = self.fin.shape[1:]
        out = self.outs[i]
        if self.kinds[i] == "cols":
            return out.at[:, pl.ds(pl.multiple_of((2 * j + core) * cols, cols), cols)]
        return out.at[pl.ds(pl.multiple_of(j * rows, rows), rows), pl.ds(pl.multiple_of(core * cols, cols), cols)]

    def load_copy(self, k, src):
        return pltpu.make_async_copy(src.at[self.p.core], self.own.at[k], self.load.at[k])

    def core_copy(self, k, src):
        p = self.p
        return remote(src.at[1 - p.core], self.cb.at[k], self.cs.at[k], self.cr.at[k], (p.partner, p.me))

    def begin(self, k):
        def go(i, j):
            self.core_copy(k, self.srcs[i].at[j]).start()
            self.load_copy(k, self.srcs[i].at[j]).start()
        self.source(k, go)

    def slot(self, order, t, mask):
        base = sum(self.p.groups >> (u + 1) for u in range(t))
        return base + subsets(order[t + 1:]).index(mask)

    def group_copy(self, k, color, t, mask):
        p = self.p
        order = p.orders[color]
        i = self.slot(order, t, mask)
        return remote(self.own.at[k, xor(p.me, (1 << order[t]) | mask), color], self.xb.at[k, color, i],
                      self.xs.at[k, color, i], self.xr.at[k, color, i], (p.dp, flip(p.me, order[t])))

    def group_send(self, k, t):
        for color in (0, 1):
            for mask in subsets(self.p.orders[color][t + 1:]):
                self.group_copy(k, color, t, mask).start()

    def core_add(self, k):
        self.load_copy(k, self.srcs[0].at[0]).wait()
        self.core_copy(k, self.srcs[0].at[0]).wait_recv()
        for f in range(self.p.groups):
            for color in (0, 1):
                self.own[k, f, color] = (self.own[k, f, color].astype(f32) + self.cb[k, f, color].astype(f32)).astype(bf16)
        self.group_send(k, 0)

    def group_add(self, t, k):
        p = self.p
        for color in (0, 1):
            order = p.orders[color]
            for mask in subsets(order[t + 1:]):
                self.group_copy(k, color, t, mask).wait_recv()
                blk, i = xor(p.me, mask), self.slot(order, t, mask)
                total = self.own[k, blk, color].astype(f32) + self.xb[k, color, i].astype(f32)
                if t == p.bits - 1:
                    self.u2[k, self.part(color)] = total.astype(bf16)
                else:
                    self.own[k, blk, color] = total.astype(bf16)
        if t < p.bits - 1:
            self.group_send(k, t + 1)
        else:
            @pl.when(self.e == 0)
            def _():
                (self.climb_copy(k) if self.last > 0 else self.middle_copy(k)).start()

    def part(self, color):
        half = self.u2.shape[1] // 2
        return slice(color * half, (color + 1) * half)

    def climb_copy(self, k):
        return remote(self.u2.at[k], self.zb.at[k], self.zs.at[k], self.zr.at[k], self.inner)

    def middle_copy(self, k):
        return remote(self.u2.at[k], self.mb.at[k], self.ms.at[k], self.mr.at[k], self.inner)

    def climb(self, j, k):
        @pl.when(self.e == j)
        def _():
            self.climb_copy(k).wait_recv()
            for color in (0, 1):
                total = self.u2[k, self.part(color)].astype(f32) + self.zb[k, self.part(color)].astype(f32)
                self.u2[k, self.part(color)] = total.astype(bf16)
            (self.middle_copy(k) if j == self.last else self.climb_copy(k)).start()

    def share_copy(self, k):
        return remote(self.fin.at[k], self.fin.at[k], self.fs.at[k], self.fr.at[k], self.outer)

    def share_wait(self, k):
        return remote(self.fin.at[k], self.fin.at[k], self.fs.at[k], self.fr.at[k], self.inner)

    def pass_copy(self, k, dst):
        p = self.p
        return remote(self.fin.at[k], dst, self.ps.at[k], self.pr.at[k], (p.partner, p.me))

    def store_copy(self, k, dst):
        return pltpu.make_async_copy(self.fin.at[k], dst, self.st.at[k])

    def done(self, k):
        def go(i, j):
            self.pass_copy(k, self.target(i, j, self.p.core)).start()
            self.store_copy(k, self.target(i, j, self.p.core)).start()
        self.source(k, go)

    def middle(self, k):
        @pl.when(self.e == self.last)
        def _():
            self.middle_copy(k).wait_recv()
            for color in (0, 1):
                total = self.u2[k, self.part(color)].astype(f32) + self.mb[k, self.part(color)].astype(f32)
                self.fin[k, self.part(color)] = total.astype(bf16)
            if self.last > 0:
                self.share_copy(k).start()
            self.done(k)

    def descend(self, j, k):
        @pl.when(self.e == j)
        def _():
            self.share_wait(k).wait_recv()
            if j > 0:
                self.share_copy(k).start()
            self.done(k)

    def tick(self, t):
        for s in range(len(self.stages) - 1, -1, -1):
            k = t - self.lags[s]
            @pl.when((k >= 0) & (k < self.total))
            def _(s=s, k=k):
                self.stages[s](k)

    def opening(self, step):
        @pl.when(step == 0)
        def _():
            self.greet()
        self.tick(step)

    def closing(self, step, steps):
        @pl.when(step == steps - 1)
        def _():
            @pl.loop(steps, max(self.ticks, steps))
            def _(t):
                self.tick(t)
            self.drain()

    def drain(self):
        p = self.p
        @pl.loop(0, self.total)
        def _(k):
            self.core_copy(k, self.srcs[0].at[0]).wait_send()
            for color in (0, 1):
                for t in range(p.bits):
                    for mask in subsets(p.orders[color][t + 1:]):
                        self.group_copy(k, color, t, mask).wait_send()
            @pl.when(self.e == self.last)
            def _():
                self.middle_copy(k).wait_send()
            @pl.when(self.e < self.last)
            def _():
                self.climb_copy(k).wait_send()
            @pl.when(self.e > 0)
            def _():
                self.share_copy(k).wait_send()
            def go(i, j):
                self.pass_copy(k, self.target(i, j, 1 - p.core)).wait()
                self.store_copy(k, self.target(i, j, p.core)).wait()
            self.source(k, go)


def reduced_shapes(grads, kinds):
    rows, cols = 2 * grads[0].shape[-2], 2 * grads[0].shape[-1]
    return [jax.ShapeDtypeStruct((rows, g.shape[0] * cols) if kind == "cols" else (g.shape[0] * rows, cols), bf16)
            for g, kind in zip(grads, kinds)]


def wgrad_cols_kernel(a_ref, b_ref, o_ref):
    y = dot(a_ref[...], b_ref[...], TN).astype(bf16)
    _, _, g, _, r, c = o_ref.shape
    for half in (0, 1):
        o_ref[0, half] = y[:, half * c:(half + 1) * c].reshape(g, 2, r, c)


def wgrad_cols(a, b, groups):
    s, m = a.shape
    n = b.shape[1]
    r, c = m // groups // 2, m // 2
    return pl.pallas_call(
        wgrad_cols_kernel, grid=(n // m,),
        in_specs=[pl.BlockSpec((s, m), lambda i: (0, 0)), pl.BlockSpec((s, m), lambda i: (0, i))],
        out_specs=pl.BlockSpec((1, 2, groups, 2, r, c), lambda i: (i, 0, 0, 0, 0, 0)),
        out_shape=jax.ShapeDtypeStruct((n // m, 2, groups, 2, r, c), bf16),
        cost_estimate=pl.CostEstimate(flops=2 * s * m * n, bytes_accessed=2 * (s * (m + n) + m * n),
                                      transcendentals=0), name="wgrad_cols")(a, b)


def wgrad_rows_kernel(a_ref, b_ref, o_ref):
    y = dot(a_ref[...], b_ref[...], TN).astype(bf16)
    q, _, _, _, r, c = o_ref.shape
    for half in (0, 1):
        o_ref[:, half, 0] = y[:, half * c:(half + 1) * c].reshape(q, 2, r, c)


def wgrad_rows(a, b, groups):
    s, m = a.shape
    n = b.shape[1]
    q, r, c = m // n, n // groups // 2, n // 2
    return pl.pallas_call(
        wgrad_rows_kernel, grid=(groups,),
        in_specs=[pl.BlockSpec((s, m // groups), lambda i: (0, i)), pl.BlockSpec((s, n), lambda i: (0, 0))],
        out_specs=pl.BlockSpec((q, 2, 1, 2, r, c), lambda i: (0, 0, i, 0, 0, 0)),
        out_shape=jax.ShapeDtypeStruct((q, 2, groups, 2, r, c), bf16),
        cost_estimate=pl.CostEstimate(flops=2 * s * m * n, bytes_accessed=2 * (s * (m + n) + m * n),
                                      transcendentals=0), name="wgrad_rows")(a, b)


def attn_fwd_kernel(shape, count, rows, *refs):
    len_ref, q_ref, k_ref, v_ref = refs[:4]
    ins = refs[4:4 + count]
    o_ref, lse_ref = refs[4 + count:6 + count]
    outs = refs[6 + count:6 + 2 * count]
    step, steps = pl.program_id(0), pl.num_programs(0)
    p = Place(shape)
    g = Gather(p, ins, outs, refs[6 + 2 * count:])
    @pl.when(step == 0)
    def _():
        greet(gather_peers(p, False))
        for w in range(count):
            g.start(w)
    for w, at in ((0, 2), (1, 4)):
        @pl.when(step == at)
        def _(w=w):
            g.after(w, 0)
    attn_fwd_body(len_ref, q_ref, k_ref, v_ref, o_ref, lse_ref, rows)
    @pl.when(step == steps - 1)
    def _():
        for w in range(2, count):
            g.after(w, 0)
        for t in range(1, p.bits):
            for w in range(count):
                g.after(w, t)
        for w in range(count):
            g.finish(w)


def attn_fwd_call(shape, length, qkv, ws, rows=256):
    groups = shape["fsdp"]
    s, d3 = qkv.shape
    d = d3 // 3
    np_ = d // 128
    sd = jax.ShapeDtypeStruct
    res = pl.pallas_call(
        functools.partial(attn_fwd_kernel, shape, len(ws), rows), grid=(np_,),
        in_specs=[pl.BlockSpec(memory_space=pltpu.SMEM), pl.BlockSpec((s, 128), lambda i: (0, i)),
                  pl.BlockSpec((s, 128), lambda i: (0, np_ + i)),
                  pl.BlockSpec((s, 128), lambda i: (0, 2 * np_ + i))] + [ANY] * len(ws),
        out_specs=[pl.BlockSpec((s, 128), lambda i: (0, i)), pl.BlockSpec((s, 128), lambda i: (0, 0))]
        + [ANY] * len(ws),
        out_shape=[sd((s, d), bf16), sd((s, 128), f32)] + [gather_shape(w, groups) for w in ws],
        scratch_shapes=Gather.scratch(len(ws), groups),
        compiler_params=pltpu.CompilerParams(collective_id=2, has_side_effects=True),
        cost_estimate=pl.CostEstimate(flops=8 * s * s * d, bytes_accessed=8 * s * d, transcendentals=s * s * 12),
        name="attn_fwd")(length, qkv, qkv, qkv, *[quarter(w) for w in ws])
    return res[0], res[1], [r.reshape(-1, r.shape[-1]) for r in res[2:]]


def attn_bwd_kernel(shape, counts, kinds, pairs, rows, *refs):
    n = len(counts)
    ins, srcs, grads, outs = refs[:9], refs[9:9 + n], refs[9 + n:12 + n], refs[12 + n:12 + 2 * n]
    work, scratch = refs[12 + 2 * n:15 + 2 * n], refs[15 + 2 * n:]
    step = pl.program_id(0) * 2 + pl.program_id(1)
    r = Reduce(Place(shape), counts, kinds, srcs, outs, scratch)
    r.opening(step)
    attn_bwd_body(*ins, *grads, *work, rows)
    r.closing(step, 2 * pairs)


def attn_bwd_call(shape, length, qkv, att, gatt, lse, cos, sin, grads, kinds, rows=256):
    groups = shape["fsdp"]
    s, d3 = qkv.shape
    d = d3 // 3
    np_ = d // 128
    counts = [g.shape[0] for g in grads]
    r, c = 2 * grads[0].shape[-2], grads[0].shape[-1]
    col = pl.BlockSpec((s, 128), lambda i, h: (0, i))
    const = pl.BlockSpec((s, 128), lambda i, h: (0, 0))
    res = pl.pallas_call(
        functools.partial(attn_bwd_kernel, shape, counts, kinds, np_, rows), grid=(np_, 2),
        in_specs=[pl.BlockSpec(memory_space=pltpu.SMEM), col,
                  pl.BlockSpec((s, 128), lambda i, h: (0, np_ + i)),
                  pl.BlockSpec((s, 128), lambda i, h: (0, 2 * np_ + i)), col, col, const, const, const]
        + [ANY] * len(grads),
        out_specs=[col, col, col] + [ANY] * len(grads),
        out_shape=[jax.ShapeDtypeStruct((s, d), bf16)] * 3 + reduced_shapes(grads, kinds),
        scratch_shapes=[pltpu.VMEM((128, s), f32), pltpu.VMEM((s, 128), f32), pltpu.VMEM((s, 128), f32)]
        + Reduce.scratch(sum(counts), groups, r, c),
        compiler_params=pltpu.CompilerParams(collective_id=3, has_side_effects=True, vmem_limit_bytes=64000 * 1024),
        cost_estimate=pl.CostEstimate(flops=20 * s * s * d, bytes_accessed=16 * s * d, transcendentals=s * s * 12),
        name="attn_bwd")(length, qkv, qkv, qkv, att, gatt, lse, cos, sin, *grads)
    return res[:3], res[3:]


def post_kernel(shape, counts, kinds, steps, *refs):
    n = len(counts)
    ins, srcs, outs, reduced = refs[:8], refs[8:8 + n], refs[8 + n:10 + n], refs[10 + n:10 + 2 * n]
    r = Reduce(Place(shape), counts, kinds, srcs, reduced, refs[10 + 2 * n:])
    step = pl.program_id(0)
    r.opening(step)
    post_body(*ins, *outs)
    r.closing(step, steps)


def post_call(shape, dq, dk, dv, tok, flag, gh1, vec, w, grads, kinds, rows=128):
    s, d = tok.shape
    row = lambda c: pl.BlockSpec((rows, c), lambda i: (i, 0))
    whole = lambda a: pl.BlockSpec(a.shape, lambda i: (0, 0))
    sd = jax.ShapeDtypeStruct
    counts = [g.shape[0] for g in grads]
    r, c = 2 * grads[0].shape[-2], grads[0].shape[-1]
    res = pl.pallas_call(
        functools.partial(post_kernel, shape, counts, kinds, s // rows), grid=(s // rows,),
        in_specs=[row(d), row(d), row(d), row(d), row(1), row(d), whole(vec), whole(w)] + [ANY] * len(grads),
        out_specs=[row(d), pl.BlockSpec((8, d), lambda i: (0, 0))] + [ANY] * len(grads),
        out_shape=[sd((s, d), bf16), sd((8, d), f32)] + reduced_shapes(grads, kinds),
        scratch_shapes=Reduce.scratch(sum(counts), shape["fsdp"], r, c),
        compiler_params=pltpu.CompilerParams(collective_id=4, has_side_effects=True, vmem_limit_bytes=64000 * 1024),
        cost_estimate=pl.CostEstimate(flops=6 * s * d * d, bytes_accessed=16 * s * d, transcendentals=0),
        name="post")(dq, dk, dv, tok, flag, gh1, vec, w, *grads)
    return res[0], res[1], res[2:]

def f32_rows_dot(row, weights):
    parts = split3(row)
    stack = jnp.concatenate(list(parts) + [jnp.zeros((5, row.shape[1]), f32)], axis=0).astype(bf16)
    return colsum(dot(stack, weights))


class Small:
    def __init__(self, place, scratch):
        self.p = place
        (self.ag, self.rows, self.ab, self.bs, self.bm, self.bb, self.bg, self.s1, self.r1, self.s2, self.r2) = scratch

    @staticmethod
    def widths(shape, d, ff, n_mod):
        groups = shape["fsdp"]
        part = n_mod // groups
        return -(-(d // groups) // 128) * 128, ff // groups, part if part % 128 == 0 else n_mod

    @staticmethod
    def scratch(shape, d, ff, n_mod):
        groups, lines = shape["fsdp"], shape["dp"]
        wide, fpart, gpart = Small.widths(shape, d, ff, n_mod)
        vm = lambda *dims: pltpu.VMEM(dims, f32)
        sem = pltpu.SemaphoreType.DMA
        return [vm(groups, 1, n_mod), vm(groups, 8, d), vm(groups, 1, ff), vm(lines, 8, wide), vm(lines, groups, 384),
                vm(lines, 1, fpart), vm(lines, groups, gpart), sem((groups, 3)), sem((groups, 3)), sem((lines, 4)),
                sem((lines, 4))]

    def peers(self):
        p = self.p
        return [(p.dp, xor(p.me, m)) for m in range(1, p.groups)] + [(xor(p.dp, m), p.me) for m in range(1, p.lines)]

    def copies(self, stage, m, arrived):
        p = self.p
        if stage == 1:
            bufs, ss, rs = (self.ag, self.rows, self.ab), self.s1, self.r1
            where, slot = (p.dp, xor(p.me, m)), xor(p.me, m) if arrived else p.me
        else:
            bufs, ss, rs = (self.bs, self.bm, self.bb, self.bg), self.s2, self.r2
            where, slot = (xor(p.dp, m), p.me), xor(p.dp, m) if arrived else p.dp
        return [remote(b.at[slot], b.at[slot], ss.at[m, i], rs.at[m, i], where) for i, b in enumerate(bufs)]

    def spread(self, stage):
        for m in range(1, self.p.groups if stage == 1 else self.p.lines):
            for c in self.copies(stage, m, False):
                c.start()

    def collect(self, stage):
        for m in range(1, self.p.groups if stage == 1 else self.p.lines):
            for c in self.copies(stage, m, True):
                c.wait_recv()

    def settle(self):
        for stage in (1, 2):
            for m in range(1, self.p.groups if stage == 1 else self.p.lines):
                for c in self.copies(stage, m, False):
                    c.wait_send()

    def first(self, sums, sb1, sums1, vec_pre, vec_mid, condp, meta, ada):
        me = self.p.me
        d = sums.shape[1]
        ggm, gb2, a2, s2, gga, st0, st1, st2 = (sums[i:i + 1] for i in range(8))
        a1, s1, gemb = (sums1[i:i + 1] for i in range(3))
        gain1, scale_a, gain2, scale_m = vec_pre[1:2], vec_pre[2:3], vec_mid[1:2], vec_mid[2:3]
        gm = jnp.concatenate([s1, a1 * gain1, gga, s2, a2 * gain2, ggm], axis=1)
        sig = 1.0 / (1.0 + jnp.exp(-condp))
        gc = f32_rows_dot(gm, ada) * (sig * (1.0 + condp * (1.0 - sig)))
        lane = lax.broadcasted_iota(jnp.int32, (1, 128), 1)
        total = lambda x: jnp.sum(x, axis=1, keepdims=True)
        stat = jnp.where(lane == 0, total(st0), jnp.where(lane == 1, total(st1), jnp.where(lane == 2, total(st2), meta)))
        tail = jnp.concatenate([gc, condp * sig, stat, jnp.zeros((1, d - 384), f32)], axis=1)
        self.ag[me] = gm
        self.ab[me] = sb1
        self.rows[me] = jnp.concatenate([(1.0 + scale_a) * a1, (1.0 + scale_m) * a2, gb2, gemb, tail,
                                         jnp.zeros((3, d), f32)], axis=0)
        self.spread(1)

    def second(self):
        p = self.p
        self.collect(1)
        d = self.rows.shape[2]
        wide, fpart, gpart = self.bs.shape[2], self.bb.shape[2], self.bg.shape[2]
        total = self.rows[0]
        for f in range(1, p.groups):
            total = total + self.rows[f]
        self.bs[p.dp] = pltpu.roll(total, (d - p.me * (d // p.groups)) % d, 1)[:, :wide]
        self.bm[p.dp] = jnp.concatenate([self.rows[f, 4:5, :384] for f in range(p.groups)], axis=0)
        cut = pl.ds(pl.multiple_of(p.me * fpart, 128), fpart)
        part = self.ab[0, :, cut]
        for f in range(1, p.groups):
            part = part + self.ab[f, :, cut]
        self.bb[p.dp] = part
        n_mod = self.ag.shape[2]
        cut = slice(None) if gpart == n_mod else pl.ds(pl.multiple_of(p.me * gpart, 128), gpart)
        self.bg[p.dp] = jnp.concatenate([self.ag[f, :, cut] for f in range(p.groups)], axis=0)
        self.spread(2)

    def third(self, norms_ref, gb1_ref, gada_ref, gbada_ref, table_ref, rms_ref, d):
        p = self.p
        self.collect(2)
        total, part = self.bs[0], self.bb[0]
        for z in range(1, p.lines):
            total = total + self.bs[z]
            part = part + self.bb[z]
        norms_ref[...] = total
        gb1_ref[...] = part
        mods = jnp.concatenate([self.bg[z] for z in range(p.lines)], axis=0)
        info = jnp.concatenate([self.bm[z] for z in range(p.lines)], axis=0)
        gcs, conds, stat = info[:, :128], info[:, 128:256], info[:, 256:384]
        highest = lax.Precision.HIGHEST
        gada_ref[...] = lax.dot_general(mods, conds, TN, precision=highest, preferred_element_type=f32)
        gbada_ref[...] = colsum(mods)
        ids = stat[:, 4:5].astype(jnp.int32)
        hot = (lax.broadcasted_iota(jnp.int32, (ids.shape[0], table_ref.shape[0]), 1) == ids).astype(f32)
        table_ref[...] = lax.dot_general(hot, gcs, TN, precision=highest, preferred_element_type=f32)
        stat = colsum(stat)
        rms_ref[...] = jnp.sqrt(stat / (stat[:, 3:4] * d))


def small_kernel(shape, sums, sb1, sums1, vec_pre, vec_mid, condp, meta, ada, norms, gb1, gada, gbada, table, rms,
                 *scratch):
    s = Small(Place(shape), scratch)
    greet(s.peers())
    s.first(sums[...], sb1[...], sums1[...], vec_pre[...], vec_mid[...], condp[...], meta[...], ada[...])
    s.second()
    s.third(norms, gb1, gada, gbada, table, rms, sums.shape[1])
    s.settle()


def small_shapes(shape, d, ff, n_mod, table_rows):
    wide, fpart, gpart = Small.widths(shape, d, ff, n_mod)
    sd = lambda *dims: jax.ShapeDtypeStruct(dims, f32)
    return [sd(8, wide), sd(1, fpart), sd(gpart, 128), sd(1, gpart), sd(table_rows, 128), sd(1, 128)]


def small_call(shape, sums, sb1, sums1, vec_pre, vec_mid, condp, meta, ada, table_rows):
    d, ff, n_mod = sums.shape[1], sb1.shape[1], ada.shape[0]
    vm = pl.BlockSpec(memory_space=pltpu.VMEM)
    return pl.pallas_call(
        functools.partial(small_kernel, shape), in_specs=[vm] * 8, out_specs=[vm] * 6,
        out_shape=small_shapes(shape, d, ff, n_mod, table_rows), scratch_shapes=Small.scratch(shape, d, ff, n_mod),
        compiler_params=pltpu.CompilerParams(collective_id=5, has_side_effects=True), name="small",
    )(sums, sb1, sums1, vec_pre, vec_mid, condp, meta, ada)


def small_results(shape, res, sizes):
    norms, gb1, gada, gbada, table, rms = res
    n_ada = sizes[5]
    if gada.shape[0] != n_ada:
        me = lax.axis_index("fsdp")
        gada = lax.dynamic_slice_in_dim(gada, me * n_ada, n_ada, axis=0)
        gbada = lax.dynamic_slice_in_dim(gbada, me * n_ada, n_ada, axis=1)
    g1, g2, gb2, gemb = (norms[i, :sizes[i]] for i in range(4))
    return g1, g2, gb2, gemb, gb1[0], gada, gbada[0], table, rms[0, :3]
from jax.sharding import PartitionSpec as P

highest = lax.Precision.HIGHEST


def rotary_tables(length):
    half = HD // 2
    rate = 1.0 / 10000.0 ** (jnp.arange(half, dtype=f32) * 2.0 / HD)
    angle = jnp.arange(length, dtype=f32)[:, None] * rate[None, :]
    angle = jnp.concatenate([angle] * (128 // half), axis=-1)
    sign = jnp.where(jnp.arange(128) % HD < half, -1.0, 1.0)
    return jnp.cos(angle), jnp.sin(angle) * sign


def per_device(shape, tokens, hidden_token_indicator, lengths, time_ids, cotangent, gain_one, w_qkv, w_out, gain_two,
               w_fc1, b_fc1, w_fc2, b_fc2, w_ada, b_ada, mask_embed, time_table):
    groups = shape["fsdp"]
    s, d = tokens.shape[1:]
    ff = b_fc1.shape[0] * groups
    tok, cot = tokens[0], cotangent[0]
    flag = hidden_token_indicator.reshape(s, 1)
    sizes = [v.shape[0] for v in (gain_one, gain_two, b_fc2, mask_embed, b_fc1, b_ada)]
    small = jnp.concatenate([gain_one, gain_two, b_fc2, mask_embed, b_fc1, b_ada])[None]
    (ada_all, qkv_all), packed = head_call(shape, small, [w_ada, w_qkv])
    packed = packed[:, 0]
    cuts = [sum(sizes[:i]) for i in range(len(sizes) + 1)]
    gain1, gain2, b2, emb, b1, bada = (
        packed[:, cuts[i]:cuts[i + 1]].reshape(1, -1).astype(f32) for i in range(len(sizes)))
    cond_pre = lax.dynamic_slice_in_dim(time_table, time_ids[0], 1, axis=0)
    cond = jax.nn.silu(cond_pre)
    modulation = jnp.dot(cond, ada_all.astype(f32).T, precision=highest) + bada
    shift_a, scale_a, gate_a, shift_m, scale_m, gate_m = (modulation[:, i * d:(i + 1) * d] for i in range(6))
    cos, sin = rotary_tables(s)
    zero = jnp.zeros((1, d), f32)
    vec_pre = jnp.concatenate([emb, gain1, scale_a, shift_a] + [zero] * 4, axis=0)
    vec_mid = jnp.concatenate([emb, gain2, scale_m, shift_m, gate_a, gate_m, b2, zero], axis=0)
    n1, qkv = pre_call(tok, flag, vec_pre, qkv_all, cos, sin)
    att, lse, (out_all, fc1_all, fc2_all) = attn_fwd_call(shape, lengths, qkv, [w_out, w_fc1, w_fc2])
    out, gh1, gatt, n2, act, gm, gpre, gap, sums, gb1 = mid_call(
        lengths, att, tok, flag, cot, vec_mid, b1, out_all, fc1_all, fc2_all)
    g_fc2 = wgrad_rows(act, gm, groups)
    g_fc1 = wgrad_cols(n2, gpre, groups)
    g_out = wgrad_cols(att, gap, groups)
    (dq, dk, dv), (r_fc2, r_fc1, r_out) = attn_bwd_call(
        shape, lengths, qkv, att, gatt, lse, cos, sin, [g_fc2, g_fc1, g_out], ["rows", "cols", "cols"])
    g_qkv = [wgrad_cols(n1, x, groups) for x in (dq, dk, dv)]
    igrad, sums1, r_qkv = post_call(shape, dq, dk, dv, tok, flag, gh1, vec_pre, qkv_all, g_qkv, ["cols"] * 3)
    meta = jnp.concatenate([jnp.zeros((3,), f32), lengths.astype(f32), time_ids.astype(f32), jnp.zeros((123,), f32)])[None]
    g1, g2, gb2, gemb, gb1, g_ada, gbada, table, rms = small_results(
        shape, small_call(shape, sums, gb1, sums1, vec_pre, vec_mid, cond_pre, meta, ada_all, time_table.shape[0]), sizes)
    return (out[None], igrad[None], g1, jnp.concatenate(r_qkv, axis=1).astype(f32), r_out.astype(f32), g2, r_fc1.astype(f32), gb1,
            r_fc2.astype(f32), gb2,
            g_ada, gbada, gemb, table, rms)


def solution(mesh):
    both = ("dp", "fsdp")
    f1, f2 = P("fsdp"), P("fsdp", None)
    placed = (P(both, None, None), P(both, None), P(both), P(both), P(both, None, None), f1, f2, f2, f1, f2, f1, f2, f1,
              f2, f1, f1, P())
    outs = (P(both, None, None), P(both, None, None), f1, f2, f2, f1, f2, f1, f2, f1, f2, f1, f1, P(), P())
    return jax.shard_map(functools.partial(per_device, dict(mesh.shape)), mesh=mesh, in_specs=placed, out_specs=outs,
                         check_vma=False)
```

```python
import functools, math
import jax, jax.numpy as jnp
from jax import lax
from jax.experimental import pallas as pl
from jax.experimental.pallas import tpu as pltpu

HD = 64
EPS = 1e-5
LOG2E = math.log2(math.e)
QSCALE = LOG2E * HD ** -0.5
f32, bf16 = jnp.float32, jnp.bfloat16
NT = (((1,), (1,)), ((), ()))
NN = (((1,), (0,)), ((), ()))
TN = (((0,), (0,)), ((), ()))

def dot(a, b, dims=NN):
    return lax.dot_general(a, b, dims, preferred_element_type=f32)

def norm_parts(x):
    mean = jnp.mean(x, axis=-1, keepdims=True)
    cen = x - mean
    rs = lax.rsqrt(jnp.mean(cen * cen, axis=-1, keepdims=True) + EPS)
    return cen * rs, rs

def swap_halves(u):
    lane = lax.broadcasted_iota(jnp.int32, u.shape, 1)
    return jnp.where(lane % HD < HD // 2, pltpu.roll(u, 96, 1), pltpu.roll(u, 32, 1))

def pre_kernel(tok_ref, flag_ref, vec_ref, w_ref, cos_ref, sin_ref, n1_ref, qkv_ref):
    emb, gain, scale, shift = (vec_ref[i:i + 1, :] for i in range(4))
    h0 = jnp.where(flag_ref[...] == 1, emb, tok_ref[...].astype(f32))
    n, _ = norm_parts(h0)
    n1 = (n * gain * (1.0 + scale) + shift).astype(bf16)
    n1_ref[...] = n1.astype(f32).T.astype(bf16)
    d = n1.shape[1]
    cos, sin = cos_ref[...], sin_ref[...]
    for part in range(3):
        y = dot(n1, w_ref[:, part * d:(part + 1) * d])
        for c in range(d // 128):
            lo = part * d + c * 128
            u = y[:, c * 128:(c + 1) * 128]
            if part < 2:
                u = u * cos + swap_halves(u) * sin
                if part == 0:
                    u = u * QSCALE
            qkv_ref[:, lo:lo + 128] = u.astype(bf16)

def pre_call(tok, flag, vecs, w, cos, sin, rows=256):
    s, d = tok.shape
    return pl.pallas_call(
        pre_kernel, grid=(s // rows,),
        in_specs=[pl.BlockSpec((rows, d), lambda i: (i, 0)), pl.BlockSpec((rows, 1), lambda i: (i, 0)),
                  pl.BlockSpec((8, d), lambda i: (0, 0)), pl.BlockSpec((d, 3 * d), lambda i: (0, 0)),
                  pl.BlockSpec((rows, 128), lambda i: (i, 0)), pl.BlockSpec((rows, 128), lambda i: (i, 0))],
        out_specs=[pl.BlockSpec((d, rows), lambda i: (0, i)), pl.BlockSpec((rows, 3 * d), lambda i: (i, 0))],
        out_shape=[jax.ShapeDtypeStruct((d, s), bf16), jax.ShapeDtypeStruct((s, 3 * d), bf16)],
        cost_estimate=pl.CostEstimate(flops=2 * s * d * 3 * d, bytes_accessed=12 * s * d, transcendentals=0),
        name="pre")(tok, flag, vecs, w, cos, sin)

def attn_fwd_body(len_ref, q_ref, k_ref, v_ref, o_ref, lse_ref, rows):
    p = pl.program_id(0)
    s = q_ref.shape[0]
    length = len_ref[0]
    lane = lax.broadcasted_iota(jnp.int32, (s, 128), 1)
    pos = lax.broadcasted_iota(jnp.int32, (s, 128), 0)
    lane_q = lax.broadcasted_iota(jnp.int32, (rows, 128), 1)
    k = k_ref[...].astype(f32)
    v = v_ref[...].astype(f32)
    kx, vx = [], []
    for h in (0, 1):
        extra = HD * (1 - h)
        mine = (lane >= HD) if h else (lane < HD)
        bias = jnp.where(pos >= length, -1e30, 0.0)
        kx.append(jnp.where(mine, k, jnp.where(lane == extra, bias, 0.0)).astype(bf16))
        vx.append(jnp.where(mine, v, jnp.where(lane == extra, 1.0, 0.0)).astype(bf16))
    for b in range(s // rows):
        q = q_ref[b * rows:(b + 1) * rows, :].astype(f32)
        outs, lses = [], []
        for h in (0, 1):
            extra = HD * (1 - h)
            mine = (lane_q >= HD) if h else (lane_q < HD)
            qx = jnp.where(mine, q, jnp.where(lane_q == extra, 1.0, 0.0)).astype(bf16)
            sc = dot(qx, kx[h], NT)
            m = jnp.max(sc, axis=1, keepdims=True)
            pr = jnp.exp2(sc - m).astype(bf16)
            o = dot(pr, vx[h])
            tot = o[:, extra:extra + 1]
            outs.append(o * (1.0 / tot))
            lses.append(m + jnp.log(tot) * LOG2E)
        o_ref[b * rows:(b + 1) * rows, :] = jnp.where(lane_q < HD, outs[0], outs[1]).astype(bf16)
        old = jnp.where(p == 0, 0.0, lse_ref[b * rows:(b + 1) * rows, :])
        lse_ref[b * rows:(b + 1) * rows, :] = jnp.where(
            lane_q == 2 * p, lses[0], jnp.where(lane_q == 2 * p + 1, lses[1], old))

def split3(x):
    hi = x.astype(bf16).astype(f32)
    r = x - hi
    mid = r.astype(bf16).astype(f32)
    return hi, mid, r - mid

def attn_bwd_body(len_ref, q_ref, k_ref, v_ref, o_ref, g_ref, lse_ref, cos_ref, sin_ref,
                  dqs, dks, dvs, rows, p, h, emit):
    s = q_ref.shape[0]
    length = len_ref[0]
    lane = lax.broadcasted_iota(jnp.int32, (s, 128), 1)
    pos = lax.broadcasted_iota(jnp.int32, (s, 128), 0)
    lane_q = lax.broadcasted_iota(jnp.int32, (rows, 128), 1)
    e = HD * (1 - h)
    mine, mine_q = lane // HD == h, lane_q // HD == h
    k = k_ref[...].astype(f32)
    v = v_ref[...].astype(f32)
    ones = jnp.where((lane >= e) & (lane < e + 3), 1.0, 0.0)
    bias = jnp.where(pos >= length, -1e30, 0.0)
    kx = jnp.where(mine, k, jnp.where(lane == e + 3, bias, ones)).astype(bf16)
    vx = jnp.where(mine, v, ones).astype(bf16)
    kt = jnp.where(mine, k, 0.0).T.astype(bf16)
    dk = jnp.zeros((s, 128), f32)
    dv = jnp.zeros((s, 128), f32)
    for b in range(s // rows):
        sl = slice(b * rows, (b + 1) * rows)
        qb = q_ref[sl, :]
        gb = g_ref[sl, :]
        q = qb.astype(f32)
        g = gb.astype(f32)
        lse = jnp.sum(jnp.where(lane_q == 2 * p + h, lse_ref[sl, :], 0.0), axis=1, keepdims=True)
        dd = jnp.sum(jnp.where(mine_q, g * o_ref[sl, :].astype(f32), 0.0), axis=1, keepdims=True)
        l0, l1, l2 = split3(-lse)
        d0, d1, d2 = split3(-dd)
        qx = jnp.where(mine_q, q, jnp.where(lane_q == e, l0, jnp.where(lane_q == e + 1, l1, jnp.where(
            lane_q == e + 2, l2, jnp.where(lane_q == e + 3, 1.0, 0.0))))).astype(bf16)
        gx = jnp.where(mine_q, g, jnp.where(lane_q == e, d0, jnp.where(lane_q == e + 1, d1, jnp.where(
            lane_q == e + 2, d2, 0.0)))).astype(bf16)
        pt = jnp.exp2(dot(kx, qx, NT))
        dst = (pt * dot(vx, gx, NT)).astype(bf16)
        dv = dv + dot(pt.astype(bf16), gb)
        dk = dk + dot(dst, qb)
        dqt = dot(kt, dst)
        dqs[:, sl] = jnp.where(h == 0, dqt, dqs[:, sl] + dqt)
    @pl.when(h == 0)
    def _():
        dks[...] = dk
        dvs[...] = dv
    @pl.when(h == 1)
    def _():
        cos, sin = cos_ref[...], sin_ref[...]
        dq = dqs[...].T * (HD ** -0.5)
        dkk = jnp.where(lane < HD, dks[...], dk) * (1.0 / LOG2E)
        emit((dq * cos - swap_halves(dq) * sin).astype(bf16), (dkk * cos - swap_halves(dkk) * sin).astype(bf16),
             jnp.where(lane < HD, dvs[...], dv).astype(bf16))


def gelu_both(v):
    a, b = 0.7978845608028654, 0.044715
    v2 = v * v
    t = jnp.tanh(a * v * (1.0 + b * v2))
    half = 0.5 + 0.5 * t
    return v * half, half + (0.5 * a) * v * (1.0 - t * t) * (1.0 + 3.0 * b * v2)

def colsum(x):
    return jnp.sum(x, axis=0, keepdims=True)

def mid_kernel(len_ref, att_ref, tok_ref, flag_ref, cot_ref, vec_ref, b1_ref, wo_ref, w1_ref, w2_ref,
               out_ref, gh1_ref, gatt_ref, n2_ref, act_ref, gm_ref, gpre_ref, gap_ref, sum_ref, sb1_ref,
               gp_s, *, cut):
    i = pl.program_id(0)
    rows, d = att_ref.shape
    ff = w1_ref.shape[1]
    emb, gain, scale, shift, gate_a, gate_m, b2 = (vec_ref[r:r + 1, :] for r in range(7))
    h0 = jnp.where(flag_ref[...] == 1, emb, tok_ref[...].astype(f32))
    ap = dot(att_ref[...], wo_ref[...])
    br_a = gate_a * ap
    h1 = h0 + br_a
    n, rs = norm_parts(h1)
    n2 = (n * gain * (1.0 + scale) + shift).astype(bf16)
    n2_ref[...] = n2
    mp = jnp.zeros((rows, d), f32) + b2
    for j in range(ff // cut):
        sl = slice(j * cut, (j + 1) * cut)
        act, gp = gelu_both(dot(n2, w1_ref[:, sl]) + b1_ref[:, sl])
        act = act.astype(bf16)
        act_ref[:, sl] = act
        gp_s[:, sl] = gp
        mp = mp + dot(act, w2_ref[sl, :])
    br_m = gate_m * mp
    bo = h1 + br_m
    out_ref[...] = bo.astype(bf16)
    pos = lax.broadcasted_iota(jnp.int32, (rows, 1), 0) + i * rows
    valid = jnp.where(pos < len_ref[0], 1.0, 0.0)
    cot = cot_ref[...].astype(f32)
    gm = (gate_m * cot).astype(bf16)
    gm_ref[...] = gm
    gn2 = jnp.zeros((rows, d), f32)
    sb1 = []
    for j in range(ff // cut):
        sl = slice(j * cut, (j + 1) * cut)
        gpre = (dot(gm, w2_ref[sl, :], NT) * gp_s[:, sl]).astype(bf16)
        gpre_ref[:, sl] = gpre
        sb1.append(colsum(gpre.astype(f32)))
        gn2 = gn2 + dot(gpre, w1_ref[:, sl], NT)
    e = gn2 * (gain * (1.0 + scale))
    gh1 = cot + rs * (e - jnp.mean(e, axis=1, keepdims=True) - n * jnp.mean(e * n, axis=1, keepdims=True))
    gh1_ref[...] = gh1
    gap = (gate_a * gh1).astype(bf16)
    gap_ref[...] = gap
    gatt_ref[...] = dot(gap, wo_ref[...], NT).astype(bf16)
    new = jnp.concatenate([
        colsum(cot * mp), colsum(gm.astype(f32)), colsum(gn2 * n), colsum(gn2), colsum(gh1 * ap),
        colsum(valid * bo * bo), colsum(valid * br_a * br_a), colsum(valid * br_m * br_m)], axis=0)
    sb1 = jnp.concatenate(sb1, axis=1)
    @pl.when(i == 0)
    def _():
        sum_ref[...] = new
        sb1_ref[...] = sb1
    @pl.when(i > 0)
    def _():
        sum_ref[...] += new
        sb1_ref[...] += sb1

def mid_call(length, att, tok, flag, cot, vec, b1, wo, w1, w2, rows=256, cut=768):
    s, d = tok.shape
    ff = w1.shape[1]
    row = lambda c: pl.BlockSpec((rows, c), lambda i: (i, 0))
    whole = lambda a: pl.BlockSpec(a.shape, lambda i: (0, 0))
    sd = jax.ShapeDtypeStruct
    return pl.pallas_call(
        functools.partial(mid_kernel, cut=cut), grid=(s // rows,),
        in_specs=[pl.BlockSpec(memory_space=pltpu.SMEM), row(d), row(d), row(1), row(d), whole(vec), whole(b1),
                  whole(wo), whole(w1), whole(w2)],
        out_specs=[row(d), row(d), row(d), row(d), row(ff), row(d), row(ff), row(d),
                   pl.BlockSpec((8, d), lambda i: (0, 0)), pl.BlockSpec((1, ff), lambda i: (0, 0))],
        out_shape=[sd((s, d), bf16), sd((s, d), f32), sd((s, d), bf16), sd((s, d), bf16), sd((s, ff), bf16),
                   sd((s, d), bf16), sd((s, ff), bf16), sd((s, d), bf16), sd((8, d), f32), sd((1, ff), f32)],
        scratch_shapes=[pltpu.VMEM((rows, ff), f32)],
        compiler_params=pltpu.CompilerParams(vmem_limit_bytes=60000 * 1024),
        cost_estimate=pl.CostEstimate(flops=2 * s * d * (2 * d + 4 * ff), bytes_accessed=30 * s * d,
                                      transcendentals=s * ff),
        name="mid")(length, att, tok, flag, cot, vec, b1, wo, w1, w2)

def post_rows(grads, h0, masked, gh1, gain, scale, w_ref):
    d = h0.shape[1]
    n, rs = norm_parts(h0)
    gn1 = sum(dot(g, w_ref[:, i * d:(i + 1) * d], NT) for i, g in enumerate(grads))
    e = gn1 * (gain * (1.0 + scale))
    gh0 = gh1 + rs * (e - jnp.mean(e, axis=1, keepdims=True) - n * jnp.mean(e * n, axis=1, keepdims=True))
    sums = jnp.concatenate([colsum(gn1 * n), colsum(gn1), colsum(jnp.where(masked, gh0, 0.0)),
                            jnp.zeros((5, d), f32)], axis=0)
    return jnp.where(masked, 0.0, gh0).astype(bf16), sums

MESH = pl.DeviceIdType.MESH


def flip(i, b):
    return i + 2 ** b * (1 - 2 * ((i // 2 ** b) % 2))


def xor(i, mask):
    b = 0
    while mask >> b:
        if (mask >> b) & 1:
            i = flip(i, b)
        b += 1
    return i


def subsets(bits):
    masks = [0]
    for b in bits:
        masks = masks + [m | (1 << b) for m in masks]
    return masks


def log2(n):
    return n.bit_length() - 1


class Place:
    def __init__(self, shape):
        self.groups, self.lines = shape["fsdp"], shape["dp"]
        self.bits = log2(self.groups)
        self.orders = [list(range(self.bits)), list(range(self.bits))[::-1]]
        self.me = lax.axis_index("fsdp")
        self.dp = lax.axis_index("dp")
        self.core = self.dp % 2
        self.partner = flip(self.dp, 0)


def remote(src, dst, ssem, rsem, where):
    return pltpu.make_async_remote_copy(src_ref=src, dst_ref=dst, send_sem=ssem, recv_sem=rsem, device_id=where,
                                        device_id_type=MESH)


class Gather:
    def __init__(self, place, ins, outs, sems):
        self.p, self.ins, self.outs = place, ins, outs
        self.ss, self.rs, self.fs, self.fr, self.os, self.orr = sems

    @staticmethod
    def scratch(count, groups):
        a = pltpu.SemaphoreType.DMA((count, 2, groups - 1))
        b = pltpu.SemaphoreType.DMA((count,))
        return [a, a, a, a, b, b]

    def send(self, w, color, t, mask):
        p = self.p
        order = p.orders[color]
        e = 2 ** t - 1 + subsets(order[:t]).index(mask)
        piece = p.core * 2 + color
        blk = xor(p.me, mask)
        src = self.ins[w].at[piece] if mask == 0 else self.outs[w].at[blk, piece]
        return remote(src, self.outs[w].at[blk, piece], self.ss.at[w, color, e], self.rs.at[w, color, e],
                      (p.dp, flip(p.me, order[t])))

    def arrival(self, w, color, t, mask):
        p = self.p
        order = p.orders[color]
        e = 2 ** t - 1 + subsets(order[:t]).index(mask)
        got = self.outs[w].at[xor(p.me, mask | (1 << order[t])), p.core * 2 + color]
        return e, got

    def landed(self, w, color, e, got):
        return remote(got, got, self.ss.at[w, color, e], self.rs.at[w, color, e], (self.p.partner, self.p.me))

    def forward(self, w, color, e, got):
        return remote(got, got, self.fs.at[w, color, e], self.fr.at[w, color, e], (self.p.partner, self.p.me))

    def own(self, w):
        p = self.p
        return remote(self.ins[w], self.outs[w].at[p.me], self.os.at[w], self.orr.at[w], (p.partner, p.me))

    def start(self, w):
        for t in range(self.p.bits):
            for color in (0, 1):
                self.send(w, color, t, 0).start()
        self.own(w).start()

    def after(self, w, t):
        for color in (0, 1):
            order = self.p.orders[color]
            for mask in subsets(order[:t]):
                e, got = self.arrival(w, color, t, mask)
                self.landed(w, color, e, got).wait_recv()
                for later in range(t + 1, self.p.bits):
                    self.send(w, color, later, mask | (1 << order[t])).start()
                self.forward(w, color, e, got).start()

    def finish(self, w):
        p = self.p
        for color in (0, 1):
            order = p.orders[color]
            for t in range(p.bits):
                for mask in subsets(order[:t]):
                    e, got = self.arrival(w, color, t, mask)
                    other = self.outs[w].at[xor(p.me, mask | (1 << order[t])), (1 - p.core) * 2 + color]
                    self.forward(w, color, e, other).wait_recv()
                    self.forward(w, color, e, got).wait_send()
                    self.send(w, color, t, mask).wait_send()
        self.own(w).wait()


class Direct:
    def __init__(self, place, src, out, sems):
        self.p, self.src, self.out = place, src, out
        self.ss, self.rs = sems

    @staticmethod
    def scratch(groups):
        return [pltpu.SemaphoreType.DMA((groups,))] * 2

    def copy(self, m, arrived):
        p = self.p
        where = (p.partner, p.me) if m == 0 else (p.dp, xor(p.me, m))
        slot = xor(p.me, m) if arrived else p.me
        return remote(self.src, self.out.at[slot], self.ss.at[m], self.rs.at[m], where)

    def start(self):
        for m in range(self.p.groups):
            self.copy(m, False).start()

    def finish(self):
        for m in range(self.p.groups):
            self.copy(m, True).wait_recv()
            self.copy(m, False).wait_send()


def greet(devices):
    barrier = pltpu.get_barrier_semaphore()
    for where in devices:
        pl.semaphore_signal(barrier, inc=1, device_id=where, device_id_type=MESH)
    pl.semaphore_wait(barrier, len(devices))


def gather_peers(p, everyone):
    masks = range(1, p.groups) if everyone else [1 << b for b in range(p.bits)]
    return [(p.partner, p.me)] + [(p.dp, xor(p.me, m)) for m in masks]


def quarter(w):
    return w.reshape(4, w.shape[0] // 4, w.shape[1])


def gather_shape(w, groups):
    return jax.ShapeDtypeStruct((groups, 4, w.shape[0] // 4, w.shape[1]), w.dtype)


ANY = pl.BlockSpec(memory_space=pl.ANY)


def head_kernel(shape, count, *refs):
    ins, small, outs, small_out = refs[:count], refs[count], refs[count + 1:2 * count + 1], refs[2 * count + 1]
    sems = refs[2 * count + 2:]
    p = Place(shape)
    g = Gather(p, ins, outs, sems[:6])
    s = Direct(p, small, small_out, sems[6:])
    greet(gather_peers(p, True))
    s.start()
    for w in range(count):
        g.start(w)
    for t in range(p.bits):
        for w in range(count):
            g.after(w, t)
    for w in range(count):
        g.finish(w)
    s.finish()


def head_call(shape, small, ws):
    groups = shape["fsdp"]
    outs = [gather_shape(w, groups) for w in ws] + [jax.ShapeDtypeStruct((groups,) + small.shape, small.dtype)]
    res = pl.pallas_call(
        functools.partial(head_kernel, shape, len(ws)), in_specs=[ANY] * (len(ws) + 1), out_specs=[ANY] * len(outs),
        out_shape=outs, scratch_shapes=Gather.scratch(len(ws), groups) + Direct.scratch(groups),
        compiler_params=pltpu.CompilerParams(collective_id=1, has_side_effects=True), name="head",
    )(*[quarter(w) for w in ws], small)
    return [r.reshape(-1, r.shape[-1]) for r in res[:-1]], res[-1]


class Reduce:
    def __init__(self, place, counts, kinds, srcs, outs, scratch, lag, gap):
        self.p, self.counts, self.kinds, self.srcs, self.outs = place, counts, kinds, srcs, outs
        (self.own, self.cb, self.xb, self.zb, self.mb, self.u2, self.fin,
         self.load, self.cs, self.cr, self.xs, self.xr, self.zs, self.zr, self.ms, self.mr, self.fs, self.fr,
         self.ps, self.pr, self.st) = scratch
        p = place
        self.total = sum(counts)
        self.n = p.lines // 2
        self.zi = p.dp // 2
        left = self.zi // (self.n // 2)
        self.e = self.zi * (1 - left) + (self.n - 1 - self.zi) * left
        step = 2 * (1 - 2 * left)
        self.inner = (p.dp + step, p.me)
        self.outer = (p.dp - step, p.me)
        self.last = self.n // 2 - 1
        self.stages = ([self.begin, self.core_add] + [functools.partial(self.group_add, t) for t in range(p.bits)]
                       + [functools.partial(self.climb, j) for j in range(1, self.last + 1)] + [self.middle]
                       + [functools.partial(self.descend, j) for j in range(self.last - 1, -1, -1)])
        self.lags = [lag * i for i in range(len(self.stages))]
        self.gap = gap
        self.ticks = self.total + gap + self.lags[-1]

    @staticmethod
    def scratch(total, groups, rows, cols):
        sem = pltpu.SemaphoreType.DMA
        vm = lambda *lead: pltpu.VMEM((total,) + lead + (rows // 2, cols), bf16)
        one = sem((total,))
        line = pltpu.VMEM((total, rows, cols), bf16)
        return [vm(groups, 2), vm(groups, 2), vm(2, groups - 1), line, line, line, line,
                one, one, one, sem((total, 2, groups - 1)), sem((total, 2, groups - 1)),
                one, one, one, one, one, one, sem((total, 3)), sem((total, 3)), sem((total, 3))]

    def greet(self, peers):
        p = self.p
        barrier = pltpu.get_barrier_semaphore()
        for where in peers:
            pl.semaphore_signal(barrier, inc=1, device_id=where, device_id_type=MESH)
        pl.semaphore_wait(barrier, len(peers))

    def source(self, k, fn):
        base = 0
        for i, count in enumerate(self.counts):
            @pl.when((k >= base) & (k < base + count))
            def _(i=i, base=base):
                fn(i, k - base)
            base += count

    def targets(self, k, i, j, core):
        rows, cols = self.fin.shape[1:]
        out, fin = self.outs[i], self.fin.at[k]
        if self.kinds[i] == "rows":
            cut = pl.ds(pl.multiple_of(core * cols, cols), cols)
            return [(fin, out.at[pl.ds(pl.multiple_of(j * rows, rows), rows), cut])]
        down = pl.ds(pl.multiple_of((j % 2) * rows, rows), rows)
        if self.kinds[i] == "cols":
            return [(fin, out.at[down, pl.ds(pl.multiple_of((2 * (j // 2) + core) * cols, cols), cols)])]
        width = out.shape[1] // 3
        pair = 2 * (j // 2) + core
        return [(fin.at[:, part * 128:(part + 1) * 128],
                 out.at[down, pl.ds(pl.multiple_of(part * width + pair * 128, 128), 128)]) for part in range(3)]

    def load_copy(self, k, src):
        return pltpu.make_async_copy(src.at[self.p.core], self.own.at[k], self.load.at[k])

    def core_copy(self, k, src):
        p = self.p
        return remote(src.at[1 - p.core], self.cb.at[k], self.cs.at[k], self.cr.at[k], (p.partner, p.me))

    def begin(self, k):
        def go(i, j):
            self.core_copy(k, self.srcs[i].at[j]).start()
            self.load_copy(k, self.srcs[i].at[j]).start()
        self.source(k, go)

    def slot(self, order, t, mask):
        base = sum(self.p.groups >> (u + 1) for u in range(t))
        return base + subsets(order[t + 1:]).index(mask)

    def group_copy(self, k, color, t, mask):
        p = self.p
        order = p.orders[color]
        i = self.slot(order, t, mask)
        return remote(self.own.at[k, xor(p.me, (1 << order[t]) | mask), color], self.xb.at[k, color, i],
                      self.xs.at[k, color, i], self.xr.at[k, color, i], (p.dp, flip(p.me, order[t])))

    def group_send(self, k, t):
        for color in (0, 1):
            for mask in subsets(self.p.orders[color][t + 1:]):
                self.group_copy(k, color, t, mask).start()

    def core_add(self, k):
        self.load_copy(k, self.srcs[0].at[0]).wait()
        self.core_copy(k, self.srcs[0].at[0]).wait_recv()
        for f in range(self.p.groups):
            for color in (0, 1):
                self.own[k, f, color] = (self.own[k, f, color].astype(f32) + self.cb[k, f, color].astype(f32)).astype(bf16)
        self.group_send(k, 0)

    def group_add(self, t, k):
        p = self.p
        for color in (0, 1):
            order = p.orders[color]
            for mask in subsets(order[t + 1:]):
                self.group_copy(k, color, t, mask).wait_recv()
                blk, i = xor(p.me, mask), self.slot(order, t, mask)
                total = self.own[k, blk, color].astype(f32) + self.xb[k, color, i].astype(f32)
                if t == p.bits - 1:
                    self.u2[k, self.part(color)] = total.astype(bf16)
                else:
                    self.own[k, blk, color] = total.astype(bf16)
        if t < p.bits - 1:
            self.group_send(k, t + 1)
        else:
            @pl.when(self.e == 0)
            def _():
                (self.climb_copy(k) if self.last > 0 else self.middle_copy(k)).start()

    def part(self, color):
        half = self.u2.shape[1] // 2
        return slice(color * half, (color + 1) * half)

    def climb_copy(self, k):
        return remote(self.u2.at[k], self.zb.at[k], self.zs.at[k], self.zr.at[k], self.inner)

    def middle_copy(self, k):
        return remote(self.u2.at[k], self.mb.at[k], self.ms.at[k], self.mr.at[k], self.inner)

    def climb(self, j, k):
        @pl.when(self.e == j)
        def _():
            self.climb_copy(k).wait_recv()
            for color in (0, 1):
                total = self.u2[k, self.part(color)].astype(f32) + self.zb[k, self.part(color)].astype(f32)
                self.u2[k, self.part(color)] = total.astype(bf16)
            (self.middle_copy(k) if j == self.last else self.climb_copy(k)).start()

    def share_copy(self, k):
        return remote(self.fin.at[k], self.fin.at[k], self.fs.at[k], self.fr.at[k], self.outer)

    def share_wait(self, k):
        return remote(self.fin.at[k], self.fin.at[k], self.fs.at[k], self.fr.at[k], self.inner)

    def out_copies(self, k, i, j):
        p = self.p
        mine, other = self.targets(k, i, j, p.core), self.targets(k, i, j, 1 - p.core)
        sent = [remote(s, d, self.ps.at[k, n], self.pr.at[k, n], (p.partner, p.me)) for n, (s, d) in enumerate(mine)]
        kept = [pltpu.make_async_copy(s, d, self.st.at[k, n]) for n, (s, d) in enumerate(mine)]
        return sent, kept, other

    def done(self, k):
        def go(i, j):
            sent, kept, _ = self.out_copies(k, i, j)
            for c in sent + kept:
                c.start()
        self.source(k, go)

    def retire(self, k):
        p = self.p
        def go(i, j):
            sent, kept, other = self.out_copies(k, i, j)
            for n, c in enumerate(sent):
                c.wait_send()
                s, d = other[n]
                remote(s, d, self.ps.at[k, n], self.pr.at[k, n], (p.partner, p.me)).wait_recv()
            for c in kept:
                c.wait()
        self.source(k, go)

    def middle(self, k):
        @pl.when(self.e == self.last)
        def _():
            self.middle_copy(k).wait_recv()
            for color in (0, 1):
                total = self.u2[k, self.part(color)].astype(f32) + self.mb[k, self.part(color)].astype(f32)
                self.fin[k, self.part(color)] = total.astype(bf16)
            if self.last > 0:
                self.share_copy(k).start()
            self.done(k)

    def descend(self, j, k):
        @pl.when(self.e == j)
        def _():
            self.share_wait(k).wait_recv()
            if j > 0:
                self.share_copy(k).start()
            self.done(k)

    def tick(self, t):
        for s in range(len(self.stages) - 1, -1, -1):
            k = t - self.lags[s]
            @pl.when((k >= 0) & (k < self.total + self.gap) & ((k < self.total - self.gap) | (k >= self.total)))
            def _(s=s, k=k):
                self.stages[s](k - self.gap * (k // self.total))

    def drain(self):
        p = self.p
        @pl.loop(0, self.total)
        def _(k):
            self.core_copy(k, self.srcs[0].at[0]).wait_send()
            for color in (0, 1):
                for t in range(p.bits):
                    for mask in subsets(p.orders[color][t + 1:]):
                        self.group_copy(k, color, t, mask).wait_send()
            @pl.when(self.e == self.last)
            def _():
                self.middle_copy(k).wait_send()
            @pl.when(self.e < self.last)
            def _():
                self.climb_copy(k).wait_send()
            @pl.when(self.e > 0)
            def _():
                self.share_copy(k).wait_send()
            self.retire(k)


def wgrad_cols_kernel(a_ref, b_ref, o_ref):
    y = dot(a_ref[...], b_ref[...], TN).astype(bf16)
    _, _, g, _, r, c = o_ref.shape
    for core in (0, 1):
        z = y[:, core * c:(core + 1) * c].reshape(g, 2, 2, r, c)
        for half in (0, 1):
            o_ref[half, core] = z[:, half]


def wgrad_cols(a, b, groups):
    s, m = a.shape
    n = b.shape[1]
    r, c = m // groups // 4, m // 2
    return pl.pallas_call(
        wgrad_cols_kernel, grid=(n // m,),
        in_specs=[pl.BlockSpec((s, m), lambda i: (0, 0)), pl.BlockSpec((s, m), lambda i: (0, i))],
        out_specs=pl.BlockSpec((2, 2, groups, 2, r, c), lambda i: (i, 0, 0, 0, 0, 0)),
        out_shape=jax.ShapeDtypeStruct((2 * n // m, 2, groups, 2, r, c), bf16),
        cost_estimate=pl.CostEstimate(flops=2 * s * m * n, bytes_accessed=2 * (s * (m + n) + m * n),
                                      transcendentals=0), name="wgrad_cols")(a, b)


def wgrad_rows_kernel(a_ref, b_ref, o_ref):
    y = dot(a_ref[...], b_ref[...], TN).astype(bf16)
    q, _, _, _, r, c = o_ref.shape
    for core in (0, 1):
        o_ref[:, core, 0] = y[:, core * c:(core + 1) * c].reshape(q, 2, r, c)


def wgrad_rows(a, b, groups):
    s, m = a.shape
    n = b.shape[1]
    q, r, c = 2 * m // n, n // groups // 4, n // 2
    return pl.pallas_call(
        wgrad_rows_kernel, grid=(groups,),
        in_specs=[pl.BlockSpec((s, m // groups), lambda i: (0, i)), pl.BlockSpec((s, n), lambda i: (0, 0))],
        out_specs=pl.BlockSpec((q, 2, 1, 2, r, c), lambda i: (0, 0, i, 0, 0, 0)),
        out_shape=jax.ShapeDtypeStruct((q, 2, groups, 2, r, c), bf16),
        cost_estimate=pl.CostEstimate(flops=2 * s * m * n, bytes_accessed=2 * (s * (m + n) + m * n),
                                      transcendentals=0), name="wgrad_rows")(a, b)


def attn_fwd_kernel(shape, count, rows, *refs):
    len_ref, q_ref, k_ref, v_ref = refs[:4]
    ins = refs[4:4 + count]
    o_ref, lse_ref = refs[4 + count:6 + count]
    outs = refs[6 + count:6 + 2 * count]
    step, steps = pl.program_id(0), pl.num_programs(0)
    p = Place(shape)
    g = Gather(p, ins, outs, refs[6 + 2 * count:])
    @pl.when(step == 0)
    def _():
        greet(gather_peers(p, False))
        for w in range(count):
            g.start(w)
    for w, at in ((0, 2), (1, 4)):
        @pl.when(step == at)
        def _(w=w):
            g.after(w, 0)
    attn_fwd_body(len_ref, q_ref, k_ref, v_ref, o_ref, lse_ref, rows)
    @pl.when(step == steps - 1)
    def _():
        for w in range(2, count):
            g.after(w, 0)
        for t in range(1, p.bits):
            for w in range(count):
                g.after(w, t)
        for w in range(count):
            g.finish(w)


def attn_fwd_call(shape, length, qkv, ws, rows=256):
    groups = shape["fsdp"]
    s, d3 = qkv.shape
    d = d3 // 3
    np_ = d // 128
    sd = jax.ShapeDtypeStruct
    res = pl.pallas_call(
        functools.partial(attn_fwd_kernel, shape, len(ws), rows), grid=(np_,),
        in_specs=[pl.BlockSpec(memory_space=pltpu.SMEM), pl.BlockSpec((s, 128), lambda i: (0, i)),
                  pl.BlockSpec((s, 128), lambda i: (0, np_ + i)),
                  pl.BlockSpec((s, 128), lambda i: (0, 2 * np_ + i))] + [ANY] * len(ws),
        out_specs=[pl.BlockSpec((s, 128), lambda i: (0, i)), pl.BlockSpec((s, 128), lambda i: (0, 0))]
        + [ANY] * len(ws),
        out_shape=[sd((s, d), bf16), sd((s, 128), f32)] + [gather_shape(w, groups) for w in ws],
        scratch_shapes=Gather.scratch(len(ws), groups),
        compiler_params=pltpu.CompilerParams(collective_id=2, has_side_effects=True),
        cost_estimate=pl.CostEstimate(flops=8 * s * s * d, bytes_accessed=8 * s * d, transcendentals=s * s * 12),
        name="attn_fwd")(length, qkv, qkv, qkv, *[quarter(w) for w in ws])
    return res[0], res[1], [r.reshape(-1, r.shape[-1]) for r in res[2:]]


def f32_rows_dot(row, weights):
    parts = split3(row)
    stack = jnp.concatenate(list(parts) + [jnp.zeros((5, row.shape[1]), f32)], axis=0).astype(bf16)
    return colsum(dot(stack, weights))


class Small:
    def __init__(self, place, scratch):
        self.p = place
        (self.ag, self.rows, self.ab, self.bs, self.bm, self.bb, self.bg, self.s1, self.r1, self.s2, self.r2) = scratch

    @staticmethod
    def widths(shape, d, ff, n_mod):
        groups = shape["fsdp"]
        part = n_mod // groups
        return -(-(d // groups) // 128) * 128, ff // groups, part if part % 128 == 0 else n_mod

    @staticmethod
    def scratch(shape, d, ff, n_mod):
        groups, lines = shape["fsdp"], shape["dp"]
        wide, fpart, gpart = Small.widths(shape, d, ff, n_mod)
        vm = lambda *dims: pltpu.VMEM(dims, f32)
        sem = pltpu.SemaphoreType.DMA
        return [vm(groups, 1, n_mod), vm(groups, 8, d), vm(groups, 1, ff), vm(lines, 8, wide), vm(lines, groups, 384),
                vm(lines, 1, fpart), vm(lines, groups, gpart), sem((groups, 3)), sem((groups, 3)), sem((lines, 4)),
                sem((lines, 4))]

    def peers(self):
        p = self.p
        return [(p.dp, xor(p.me, m)) for m in range(1, p.groups)] + [(xor(p.dp, m), p.me) for m in range(1, p.lines)]

    def copies(self, stage, m, arrived):
        p = self.p
        if stage == 1:
            bufs, ss, rs = (self.ag, self.rows, self.ab), self.s1, self.r1
            where, slot = (p.dp, xor(p.me, m)), xor(p.me, m) if arrived else p.me
        else:
            bufs, ss, rs = (self.bs, self.bm, self.bb, self.bg), self.s2, self.r2
            where, slot = (xor(p.dp, m), p.me), xor(p.dp, m) if arrived else p.dp
        return [remote(b.at[slot], b.at[slot], ss.at[m, i], rs.at[m, i], where) for i, b in enumerate(bufs)]

    def spread(self, stage):
        for m in range(1, self.p.groups if stage == 1 else self.p.lines):
            for c in self.copies(stage, m, False):
                c.start()

    def collect(self, stage):
        for m in range(1, self.p.groups if stage == 1 else self.p.lines):
            for c in self.copies(stage, m, True):
                c.wait_recv()

    def settle(self):
        for stage in (1, 2):
            for m in range(1, self.p.groups if stage == 1 else self.p.lines):
                for c in self.copies(stage, m, False):
                    c.wait_send()

    def first(self, sums, sb1, sums1, vec_pre, vec_mid, condp, meta, ada):
        me = self.p.me
        d = sums.shape[1]
        ggm, gb2, a2, s2, gga, st0, st1, st2 = (sums[i:i + 1] for i in range(8))
        a1, s1, gemb = (sums1[i:i + 1] for i in range(3))
        gain1, scale_a, gain2, scale_m = vec_pre[1:2], vec_pre[2:3], vec_mid[1:2], vec_mid[2:3]
        gm = jnp.concatenate([s1, a1 * gain1, gga, s2, a2 * gain2, ggm], axis=1)
        sig = 1.0 / (1.0 + jnp.exp(-condp))
        gc = f32_rows_dot(gm, ada) * (sig * (1.0 + condp * (1.0 - sig)))
        lane = lax.broadcasted_iota(jnp.int32, (1, 128), 1)
        total = lambda x: jnp.sum(x, axis=1, keepdims=True)
        stat = jnp.where(lane == 0, total(st0), jnp.where(lane == 1, total(st1), jnp.where(lane == 2, total(st2), meta)))
        tail = jnp.concatenate([gc, condp * sig, stat, jnp.zeros((1, d - 384), f32)], axis=1)
        self.ag[me] = gm
        self.ab[me] = sb1
        self.rows[me] = jnp.concatenate([(1.0 + scale_a) * a1, (1.0 + scale_m) * a2, gb2, gemb, tail,
                                         jnp.zeros((3, d), f32)], axis=0)
        self.spread(1)

    def second(self):
        p = self.p
        self.collect(1)
        d = self.rows.shape[2]
        wide, fpart, gpart = self.bs.shape[2], self.bb.shape[2], self.bg.shape[2]
        total = self.rows[0]
        for f in range(1, p.groups):
            total = total + self.rows[f]
        self.bs[p.dp] = pltpu.roll(total, (d - p.me * (d // p.groups)) % d, 1)[:, :wide]
        self.bm[p.dp] = jnp.concatenate([self.rows[f, 4:5, :384] for f in range(p.groups)], axis=0)
        cut = pl.ds(pl.multiple_of(p.me * fpart, 128), fpart)
        part = self.ab[0, :, cut]
        for f in range(1, p.groups):
            part = part + self.ab[f, :, cut]
        self.bb[p.dp] = part
        n_mod = self.ag.shape[2]
        cut = slice(None) if gpart == n_mod else pl.ds(pl.multiple_of(p.me * gpart, 128), gpart)
        self.bg[p.dp] = jnp.concatenate([self.ag[f, :, cut] for f in range(p.groups)], axis=0)
        self.spread(2)

    def third(self, norms_ref, gb1_ref, gada_ref, gbada_ref, table_ref, rms_ref, d):
        p = self.p
        self.collect(2)
        total, part = self.bs[0], self.bb[0]
        for z in range(1, p.lines):
            total = total + self.bs[z]
            part = part + self.bb[z]
        norms_ref[...] = total
        gb1_ref[...] = part
        mods = jnp.concatenate([self.bg[z] for z in range(p.lines)], axis=0)
        info = jnp.concatenate([self.bm[z] for z in range(p.lines)], axis=0)
        gcs, conds, stat = info[:, :128], info[:, 128:256], info[:, 256:384]
        highest = lax.Precision.HIGHEST
        gada_ref[...] = lax.dot_general(mods, conds, TN, precision=highest, preferred_element_type=f32)
        gbada_ref[...] = colsum(mods)
        ids = stat[:, 4:5].astype(jnp.int32)
        hot = (lax.broadcasted_iota(jnp.int32, (ids.shape[0], table_ref.shape[0]), 1) == ids).astype(f32)
        table_ref[...] = lax.dot_general(hot, gcs, TN, precision=highest, preferred_element_type=f32)
        stat = colsum(stat)
        rms_ref[...] = jnp.sqrt(stat / (stat[:, 3:4] * d))


def small_shapes(shape, d, ff, n_mod, table_rows):
    wide, fpart, gpart = Small.widths(shape, d, ff, n_mod)
    sd = lambda *dims: jax.ShapeDtypeStruct(dims, f32)
    return [sd(8, wide), sd(1, fpart), sd(gpart, 128), sd(1, gpart), sd(table_rows, 128), sd(1, 128)]


def small_results(shape, res, sizes):
    norms, gb1, gada, gbada, table, rms = res
    n_ada = sizes[5]
    if gada.shape[0] != n_ada:
        me = lax.axis_index("fsdp")
        gada = lax.dynamic_slice_in_dim(gada, me * n_ada, n_ada, axis=0)
        gbada = lax.dynamic_slice_in_dim(gbada, me * n_ada, n_ada, axis=1)
    g1, g2, gb2, gemb = (norms[i, :sizes[i]] for i in range(4))
    return g1, g2, gb2, gemb, gb1[0], gada, gbada[0], table, rms[0, :3]


def tail_kernel(shape, counts, rows, post, pairs, *refs):
    n = len(counts)
    (len_ref, q_ref, k_ref, v_ref, o_ref, g_ref, lse_ref, cos_ref, sin_ref, n1_ref, w_ref, tok_ref, flag_ref, gh1_ref,
     vpre_ref, vmid_ref, sums_ref, sb1_ref, condp_ref, meta_ref, ada_ref) = refs[:21]
    srcs = refs[21:20 + n]
    outs = refs[20 + n:21 + 2 * n]
    igrad_ref, reduced, small_out = outs[0], outs[1:1 + n], refs[21 + 2 * n:27 + 2 * n]
    dqs, dks, dvs, dqkv, gq, sums1 = refs[27 + 2 * n:33 + 2 * n]
    rscratch, sscratch = refs[33 + 2 * n:54 + 2 * n], refs[54 + 2 * n:]
    step, steps = pl.program_id(0), 2 * pairs + post
    p = Place(shape)
    r = Reduce(p, counts, ["rows"] + ["cols"] * (n - 2) + ["qkv"], list(srcs) + [gq], reduced, rscratch, 2, 2)
    small = Small(p, sscratch)

    @pl.when(step == 0)
    def _():
        r.greet(small.peers())

    @pl.loop(2 * step, 2 * step + 2)
    def _(t):
        r.tick(t)

    @pl.when(step < 2 * pairs)
    def _():
        pair, head = step // 2, step % 2

        def emit(*parts):
            for i, x in enumerate(parts):
                dqkv[i, pair] = x
            y = dot(n1_ref[...], jnp.concatenate(parts, axis=1)).astype(bf16)
            _, _, g, _, rr, c = gq.shape
            y = y.reshape(g, 2, 2, rr, c)
            for half in (0, 1):
                gq[2 * (pair // 2) + half, pair % 2] = y[:, half]

        attn_bwd_body(len_ref, q_ref, k_ref, v_ref, o_ref, g_ref, lse_ref, cos_ref, sin_ref, dqs, dks, dvs, rows,
                      pair, head, emit)

    @pl.when(step >= 2 * pairs)
    def _():
        i = step - 2 * pairs
        m = tok_ref.shape[0]
        cut = pl.ds(pl.multiple_of(i * m, m), m)
        grads = [jnp.concatenate([dqkv[a, b, cut, :] for b in range(pairs)], axis=1) for a in range(3)]
        masked = flag_ref[...] == 1
        h0 = jnp.where(masked, vpre_ref[0:1, :], tok_ref[...].astype(f32))
        igrad_ref[...], new = post_rows(grads, h0, masked, gh1_ref[...], vpre_ref[1:2, :], vpre_ref[2:3, :], w_ref)
        sums1[...] = jnp.where(i == 0, new, sums1[...] + new)

    @pl.when(step == steps - 1)
    def _():
        small.first(sums_ref[...], sb1_ref[...], sums1[...], vpre_ref[...], vmid_ref[...], condp_ref[...], meta_ref[...],
                    ada_ref[...])
        small.second()
        @pl.loop(2 * steps, max(r.ticks, 2 * steps))
        def _(t):
            r.tick(t)
        small.third(*small_out, sums1.shape[1])
        r.drain()
        small.settle()


def tail_call(shape, length, qkv, att, gatt, lse, cos, sin, n1t, w, tok, flag, gh1, vpre, vmid, sums, sb1, condp, meta,
              ada, grads, table_rows, rows=256, post=128):
    groups = shape["fsdp"]
    s, d3 = qkv.shape
    d = d3 // 3
    pairs = d // 128
    blocks = s // post
    steps = 2 * pairs + blocks
    ff, n_mod = sb1.shape[1], ada.shape[0]
    r, c = 2 * grads[0].shape[-2], grads[0].shape[-1]
    counts = [g.shape[0] for g in grads] + [pairs]
    pair = lambda i: jnp.minimum(i // 2, pairs - 1)
    blk = lambda i: jnp.maximum(i - 2 * pairs, 0)
    once = pl.Buffered(1)
    col = lambda base: pl.BlockSpec((s, 128), lambda i: (0, base + pair(i)))
    whole = lambda a: pl.BlockSpec(a.shape, lambda i: (0,) * a.ndim, pipeline_mode=once)
    row = lambda cc: pl.BlockSpec((post, cc), lambda i: (blk(i), 0))
    sd = jax.ShapeDtypeStruct
    shard = d // groups
    red = [sd((shard * (g.shape[0] // 2), d), bf16) if i == 0 else sd((shard, d * (g.shape[0] // 2)), bf16)
           for i, g in enumerate(grads)] + [sd((shard, d3), bf16)]
    smalls = small_shapes(shape, d, ff, n_mod, table_rows)
    const = lambda x: pl.BlockSpec(x.shape, lambda i: (0, 0), pipeline_mode=once)
    res = pl.pallas_call(
        functools.partial(tail_kernel, shape, counts, rows, blocks, pairs), grid=(steps,),
        in_specs=[pl.BlockSpec(memory_space=pltpu.SMEM), col(0), col(pairs), col(2 * pairs), col(0), col(0), whole(lse),
                  whole(cos), whole(sin), whole(n1t), whole(w), row(d), row(1), row(d)]
        + [whole(x) for x in (vpre, vmid, sums, sb1, condp, meta, ada)] + [ANY] * len(grads),
        out_specs=[row(d)] + [ANY] * len(red) + [const(x) for x in smalls],
        out_shape=[sd((s, d), bf16)] + red + smalls,
        scratch_shapes=[pltpu.VMEM((128, s), f32), pltpu.VMEM((s, 128), f32), pltpu.VMEM((s, 128), f32),
                        pltpu.VMEM((3, pairs, s, 128), bf16), pltpu.VMEM((pairs, 2, groups, 2, r // 2, c), bf16),
                        pltpu.VMEM((8, d), f32)]
        + Reduce.scratch(sum(counts), groups, r, c) + Small.scratch(shape, d, ff, n_mod),
        compiler_params=pltpu.CompilerParams(collective_id=3, has_side_effects=True, vmem_limit_bytes=65000 * 1024),
        cost_estimate=pl.CostEstimate(flops=30 * s * s * d, bytes_accessed=40 * s * d, transcendentals=s * s * 12),
        name="tail")(length, qkv, qkv, qkv, att, gatt, lse, cos, sin, n1t, w, tok, flag, gh1, vpre, vmid, sums, sb1, condp,
                     meta, ada, *grads)
    return res[0], res[1:1 + len(red)], res[1 + len(red):]
from jax.sharding import PartitionSpec as P

highest = lax.Precision.HIGHEST


def rotary_tables(length):
    half = HD // 2
    rate = 1.0 / 10000.0 ** (jnp.arange(half, dtype=f32) * 2.0 / HD)
    angle = jnp.arange(length, dtype=f32)[:, None] * rate[None, :]
    angle = jnp.concatenate([angle] * (128 // half), axis=-1)
    sign = jnp.where(jnp.arange(128) % HD < half, -1.0, 1.0)
    return jnp.cos(angle), jnp.sin(angle) * sign


def per_device(shape, tokens, hidden_token_indicator, lengths, time_ids, cotangent, gain_one, w_qkv, w_out, gain_two,
               w_fc1, b_fc1, w_fc2, b_fc2, w_ada, b_ada, mask_embed, time_table):
    groups = shape["fsdp"]
    s, d = tokens.shape[1:]
    ff = b_fc1.shape[0] * groups
    tok, cot = tokens[0], cotangent[0]
    flag = hidden_token_indicator.reshape(s, 1)
    sizes = [v.shape[0] for v in (gain_one, gain_two, b_fc2, mask_embed, b_fc1, b_ada)]
    small = jnp.concatenate([gain_one, gain_two, b_fc2, mask_embed, b_fc1, b_ada])[None]
    (ada_all, qkv_all), packed = head_call(shape, small, [w_ada, w_qkv])
    packed = packed[:, 0]
    cuts = [sum(sizes[:i]) for i in range(len(sizes) + 1)]
    gain1, gain2, b2, emb, b1, bada = (
        packed[:, cuts[i]:cuts[i + 1]].reshape(1, -1).astype(f32) for i in range(len(sizes)))
    cond_pre = lax.dynamic_slice_in_dim(time_table, time_ids[0], 1, axis=0)
    cond = jax.nn.silu(cond_pre)
    modulation = jnp.dot(cond, ada_all.astype(f32).T, precision=highest) + bada
    shift_a, scale_a, gate_a, shift_m, scale_m, gate_m = (modulation[:, i * d:(i + 1) * d] for i in range(6))
    cos, sin = rotary_tables(s)
    zero = jnp.zeros((1, d), f32)
    vec_pre = jnp.concatenate([emb, gain1, scale_a, shift_a] + [zero] * 4, axis=0)
    vec_mid = jnp.concatenate([emb, gain2, scale_m, shift_m, gate_a, gate_m, b2, zero], axis=0)
    n1, qkv = pre_call(tok, flag, vec_pre, qkv_all, cos, sin)
    att, lse, (out_all, fc1_all, fc2_all) = attn_fwd_call(shape, lengths, qkv, [w_out, w_fc1, w_fc2])
    out, gh1, gatt, n2, act, gm, gpre, gap, sums, gb1 = mid_call(
        lengths, att, tok, flag, cot, vec_mid, b1, out_all, fc1_all, fc2_all)
    g_fc2 = wgrad_rows(act, gm, groups)
    g_fc1 = wgrad_cols(n2, gpre, groups)
    g_out = wgrad_cols(att, gap, groups)
    meta = jnp.concatenate([jnp.zeros((3,), f32), lengths.astype(f32), time_ids.astype(f32), jnp.zeros((123,), f32)])[None]
    igrad, (r_fc2, r_fc1, r_out, r_qkv), smalls = tail_call(
        shape, lengths, qkv, att, gatt, lse, cos, sin, n1, qkv_all, tok, flag, gh1, vec_pre, vec_mid, sums, gb1, cond_pre,
        meta, ada_all, [g_fc2, g_fc1, g_out], time_table.shape[0])
    g1, g2, gb2, gemb, gb1, g_ada, gbada, table, rms = small_results(shape, smalls, sizes)
    return (out[None], igrad[None], g1, r_qkv.astype(f32), r_out.astype(f32), g2, r_fc1.astype(f32), gb1,
            r_fc2.astype(f32), gb2,
            g_ada, gbada, gemb, table, rms)


def solution(mesh):
    both = ("dp", "fsdp")
    f1, f2 = P("fsdp"), P("fsdp", None)
    placed = (P(both, None, None), P(both, None), P(both), P(both), P(both, None, None), f1, f2, f2, f1, f2, f1, f2, f1,
              f2, f1, f1, P())
    outs = (P(both, None, None), P(both, None, None), f1, f2, f2, f1, f2, f1, f2, f1, f2, f1, f1, P(), P())
    return jax.shard_map(functools.partial(per_device, dict(mesh.shape)), mesh=mesh, in_specs=placed, out_specs=outs,
                         check_vma=False)
```

```python
import functools, math
import jax, jax.numpy as jnp
from jax import lax
from jax.experimental import pallas as pl
from jax.experimental.pallas import tpu as pltpu

HD = 64
EPS = 1e-5
LOG2E = math.log2(math.e)
QSCALE = LOG2E * HD ** -0.5
f32, bf16 = jnp.float32, jnp.bfloat16
NT = (((1,), (1,)), ((), ()))
NN = (((1,), (0,)), ((), ()))
TN = (((0,), (0,)), ((), ()))

def dot(a, b, dims=NN):
    return lax.dot_general(a, b, dims, preferred_element_type=f32)

def norm_parts(x):
    mean = jnp.mean(x, axis=-1, keepdims=True)
    cen = x - mean
    rs = lax.rsqrt(jnp.mean(cen * cen, axis=-1, keepdims=True) + EPS)
    return cen * rs, rs

def swap_halves(u):
    lane = lax.broadcasted_iota(jnp.int32, u.shape, 1)
    return jnp.where(lane % HD < HD // 2, pltpu.roll(u, 96, 1), pltpu.roll(u, 32, 1))

def pre_kernel(tok_ref, flag_ref, vec_ref, w_ref, cos_ref, sin_ref, n1_ref, qkv_ref):
    emb, gain, scale, shift = (vec_ref[i:i + 1, :] for i in range(4))
    h0 = jnp.where(flag_ref[...] == 1, emb, tok_ref[...].astype(f32))
    n, _ = norm_parts(h0)
    n1 = (n * gain * (1.0 + scale) + shift).astype(bf16)
    n1_ref[...] = n1.astype(f32).T.astype(bf16)
    d = n1.shape[1]
    cos, sin = cos_ref[...], sin_ref[...]
    for part in range(3):
        y = dot(n1, w_ref[:, part * d:(part + 1) * d])
        for c in range(d // 128):
            lo = part * d + c * 128
            u = y[:, c * 128:(c + 1) * 128]
            if part < 2:
                u = u * cos + swap_halves(u) * sin
                if part == 0:
                    u = u * QSCALE
            qkv_ref[:, lo:lo + 128] = u.astype(bf16)

def pre_call(tok, flag, vecs, w, cos, sin, rows=256):
    s, d = tok.shape
    return pl.pallas_call(
        pre_kernel, grid=(s // rows,),
        in_specs=[pl.BlockSpec((rows, d), lambda i: (i, 0)), pl.BlockSpec((rows, 1), lambda i: (i, 0)),
                  pl.BlockSpec((8, d), lambda i: (0, 0)), pl.BlockSpec((d, 3 * d), lambda i: (0, 0)),
                  pl.BlockSpec((rows, 128), lambda i: (i, 0)), pl.BlockSpec((rows, 128), lambda i: (i, 0))],
        out_specs=[pl.BlockSpec((d, rows), lambda i: (0, i)), pl.BlockSpec((rows, 3 * d), lambda i: (i, 0))],
        out_shape=[jax.ShapeDtypeStruct((d, s), bf16), jax.ShapeDtypeStruct((s, 3 * d), bf16)],
        cost_estimate=pl.CostEstimate(flops=2 * s * d * 3 * d, bytes_accessed=12 * s * d, transcendentals=0),
        name="pre")(tok, flag, vecs, w, cos, sin)

def attn_fwd_body(len_ref, q_ref, k_ref, v_ref, o_ref, lse_ref, rows):
    p = pl.program_id(0)
    s = q_ref.shape[0]
    length = len_ref[0]
    lane = lax.broadcasted_iota(jnp.int32, (s, 128), 1)
    pos = lax.broadcasted_iota(jnp.int32, (s, 128), 0)
    lane_q = lax.broadcasted_iota(jnp.int32, (rows, 128), 1)
    k = k_ref[...].astype(f32)
    v = v_ref[...].astype(f32)
    kx, vx = [], []
    for h in (0, 1):
        extra = HD * (1 - h)
        mine = (lane >= HD) if h else (lane < HD)
        bias = jnp.where(pos >= length, -1e30, 0.0)
        kx.append(jnp.where(mine, k, jnp.where(lane == extra, bias, 0.0)).astype(bf16))
        vx.append(jnp.where(mine, v, jnp.where(lane == extra, 1.0, 0.0)).astype(bf16))
    for b in range(s // rows):
        q = q_ref[b * rows:(b + 1) * rows, :].astype(f32)
        outs, lses = [], []
        for h in (0, 1):
            extra = HD * (1 - h)
            mine = (lane_q >= HD) if h else (lane_q < HD)
            qx = jnp.where(mine, q, jnp.where(lane_q == extra, 1.0, 0.0)).astype(bf16)
            sc = dot(qx, kx[h], NT)
            m = jnp.max(sc, axis=1, keepdims=True)
            pr = jnp.exp2(sc - m).astype(bf16)
            o = dot(pr, vx[h])
            tot = o[:, extra:extra + 1]
            outs.append(o * (1.0 / tot))
            lses.append(m + jnp.log(tot) * LOG2E)
        o_ref[b * rows:(b + 1) * rows, :] = jnp.where(lane_q < HD, outs[0], outs[1]).astype(bf16)
        old = jnp.where(p == 0, 0.0, lse_ref[b * rows:(b + 1) * rows, :])
        lse_ref[b * rows:(b + 1) * rows, :] = jnp.where(
            lane_q == 2 * p, lses[0], jnp.where(lane_q == 2 * p + 1, lses[1], old))

def split3(x):
    hi = x.astype(bf16).astype(f32)
    r = x - hi
    mid = r.astype(bf16).astype(f32)
    return hi, mid, r - mid

def attn_bwd_body(len_ref, q_ref, k_ref, v_ref, o_ref, g_ref, lse_ref, cos_ref, sin_ref,
                  dqs, dks, dvs, rows, p, h, emit):
    s = q_ref.shape[0]
    length = len_ref[0]
    lane = lax.broadcasted_iota(jnp.int32, (s, 128), 1)
    pos = lax.broadcasted_iota(jnp.int32, (s, 128), 0)
    lane_q = lax.broadcasted_iota(jnp.int32, (rows, 128), 1)
    e = HD * (1 - h)
    mine, mine_q = lane // HD == h, lane_q // HD == h
    k = k_ref[...].astype(f32)
    v = v_ref[...].astype(f32)
    ones = jnp.where((lane >= e) & (lane < e + 3), 1.0, 0.0)
    bias = jnp.where(pos >= length, -1e30, 0.0)
    kx = jnp.where(mine, k, jnp.where(lane == e + 3, bias, ones)).astype(bf16)
    vx = jnp.where(mine, v, ones).astype(bf16)
    kt = jnp.where(mine, k, 0.0).T.astype(bf16)
    dk = jnp.zeros((s, 128), f32)
    dv = jnp.zeros((s, 128), f32)
    for b in range(s // rows):
        sl = slice(b * rows, (b + 1) * rows)
        qb = q_ref[sl, :]
        gb = g_ref[sl, :]
        q = qb.astype(f32)
        g = gb.astype(f32)
        lse = jnp.sum(jnp.where(lane_q == 2 * p + h, lse_ref[sl, :], 0.0), axis=1, keepdims=True)
        dd = jnp.sum(jnp.where(mine_q, g * o_ref[sl, :].astype(f32), 0.0), axis=1, keepdims=True)
        l0, l1, l2 = split3(-lse)
        d0, d1, d2 = split3(-dd)
        qx = jnp.where(mine_q, q, jnp.where(lane_q == e, l0, jnp.where(lane_q == e + 1, l1, jnp.where(
            lane_q == e + 2, l2, jnp.where(lane_q == e + 3, 1.0, 0.0))))).astype(bf16)
        gx = jnp.where(mine_q, g, jnp.where(lane_q == e, d0, jnp.where(lane_q == e + 1, d1, jnp.where(
            lane_q == e + 2, d2, 0.0)))).astype(bf16)
        pt = jnp.exp2(dot(kx, qx, NT))
        dst = (pt * dot(vx, gx, NT)).astype(bf16)
        dv = dv + dot(pt.astype(bf16), gb)
        dk = dk + dot(dst, qb)
        dqt = dot(kt, dst)
        dqs[:, sl] = jnp.where(h == 0, dqt, dqs[:, sl] + dqt)
    @pl.when(h == 0)
    def _():
        dks[...] = dk
        dvs[...] = dv
    @pl.when(h == 1)
    def _():
        cos, sin = cos_ref[...], sin_ref[...]
        dq = dqs[...].T * (HD ** -0.5)
        dkk = jnp.where(lane < HD, dks[...], dk) * (1.0 / LOG2E)
        emit((dq * cos - swap_halves(dq) * sin).astype(bf16), (dkk * cos - swap_halves(dkk) * sin).astype(bf16),
             jnp.where(lane < HD, dvs[...], dv).astype(bf16))


def gelu_both(v):
    a, b = 0.7978845608028654, 0.044715
    v2 = v * v
    t = jnp.tanh(a * v * (1.0 + b * v2))
    half = 0.5 + 0.5 * t
    return v * half, half + (0.5 * a) * v * (1.0 - t * t) * (1.0 + 3.0 * b * v2)

def colsum(x):
    return jnp.sum(x, axis=0, keepdims=True)

def mid_kernel(len_ref, att_ref, tok_ref, flag_ref, cot_ref, vec_ref, b1_ref, wo_ref, w1_ref, w2_ref,
               out_ref, gh1_ref, gatt_ref, n2_ref, act_ref, gm_ref, gpre_ref, gap_ref, sum_ref, sb1_ref,
               gp_s, *, cut):
    i = pl.program_id(0)
    rows, d = att_ref.shape
    ff = w1_ref.shape[1]
    emb, gain, scale, shift, gate_a, gate_m, b2 = (vec_ref[r:r + 1, :] for r in range(7))
    h0 = jnp.where(flag_ref[...] == 1, emb, tok_ref[...].astype(f32))
    ap = dot(att_ref[...], wo_ref[...])
    br_a = gate_a * ap
    h1 = h0 + br_a
    n, rs = norm_parts(h1)
    n2 = (n * gain * (1.0 + scale) + shift).astype(bf16)
    n2_ref[...] = n2
    mp = jnp.zeros((rows, d), f32) + b2
    for j in range(ff // cut):
        sl = slice(j * cut, (j + 1) * cut)
        act, gp = gelu_both(dot(n2, w1_ref[:, sl]) + b1_ref[:, sl])
        act = act.astype(bf16)
        act_ref[:, sl] = act
        gp_s[:, sl] = gp
        mp = mp + dot(act, w2_ref[sl, :])
    br_m = gate_m * mp
    bo = h1 + br_m
    out_ref[...] = bo.astype(bf16)
    pos = lax.broadcasted_iota(jnp.int32, (rows, 1), 0) + i * rows
    valid = jnp.where(pos < len_ref[0], 1.0, 0.0)
    cot = cot_ref[...].astype(f32)
    gm = (gate_m * cot).astype(bf16)
    gm_ref[...] = gm
    gn2 = jnp.zeros((rows, d), f32)
    sb1 = []
    for j in range(ff // cut):
        sl = slice(j * cut, (j + 1) * cut)
        gpre = (dot(gm, w2_ref[sl, :], NT) * gp_s[:, sl]).astype(bf16)
        gpre_ref[:, sl] = gpre
        sb1.append(colsum(gpre.astype(f32)))
        gn2 = gn2 + dot(gpre, w1_ref[:, sl], NT)
    e = gn2 * (gain * (1.0 + scale))
    gh1 = cot + rs * (e - jnp.mean(e, axis=1, keepdims=True) - n * jnp.mean(e * n, axis=1, keepdims=True))
    gh1_ref[...] = gh1
    gap = (gate_a * gh1).astype(bf16)
    gap_ref[...] = gap
    gatt_ref[...] = dot(gap, wo_ref[...], NT).astype(bf16)
    new = jnp.concatenate([
        colsum(cot * mp), colsum(gm.astype(f32)), colsum(gn2 * n), colsum(gn2), colsum(gh1 * ap),
        colsum(valid * bo * bo), colsum(valid * br_a * br_a), colsum(valid * br_m * br_m)], axis=0)
    sb1 = jnp.concatenate(sb1, axis=1)
    @pl.when(i == 0)
    def _():
        sum_ref[...] = new
        sb1_ref[...] = sb1
    @pl.when(i > 0)
    def _():
        sum_ref[...] += new
        sb1_ref[...] += sb1

def mid_call(length, att, tok, flag, cot, vec, b1, wo, w1, w2, rows=256, cut=768):
    s, d = tok.shape
    ff = w1.shape[1]
    row = lambda c: pl.BlockSpec((rows, c), lambda i: (i, 0))
    whole = lambda a: pl.BlockSpec(a.shape, lambda i: (0, 0))
    sd = jax.ShapeDtypeStruct
    return pl.pallas_call(
        functools.partial(mid_kernel, cut=cut), grid=(s // rows,),
        in_specs=[pl.BlockSpec(memory_space=pltpu.SMEM), row(d), row(d), row(1), row(d), whole(vec), whole(b1),
                  whole(wo), whole(w1), whole(w2)],
        out_specs=[row(d), row(d), row(d), row(d), row(ff), row(d), row(ff), row(d),
                   pl.BlockSpec((8, d), lambda i: (0, 0)), pl.BlockSpec((1, ff), lambda i: (0, 0))],
        out_shape=[sd((s, d), bf16), sd((s, d), f32), sd((s, d), bf16), sd((s, d), bf16), sd((s, ff), bf16),
                   sd((s, d), bf16), sd((s, ff), bf16), sd((s, d), bf16), sd((8, d), f32), sd((1, ff), f32)],
        scratch_shapes=[pltpu.VMEM((rows, ff), f32)],
        compiler_params=pltpu.CompilerParams(vmem_limit_bytes=60000 * 1024),
        cost_estimate=pl.CostEstimate(flops=2 * s * d * (2 * d + 4 * ff), bytes_accessed=30 * s * d,
                                      transcendentals=s * ff),
        name="mid")(length, att, tok, flag, cot, vec, b1, wo, w1, w2)

def post_rows(grads, h0, masked, gh1, gain, scale, w_ref):
    d = h0.shape[1]
    n, rs = norm_parts(h0)
    gn1 = sum(dot(g, w_ref[:, i * d:(i + 1) * d], NT) for i, g in enumerate(grads))
    e = gn1 * (gain * (1.0 + scale))
    gh0 = gh1 + rs * (e - jnp.mean(e, axis=1, keepdims=True) - n * jnp.mean(e * n, axis=1, keepdims=True))
    sums = jnp.concatenate([colsum(gn1 * n), colsum(gn1), colsum(jnp.where(masked, gh0, 0.0)),
                            jnp.zeros((5, d), f32)], axis=0)
    return jnp.where(masked, 0.0, gh0).astype(bf16), sums

MESH = pl.DeviceIdType.MESH


def flip(i, b):
    return i + 2 ** b * (1 - 2 * ((i // 2 ** b) % 2))


def xor(i, mask):
    b = 0
    while mask >> b:
        if (mask >> b) & 1:
            i = flip(i, b)
        b += 1
    return i


def subsets(bits):
    masks = [0]
    for b in bits:
        masks = masks + [m | (1 << b) for m in masks]
    return masks


def log2(n):
    return n.bit_length() - 1


class Place:
    def __init__(self, shape):
        self.groups, self.lines = shape["fsdp"], shape["dp"]
        self.bits = log2(self.groups)
        self.orders = [list(range(self.bits)), list(range(self.bits))[::-1]]
        self.me = lax.axis_index("fsdp")
        self.dp = lax.axis_index("dp")
        self.core = self.dp % 2
        self.partner = flip(self.dp, 0)


def remote(src, dst, ssem, rsem, where):
    return pltpu.make_async_remote_copy(src_ref=src, dst_ref=dst, send_sem=ssem, recv_sem=rsem, device_id=where,
                                        device_id_type=MESH)


class Gather:
    def __init__(self, place, ins, outs, sems):
        self.p, self.ins, self.outs = place, ins, outs
        self.ss, self.rs, self.fs, self.fr, self.os, self.orr = sems

    @staticmethod
    def scratch(count, groups):
        a = pltpu.SemaphoreType.DMA((count, 2, groups - 1))
        b = pltpu.SemaphoreType.DMA((count,))
        return [a, a, a, a, b, b]

    def send(self, w, color, t, mask):
        p = self.p
        order = p.orders[color]
        e = 2 ** t - 1 + subsets(order[:t]).index(mask)
        piece = p.core * 2 + color
        blk = xor(p.me, mask)
        src = self.ins[w].at[piece] if mask == 0 else self.outs[w].at[blk, piece]
        return remote(src, self.outs[w].at[blk, piece], self.ss.at[w, color, e], self.rs.at[w, color, e],
                      (p.dp, flip(p.me, order[t])))

    def arrival(self, w, color, t, mask):
        p = self.p
        order = p.orders[color]
        e = 2 ** t - 1 + subsets(order[:t]).index(mask)
        got = self.outs[w].at[xor(p.me, mask | (1 << order[t])), p.core * 2 + color]
        return e, got

    def landed(self, w, color, e, got):
        return remote(got, got, self.ss.at[w, color, e], self.rs.at[w, color, e], (self.p.partner, self.p.me))

    def forward(self, w, color, e, got):
        return remote(got, got, self.fs.at[w, color, e], self.fr.at[w, color, e], (self.p.partner, self.p.me))

    def own(self, w):
        p = self.p
        return remote(self.ins[w], self.outs[w].at[p.me], self.os.at[w], self.orr.at[w], (p.partner, p.me))

    def start(self, w):
        for t in range(self.p.bits):
            for color in (0, 1):
                self.send(w, color, t, 0).start()
        self.own(w).start()

    def after(self, w, t):
        for color in (0, 1):
            order = self.p.orders[color]
            for mask in subsets(order[:t]):
                e, got = self.arrival(w, color, t, mask)
                self.landed(w, color, e, got).wait_recv()
                for later in range(t + 1, self.p.bits):
                    self.send(w, color, later, mask | (1 << order[t])).start()
                self.forward(w, color, e, got).start()

    def finish(self, w):
        p = self.p
        for color in (0, 1):
            order = p.orders[color]
            for t in range(p.bits):
                for mask in subsets(order[:t]):
                    e, got = self.arrival(w, color, t, mask)
                    other = self.outs[w].at[xor(p.me, mask | (1 << order[t])), (1 - p.core) * 2 + color]
                    self.forward(w, color, e, other).wait_recv()
                    self.forward(w, color, e, got).wait_send()
                    self.send(w, color, t, mask).wait_send()
        self.own(w).wait()


class Direct:
    def __init__(self, place, src, out, sems):
        self.p, self.src, self.out = place, src, out
        self.ss, self.rs = sems

    @staticmethod
    def scratch(groups):
        return [pltpu.SemaphoreType.DMA((groups,))] * 2

    def copy(self, m, arrived):
        p = self.p
        where = (p.partner, p.me) if m == 0 else (p.dp, xor(p.me, m))
        slot = xor(p.me, m) if arrived else p.me
        return remote(self.src, self.out.at[slot], self.ss.at[m], self.rs.at[m], where)

    def start(self):
        for m in range(self.p.groups):
            self.copy(m, False).start()

    def finish(self):
        for m in range(self.p.groups):
            self.copy(m, True).wait_recv()
            self.copy(m, False).wait_send()


def greet(devices):
    barrier = pltpu.get_barrier_semaphore()
    for where in devices:
        pl.semaphore_signal(barrier, inc=1, device_id=where, device_id_type=MESH)
    pl.semaphore_wait(barrier, len(devices))


def gather_peers(p, everyone):
    masks = range(1, p.groups) if everyone else [1 << b for b in range(p.bits)]
    return [(p.partner, p.me)] + [(p.dp, xor(p.me, m)) for m in masks]


def quarter(w):
    return w.reshape(4, w.shape[0] // 4, w.shape[1])


def gather_shape(w, groups):
    return jax.ShapeDtypeStruct((groups, 4, w.shape[0] // 4, w.shape[1]), w.dtype)


ANY = pl.BlockSpec(memory_space=pl.ANY)


def head_kernel(shape, count, *refs):
    ins, small, outs, small_out = refs[:count], refs[count], refs[count + 1:2 * count + 1], refs[2 * count + 1]
    sems = refs[2 * count + 2:]
    p = Place(shape)
    g = Gather(p, ins, outs, sems[:6])
    s = Direct(p, small, small_out, sems[6:])
    greet(gather_peers(p, True))
    s.start()
    for w in range(count):
        g.start(w)
    for t in range(p.bits):
        for w in range(count):
            g.after(w, t)
    for w in range(count):
        g.finish(w)
    s.finish()


def head_call(shape, small, ws):
    groups = shape["fsdp"]
    outs = [gather_shape(w, groups) for w in ws] + [jax.ShapeDtypeStruct((groups,) + small.shape, small.dtype)]
    res = pl.pallas_call(
        functools.partial(head_kernel, shape, len(ws)), in_specs=[ANY] * (len(ws) + 1), out_specs=[ANY] * len(outs),
        out_shape=outs, scratch_shapes=Gather.scratch(len(ws), groups) + Direct.scratch(groups),
        compiler_params=pltpu.CompilerParams(collective_id=1, has_side_effects=True), name="head",
    )(*[quarter(w) for w in ws], small)
    return [r.reshape(-1, r.shape[-1]) for r in res[:-1]], res[-1]


class Reduce:
    def __init__(self, place, counts, kinds, srcs, outs, scratch, lag, gap):
        self.p, self.counts, self.kinds, self.srcs, self.outs = place, counts, kinds, srcs, outs
        (self.own, self.cb, self.xb, self.zb, self.mb, self.u2, self.fin,
         self.load, self.cs, self.cr, self.xs, self.xr, self.zs, self.zr, self.ms, self.mr, self.fs, self.fr,
         self.ps, self.pr, self.st) = scratch
        p = place
        self.total = sum(counts)
        self.n = p.lines // 2
        self.zi = p.dp // 2
        left = self.zi // (self.n // 2)
        self.e = self.zi * (1 - left) + (self.n - 1 - self.zi) * left
        step = 2 * (1 - 2 * left)
        self.inner = (p.dp + step, p.me)
        self.outer = (p.dp - step, p.me)
        self.last = self.n // 2 - 1
        self.stages = ([self.begin, self.core_add] + [functools.partial(self.group_add, t) for t in range(p.bits)]
                       + [functools.partial(self.climb, j) for j in range(1, self.last + 1)] + [self.middle]
                       + [functools.partial(self.descend, j) for j in range(self.last - 1, -1, -1)])
        self.lags = [0, 1] + [1 + lag * (i + 1) for i in range(len(self.stages) - 2)]
        self.early = self.total - counts[-1]
        self.gap = gap
        self.ticks = self.total + gap + self.lags[-1]

    @staticmethod
    def scratch(total, groups, rows, cols):
        sem = pltpu.SemaphoreType.DMA
        vm = lambda *lead: pltpu.VMEM((total,) + lead + (rows // 2, cols), bf16)
        one = sem((total,))
        line = pltpu.VMEM((total, rows, cols), bf16)
        return [vm(groups, 2), vm(groups, 2), vm(2, groups - 1), line, line, line, line,
                one, one, one, sem((total, 2, groups - 1)), sem((total, 2, groups - 1)),
                one, one, one, one, one, one, sem((total, 3)), sem((total, 3)), sem((total, 3))]

    def greet(self, peers):
        p = self.p
        barrier = pltpu.get_barrier_semaphore()
        for where in peers:
            pl.semaphore_signal(barrier, inc=1, device_id=where, device_id_type=MESH)
        pl.semaphore_wait(barrier, len(peers))

    def source(self, k, fn):
        base = 0
        for i, count in enumerate(self.counts):
            @pl.when((k >= base) & (k < base + count))
            def _(i=i, base=base):
                fn(i, k - base)
            base += count

    def targets(self, k, i, j, core):
        rows, cols = self.fin.shape[1:]
        out, fin = self.outs[i], self.fin.at[k]
        if self.kinds[i] == "rows":
            cut = pl.ds(pl.multiple_of(core * cols, cols), cols)
            return [(fin, out.at[pl.ds(pl.multiple_of(j * rows, rows), rows), cut])]
        down = pl.ds(pl.multiple_of((j % 2) * rows, rows), rows)
        if self.kinds[i] == "cols":
            return [(fin, out.at[down, pl.ds(pl.multiple_of((2 * (j // 2) + core) * cols, cols), cols)])]
        width = out.shape[1] // 3
        pair = 2 * (j // 2) + core
        return [(fin.at[:, part * 128:(part + 1) * 128],
                 out.at[down, pl.ds(pl.multiple_of(part * width + pair * 128, 128), 128)]) for part in range(3)]

    def load_copy(self, k, src):
        return pltpu.make_async_copy(src.at[self.p.core], self.own.at[k], self.load.at[k])

    def core_copy(self, k, src):
        p = self.p
        return remote(src.at[1 - p.core], self.cb.at[k], self.cs.at[k], self.cr.at[k], (p.partner, p.me))

    def begin(self, k):
        def go(i, j):
            self.core_copy(k, self.srcs[i].at[j]).start()
            self.load_copy(k, self.srcs[i].at[j]).start()
        self.source(k, go)

    def slot(self, order, t, mask):
        base = sum(self.p.groups >> (u + 1) for u in range(t))
        return base + subsets(order[t + 1:]).index(mask)

    def group_copy(self, k, color, t, mask):
        p = self.p
        order = p.orders[color]
        i = self.slot(order, t, mask)
        return remote(self.own.at[k, xor(p.me, (1 << order[t]) | mask), color], self.xb.at[k, color, i],
                      self.xs.at[k, color, i], self.xr.at[k, color, i], (p.dp, flip(p.me, order[t])))

    def group_send(self, k, t):
        for color in (0, 1):
            for mask in subsets(self.p.orders[color][t + 1:]):
                self.group_copy(k, color, t, mask).start()

    def core_add(self, k):
        self.load_copy(k, self.srcs[0].at[0]).wait()
        self.core_copy(k, self.srcs[0].at[0]).wait_recv()
        for f in range(self.p.groups):
            for color in (0, 1):
                self.own[k, f, color] = (self.own[k, f, color].astype(f32) + self.cb[k, f, color].astype(f32)).astype(bf16)
        self.group_send(k, 0)

    def group_add(self, t, k):
        p = self.p
        for color in (0, 1):
            order = p.orders[color]
            for mask in subsets(order[t + 1:]):
                self.group_copy(k, color, t, mask).wait_recv()
                blk, i = xor(p.me, mask), self.slot(order, t, mask)
                total = self.own[k, blk, color].astype(f32) + self.xb[k, color, i].astype(f32)
                if t == p.bits - 1:
                    self.u2[k, self.part(color)] = total.astype(bf16)
                else:
                    self.own[k, blk, color] = total.astype(bf16)
        if t < p.bits - 1:
            self.group_send(k, t + 1)
        else:
            @pl.when(self.e == 0)
            def _():
                (self.climb_copy(k) if self.last > 0 else self.middle_copy(k)).start()

    def part(self, color):
        half = self.u2.shape[1] // 2
        return slice(color * half, (color + 1) * half)

    def climb_copy(self, k):
        return remote(self.u2.at[k], self.zb.at[k], self.zs.at[k], self.zr.at[k], self.inner)

    def middle_copy(self, k):
        return remote(self.u2.at[k], self.mb.at[k], self.ms.at[k], self.mr.at[k], self.inner)

    def climb(self, j, k):
        @pl.when(self.e == j)
        def _():
            self.climb_copy(k).wait_recv()
            for color in (0, 1):
                total = self.u2[k, self.part(color)].astype(f32) + self.zb[k, self.part(color)].astype(f32)
                self.u2[k, self.part(color)] = total.astype(bf16)
            (self.middle_copy(k) if j == self.last else self.climb_copy(k)).start()

    def share_copy(self, k):
        return remote(self.fin.at[k], self.fin.at[k], self.fs.at[k], self.fr.at[k], self.outer)

    def share_wait(self, k):
        return remote(self.fin.at[k], self.fin.at[k], self.fs.at[k], self.fr.at[k], self.inner)

    def out_copies(self, k, i, j):
        p = self.p
        mine, other = self.targets(k, i, j, p.core), self.targets(k, i, j, 1 - p.core)
        sent = [remote(s, d, self.ps.at[k, n], self.pr.at[k, n], (p.partner, p.me)) for n, (s, d) in enumerate(mine)]
        kept = [pltpu.make_async_copy(s, d, self.st.at[k, n]) for n, (s, d) in enumerate(mine)]
        return sent, kept, other

    def done(self, k):
        def go(i, j):
            sent, kept, _ = self.out_copies(k, i, j)
            for c in sent + kept:
                c.start()
        self.source(k, go)

    def retire(self, k):
        p = self.p
        def go(i, j):
            sent, kept, other = self.out_copies(k, i, j)
            for n, c in enumerate(sent):
                c.wait_send()
                s, d = other[n]
                remote(s, d, self.ps.at[k, n], self.pr.at[k, n], (p.partner, p.me)).wait_recv()
            for c in kept:
                c.wait()
        self.source(k, go)

    def middle(self, k):
        @pl.when(self.e == self.last)
        def _():
            self.middle_copy(k).wait_recv()
            for color in (0, 1):
                total = self.u2[k, self.part(color)].astype(f32) + self.mb[k, self.part(color)].astype(f32)
                self.fin[k, self.part(color)] = total.astype(bf16)
            if self.last > 0:
                self.share_copy(k).start()
            self.done(k)

    def descend(self, j, k):
        @pl.when(self.e == j)
        def _():
            self.share_wait(k).wait_recv()
            if j > 0:
                self.share_copy(k).start()
            self.done(k)

    def tick(self, t):
        for s in range(len(self.stages) - 1, 0, -1):
            k = t - self.lags[s]
            @pl.when((k >= 0) & (k < self.total + self.gap) & ((k < self.total - self.gap) | (k >= self.total)))
            def _(s=s, k=k):
                self.stages[s](k - self.gap * (k // self.total))
        @pl.when(t + 1 < self.early)
        def _():
            self.begin(t + 1)
        @pl.when((t >= self.early) & (t < self.total + self.gap) & ((t < self.total - self.gap) | (t >= self.total)))
        def _():
            self.begin(t - self.gap * (t // self.total))

    def drain(self):
        p = self.p
        @pl.loop(0, self.total)
        def _(k):
            self.core_copy(k, self.srcs[0].at[0]).wait_send()
            for color in (0, 1):
                for t in range(p.bits):
                    for mask in subsets(p.orders[color][t + 1:]):
                        self.group_copy(k, color, t, mask).wait_send()
            @pl.when(self.e == self.last)
            def _():
                self.middle_copy(k).wait_send()
            @pl.when(self.e < self.last)
            def _():
                self.climb_copy(k).wait_send()
            @pl.when(self.e > 0)
            def _():
                self.share_copy(k).wait_send()
            self.retire(k)


def wgrad_cols_kernel(a_ref, b_ref, o_ref):
    y = dot(a_ref[...], b_ref[...], TN).astype(bf16)
    _, _, g, _, r, c = o_ref.shape
    for core in (0, 1):
        z = y[:, core * c:(core + 1) * c].reshape(g, 2, 2, r, c)
        for half in (0, 1):
            o_ref[half, core] = z[:, half]


def wgrad_cols(a, b, groups):
    s, m = a.shape
    n = b.shape[1]
    r, c = m // groups // 4, m // 2
    return pl.pallas_call(
        wgrad_cols_kernel, grid=(n // m,),
        in_specs=[pl.BlockSpec((s, m), lambda i: (0, 0)), pl.BlockSpec((s, m), lambda i: (0, i))],
        out_specs=pl.BlockSpec((2, 2, groups, 2, r, c), lambda i: (i, 0, 0, 0, 0, 0)),
        out_shape=jax.ShapeDtypeStruct((2 * n // m, 2, groups, 2, r, c), bf16),
        cost_estimate=pl.CostEstimate(flops=2 * s * m * n, bytes_accessed=2 * (s * (m + n) + m * n),
                                      transcendentals=0), name="wgrad_cols")(a, b)


def wgrad_rows_kernel(a_ref, b_ref, o_ref):
    y = dot(a_ref[...], b_ref[...], TN).astype(bf16)
    q, _, _, _, r, c = o_ref.shape
    for core in (0, 1):
        o_ref[:, core, 0] = y[:, core * c:(core + 1) * c].reshape(q, 2, r, c)


def wgrad_rows(a, b, groups):
    s, m = a.shape
    n = b.shape[1]
    q, r, c = 2 * m // n, n // groups // 4, n // 2
    return pl.pallas_call(
        wgrad_rows_kernel, grid=(groups,),
        in_specs=[pl.BlockSpec((s, m // groups), lambda i: (0, i)), pl.BlockSpec((s, n), lambda i: (0, 0))],
        out_specs=pl.BlockSpec((q, 2, 1, 2, r, c), lambda i: (0, 0, i, 0, 0, 0)),
        out_shape=jax.ShapeDtypeStruct((q, 2, groups, 2, r, c), bf16),
        cost_estimate=pl.CostEstimate(flops=2 * s * m * n, bytes_accessed=2 * (s * (m + n) + m * n),
                                      transcendentals=0), name="wgrad_rows")(a, b)


def attn_fwd_kernel(shape, count, rows, *refs):
    len_ref, q_ref, k_ref, v_ref = refs[:4]
    ins = refs[4:4 + count]
    o_ref, lse_ref = refs[4 + count:6 + count]
    outs = refs[6 + count:6 + 2 * count]
    step, steps = pl.program_id(0), pl.num_programs(0)
    p = Place(shape)
    g = Gather(p, ins, outs, refs[6 + 2 * count:])
    @pl.when(step == 0)
    def _():
        greet(gather_peers(p, False))
        for w in range(count):
            g.start(w)
    for w, at in ((0, 2), (1, 4)):
        @pl.when(step == at)
        def _(w=w):
            g.after(w, 0)
    attn_fwd_body(len_ref, q_ref, k_ref, v_ref, o_ref, lse_ref, rows)
    @pl.when(step == steps - 1)
    def _():
        for w in range(2, count):
            g.after(w, 0)
        for t in range(1, p.bits):
            for w in range(count):
                g.after(w, t)
        for w in range(count):
            g.finish(w)


def attn_fwd_call(shape, length, qkv, ws, rows=256):
    groups = shape["fsdp"]
    s, d3 = qkv.shape
    d = d3 // 3
    np_ = d // 128
    sd = jax.ShapeDtypeStruct
    res = pl.pallas_call(
        functools.partial(attn_fwd_kernel, shape, len(ws), rows), grid=(np_,),
        in_specs=[pl.BlockSpec(memory_space=pltpu.SMEM), pl.BlockSpec((s, 128), lambda i: (0, i)),
                  pl.BlockSpec((s, 128), lambda i: (0, np_ + i)),
                  pl.BlockSpec((s, 128), lambda i: (0, 2 * np_ + i))] + [ANY] * len(ws),
        out_specs=[pl.BlockSpec((s, 128), lambda i: (0, i)), pl.BlockSpec((s, 128), lambda i: (0, 0))]
        + [ANY] * len(ws),
        out_shape=[sd((s, d), bf16), sd((s, 128), f32)] + [gather_shape(w, groups) for w in ws],
        scratch_shapes=Gather.scratch(len(ws), groups),
        compiler_params=pltpu.CompilerParams(collective_id=2, has_side_effects=True),
        cost_estimate=pl.CostEstimate(flops=8 * s * s * d, bytes_accessed=8 * s * d, transcendentals=s * s * 12),
        name="attn_fwd")(length, qkv, qkv, qkv, *[quarter(w) for w in ws])
    return res[0], res[1], [r.reshape(-1, r.shape[-1]) for r in res[2:]]


def f32_rows_dot(row, weights):
    parts = split3(row)
    stack = jnp.concatenate(list(parts) + [jnp.zeros((5, row.shape[1]), f32)], axis=0).astype(bf16)
    return colsum(dot(stack, weights))


class Small:
    def __init__(self, place, scratch):
        self.p = place
        (self.ag, self.rows, self.ab, self.bs, self.bm, self.bb, self.bg, self.s1, self.r1, self.s2, self.r2) = scratch

    @staticmethod
    def widths(shape, d, ff, n_mod):
        groups = shape["fsdp"]
        part = n_mod // groups
        return -(-(d // groups) // 128) * 128, ff // groups, part if part % 128 == 0 else n_mod

    @staticmethod
    def scratch(shape, d, ff, n_mod):
        groups, lines = shape["fsdp"], shape["dp"]
        wide, fpart, gpart = Small.widths(shape, d, ff, n_mod)
        vm = lambda *dims: pltpu.VMEM(dims, f32)
        sem = pltpu.SemaphoreType.DMA
        return [vm(groups, 1, n_mod), vm(groups, 8, d), vm(groups, 1, ff), vm(lines, 8, wide), vm(lines, groups, 384),
                vm(lines, 1, fpart), vm(lines, groups, gpart), sem((groups, 3)), sem((groups, 3)), sem((lines, 4)),
                sem((lines, 4))]

    def peers(self):
        p = self.p
        return [(p.dp, xor(p.me, m)) for m in range(1, p.groups)] + [(xor(p.dp, m), p.me) for m in range(1, p.lines)]

    def copies(self, stage, m, arrived):
        p = self.p
        if stage == 1:
            bufs, ss, rs = (self.ag, self.rows, self.ab), self.s1, self.r1
            where, slot = (p.dp, xor(p.me, m)), xor(p.me, m) if arrived else p.me
        else:
            bufs, ss, rs = (self.bs, self.bm, self.bb, self.bg), self.s2, self.r2
            where, slot = (xor(p.dp, m), p.me), xor(p.dp, m) if arrived else p.dp
        return [remote(b.at[slot], b.at[slot], ss.at[m, i], rs.at[m, i], where) for i, b in enumerate(bufs)]

    def spread(self, stage):
        for m in range(1, self.p.groups if stage == 1 else self.p.lines):
            for c in self.copies(stage, m, False):
                c.start()

    def collect(self, stage):
        for m in range(1, self.p.groups if stage == 1 else self.p.lines):
            for c in self.copies(stage, m, True):
                c.wait_recv()

    def settle(self):
        for stage in (1, 2):
            for m in range(1, self.p.groups if stage == 1 else self.p.lines):
                for c in self.copies(stage, m, False):
                    c.wait_send()

    def first(self, sums, sb1, sums1, vec_pre, vec_mid, condp, meta, ada):
        me = self.p.me
        d = sums.shape[1]
        ggm, gb2, a2, s2, gga, st0, st1, st2 = (sums[i:i + 1] for i in range(8))
        a1, s1, gemb = (sums1[i:i + 1] for i in range(3))
        gain1, scale_a, gain2, scale_m = vec_pre[1:2], vec_pre[2:3], vec_mid[1:2], vec_mid[2:3]
        gm = jnp.concatenate([s1, a1 * gain1, gga, s2, a2 * gain2, ggm], axis=1)
        sig = 1.0 / (1.0 + jnp.exp(-condp))
        gc = f32_rows_dot(gm, ada) * (sig * (1.0 + condp * (1.0 - sig)))
        lane = lax.broadcasted_iota(jnp.int32, (1, 128), 1)
        total = lambda x: jnp.sum(x, axis=1, keepdims=True)
        stat = jnp.where(lane == 0, total(st0), jnp.where(lane == 1, total(st1), jnp.where(lane == 2, total(st2), meta)))
        tail = jnp.concatenate([gc, condp * sig, stat, jnp.zeros((1, d - 384), f32)], axis=1)
        self.ag[me] = gm
        self.ab[me] = sb1
        self.rows[me] = jnp.concatenate([(1.0 + scale_a) * a1, (1.0 + scale_m) * a2, gb2, gemb, tail,
                                         jnp.zeros((3, d), f32)], axis=0)
        self.spread(1)

    def second(self):
        p = self.p
        self.collect(1)
        d = self.rows.shape[2]
        wide, fpart, gpart = self.bs.shape[2], self.bb.shape[2], self.bg.shape[2]
        total = self.rows[0]
        for f in range(1, p.groups):
            total = total + self.rows[f]
        self.bs[p.dp] = pltpu.roll(total, (d - p.me * (d // p.groups)) % d, 1)[:, :wide]
        self.bm[p.dp] = jnp.concatenate([self.rows[f, 4:5, :384] for f in range(p.groups)], axis=0)
        cut = pl.ds(pl.multiple_of(p.me * fpart, 128), fpart)
        part = self.ab[0, :, cut]
        for f in range(1, p.groups):
            part = part + self.ab[f, :, cut]
        self.bb[p.dp] = part
        n_mod = self.ag.shape[2]
        cut = slice(None) if gpart == n_mod else pl.ds(pl.multiple_of(p.me * gpart, 128), gpart)
        self.bg[p.dp] = jnp.concatenate([self.ag[f, :, cut] for f in range(p.groups)], axis=0)
        self.spread(2)

    def third(self, norms_ref, gb1_ref, gada_ref, gbada_ref, table_ref, rms_ref, d):
        p = self.p
        self.collect(2)
        total, part = self.bs[0], self.bb[0]
        for z in range(1, p.lines):
            total = total + self.bs[z]
            part = part + self.bb[z]
        norms_ref[...] = total
        gb1_ref[...] = part
        mods = jnp.concatenate([self.bg[z] for z in range(p.lines)], axis=0)
        info = jnp.concatenate([self.bm[z] for z in range(p.lines)], axis=0)
        gcs, conds, stat = info[:, :128], info[:, 128:256], info[:, 256:384]
        highest = lax.Precision.HIGHEST
        gada_ref[...] = lax.dot_general(mods, conds, TN, precision=highest, preferred_element_type=f32)
        gbada_ref[...] = colsum(mods)
        ids = stat[:, 4:5].astype(jnp.int32)
        hot = (lax.broadcasted_iota(jnp.int32, (ids.shape[0], table_ref.shape[0]), 1) == ids).astype(f32)
        table_ref[...] = lax.dot_general(hot, gcs, TN, precision=highest, preferred_element_type=f32)
        stat = colsum(stat)
        rms_ref[...] = jnp.sqrt(stat / (stat[:, 3:4] * d))


def small_shapes(shape, d, ff, n_mod, table_rows):
    wide, fpart, gpart = Small.widths(shape, d, ff, n_mod)
    sd = lambda *dims: jax.ShapeDtypeStruct(dims, f32)
    return [sd(8, wide), sd(1, fpart), sd(gpart, 128), sd(1, gpart), sd(table_rows, 128), sd(1, 128)]


def small_results(shape, res, sizes):
    norms, gb1, gada, gbada, table, rms = res
    n_ada = sizes[5]
    if gada.shape[0] != n_ada:
        me = lax.axis_index("fsdp")
        gada = lax.dynamic_slice_in_dim(gada, me * n_ada, n_ada, axis=0)
        gbada = lax.dynamic_slice_in_dim(gbada, me * n_ada, n_ada, axis=1)
    g1, g2, gb2, gemb = (norms[i, :sizes[i]] for i in range(4))
    return g1, g2, gb2, gemb, gb1[0], gada, gbada[0], table, rms[0, :3]


def tail_kernel(shape, counts, rows, post, pairs, *refs):
    n = len(counts)
    (len_ref, q_ref, k_ref, v_ref, o_ref, g_ref, lse_ref, cos_ref, sin_ref, n1_ref, w_ref, tok_ref, flag_ref, gh1_ref,
     vpre_ref, vmid_ref, sums_ref, sb1_ref, condp_ref, meta_ref, ada_ref) = refs[:21]
    srcs = refs[21:20 + n]
    outs = refs[20 + n:21 + 2 * n]
    igrad_ref, reduced, small_out = outs[0], outs[1:1 + n], refs[21 + 2 * n:27 + 2 * n]
    dqs, dks, dvs, dqkv, gq, sums1 = refs[27 + 2 * n:33 + 2 * n]
    rscratch, sscratch = refs[33 + 2 * n:54 + 2 * n], refs[54 + 2 * n:]
    step, steps = pl.program_id(0), 2 * pairs + post
    p = Place(shape)
    r = Reduce(p, counts, ["rows"] + ["cols"] * (n - 2) + ["qkv"], list(srcs) + [gq], reduced, rscratch, 3, 2)
    small = Small(p, sscratch)

    @pl.when(step == 0)
    def _():
        r.greet(small.peers())
        r.begin(0)

    @pl.loop(2 * step, 2 * step + 2)
    def _(t):
        r.tick(t)

    @pl.when(step < 2 * pairs)
    def _():
        pair, head = step // 2, step % 2

        def emit(*parts):
            for i, x in enumerate(parts):
                dqkv[i, pair] = x
            y = dot(n1_ref[...], jnp.concatenate(parts, axis=1)).astype(bf16)
            _, _, g, _, rr, c = gq.shape
            y = y.reshape(g, 2, 2, rr, c)
            for half in (0, 1):
                gq[2 * (pair // 2) + half, pair % 2] = y[:, half]

        attn_bwd_body(len_ref, q_ref, k_ref, v_ref, o_ref, g_ref, lse_ref, cos_ref, sin_ref, dqs, dks, dvs, rows,
                      pair, head, emit)

    @pl.when(step >= 2 * pairs)
    def _():
        i = step - 2 * pairs
        m = tok_ref.shape[0]
        cut = pl.ds(pl.multiple_of(i * m, m), m)
        grads = [jnp.concatenate([dqkv[a, b, cut, :] for b in range(pairs)], axis=1) for a in range(3)]
        masked = flag_ref[...] == 1
        h0 = jnp.where(masked, vpre_ref[0:1, :], tok_ref[...].astype(f32))
        igrad_ref[...], new = post_rows(grads, h0, masked, gh1_ref[...], vpre_ref[1:2, :], vpre_ref[2:3, :], w_ref)
        sums1[...] = jnp.where(i == 0, new, sums1[...] + new)

    @pl.when(step == steps - 1)
    def _():
        small.first(sums_ref[...], sb1_ref[...], sums1[...], vpre_ref[...], vmid_ref[...], condp_ref[...], meta_ref[...],
                    ada_ref[...])
        last = max(r.ticks, 2 * steps)
        marks = [2 * steps, min(2 * steps + SPLIT[0], last), min(2 * steps + SPLIT[1], last), last]
        for n in range(3):
            @pl.loop(marks[n], marks[n + 1])
            def _(t):
                r.tick(t)
            if n == 0:
                small.second()
            if n == 1:
                small.third(*small_out, sums1.shape[1])
        r.drain()
        small.settle()


SPLIT = (3, 8)


def tail_call(shape, length, qkv, att, gatt, lse, cos, sin, n1t, w, tok, flag, gh1, vpre, vmid, sums, sb1, condp, meta,
              ada, grads, table_rows, rows=256):
    groups = shape["fsdp"]
    s, d3 = qkv.shape
    d = d3 // 3
    pairs = d // 128
    r, c = 2 * grads[0].shape[-2], grads[0].shape[-1]
    post = 256 if r % 32 == 0 else 128
    blocks = s // post
    steps = 2 * pairs + blocks
    ff, n_mod = sb1.shape[1], ada.shape[0]
    counts = [g.shape[0] for g in grads] + [pairs]
    pair = lambda i: jnp.minimum(i // 2, pairs - 1)
    blk = lambda i: jnp.maximum(i - 2 * pairs, 0)
    once = pl.Buffered(1)
    col = lambda base: pl.BlockSpec((s, 128), lambda i: (0, base + pair(i)))
    whole = lambda a: pl.BlockSpec(a.shape, lambda i: (0,) * a.ndim, pipeline_mode=once)
    row = lambda cc: pl.BlockSpec((post, cc), lambda i: (blk(i), 0))
    sd = jax.ShapeDtypeStruct
    shard = d // groups
    red = [sd((shard * (g.shape[0] // 2), d), bf16) if i == 0 else sd((shard, d * (g.shape[0] // 2)), bf16)
           for i, g in enumerate(grads)] + [sd((shard, d3), bf16)]
    smalls = small_shapes(shape, d, ff, n_mod, table_rows)
    const = lambda x: pl.BlockSpec(x.shape, lambda i: (0, 0), pipeline_mode=once)
    res = pl.pallas_call(
        functools.partial(tail_kernel, shape, counts, rows, blocks, pairs), grid=(steps,),
        in_specs=[pl.BlockSpec(memory_space=pltpu.SMEM), col(0), col(pairs), col(2 * pairs), col(0), col(0), whole(lse),
                  whole(cos), whole(sin), whole(n1t), whole(w), row(d), row(1), row(d)]
        + [whole(x) for x in (vpre, vmid, sums, sb1, condp, meta, ada)] + [ANY] * len(grads),
        out_specs=[row(d)] + [ANY] * len(red) + [const(x) for x in smalls],
        out_shape=[sd((s, d), bf16)] + red + smalls,
        scratch_shapes=[pltpu.VMEM((128, s), f32), pltpu.VMEM((s, 128), f32), pltpu.VMEM((s, 128), f32),
                        pltpu.VMEM((3, pairs, s, 128), bf16), pltpu.VMEM((pairs, 2, groups, 2, r // 2, c), bf16),
                        pltpu.VMEM((8, d), f32)]
        + Reduce.scratch(sum(counts), groups, r, c) + Small.scratch(shape, d, ff, n_mod),
        compiler_params=pltpu.CompilerParams(collective_id=3, has_side_effects=True, vmem_limit_bytes=65000 * 1024),
        cost_estimate=pl.CostEstimate(flops=30 * s * s * d, bytes_accessed=40 * s * d, transcendentals=s * s * 12),
        name="tail")(length, qkv, qkv, qkv, att, gatt, lse, cos, sin, n1t, w, tok, flag, gh1, vpre, vmid, sums, sb1, condp,
                     meta, ada, *grads)
    return res[0], res[1:1 + len(red)], res[1 + len(red):]
from jax.sharding import PartitionSpec as P

highest = lax.Precision.HIGHEST


def rotary_tables(length):
    half = HD // 2
    rate = 1.0 / 10000.0 ** (jnp.arange(half, dtype=f32) * 2.0 / HD)
    angle = jnp.arange(length, dtype=f32)[:, None] * rate[None, :]
    angle = jnp.concatenate([angle] * (128 // half), axis=-1)
    sign = jnp.where(jnp.arange(128) % HD < half, -1.0, 1.0)
    return jnp.cos(angle), jnp.sin(angle) * sign


def per_device(shape, tokens, hidden_token_indicator, lengths, time_ids, cotangent, gain_one, w_qkv, w_out, gain_two,
               w_fc1, b_fc1, w_fc2, b_fc2, w_ada, b_ada, mask_embed, time_table):
    groups = shape["fsdp"]
    s, d = tokens.shape[1:]
    ff = b_fc1.shape[0] * groups
    tok, cot = tokens[0], cotangent[0]
    flag = hidden_token_indicator.reshape(s, 1)
    sizes = [v.shape[0] for v in (gain_one, gain_two, b_fc2, mask_embed, b_fc1, b_ada)]
    small = jnp.concatenate([v[None].astype(f32) for v in (gain_one, gain_two, b_fc2, mask_embed, b_fc1, b_ada)], axis=1)
    (ada_all, qkv_all), packed = head_call(shape, small, [w_ada, w_qkv])
    packed = packed[:, 0]
    cuts = [sum(sizes[:i]) for i in range(len(sizes) + 1)]
    gain1, gain2, b2, emb, b1, bada = (
        packed[:, cuts[i]:cuts[i + 1]].reshape(1, -1) for i in range(len(sizes)))
    cond_pre = lax.dynamic_slice_in_dim(time_table, time_ids[0], 1, axis=0)
    cond = jax.nn.silu(cond_pre)
    modulation = jnp.dot(cond, ada_all.astype(f32).T, precision=highest) + bada
    shift_a, scale_a, gate_a, shift_m, scale_m, gate_m = (modulation[:, i * d:(i + 1) * d] for i in range(6))
    cos, sin = rotary_tables(s)
    zero = jnp.zeros((1, d), f32)
    vec_pre = jnp.concatenate([emb, gain1, scale_a, shift_a] + [zero] * 4, axis=0)
    vec_mid = jnp.concatenate([emb, gain2, scale_m, shift_m, gate_a, gate_m, b2, zero], axis=0)
    n1, qkv = pre_call(tok, flag, vec_pre, qkv_all, cos, sin)
    att, lse, (out_all, fc1_all, fc2_all) = attn_fwd_call(shape, lengths, qkv, [w_out, w_fc1, w_fc2])
    out, gh1, gatt, n2, act, gm, gpre, gap, sums, gb1 = mid_call(
        lengths, att, tok, flag, cot, vec_mid, b1, out_all, fc1_all, fc2_all)
    g_fc2 = wgrad_rows(act, gm, groups)
    g_fc1 = wgrad_cols(n2, gpre, groups)
    g_out = wgrad_cols(att, gap, groups)
    meta = jnp.concatenate([jnp.zeros((3,), f32), lengths.astype(f32), time_ids.astype(f32), jnp.zeros((123,), f32)])[None]
    igrad, (r_fc2, r_fc1, r_out, r_qkv), smalls = tail_call(
        shape, lengths, qkv, att, gatt, lse, cos, sin, n1, qkv_all, tok, flag, gh1, vec_pre, vec_mid, sums, gb1, cond_pre,
        meta, ada_all, [g_fc2, g_fc1, g_out], time_table.shape[0])
    g1, g2, gb2, gemb, gb1, g_ada, gbada, table, rms = small_results(shape, smalls, sizes)
    return (out[None], igrad[None], g1, r_qkv.astype(f32), r_out.astype(f32), g2, r_fc1.astype(f32), gb1,
            r_fc2.astype(f32), gb2,
            g_ada, gbada, gemb, table, rms)


def solution(mesh):
    both = ("dp", "fsdp")
    f1, f2 = P("fsdp"), P("fsdp", None)
    placed = (P(both, None, None), P(both, None), P(both), P(both), P(both, None, None), f1, f2, f2, f1, f2, f1, f2, f1,
              f2, f1, f1, P())
    outs = (P(both, None, None), P(both, None, None), f1, f2, f2, f1, f2, f1, f2, f1, f2, f1, f1, P(), P())
    return jax.shard_map(functools.partial(per_device, dict(mesh.shape)), mesh=mesh, in_specs=placed, out_specs=outs,
                         check_vma=False)
```

```python
import functools, math
import jax, jax.numpy as jnp
from jax import lax
from jax.experimental import pallas as pl
from jax.experimental.pallas import tpu as pltpu

HD = 64
EPS = 1e-5
LOG2E = math.log2(math.e)
QSCALE = LOG2E * HD ** -0.5
f32, bf16 = jnp.float32, jnp.bfloat16
NT = (((1,), (1,)), ((), ()))
NN = (((1,), (0,)), ((), ()))
TN = (((0,), (0,)), ((), ()))

def dot(a, b, dims=NN):
    return lax.dot_general(a, b, dims, preferred_element_type=f32)

def norm_parts(x):
    mean = jnp.mean(x, axis=-1, keepdims=True)
    cen = x - mean
    rs = lax.rsqrt(jnp.mean(cen * cen, axis=-1, keepdims=True) + EPS)
    return cen * rs, rs

def swap_halves(u):
    lane = lax.broadcasted_iota(jnp.int32, u.shape, 1)
    return jnp.where(lane % HD < HD // 2, pltpu.roll(u, 96, 1), pltpu.roll(u, 32, 1))

def attn_fwd_body(len_ref, q_ref, k_ref, v_ref, o_ref, lse_ref, rows, p):
    s = q_ref.shape[0]
    length = len_ref[0]
    lane = lax.broadcasted_iota(jnp.int32, (s, 128), 1)
    pos = lax.broadcasted_iota(jnp.int32, (s, 128), 0)
    lane_q = lax.broadcasted_iota(jnp.int32, (rows, 128), 1)
    k = k_ref[...].astype(f32)
    v = v_ref[...].astype(f32)
    kx, vx = [], []
    for h in (0, 1):
        extra = HD * (1 - h)
        mine = (lane >= HD) if h else (lane < HD)
        bias = jnp.where(pos >= length, -1e30, 0.0)
        kx.append(jnp.where(mine, k, jnp.where(lane == extra, bias, 0.0)).astype(bf16))
        vx.append(jnp.where(mine, v, jnp.where(lane == extra, 1.0, 0.0)).astype(bf16))
    for b in range(s // rows):
        q = q_ref[b * rows:(b + 1) * rows, :].astype(f32)
        outs, lses = [], []
        for h in (0, 1):
            extra = HD * (1 - h)
            mine = (lane_q >= HD) if h else (lane_q < HD)
            qx = jnp.where(mine, q, jnp.where(lane_q == extra, 1.0, 0.0)).astype(bf16)
            sc = dot(qx, kx[h], NT)
            m = jnp.max(sc, axis=1, keepdims=True)
            pr = jnp.exp2(sc - m).astype(bf16)
            o = dot(pr, vx[h])
            tot = o[:, extra:extra + 1]
            outs.append(o * (1.0 / tot))
            lses.append(m + jnp.log(tot) * LOG2E)
        o_ref[b * rows:(b + 1) * rows, :] = jnp.where(lane_q < HD, outs[0], outs[1]).astype(bf16)
        old = jnp.where(p == 0, 0.0, lse_ref[b * rows:(b + 1) * rows, :])
        lse_ref[b * rows:(b + 1) * rows, :] = jnp.where(
            lane_q == 2 * p, lses[0], jnp.where(lane_q == 2 * p + 1, lses[1], old))

def split3(x):
    hi = x.astype(bf16).astype(f32)
    r = x - hi
    mid = r.astype(bf16).astype(f32)
    return hi, mid, r - mid

def attn_bwd_body(len_ref, q_ref, k_ref, v_ref, o_ref, g_ref, lse_ref, cos_ref, sin_ref,
                  dqs, dks, dvs, rows, p, h, emit):
    s = q_ref.shape[0]
    length = len_ref[0]
    lane = lax.broadcasted_iota(jnp.int32, (s, 128), 1)
    pos = lax.broadcasted_iota(jnp.int32, (s, 128), 0)
    lane_q = lax.broadcasted_iota(jnp.int32, (rows, 128), 1)
    e = HD * (1 - h)
    mine, mine_q = lane // HD == h, lane_q // HD == h
    k = k_ref[...].astype(f32)
    v = v_ref[...].astype(f32)
    ones = jnp.where((lane >= e) & (lane < e + 3), 1.0, 0.0)
    bias = jnp.where(pos >= length, -1e30, 0.0)
    kx = jnp.where(mine, k, jnp.where(lane == e + 3, bias, ones)).astype(bf16)
    vx = jnp.where(mine, v, ones).astype(bf16)
    kt = jnp.where(mine, k, 0.0).T.astype(bf16)
    dk = jnp.zeros((s, 128), f32)
    dv = jnp.zeros((s, 128), f32)
    for b in range(s // rows):
        sl = slice(b * rows, (b + 1) * rows)
        qb = q_ref[sl, :]
        gb = g_ref[sl, :]
        q = qb.astype(f32)
        g = gb.astype(f32)
        lse = jnp.sum(jnp.where(lane_q == 2 * p + h, lse_ref[sl, :], 0.0), axis=1, keepdims=True)
        dd = jnp.sum(jnp.where(mine_q, g * o_ref[sl, :].astype(f32), 0.0), axis=1, keepdims=True)
        l0, l1, l2 = split3(-lse)
        d0, d1, d2 = split3(-dd)
        qx = jnp.where(mine_q, q, jnp.where(lane_q == e, l0, jnp.where(lane_q == e + 1, l1, jnp.where(
            lane_q == e + 2, l2, jnp.where(lane_q == e + 3, 1.0, 0.0))))).astype(bf16)
        gx = jnp.where(mine_q, g, jnp.where(lane_q == e, d0, jnp.where(lane_q == e + 1, d1, jnp.where(
            lane_q == e + 2, d2, 0.0)))).astype(bf16)
        pt = jnp.exp2(dot(kx, qx, NT))
        dst = (pt * dot(vx, gx, NT)).astype(bf16)
        dv = dv + dot(pt.astype(bf16), gb)
        dk = dk + dot(dst, qb)
        dqt = dot(kt, dst)
        dqs[:, sl] = jnp.where(h == 0, dqt, dqs[:, sl] + dqt)
    @pl.when(h == 0)
    def _():
        dks[...] = dk
        dvs[...] = dv
    @pl.when(h == 1)
    def _():
        cos, sin = cos_ref[...], sin_ref[...]
        dq = dqs[...].T * (HD ** -0.5)
        dkk = jnp.where(lane < HD, dks[...], dk) * (1.0 / LOG2E)
        emit((dq * cos - swap_halves(dq) * sin).astype(bf16), (dkk * cos - swap_halves(dkk) * sin).astype(bf16),
             jnp.where(lane < HD, dvs[...], dv).astype(bf16))


def gelu_both(v):
    a, b = 0.7978845608028654, 0.044715
    v2 = v * v
    t = jnp.tanh(a * v * (1.0 + b * v2))
    half = 0.5 + 0.5 * t
    return v * half, half + (0.5 * a) * v * (1.0 - t * t) * (1.0 + 3.0 * b * v2)

def colsum(x):
    return jnp.sum(x, axis=0, keepdims=True)

def mid_kernel(len_ref, att_ref, tok_ref, flag_ref, cot_ref, vec_ref, b1_ref, wo_ref, w1_ref, w2_ref,
               out_ref, gh1_ref, gatt_ref, n2_ref, act_ref, gm_ref, gpre_ref, gap_ref, sum_ref, sb1_ref,
               gp_s, *, cut):
    i = pl.program_id(0)
    rows, d = att_ref.shape
    ff = w1_ref.shape[1]
    emb, gain, scale, shift, gate_a, gate_m, b2 = (vec_ref[r:r + 1, :] for r in range(7))
    h0 = jnp.where(flag_ref[...] == 1, emb, tok_ref[...].astype(f32))
    ap = dot(att_ref[...], wo_ref[...])
    br_a = gate_a * ap
    h1 = h0 + br_a
    n, rs = norm_parts(h1)
    n2 = (n * gain * (1.0 + scale) + shift).astype(bf16)
    n2_ref[...] = n2
    mp = jnp.zeros((rows, d), f32) + b2
    for j in range(ff // cut):
        sl = slice(j * cut, (j + 1) * cut)
        act, gp = gelu_both(dot(n2, w1_ref[:, sl]) + b1_ref[:, sl])
        act = act.astype(bf16)
        act_ref[:, sl] = act
        gp_s[:, sl] = gp
        mp = mp + dot(act, w2_ref[sl, :])
    br_m = gate_m * mp
    bo = h1 + br_m
    out_ref[...] = bo.astype(bf16)
    pos = lax.broadcasted_iota(jnp.int32, (rows, 1), 0) + i * rows
    valid = jnp.where(pos < len_ref[0], 1.0, 0.0)
    cot = cot_ref[...].astype(f32)
    gm = (gate_m * cot).astype(bf16)
    gm_ref[...] = gm
    gn2 = jnp.zeros((rows, d), f32)
    sb1 = []
    for j in range(ff // cut):
        sl = slice(j * cut, (j + 1) * cut)
        gpre = (dot(gm, w2_ref[sl, :], NT) * gp_s[:, sl]).astype(bf16)
        gpre_ref[:, sl] = gpre
        sb1.append(colsum(gpre.astype(f32)))
        gn2 = gn2 + dot(gpre, w1_ref[:, sl], NT)
    e = gn2 * (gain * (1.0 + scale))
    gh1 = cot + rs * (e - jnp.mean(e, axis=1, keepdims=True) - n * jnp.mean(e * n, axis=1, keepdims=True))
    gh1_ref[...] = gh1
    gap = (gate_a * gh1).astype(bf16)
    gap_ref[...] = gap
    gatt_ref[...] = dot(gap, wo_ref[...], NT).astype(bf16)
    new = jnp.concatenate([
        colsum(cot * mp), colsum(gm.astype(f32)), colsum(gn2 * n), colsum(gn2), colsum(gh1 * ap),
        colsum(valid * bo * bo), colsum(valid * br_a * br_a), colsum(valid * br_m * br_m)], axis=0)
    sb1 = jnp.concatenate(sb1, axis=1)
    @pl.when(i == 0)
    def _():
        sum_ref[...] = new
        sb1_ref[...] = sb1
    @pl.when(i > 0)
    def _():
        sum_ref[...] += new
        sb1_ref[...] += sb1

def mid_call(length, att, tok, flag, cot, vec, b1, wo, w1, w2, rows=256, cut=768):
    s, d = tok.shape
    ff = w1.shape[1]
    row = lambda c: pl.BlockSpec((rows, c), lambda i: (i, 0))
    whole = lambda a: pl.BlockSpec(a.shape, lambda i: (0, 0))
    sd = jax.ShapeDtypeStruct
    return pl.pallas_call(
        functools.partial(mid_kernel, cut=cut), grid=(s // rows,),
        in_specs=[pl.BlockSpec(memory_space=pltpu.SMEM), row(d), row(d), row(1), row(d), whole(vec), whole(b1),
                  whole(wo), whole(w1), whole(w2)],
        out_specs=[row(d), row(d), row(d), row(d), row(ff), row(d), row(ff), row(d),
                   pl.BlockSpec((8, d), lambda i: (0, 0)), pl.BlockSpec((1, ff), lambda i: (0, 0))],
        out_shape=[sd((s, d), bf16), sd((s, d), f32), sd((s, d), bf16), sd((s, d), bf16), sd((s, ff), bf16),
                   sd((s, d), bf16), sd((s, ff), bf16), sd((s, d), bf16), sd((8, d), f32), sd((1, ff), f32)],
        scratch_shapes=[pltpu.VMEM((rows, ff), f32)],
        compiler_params=pltpu.CompilerParams(vmem_limit_bytes=60000 * 1024),
        cost_estimate=pl.CostEstimate(flops=2 * s * d * (2 * d + 4 * ff), bytes_accessed=30 * s * d,
                                      transcendentals=s * ff),
        name="mid")(length, att, tok, flag, cot, vec, b1, wo, w1, w2)

def post_rows(grads, h0, masked, gh1, gain, scale, w_ref):
    d = h0.shape[1]
    n, rs = norm_parts(h0)
    gn1 = sum(dot(g, w_ref[:, i * d:(i + 1) * d], NT) for i, g in enumerate(grads))
    e = gn1 * (gain * (1.0 + scale))
    gh0 = gh1 + rs * (e - jnp.mean(e, axis=1, keepdims=True) - n * jnp.mean(e * n, axis=1, keepdims=True))
    sums = jnp.concatenate([colsum(gn1 * n), colsum(gn1), colsum(jnp.where(masked, gh0, 0.0)),
                            jnp.zeros((5, d), f32)], axis=0)
    return jnp.where(masked, 0.0, gh0).astype(bf16), sums

MESH = pl.DeviceIdType.MESH


def flip(i, b):
    return i + 2 ** b * (1 - 2 * ((i // 2 ** b) % 2))


def xor(i, mask):
    b = 0
    while mask >> b:
        if (mask >> b) & 1:
            i = flip(i, b)
        b += 1
    return i


def subsets(bits):
    masks = [0]
    for b in bits:
        masks = masks + [m | (1 << b) for m in masks]
    return masks


def log2(n):
    return n.bit_length() - 1


class Place:
    def __init__(self, shape):
        self.groups, self.lines = shape["fsdp"], shape["dp"]
        self.bits = log2(self.groups)
        self.orders = [list(range(self.bits)), list(range(self.bits))[::-1]]
        self.me = lax.axis_index("fsdp")
        self.dp = lax.axis_index("dp")
        self.core = self.dp % 2
        self.partner = flip(self.dp, 0)


def remote(src, dst, ssem, rsem, where):
    return pltpu.make_async_remote_copy(src_ref=src, dst_ref=dst, send_sem=ssem, recv_sem=rsem, device_id=where,
                                        device_id_type=MESH)


class Gather:
    def __init__(self, place, ins, outs, sems):
        self.p, self.ins, self.outs = place, ins, outs
        self.ss, self.rs, self.fs, self.fr, self.os, self.orr = sems

    @staticmethod
    def scratch(count, groups):
        a = pltpu.SemaphoreType.DMA((count, 2, groups - 1))
        b = pltpu.SemaphoreType.DMA((count,))
        return [a, a, a, a, b, b]

    def send(self, w, color, t, mask):
        p = self.p
        order = p.orders[color]
        e = 2 ** t - 1 + subsets(order[:t]).index(mask)
        piece = p.core * 2 + color
        blk = xor(p.me, mask)
        src = self.ins[w].at[piece] if mask == 0 else self.outs[w].at[blk, piece]
        return remote(src, self.outs[w].at[blk, piece], self.ss.at[w, color, e], self.rs.at[w, color, e],
                      (p.dp, flip(p.me, order[t])))

    def arrival(self, w, color, t, mask):
        p = self.p
        order = p.orders[color]
        e = 2 ** t - 1 + subsets(order[:t]).index(mask)
        got = self.outs[w].at[xor(p.me, mask | (1 << order[t])), p.core * 2 + color]
        return e, got

    def landed(self, w, color, e, got):
        return remote(got, got, self.ss.at[w, color, e], self.rs.at[w, color, e], (self.p.partner, self.p.me))

    def forward(self, w, color, e, got):
        return remote(got, got, self.fs.at[w, color, e], self.fr.at[w, color, e], (self.p.partner, self.p.me))

    def own(self, w):
        p = self.p
        return remote(self.ins[w], self.outs[w].at[p.me], self.os.at[w], self.orr.at[w], (p.partner, p.me))

    def start(self, w):
        for t in range(self.p.bits):
            for color in (0, 1):
                self.send(w, color, t, 0).start()
        self.own(w).start()

    def after(self, w, t):
        for color in (0, 1):
            order = self.p.orders[color]
            for mask in subsets(order[:t]):
                e, got = self.arrival(w, color, t, mask)
                self.landed(w, color, e, got).wait_recv()
                for later in range(t + 1, self.p.bits):
                    self.send(w, color, later, mask | (1 << order[t])).start()
                self.forward(w, color, e, got).start()

    def finish(self, w):
        p = self.p
        for color in (0, 1):
            order = p.orders[color]
            for t in range(p.bits):
                for mask in subsets(order[:t]):
                    e, got = self.arrival(w, color, t, mask)
                    other = self.outs[w].at[xor(p.me, mask | (1 << order[t])), (1 - p.core) * 2 + color]
                    self.forward(w, color, e, other).wait_recv()
                    self.forward(w, color, e, got).wait_send()
                    self.send(w, color, t, mask).wait_send()
        self.own(w).wait()


class Direct:
    def __init__(self, place, src, out, sems):
        self.p, self.src, self.out = place, src, out
        self.ss, self.rs = sems

    @staticmethod
    def scratch(groups):
        return [pltpu.SemaphoreType.DMA((groups,))] * 2

    def copy(self, m, arrived):
        p = self.p
        where = (p.partner, p.me) if m == 0 else (p.dp, xor(p.me, m))
        slot = xor(p.me, m) if arrived else p.me
        return remote(self.src, self.out.at[slot], self.ss.at[m], self.rs.at[m], where)

    def start(self):
        for m in range(self.p.groups):
            self.copy(m, False).start()

    def finish(self):
        for m in range(self.p.groups):
            self.copy(m, True).wait_recv()
            self.copy(m, False).wait_send()


def greet(devices):
    barrier = pltpu.get_barrier_semaphore()
    for where in devices:
        pl.semaphore_signal(barrier, inc=1, device_id=where, device_id_type=MESH)
    pl.semaphore_wait(barrier, len(devices))


def gather_peers(p, everyone):
    masks = range(1, p.groups) if everyone else [1 << b for b in range(p.bits)]
    return [(p.partner, p.me)] + [(p.dp, xor(p.me, m)) for m in masks]


def quarter(w):
    return w.reshape(4, w.shape[0] // 4, w.shape[1])


def gather_shape(w, groups):
    return jax.ShapeDtypeStruct((groups, 4, w.shape[0] // 4, w.shape[1]), w.dtype)


ANY = pl.BlockSpec(memory_space=pl.ANY)


class Reduce:
    def __init__(self, place, counts, kinds, srcs, outs, scratch, lag, gap):
        self.p, self.counts, self.kinds, self.srcs, self.outs = place, counts, kinds, srcs, outs
        (self.own, self.cb, self.xb, self.zb, self.mb, self.u2, self.fin,
         self.load, self.cs, self.cr, self.xs, self.xr, self.zs, self.zr, self.ms, self.mr, self.fs, self.fr,
         self.ps, self.pr, self.st) = scratch
        p = place
        self.total = sum(counts)
        self.n = p.lines // 2
        self.zi = p.dp // 2
        left = self.zi // (self.n // 2)
        self.e = self.zi * (1 - left) + (self.n - 1 - self.zi) * left
        step = 2 * (1 - 2 * left)
        self.inner = (p.dp + step, p.me)
        self.outer = (p.dp - step, p.me)
        self.last = self.n // 2 - 1
        self.stages = ([self.begin, self.core_add] + [functools.partial(self.group_add, t) for t in range(p.bits)]
                       + [functools.partial(self.climb, j) for j in range(1, self.last + 1)] + [self.middle]
                       + [functools.partial(self.descend, j) for j in range(self.last - 1, -1, -1)])
        self.lags = [0, 1] + [1 + lag * (i + 1) for i in range(len(self.stages) - 2)]
        self.early = self.total - counts[-1]
        self.gap = gap
        self.ticks = self.total + gap + self.lags[-1]

    @staticmethod
    def scratch(total, groups, rows, cols):
        sem = pltpu.SemaphoreType.DMA
        vm = lambda *lead: pltpu.VMEM((total,) + lead + (rows // 2, cols), bf16)
        one = sem((total,))
        line = pltpu.VMEM((total, rows, cols), bf16)
        return [vm(groups, 2), vm(groups, 2), vm(2, groups - 1), line, line, line, line,
                one, one, one, sem((total, 2, groups - 1)), sem((total, 2, groups - 1)),
                one, one, one, one, one, one, sem((total, 3)), sem((total, 3)), sem((total, 3))]

    def greet(self, peers):
        p = self.p
        barrier = pltpu.get_barrier_semaphore()
        for where in peers:
            pl.semaphore_signal(barrier, inc=1, device_id=where, device_id_type=MESH)
        pl.semaphore_wait(barrier, len(peers))

    def source(self, k, fn):
        base = 0
        for i, count in enumerate(self.counts):
            @pl.when((k >= base) & (k < base + count))
            def _(i=i, base=base):
                fn(i, k - base)
            base += count

    def targets(self, k, i, j, core):
        rows, cols = self.fin.shape[1:]
        out, fin = self.outs[i], self.fin.at[k]
        if self.kinds[i] == "rows":
            cut = pl.ds(pl.multiple_of(core * cols, cols), cols)
            return [(fin, out.at[pl.ds(pl.multiple_of(j * rows, rows), rows), cut])]
        down = pl.ds(pl.multiple_of((j % 2) * rows, rows), rows)
        if self.kinds[i] == "cols":
            return [(fin, out.at[down, pl.ds(pl.multiple_of((2 * (j // 2) + core) * cols, cols), cols)])]
        width = out.shape[1] // 3
        pair = 2 * (j // 2) + core
        return [(fin.at[:, part * 128:(part + 1) * 128],
                 out.at[down, pl.ds(pl.multiple_of(part * width + pair * 128, 128), 128)]) for part in range(3)]

    def load_copy(self, k, src):
        return pltpu.make_async_copy(src.at[self.p.core], self.own.at[k], self.load.at[k])

    def core_copy(self, k, src):
        p = self.p
        return remote(src.at[1 - p.core], self.cb.at[k], self.cs.at[k], self.cr.at[k], (p.partner, p.me))

    def begin(self, k):
        def go(i, j):
            self.core_copy(k, self.srcs[i].at[j]).start()
            self.load_copy(k, self.srcs[i].at[j]).start()
        self.source(k, go)

    def slot(self, order, t, mask):
        base = sum(self.p.groups >> (u + 1) for u in range(t))
        return base + subsets(order[t + 1:]).index(mask)

    def group_copy(self, k, color, t, mask):
        p = self.p
        order = p.orders[color]
        i = self.slot(order, t, mask)
        return remote(self.own.at[k, xor(p.me, (1 << order[t]) | mask), color], self.xb.at[k, color, i],
                      self.xs.at[k, color, i], self.xr.at[k, color, i], (p.dp, flip(p.me, order[t])))

    def group_send(self, k, t):
        for color in (0, 1):
            for mask in subsets(self.p.orders[color][t + 1:]):
                self.group_copy(k, color, t, mask).start()

    def core_add(self, k):
        self.load_copy(k, self.srcs[0].at[0]).wait()
        self.core_copy(k, self.srcs[0].at[0]).wait_recv()
        for f in range(self.p.groups):
            for color in (0, 1):
                self.own[k, f, color] = (self.own[k, f, color].astype(f32) + self.cb[k, f, color].astype(f32)).astype(bf16)
        self.group_send(k, 0)

    def group_add(self, t, k):
        p = self.p
        for color in (0, 1):
            order = p.orders[color]
            for mask in subsets(order[t + 1:]):
                self.group_copy(k, color, t, mask).wait_recv()
                blk, i = xor(p.me, mask), self.slot(order, t, mask)
                total = self.own[k, blk, color].astype(f32) + self.xb[k, color, i].astype(f32)
                if t == p.bits - 1:
                    self.u2[k, self.part(color)] = total.astype(bf16)
                else:
                    self.own[k, blk, color] = total.astype(bf16)
        if t < p.bits - 1:
            self.group_send(k, t + 1)
        else:
            @pl.when(self.e == 0)
            def _():
                (self.climb_copy(k) if self.last > 0 else self.middle_copy(k)).start()

    def part(self, color):
        half = self.u2.shape[1] // 2
        return slice(color * half, (color + 1) * half)

    def climb_copy(self, k):
        return remote(self.u2.at[k], self.zb.at[k], self.zs.at[k], self.zr.at[k], self.inner)

    def middle_copy(self, k):
        return remote(self.u2.at[k], self.mb.at[k], self.ms.at[k], self.mr.at[k], self.inner)

    def climb(self, j, k):
        @pl.when(self.e == j)
        def _():
            self.climb_copy(k).wait_recv()
            for color in (0, 1):
                total = self.u2[k, self.part(color)].astype(f32) + self.zb[k, self.part(color)].astype(f32)
                self.u2[k, self.part(color)] = total.astype(bf16)
            (self.middle_copy(k) if j == self.last else self.climb_copy(k)).start()

    def share_copy(self, k):
        return remote(self.fin.at[k], self.fin.at[k], self.fs.at[k], self.fr.at[k], self.outer)

    def share_wait(self, k):
        return remote(self.fin.at[k], self.fin.at[k], self.fs.at[k], self.fr.at[k], self.inner)

    def out_copies(self, k, i, j):
        p = self.p
        mine, other = self.targets(k, i, j, p.core), self.targets(k, i, j, 1 - p.core)
        sent = [remote(s, d, self.ps.at[k, n], self.pr.at[k, n], (p.partner, p.me)) for n, (s, d) in enumerate(mine)]
        kept = [pltpu.make_async_copy(s, d, self.st.at[k, n]) for n, (s, d) in enumerate(mine)]
        return sent, kept, other

    def done(self, k):
        def go(i, j):
            sent, kept, _ = self.out_copies(k, i, j)
            for c in sent + kept:
                c.start()
        self.source(k, go)

    def retire(self, k):
        p = self.p
        def go(i, j):
            sent, kept, other = self.out_copies(k, i, j)
            for n, c in enumerate(sent):
                c.wait_send()
                s, d = other[n]
                remote(s, d, self.ps.at[k, n], self.pr.at[k, n], (p.partner, p.me)).wait_recv()
            for c in kept:
                c.wait()
        self.source(k, go)

    def middle(self, k):
        @pl.when(self.e == self.last)
        def _():
            self.middle_copy(k).wait_recv()
            for color in (0, 1):
                total = self.u2[k, self.part(color)].astype(f32) + self.mb[k, self.part(color)].astype(f32)
                self.fin[k, self.part(color)] = total.astype(bf16)
            if self.last > 0:
                self.share_copy(k).start()
            self.done(k)

    def descend(self, j, k):
        @pl.when(self.e == j)
        def _():
            self.share_wait(k).wait_recv()
            if j > 0:
                self.share_copy(k).start()
            self.done(k)

    def tick(self, t):
        for s in range(len(self.stages) - 1, 0, -1):
            k = t - self.lags[s]
            @pl.when((k >= 0) & (k < self.total + self.gap) & ((k < self.total - self.gap) | (k >= self.total)))
            def _(s=s, k=k):
                self.stages[s](k - self.gap * (k // self.total))
        @pl.when(t + 1 < self.early)
        def _():
            self.begin(t + 1)
        @pl.when((t >= self.early) & (t < self.total + self.gap) & ((t < self.total - self.gap) | (t >= self.total)))
        def _():
            self.begin(t - self.gap * (t // self.total))

    def drain(self):
        p = self.p
        @pl.loop(0, self.total)
        def _(k):
            self.core_copy(k, self.srcs[0].at[0]).wait_send()
            for color in (0, 1):
                for t in range(p.bits):
                    for mask in subsets(p.orders[color][t + 1:]):
                        self.group_copy(k, color, t, mask).wait_send()
            @pl.when(self.e == self.last)
            def _():
                self.middle_copy(k).wait_send()
            @pl.when(self.e < self.last)
            def _():
                self.climb_copy(k).wait_send()
            @pl.when(self.e > 0)
            def _():
                self.share_copy(k).wait_send()
            self.retire(k)


def wgrad_cols_kernel(a_ref, b_ref, o_ref):
    y = dot(a_ref[...], b_ref[...], TN).astype(bf16)
    _, _, g, _, r, c = o_ref.shape
    for core in (0, 1):
        z = y[:, core * c:(core + 1) * c].reshape(g, 2, 2, r, c)
        for half in (0, 1):
            o_ref[half, core] = z[:, half]


def wgrad_cols(a, b, groups):
    s, m = a.shape
    n = b.shape[1]
    r, c = m // groups // 4, m // 2
    return pl.pallas_call(
        wgrad_cols_kernel, grid=(n // m,),
        in_specs=[pl.BlockSpec((s, m), lambda i: (0, 0)), pl.BlockSpec((s, m), lambda i: (0, i))],
        out_specs=pl.BlockSpec((2, 2, groups, 2, r, c), lambda i: (i, 0, 0, 0, 0, 0)),
        out_shape=jax.ShapeDtypeStruct((2 * n // m, 2, groups, 2, r, c), bf16),
        cost_estimate=pl.CostEstimate(flops=2 * s * m * n, bytes_accessed=2 * (s * (m + n) + m * n),
                                      transcendentals=0), name="wgrad_cols")(a, b)


def wgrad_rows_kernel(a_ref, b_ref, o_ref):
    y = dot(a_ref[...], b_ref[...], TN).astype(bf16)
    q, _, _, _, r, c = o_ref.shape
    for core in (0, 1):
        o_ref[:, core, 0] = y[:, core * c:(core + 1) * c].reshape(q, 2, r, c)


def wgrad_rows(a, b, groups):
    s, m = a.shape
    n = b.shape[1]
    q, r, c = 2 * m // n, n // groups // 4, n // 2
    return pl.pallas_call(
        wgrad_rows_kernel, grid=(groups,),
        in_specs=[pl.BlockSpec((s, m // groups), lambda i: (0, i)), pl.BlockSpec((s, n), lambda i: (0, 0))],
        out_specs=pl.BlockSpec((q, 2, 1, 2, r, c), lambda i: (0, 0, i, 0, 0, 0)),
        out_shape=jax.ShapeDtypeStruct((q, 2, groups, 2, r, c), bf16),
        cost_estimate=pl.CostEstimate(flops=2 * s * m * n, bytes_accessed=2 * (s * (m + n) + m * n),
                                      transcendentals=0), name="wgrad_rows")(a, b)


def pad128(n):
    return -(-n // 128) * 128


def small_row(vectors):
    wide = [jnp.pad(v.astype(f32), (0, pad128(v.shape[0]) - v.shape[0])) for v in vectors]
    return jnp.concatenate([v[None] for v in wide], axis=1)


def unpack(ref, sizes, groups):
    out, base = [], 0
    for size in sizes:
        wide, full = pad128(size), size * groups
        total = None
        for f in range(groups):
            x = ref[f, :, base:base + wide]
            if full > wide:
                x = jnp.concatenate([x, jnp.zeros((1, full - wide), f32)], axis=1)
            if f > 0:
                x = pltpu.roll(jnp.broadcast_to(x, (8, full)), f * size, 1)[0:1]
            total = x if total is None else total + x
        out.append(total)
        base += wide
    return out


def flat(ref, lo, hi):
    groups, _, rows, _ = ref.shape
    if rows % 16 == 0:
        return ref[:, :, :, lo:hi].reshape(groups * 4 * rows, hi - lo)
    parts = [jnp.concatenate([ref[f, i, :, lo:hi].astype(f32) for i in range(4)], axis=0).astype(bf16) for f in range(groups)]
    return jnp.concatenate(parts, axis=0)


def front_kernel(shape, sizes, rows, *refs):
    len_ref, tok_ref, flag_ref, cos_ref, sin_ref, condp_ref, small_ref = refs[:7]
    ins = refs[7:12]
    att_ref, lse_ref, vpre_ref, vmid_ref, b1_ref, n1t_hbm, qkv_hbm = refs[12:19]
    outs = refs[19:24]
    n1, n1t, qkv, wq, ada, smalls, loads, stores = refs[24:32]
    gsems, dsems = refs[32:38], refs[38:40]
    step, steps = pl.program_id(0), pl.num_programs(0)
    s, d = tok_ref.shape
    p = Place(shape)
    g = Gather(p, ins, outs, gsems)
    direct = Direct(p, small_ref, smalls, dsems)
    save = [pltpu.make_async_copy(n1t, n1t_hbm, stores.at[0]), pltpu.make_async_copy(qkv, qkv_hbm, stores.at[1])]

    @pl.when(step == 0)
    def _():
        greet(gather_peers(p, True))
        direct.start()
        g.start(0)
        g.start(1)
        g.after(0, 0)
        g.after(1, 0)
        for w in (2, 3, 4):
            g.start(w)
        for t in range(1, p.bits):
            g.after(0, t)
        g.finish(0)
        direct.finish()
        fetch = pltpu.make_async_copy(outs[0], ada, loads.at[0])
        fetch.start()
        gain1, gain2, b2, emb, b1, bada = unpack(smalls, sizes, p.groups)
        fetch.wait()
        condp = condp_ref[...]
        cond = condp / (1.0 + jnp.exp(-condp))
        stack = jnp.concatenate(list(split3(cond)) + [jnp.zeros((5, cond.shape[1]), f32)], axis=0).astype(bf16)
        mod = colsum(dot(stack, flat(ada, 0, 128), NT)) + bada
        shift_a, scale_a, gate_a, shift_m, scale_m, gate_m = (mod[:, i * d:(i + 1) * d] for i in range(6))
        vpre_ref[...] = jnp.concatenate([emb, gain1, scale_a, shift_a, jnp.zeros((4, d), f32)], axis=0)
        vmid_ref[...] = jnp.concatenate([emb, gain2, scale_m, shift_m, gate_a, gate_m, b2, jnp.zeros((1, d), f32)], axis=0)
        b1_ref[...] = b1
        amp = gain1 * (1.0 + scale_a)

        @pl.loop(0, s // rows)
        def _(i):
            cut = pl.ds(pl.multiple_of(i * rows, rows), rows)
            h0 = jnp.where(flag_ref[cut, :] == 1, emb, tok_ref[cut, :].astype(f32))
            x = norm_parts(h0)[0] * amp + shift_a
            n1[cut, :] = x.astype(bf16)
            n1t[:, cut] = x.T.astype(bf16)

        for t in range(1, p.bits):
            g.after(1, t)
        g.finish(1)
        fetch = pltpu.make_async_copy(outs[1], wq, loads.at[1])
        fetch.start()
        fetch.wait()

        @pl.loop(0, s // rows)
        def _(i):
            cut = pl.ds(pl.multiple_of(i * rows, rows), rows)
            x = n1[cut, :]
            cos, sin = cos_ref[cut, :], sin_ref[cut, :]
            for part in range(3):
                y = dot(x, flat(wq, part * d, (part + 1) * d))
                for c in range(d // 128):
                    lo = part * d + c * 128
                    u = y[:, c * 128:(c + 1) * 128]
                    if part < 2:
                        u = u * cos + swap_halves(u) * sin
                        if part == 0:
                            u = u * QSCALE
                    qkv[cut, lo:lo + 128] = u.astype(bf16)

        for c in save:
            c.start()

    @pl.when(step == 1)
    def _():
        g.after(2, 0)
        g.after(3, 0)

    @pl.when(step == 4)
    def _():
        g.after(4, 0)

    @pl.when(step > 0)
    def _():
        pair = step - 1
        col = lambda base: qkv.at[:, pl.ds(pl.multiple_of(base + pair * 128, 128), 128)]
        attn_fwd_body(len_ref, col(0), col(d), col(2 * d), att_ref, lse_ref, rows, pair)

    @pl.when(step == steps - 1)
    def _():
        for t in range(1, p.bits):
            for w in (2, 3, 4):
                g.after(w, t)
        for w in (2, 3, 4):
            g.finish(w)
        for c in save:
            c.wait()


def front_call(shape, length, tok, flag, cos, sin, condp, small, ws, sizes, rows=256):
    groups = shape["fsdp"]
    s, d = tok.shape
    pairs = d // 128
    sd = jax.ShapeDtypeStruct
    once = pl.Buffered(1)
    whole = lambda dims: pl.BlockSpec(dims, lambda i: (0, 0), pipeline_mode=once)
    sem = pltpu.SemaphoreType.DMA
    gathered = [gather_shape(w, groups) for w in ws]
    ff = sizes[4] * groups
    res = pl.pallas_call(
        functools.partial(front_kernel, shape, sizes, rows), grid=(pairs + 1,),
        in_specs=[pl.BlockSpec(memory_space=pltpu.SMEM), whole((s, d)), whole((s, 1)), whole((s, 128)), whole((s, 128)),
                  whole((1, 128))] + [ANY] * (1 + len(ws)),
        out_specs=[pl.BlockSpec((s, 128), lambda i: (0, jnp.maximum(i - 1, 0))), whole((s, 128)), whole((8, d)),
                   whole((8, d)), whole((1, ff))] + [ANY] * (2 + len(ws)),
        out_shape=[sd((s, d), bf16), sd((s, 128), f32), sd((8, d), f32), sd((8, d), f32), sd((1, ff), f32),
                   sd((d, s), bf16), sd((s, 3 * d), bf16)] + gathered,
        scratch_shapes=[pltpu.VMEM((s, d), bf16), pltpu.VMEM((d, s), bf16), pltpu.VMEM((s, 3 * d), bf16),
                        pltpu.VMEM(gathered[1].shape, bf16), pltpu.VMEM(gathered[0].shape, bf16),
                        pltpu.VMEM((groups,) + small.shape, f32), sem((2,)), sem((2,))]
        + Gather.scratch(len(ws), groups) + Direct.scratch(groups),
        compiler_params=pltpu.CompilerParams(collective_id=1, has_side_effects=True, vmem_limit_bytes=60000 * 1024),
        cost_estimate=pl.CostEstimate(flops=8 * s * s * d + 6 * s * d * d, bytes_accessed=20 * s * d,
                                      transcendentals=s * s * 12),
        name="front")(length, tok, flag, cos, sin, condp, small, *[quarter(w) for w in ws])
    att, lse, vpre, vmid, b1, n1t, qkv = res[:7]
    return att, lse, vpre, vmid, b1, n1t, qkv, [r.reshape(-1, r.shape[-1]) for r in res[7:]]

def f32_rows_dot(row, weights):
    parts = split3(row)
    stack = jnp.concatenate(list(parts) + [jnp.zeros((5, row.shape[1]), f32)], axis=0).astype(bf16)
    return colsum(dot(stack, weights))


class Small:
    def __init__(self, place, scratch):
        self.p = place
        (self.ag, self.rows, self.ab, self.bs, self.bm, self.bb, self.bg, self.s1, self.r1, self.s2, self.r2) = scratch

    @staticmethod
    def widths(shape, d, ff, n_mod):
        groups = shape["fsdp"]
        part = n_mod // groups
        return -(-(d // groups) // 128) * 128, ff // groups, part if part % 128 == 0 else n_mod

    @staticmethod
    def scratch(shape, d, ff, n_mod):
        groups, lines = shape["fsdp"], shape["dp"]
        wide, fpart, gpart = Small.widths(shape, d, ff, n_mod)
        vm = lambda *dims: pltpu.VMEM(dims, f32)
        sem = pltpu.SemaphoreType.DMA
        return [vm(groups, 1, n_mod), vm(groups, 8, d), vm(groups, 1, ff), vm(lines, 8, wide), vm(lines, groups, 384),
                vm(lines, 1, fpart), vm(lines, groups, gpart), sem((groups, 3)), sem((groups, 3)), sem((lines, 4)),
                sem((lines, 4))]

    def peers(self):
        p = self.p
        return [(p.dp, xor(p.me, m)) for m in range(1, p.groups)] + [(xor(p.dp, m), p.me) for m in range(1, p.lines)]

    def copies(self, stage, m, arrived):
        p = self.p
        if stage == 1:
            bufs, ss, rs = (self.ag, self.rows, self.ab), self.s1, self.r1
            where, slot = (p.dp, xor(p.me, m)), xor(p.me, m) if arrived else p.me
        else:
            bufs, ss, rs = (self.bs, self.bm, self.bb, self.bg), self.s2, self.r2
            where, slot = (xor(p.dp, m), p.me), xor(p.dp, m) if arrived else p.dp
        return [remote(b.at[slot], b.at[slot], ss.at[m, i], rs.at[m, i], where) for i, b in enumerate(bufs)]

    def spread(self, stage):
        for m in range(1, self.p.groups if stage == 1 else self.p.lines):
            for c in self.copies(stage, m, False):
                c.start()

    def collect(self, stage):
        for m in range(1, self.p.groups if stage == 1 else self.p.lines):
            for c in self.copies(stage, m, True):
                c.wait_recv()

    def settle(self):
        for stage in (1, 2):
            for m in range(1, self.p.groups if stage == 1 else self.p.lines):
                for c in self.copies(stage, m, False):
                    c.wait_send()

    def first(self, sums, sb1, sums1, vec_pre, vec_mid, condp, meta, ada):
        me = self.p.me
        d = sums.shape[1]
        ggm, gb2, a2, s2, gga, st0, st1, st2 = (sums[i:i + 1] for i in range(8))
        a1, s1, gemb = (sums1[i:i + 1] for i in range(3))
        gain1, scale_a, gain2, scale_m = vec_pre[1:2], vec_pre[2:3], vec_mid[1:2], vec_mid[2:3]
        gm = jnp.concatenate([s1, a1 * gain1, gga, s2, a2 * gain2, ggm], axis=1)
        sig = 1.0 / (1.0 + jnp.exp(-condp))
        gc = f32_rows_dot(gm, ada) * (sig * (1.0 + condp * (1.0 - sig)))
        lane = lax.broadcasted_iota(jnp.int32, (1, 128), 1)
        total = lambda x: jnp.sum(x, axis=1, keepdims=True)
        stat = jnp.where(lane == 0, total(st0), jnp.where(lane == 1, total(st1), jnp.where(lane == 2, total(st2), meta)))
        tail = jnp.concatenate([gc, condp * sig, stat, jnp.zeros((1, d - 384), f32)], axis=1)
        self.ag[me] = gm
        self.ab[me] = sb1
        self.rows[me] = jnp.concatenate([(1.0 + scale_a) * a1, (1.0 + scale_m) * a2, gb2, gemb, tail,
                                         jnp.zeros((3, d), f32)], axis=0)
        self.spread(1)

    def second(self):
        p = self.p
        self.collect(1)
        d = self.rows.shape[2]
        wide, fpart, gpart = self.bs.shape[2], self.bb.shape[2], self.bg.shape[2]
        total = self.rows[0]
        for f in range(1, p.groups):
            total = total + self.rows[f]
        self.bs[p.dp] = pltpu.roll(total, (d - p.me * (d // p.groups)) % d, 1)[:, :wide]
        self.bm[p.dp] = jnp.concatenate([self.rows[f, 4:5, :384] for f in range(p.groups)], axis=0)
        cut = pl.ds(pl.multiple_of(p.me * fpart, 128), fpart)
        part = self.ab[0, :, cut]
        for f in range(1, p.groups):
            part = part + self.ab[f, :, cut]
        self.bb[p.dp] = part
        n_mod = self.ag.shape[2]
        cut = slice(None) if gpart == n_mod else pl.ds(pl.multiple_of(p.me * gpart, 128), gpart)
        self.bg[p.dp] = jnp.concatenate([self.ag[f, :, cut] for f in range(p.groups)], axis=0)
        self.spread(2)

    def third(self, norms_ref, gb1_ref, gada_ref, gbada_ref, table_ref, rms_ref, d):
        p = self.p
        self.collect(2)
        total, part = self.bs[0], self.bb[0]
        for z in range(1, p.lines):
            total = total + self.bs[z]
            part = part + self.bb[z]
        norms_ref[...] = total
        gb1_ref[...] = part
        mods = jnp.concatenate([self.bg[z] for z in range(p.lines)], axis=0)
        info = jnp.concatenate([self.bm[z] for z in range(p.lines)], axis=0)
        gcs, conds, stat = info[:, :128], info[:, 128:256], info[:, 256:384]
        highest = lax.Precision.HIGHEST
        gada_ref[...] = lax.dot_general(mods, conds, TN, precision=highest, preferred_element_type=f32)
        gbada_ref[...] = colsum(mods)
        ids = stat[:, 4:5].astype(jnp.int32)
        hot = (lax.broadcasted_iota(jnp.int32, (ids.shape[0], table_ref.shape[0]), 1) == ids).astype(f32)
        table_ref[...] = lax.dot_general(hot, gcs, TN, precision=highest, preferred_element_type=f32)
        stat = colsum(stat)
        rms_ref[...] = jnp.sqrt(stat / (stat[:, 3:4] * d))


def small_shapes(shape, d, ff, n_mod, table_rows):
    wide, fpart, gpart = Small.widths(shape, d, ff, n_mod)
    sd = lambda *dims: jax.ShapeDtypeStruct(dims, f32)
    return [sd(8, wide), sd(1, fpart), sd(gpart, 128), sd(1, gpart), sd(table_rows, 128), sd(1, 128)]


def small_results(shape, res, sizes):
    norms, gb1, gada, gbada, table, rms = res
    n_ada = sizes[5]
    if gada.shape[0] != n_ada:
        me = lax.axis_index("fsdp")
        gada = lax.dynamic_slice_in_dim(gada, me * n_ada, n_ada, axis=0)
        gbada = lax.dynamic_slice_in_dim(gbada, me * n_ada, n_ada, axis=1)
    g1, g2, gb2, gemb = (norms[i, :sizes[i]] for i in range(4))
    return g1, g2, gb2, gemb, gb1[0], gada, gbada[0], table, rms[0, :3]


def tail_kernel(shape, counts, rows, post, pairs, *refs):
    n = len(counts)
    (len_ref, q_ref, k_ref, v_ref, o_ref, g_ref, lse_ref, cos_ref, sin_ref, n1_ref, w_ref, tok_ref, flag_ref, gh1_ref,
     vpre_ref, vmid_ref, sums_ref, sb1_ref, condp_ref, meta_ref, ada_ref) = refs[:21]
    srcs = refs[21:20 + n]
    outs = refs[20 + n:21 + 2 * n]
    igrad_ref, reduced, small_out = outs[0], outs[1:1 + n], refs[21 + 2 * n:27 + 2 * n]
    dqs, dks, dvs, dqkv, gq, sums1 = refs[27 + 2 * n:33 + 2 * n]
    rscratch, sscratch = refs[33 + 2 * n:54 + 2 * n], refs[54 + 2 * n:]
    step, steps = pl.program_id(0), 2 * pairs + post
    p = Place(shape)
    r = Reduce(p, counts, ["rows"] + ["cols"] * (n - 2) + ["qkv"], list(srcs) + [gq], reduced, rscratch, 3, 2)
    small = Small(p, sscratch)

    @pl.when(step == 0)
    def _():
        r.greet(small.peers())
        r.begin(0)

    @pl.loop(2 * step, 2 * step + 2)
    def _(t):
        r.tick(t)

    @pl.when(step < 2 * pairs)
    def _():
        pair, head = step // 2, step % 2

        def emit(*parts):
            for i, x in enumerate(parts):
                dqkv[i, pair] = x
            y = dot(n1_ref[...], jnp.concatenate(parts, axis=1)).astype(bf16)
            _, _, g, _, rr, c = gq.shape
            y = y.reshape(g, 2, 2, rr, c)
            for half in (0, 1):
                gq[2 * (pair // 2) + half, pair % 2] = y[:, half]

        attn_bwd_body(len_ref, q_ref, k_ref, v_ref, o_ref, g_ref, lse_ref, cos_ref, sin_ref, dqs, dks, dvs, rows,
                      pair, head, emit)

    @pl.when(step >= 2 * pairs)
    def _():
        i = step - 2 * pairs
        m = tok_ref.shape[0]
        cut = pl.ds(pl.multiple_of(i * m, m), m)
        grads = [jnp.concatenate([dqkv[a, b, cut, :] for b in range(pairs)], axis=1) for a in range(3)]
        masked = flag_ref[...] == 1
        h0 = jnp.where(masked, vpre_ref[0:1, :], tok_ref[...].astype(f32))
        igrad_ref[...], new = post_rows(grads, h0, masked, gh1_ref[...], vpre_ref[1:2, :], vpre_ref[2:3, :], w_ref)
        sums1[...] = jnp.where(i == 0, new, sums1[...] + new)

    @pl.when(step == steps - 1)
    def _():
        small.first(sums_ref[...], sb1_ref[...], sums1[...], vpre_ref[...], vmid_ref[...], condp_ref[...], meta_ref[...],
                    ada_ref[...])
        last = max(r.ticks, 2 * steps)
        marks = [2 * steps, min(2 * steps + SPLIT[0], last), min(2 * steps + SPLIT[1], last), last]
        for n in range(3):
            @pl.loop(marks[n], marks[n + 1])
            def _(t):
                r.tick(t)
            if n == 0:
                small.second()
            if n == 1:
                small.third(*small_out, sums1.shape[1])
        r.drain()
        small.settle()


SPLIT = (3, 8)


def tail_call(shape, length, qkv, att, gatt, lse, cos, sin, n1t, w, tok, flag, gh1, vpre, vmid, sums, sb1, condp, meta,
              ada, grads, table_rows, rows=256):
    groups = shape["fsdp"]
    s, d3 = qkv.shape
    d = d3 // 3
    pairs = d // 128
    r, c = 2 * grads[0].shape[-2], grads[0].shape[-1]
    post = 256 if r % 32 == 0 else 128
    blocks = s // post
    steps = 2 * pairs + blocks
    ff, n_mod = sb1.shape[1], ada.shape[0]
    counts = [g.shape[0] for g in grads] + [pairs]
    pair = lambda i: jnp.minimum(i // 2, pairs - 1)
    blk = lambda i: jnp.maximum(i - 2 * pairs, 0)
    once = pl.Buffered(1)
    col = lambda base: pl.BlockSpec((s, 128), lambda i: (0, base + pair(i)))
    whole = lambda a: pl.BlockSpec(a.shape, lambda i: (0,) * a.ndim, pipeline_mode=once)
    row = lambda cc: pl.BlockSpec((post, cc), lambda i: (blk(i), 0))
    sd = jax.ShapeDtypeStruct
    shard = d // groups
    red = [sd((shard * (g.shape[0] // 2), d), bf16) if i == 0 else sd((shard, d * (g.shape[0] // 2)), bf16)
           for i, g in enumerate(grads)] + [sd((shard, d3), bf16)]
    smalls = small_shapes(shape, d, ff, n_mod, table_rows)
    const = lambda x: pl.BlockSpec(x.shape, lambda i: (0, 0), pipeline_mode=once)
    res = pl.pallas_call(
        functools.partial(tail_kernel, shape, counts, rows, blocks, pairs), grid=(steps,),
        in_specs=[pl.BlockSpec(memory_space=pltpu.SMEM), col(0), col(pairs), col(2 * pairs), col(0), col(0), whole(lse),
                  whole(cos), whole(sin), whole(n1t), whole(w), row(d), row(1), row(d)]
        + [whole(x) for x in (vpre, vmid, sums, sb1, condp, meta, ada)] + [ANY] * len(grads),
        out_specs=[row(d)] + [ANY] * len(red) + [const(x) for x in smalls],
        out_shape=[sd((s, d), bf16)] + red + smalls,
        scratch_shapes=[pltpu.VMEM((128, s), f32), pltpu.VMEM((s, 128), f32), pltpu.VMEM((s, 128), f32),
                        pltpu.VMEM((3, pairs, s, 128), bf16), pltpu.VMEM((pairs, 2, groups, 2, r // 2, c), bf16),
                        pltpu.VMEM((8, d), f32)]
        + Reduce.scratch(sum(counts), groups, r, c) + Small.scratch(shape, d, ff, n_mod),
        compiler_params=pltpu.CompilerParams(collective_id=3, has_side_effects=True, vmem_limit_bytes=65000 * 1024),
        cost_estimate=pl.CostEstimate(flops=30 * s * s * d, bytes_accessed=40 * s * d, transcendentals=s * s * 12),
        name="tail")(length, qkv, qkv, qkv, att, gatt, lse, cos, sin, n1t, w, tok, flag, gh1, vpre, vmid, sums, sb1, condp,
                     meta, ada, *grads)
    return res[0], res[1:1 + len(red)], res[1 + len(red):]
from jax.sharding import PartitionSpec as P

highest = lax.Precision.HIGHEST


def rotary_tables(length):
    half = HD // 2
    rate = 1.0 / 10000.0 ** (jnp.arange(half, dtype=f32) * 2.0 / HD)
    angle = jnp.arange(length, dtype=f32)[:, None] * rate[None, :]
    angle = jnp.concatenate([angle] * (128 // half), axis=-1)
    sign = jnp.where(jnp.arange(128) % HD < half, -1.0, 1.0)
    return jnp.cos(angle), jnp.sin(angle) * sign


def per_device(shape, tokens, hidden_token_indicator, lengths, time_ids, cotangent, gain_one, w_qkv, w_out, gain_two,
               w_fc1, b_fc1, w_fc2, b_fc2, w_ada, b_ada, mask_embed, time_table):
    groups = shape["fsdp"]
    s, d = tokens.shape[1:]
    ff = b_fc1.shape[0] * groups
    tok, cot = tokens[0], cotangent[0]
    flag = hidden_token_indicator.reshape(s, 1)
    sizes = [v.shape[0] for v in (gain_one, gain_two, b_fc2, mask_embed, b_fc1, b_ada)]
    cond_pre = lax.dynamic_slice_in_dim(time_table, time_ids[0], 1, axis=0)
    cos, sin = rotary_tables(s)
    att, lse, vec_pre, vec_mid, b1, n1, qkv, (ada_all, qkv_all, out_all, fc1_all, fc2_all) = front_call(
        shape, lengths, tok, flag, cos, sin, cond_pre, small_row((gain_one, gain_two, b_fc2, mask_embed, b_fc1, b_ada)),
        [w_ada, w_qkv, w_out, w_fc1, w_fc2], sizes)
    out, gh1, gatt, n2, act, gm, gpre, gap, sums, gb1 = mid_call(
        lengths, att, tok, flag, cot, vec_mid, b1, out_all, fc1_all, fc2_all)
    g_fc2 = wgrad_rows(act, gm, groups)
    g_fc1 = wgrad_cols(n2, gpre, groups)
    g_out = wgrad_cols(att, gap, groups)
    meta = jnp.concatenate([jnp.zeros((3,), f32), lengths.astype(f32), time_ids.astype(f32), jnp.zeros((123,), f32)])[None]
    igrad, (r_fc2, r_fc1, r_out, r_qkv), smalls = tail_call(
        shape, lengths, qkv, att, gatt, lse, cos, sin, n1, qkv_all, tok, flag, gh1, vec_pre, vec_mid, sums, gb1, cond_pre,
        meta, ada_all, [g_fc2, g_fc1, g_out], time_table.shape[0])
    g1, g2, gb2, gemb, gb1, g_ada, gbada, table, rms = small_results(shape, smalls, sizes)
    return (out[None], igrad[None], g1, r_qkv.astype(f32), r_out.astype(f32), g2, r_fc1.astype(f32), gb1,
            r_fc2.astype(f32), gb2,
            g_ada, gbada, gemb, table, rms)


def solution(mesh):
    both = ("dp", "fsdp")
    f1, f2 = P("fsdp"), P("fsdp", None)
    placed = (P(both, None, None), P(both, None), P(both), P(both), P(both, None, None), f1, f2, f2, f1, f2, f1, f2, f1,
              f2, f1, f1, P())
    outs = (P(both, None, None), P(both, None, None), f1, f2, f2, f1, f2, f1, f2, f1, f2, f1, f1, P(), P())
    return jax.shard_map(functools.partial(per_device, dict(mesh.shape)), mesh=mesh, in_specs=placed, out_specs=outs,
                         check_vma=False)
```

```python
import functools, math
import jax, jax.numpy as jnp
from jax import lax
from jax.experimental import pallas as pl
from jax.experimental.pallas import tpu as pltpu

HD = 64
EPS = 1e-5
LOG2E = math.log2(math.e)
QSCALE = LOG2E * HD ** -0.5
f32, bf16 = jnp.float32, jnp.bfloat16
NT = (((1,), (1,)), ((), ()))
NN = (((1,), (0,)), ((), ()))
TN = (((0,), (0,)), ((), ()))

def dot(a, b, dims=NN):
    return lax.dot_general(a, b, dims, preferred_element_type=f32)

def norm_parts(x):
    mean = jnp.mean(x, axis=-1, keepdims=True)
    cen = x - mean
    rs = lax.rsqrt(jnp.mean(cen * cen, axis=-1, keepdims=True) + EPS)
    return cen * rs, rs

def swap_halves(u):
    lane = lax.broadcasted_iota(jnp.int32, u.shape, 1)
    return jnp.where(lane % HD < HD // 2, pltpu.roll(u, 96, 1), pltpu.roll(u, 32, 1))

def attn_fwd_body(len_ref, q_ref, k_ref, v_ref, o_ref, lse_ref, rows, p):
    s = q_ref.shape[0]
    length = len_ref[0]
    lane = lax.broadcasted_iota(jnp.int32, (s, 128), 1)
    pos = lax.broadcasted_iota(jnp.int32, (s, 128), 0)
    lane_q = lax.broadcasted_iota(jnp.int32, (rows, 128), 1)
    k = k_ref[...].astype(f32)
    v = v_ref[...].astype(f32)
    kx, vx = [], []
    for h in (0, 1):
        extra = HD * (1 - h)
        mine = (lane >= HD) if h else (lane < HD)
        bias = jnp.where(pos >= length, -1e30, 0.0)
        kx.append(jnp.where(mine, k, jnp.where(lane == extra, bias, 0.0)).astype(bf16))
        vx.append(jnp.where(mine, v, jnp.where(lane == extra, 1.0, 0.0)).astype(bf16))
    for b in range(s // rows):
        q = q_ref[b * rows:(b + 1) * rows, :].astype(f32)
        outs, lses = [], []
        for h in (0, 1):
            extra = HD * (1 - h)
            mine = (lane_q >= HD) if h else (lane_q < HD)
            qx = jnp.where(mine, q, jnp.where(lane_q == extra, 1.0, 0.0)).astype(bf16)
            sc = dot(qx, kx[h], NT)
            m = jnp.max(sc, axis=1, keepdims=True)
            pr = jnp.exp2(sc - m).astype(bf16)
            o = dot(pr, vx[h])
            tot = o[:, extra:extra + 1]
            outs.append(o * (1.0 / tot))
            lses.append(m + jnp.log(tot) * LOG2E)
        o_ref[b * rows:(b + 1) * rows, :] = jnp.where(lane_q < HD, outs[0], outs[1]).astype(bf16)
        old = jnp.where(p == 0, 0.0, lse_ref[b * rows:(b + 1) * rows, :])
        lse_ref[b * rows:(b + 1) * rows, :] = jnp.where(
            lane_q == 2 * p, lses[0], jnp.where(lane_q == 2 * p + 1, lses[1], old))

def split3(x):
    hi = x.astype(bf16).astype(f32)
    r = x - hi
    mid = r.astype(bf16).astype(f32)
    return hi, mid, r - mid

def attn_bwd_body(len_ref, q_ref, k_ref, v_ref, o_ref, g_ref, lse_ref, cos_ref, sin_ref,
                  dqs, dks, dvs, rows, p, h, emit, pause):
    s = q_ref.shape[0]
    length = len_ref[0]
    lane = lax.broadcasted_iota(jnp.int32, (s, 128), 1)
    pos = lax.broadcasted_iota(jnp.int32, (s, 128), 0)
    lane_q = lax.broadcasted_iota(jnp.int32, (rows, 128), 1)
    e = HD * (1 - h)
    mine, mine_q = lane // HD == h, lane_q // HD == h
    k = k_ref[...].astype(f32)
    v = v_ref[...].astype(f32)
    ones = jnp.where((lane >= e) & (lane < e + 3), 1.0, 0.0)
    bias = jnp.where(pos >= length, -1e30, 0.0)
    kx = jnp.where(mine, k, jnp.where(lane == e + 3, bias, ones)).astype(bf16)
    vx = jnp.where(mine, v, ones).astype(bf16)
    kt = jnp.where(mine, k, 0.0).T.astype(bf16)
    dk = jnp.zeros((s, 128), f32)
    dv = jnp.zeros((s, 128), f32)
    for b in range(s // rows):
        sl = slice(b * rows, (b + 1) * rows)
        qb = q_ref[sl, :]
        gb = g_ref[sl, :]
        q = qb.astype(f32)
        g = gb.astype(f32)
        lse = jnp.sum(jnp.where(lane_q == 2 * p + h, lse_ref[sl, :], 0.0), axis=1, keepdims=True)
        dd = jnp.sum(jnp.where(mine_q, g * o_ref[sl, :].astype(f32), 0.0), axis=1, keepdims=True)
        l0, l1, l2 = split3(-lse)
        d0, d1, d2 = split3(-dd)
        qx = jnp.where(mine_q, q, jnp.where(lane_q == e, l0, jnp.where(lane_q == e + 1, l1, jnp.where(
            lane_q == e + 2, l2, jnp.where(lane_q == e + 3, 1.0, 0.0))))).astype(bf16)
        gx = jnp.where(mine_q, g, jnp.where(lane_q == e, d0, jnp.where(lane_q == e + 1, d1, jnp.where(
            lane_q == e + 2, d2, 0.0)))).astype(bf16)
        pt = jnp.exp2(dot(kx, qx, NT))
        dst = (pt * dot(vx, gx, NT)).astype(bf16)
        dv = dv + dot(pt.astype(bf16), gb)
        dk = dk + dot(dst, qb)
        dqt = dot(kt, dst)
        dqs[:, sl] = jnp.where(h == 0, dqt, dqs[:, sl] + dqt)
        if b == s // rows // 2 - 1:
            pause()
    @pl.when(h == 0)
    def _():
        dks[...] = dk
        dvs[...] = dv
    @pl.when(h == 1)
    def _():
        cos, sin = cos_ref[...], sin_ref[...]
        dq = dqs[...].T * (HD ** -0.5)
        dkk = jnp.where(lane < HD, dks[...], dk) * (1.0 / LOG2E)
        emit((dq * cos - swap_halves(dq) * sin).astype(bf16), (dkk * cos - swap_halves(dkk) * sin).astype(bf16),
             jnp.where(lane < HD, dvs[...], dv).astype(bf16))


def gelu_both(v):
    a, b = 0.7978845608028654, 0.044715
    v2 = v * v
    t = jnp.tanh(a * v * (1.0 + b * v2))
    half = 0.5 + 0.5 * t
    return v * half, half + (0.5 * a) * v * (1.0 - t * t) * (1.0 + 3.0 * b * v2)

def colsum(x):
    return jnp.sum(x, axis=0, keepdims=True)

def mid_kernel(len_ref, att_ref, tok_ref, flag_ref, cot_ref, vec_ref, b1_ref, wo_ref, w1_ref, w2_ref,
               out_ref, gh1_ref, gatt_ref, n2_ref, act_ref, gm_ref, gpre_ref, gap_ref, sum_ref, sb1_ref,
               gp_s, *, cut):
    i = pl.program_id(0)
    rows, d = att_ref.shape
    ff = w1_ref.shape[1]
    emb, gain, scale, shift, gate_a, gate_m, b2 = (vec_ref[r:r + 1, :] for r in range(7))
    h0 = jnp.where(flag_ref[...] == 1, emb, tok_ref[...].astype(f32))
    ap = dot(att_ref[...], wo_ref[...])
    br_a = gate_a * ap
    h1 = h0 + br_a
    n, rs = norm_parts(h1)
    n2 = (n * gain * (1.0 + scale) + shift).astype(bf16)
    n2_ref[...] = n2
    mp = jnp.zeros((rows, d), f32) + b2
    for j in range(ff // cut):
        sl = slice(j * cut, (j + 1) * cut)
        act, gp = gelu_both(dot(n2, w1_ref[:, sl]) + b1_ref[:, sl])
        act = act.astype(bf16)
        act_ref[:, sl] = act
        gp_s[:, sl] = gp
        mp = mp + dot(act, w2_ref[sl, :])
    br_m = gate_m * mp
    bo = h1 + br_m
    out_ref[...] = bo.astype(bf16)
    pos = lax.broadcasted_iota(jnp.int32, (rows, 1), 0) + i * rows
    valid = jnp.where(pos < len_ref[0], 1.0, 0.0)
    cot = cot_ref[...].astype(f32)
    gm = (gate_m * cot).astype(bf16)
    gm_ref[...] = gm
    gn2 = jnp.zeros((rows, d), f32)
    sb1 = []
    for j in range(ff // cut):
        sl = slice(j * cut, (j + 1) * cut)
        gpre = (dot(gm, w2_ref[sl, :], NT) * gp_s[:, sl]).astype(bf16)
        gpre_ref[:, sl] = gpre
        sb1.append(colsum(gpre.astype(f32)))
        gn2 = gn2 + dot(gpre, w1_ref[:, sl], NT)
    e = gn2 * (gain * (1.0 + scale))
    gh1 = cot + rs * (e - jnp.mean(e, axis=1, keepdims=True) - n * jnp.mean(e * n, axis=1, keepdims=True))
    gh1_ref[...] = gh1
    gap = (gate_a * gh1).astype(bf16)
    gap_ref[...] = gap
    gatt_ref[...] = dot(gap, wo_ref[...], NT).astype(bf16)
    new = jnp.concatenate([
        colsum(cot * mp), colsum(gm.astype(f32)), colsum(gn2 * n), colsum(gn2), colsum(gh1 * ap),
        colsum(valid * bo * bo), colsum(valid * br_a * br_a), colsum(valid * br_m * br_m)], axis=0)
    sb1 = jnp.concatenate(sb1, axis=1)
    @pl.when(i == 0)
    def _():
        sum_ref[...] = new
        sb1_ref[...] = sb1
    @pl.when(i > 0)
    def _():
        sum_ref[...] += new
        sb1_ref[...] += sb1

def mid_call(length, att, tok, flag, cot, vec, b1, wo, w1, w2, rows=256, cut=768):
    s, d = tok.shape
    ff = w1.shape[1]
    row = lambda c: pl.BlockSpec((rows, c), lambda i: (i, 0))
    whole = lambda a: pl.BlockSpec(a.shape, lambda i: (0, 0))
    sd = jax.ShapeDtypeStruct
    return pl.pallas_call(
        functools.partial(mid_kernel, cut=cut), grid=(s // rows,),
        in_specs=[pl.BlockSpec(memory_space=pltpu.SMEM), row(d), row(d), row(1), row(d), whole(vec), whole(b1),
                  whole(wo), whole(w1), whole(w2)],
        out_specs=[row(d), row(d), row(d), row(d), row(ff), row(d), row(ff), row(d),
                   pl.BlockSpec((8, d), lambda i: (0, 0)), pl.BlockSpec((1, ff), lambda i: (0, 0))],
        out_shape=[sd((s, d), bf16), sd((s, d), f32), sd((s, d), bf16), sd((s, d), bf16), sd((s, ff), bf16),
                   sd((s, d), bf16), sd((s, ff), bf16), sd((s, d), bf16), sd((8, d), f32), sd((1, ff), f32)],
        scratch_shapes=[pltpu.VMEM((rows, ff), f32)],
        compiler_params=pltpu.CompilerParams(vmem_limit_bytes=60000 * 1024),
        cost_estimate=pl.CostEstimate(flops=2 * s * d * (2 * d + 4 * ff), bytes_accessed=30 * s * d,
                                      transcendentals=s * ff),
        name="mid")(length, att, tok, flag, cot, vec, b1, wo, w1, w2)

def post_rows(grads, h0, masked, gh1, gain, scale, w_ref):
    d = h0.shape[1]
    n, rs = norm_parts(h0)
    gn1 = sum(dot(g, w_ref[:, i * d:(i + 1) * d], NT) for i, g in enumerate(grads))
    e = gn1 * (gain * (1.0 + scale))
    gh0 = gh1 + rs * (e - jnp.mean(e, axis=1, keepdims=True) - n * jnp.mean(e * n, axis=1, keepdims=True))
    sums = jnp.concatenate([colsum(gn1 * n), colsum(gn1), colsum(jnp.where(masked, gh0, 0.0)),
                            jnp.zeros((5, d), f32)], axis=0)
    return jnp.where(masked, 0.0, gh0).astype(bf16), sums

MESH = pl.DeviceIdType.MESH


def flip(i, b):
    return i + 2 ** b * (1 - 2 * ((i // 2 ** b) % 2))


def xor(i, mask):
    b = 0
    while mask >> b:
        if (mask >> b) & 1:
            i = flip(i, b)
        b += 1
    return i


def subsets(bits):
    masks = [0]
    for b in bits:
        masks = masks + [m | (1 << b) for m in masks]
    return masks


def log2(n):
    return n.bit_length() - 1


class Place:
    def __init__(self, shape):
        self.groups, self.lines = shape["fsdp"], shape["dp"]
        self.bits = log2(self.groups)
        self.orders = [list(range(self.bits)), list(range(self.bits))[::-1]]
        self.me = lax.axis_index("fsdp")
        self.dp = lax.axis_index("dp")
        self.core = self.dp % 2
        self.partner = flip(self.dp, 0)


def remote(src, dst, ssem, rsem, where):
    return pltpu.make_async_remote_copy(src_ref=src, dst_ref=dst, send_sem=ssem, recv_sem=rsem, device_id=where,
                                        device_id_type=MESH)


class Gather:
    def __init__(self, place, ins, outs, sems):
        self.p, self.ins, self.outs = place, ins, outs
        self.ss, self.rs, self.fs, self.fr, self.os, self.orr = sems

    @staticmethod
    def scratch(count, groups):
        a = pltpu.SemaphoreType.DMA((count, 2, groups - 1))
        b = pltpu.SemaphoreType.DMA((count,))
        return [a, a, a, a, b, b]

    def send(self, w, color, t, mask):
        p = self.p
        order = p.orders[color]
        e = 2 ** t - 1 + subsets(order[:t]).index(mask)
        piece = p.core * 2 + color
        blk = xor(p.me, mask)
        src = self.ins[w].at[piece] if mask == 0 else self.outs[w].at[blk, piece]
        return remote(src, self.outs[w].at[blk, piece], self.ss.at[w, color, e], self.rs.at[w, color, e],
                      (p.dp, flip(p.me, order[t])))

    def arrival(self, w, color, t, mask):
        p = self.p
        order = p.orders[color]
        e = 2 ** t - 1 + subsets(order[:t]).index(mask)
        got = self.outs[w].at[xor(p.me, mask | (1 << order[t])), p.core * 2 + color]
        return e, got

    def landed(self, w, color, e, got):
        return remote(got, got, self.ss.at[w, color, e], self.rs.at[w, color, e], (self.p.partner, self.p.me))

    def forward(self, w, color, e, got):
        return remote(got, got, self.fs.at[w, color, e], self.fr.at[w, color, e], (self.p.partner, self.p.me))

    def own(self, w):
        p = self.p
        return remote(self.ins[w], self.outs[w].at[p.me], self.os.at[w], self.orr.at[w], (p.partner, p.me))

    def start(self, w):
        for t in range(self.p.bits):
            for color in (0, 1):
                self.send(w, color, t, 0).start()
        self.own(w).start()

    def after(self, w, t):
        for color in (0, 1):
            order = self.p.orders[color]
            for mask in subsets(order[:t]):
                e, got = self.arrival(w, color, t, mask)
                self.landed(w, color, e, got).wait_recv()
                for later in range(t + 1, self.p.bits):
                    self.send(w, color, later, mask | (1 << order[t])).start()
                self.forward(w, color, e, got).start()

    def finish(self, w):
        p = self.p
        for color in (0, 1):
            order = p.orders[color]
            for t in range(p.bits):
                for mask in subsets(order[:t]):
                    e, got = self.arrival(w, color, t, mask)
                    other = self.outs[w].at[xor(p.me, mask | (1 << order[t])), (1 - p.core) * 2 + color]
                    self.forward(w, color, e, other).wait_recv()
                    self.forward(w, color, e, got).wait_send()
                    self.send(w, color, t, mask).wait_send()
        self.own(w).wait()


class Direct:
    def __init__(self, place, src, out, sems):
        self.p, self.src, self.out = place, src, out
        self.ss, self.rs = sems

    @staticmethod
    def scratch(groups):
        return [pltpu.SemaphoreType.DMA((groups,))] * 2

    def copy(self, m, arrived):
        p = self.p
        where = (p.partner, p.me) if m == 0 else (p.dp, xor(p.me, m))
        slot = xor(p.me, m) if arrived else p.me
        return remote(self.src, self.out.at[slot], self.ss.at[m], self.rs.at[m], where)

    def start(self):
        for m in range(self.p.groups):
            self.copy(m, False).start()

    def finish(self):
        for m in range(self.p.groups):
            self.copy(m, True).wait_recv()
            self.copy(m, False).wait_send()


def greet(devices):
    barrier = pltpu.get_barrier_semaphore()
    for where in devices:
        pl.semaphore_signal(barrier, inc=1, device_id=where, device_id_type=MESH)
    pl.semaphore_wait(barrier, len(devices))


def gather_peers(p, everyone):
    masks = range(1, p.groups) if everyone else [1 << b for b in range(p.bits)]
    return [(p.partner, p.me)] + [(p.dp, xor(p.me, m)) for m in masks]


def quarter(w):
    return w.reshape(4, w.shape[0] // 4, w.shape[1])


def gather_shape(w, groups):
    return jax.ShapeDtypeStruct((groups, 4, w.shape[0] // 4, w.shape[1]), w.dtype)


ANY = pl.BlockSpec(memory_space=pl.ANY)


class Reduce:
    def __init__(self, place, counts, kinds, srcs, outs, scratch, lag, gap):
        self.p, self.counts, self.kinds, self.srcs, self.outs = place, counts, kinds, srcs, outs
        (self.own, self.cb, self.xb, self.zb, self.mb, self.u2, self.fin,
         self.load, self.cs, self.cr, self.xs, self.xr, self.zs, self.zr, self.ms, self.mr, self.fs, self.fr,
         self.ps, self.pr, self.st) = scratch
        p = place
        self.total = sum(counts)
        self.n = p.lines // 2
        self.zi = p.dp // 2
        left = self.zi // (self.n // 2)
        self.e = self.zi * (1 - left) + (self.n - 1 - self.zi) * left
        step = 2 * (1 - 2 * left)
        self.inner = (p.dp + step, p.me)
        self.outer = (p.dp - step, p.me)
        self.last = self.n // 2 - 1
        self.stages = ([self.begin, self.core_add] + [functools.partial(self.group_add, t) for t in range(p.bits)]
                       + [functools.partial(self.climb, j) for j in range(1, self.last + 1)] + [self.middle]
                       + [functools.partial(self.descend, j) for j in range(self.last - 1, -1, -1)])
        self.lags = [0, 1] + [1 + lag * (i + 1) for i in range(len(self.stages) - 2)]
        self.early = self.total - counts[-1]
        self.gap = gap
        self.ticks = self.total + gap + self.lags[-1]

    @staticmethod
    def scratch(total, groups, rows, cols):
        sem = pltpu.SemaphoreType.DMA
        vm = lambda *lead: pltpu.VMEM((total,) + lead + (rows // 2, cols), bf16)
        one = sem((total,))
        line = pltpu.VMEM((total, rows, cols), bf16)
        return [vm(groups, 2), vm(groups, 2), vm(2, groups - 1), line, line, line, line,
                one, one, one, sem((total, 2, groups - 1)), sem((total, 2, groups - 1)),
                one, one, one, one, one, one, sem((total, 3)), sem((total, 3)), sem((total, 3))]

    def greet(self, peers):
        p = self.p
        barrier = pltpu.get_barrier_semaphore()
        for where in peers:
            pl.semaphore_signal(barrier, inc=1, device_id=where, device_id_type=MESH)
        pl.semaphore_wait(barrier, len(peers))

    def source(self, k, fn):
        base = 0
        for i, count in enumerate(self.counts):
            @pl.when((k >= base) & (k < base + count))
            def _(i=i, base=base):
                fn(i, k - base)
            base += count

    def targets(self, k, i, j, core):
        rows, cols = self.fin.shape[1:]
        out, fin = self.outs[i], self.fin.at[k]
        if self.kinds[i] == "rows":
            cut = pl.ds(pl.multiple_of(core * cols, cols), cols)
            return [(fin, out.at[pl.ds(pl.multiple_of(j * rows, rows), rows), cut])]
        down = pl.ds(pl.multiple_of((j % 2) * rows, rows), rows)
        if self.kinds[i] == "cols":
            return [(fin, out.at[down, pl.ds(pl.multiple_of((2 * (j // 2) + core) * cols, cols), cols)])]
        width = out.shape[1] // 3
        pair = 2 * (j // 2) + core
        return [(fin.at[:, part * 128:(part + 1) * 128],
                 out.at[down, pl.ds(pl.multiple_of(part * width + pair * 128, 128), 128)]) for part in range(3)]

    def load_copy(self, k, src):
        return pltpu.make_async_copy(src.at[self.p.core], self.own.at[k], self.load.at[k])

    def core_copy(self, k, src):
        p = self.p
        return remote(src.at[1 - p.core], self.cb.at[k], self.cs.at[k], self.cr.at[k], (p.partner, p.me))

    def begin(self, k):
        def go(i, j):
            self.core_copy(k, self.srcs[i].at[j]).start()
            self.load_copy(k, self.srcs[i].at[j]).start()
        self.source(k, go)

    def slot(self, order, t, mask):
        base = sum(self.p.groups >> (u + 1) for u in range(t))
        return base + subsets(order[t + 1:]).index(mask)

    def group_copy(self, k, color, t, mask):
        p = self.p
        order = p.orders[color]
        i = self.slot(order, t, mask)
        return remote(self.own.at[k, xor(p.me, (1 << order[t]) | mask), color], self.xb.at[k, color, i],
                      self.xs.at[k, color, i], self.xr.at[k, color, i], (p.dp, flip(p.me, order[t])))

    def group_send(self, k, t):
        for color in (0, 1):
            for mask in subsets(self.p.orders[color][t + 1:]):
                self.group_copy(k, color, t, mask).start()

    def core_add(self, k):
        self.load_copy(k, self.srcs[0].at[0]).wait()
        self.core_copy(k, self.srcs[0].at[0]).wait_recv()
        for f in range(self.p.groups):
            for color in (0, 1):
                self.own[k, f, color] = (self.own[k, f, color].astype(f32) + self.cb[k, f, color].astype(f32)).astype(bf16)
        self.group_send(k, 0)

    def group_add(self, t, k):
        p = self.p
        for color in (0, 1):
            order = p.orders[color]
            for mask in subsets(order[t + 1:]):
                self.group_copy(k, color, t, mask).wait_recv()
                blk, i = xor(p.me, mask), self.slot(order, t, mask)
                total = self.own[k, blk, color].astype(f32) + self.xb[k, color, i].astype(f32)
                if t == p.bits - 1:
                    self.u2[k, self.part(color)] = total.astype(bf16)
                else:
                    self.own[k, blk, color] = total.astype(bf16)
        if t < p.bits - 1:
            self.group_send(k, t + 1)
        else:
            @pl.when(self.e == 0)
            def _():
                (self.climb_copy(k) if self.last > 0 else self.middle_copy(k)).start()

    def part(self, color):
        half = self.u2.shape[1] // 2
        return slice(color * half, (color + 1) * half)

    def climb_copy(self, k):
        return remote(self.u2.at[k], self.zb.at[k], self.zs.at[k], self.zr.at[k], self.inner)

    def middle_copy(self, k):
        return remote(self.u2.at[k], self.mb.at[k], self.ms.at[k], self.mr.at[k], self.inner)

    def climb(self, j, k):
        @pl.when(self.e == j)
        def _():
            self.climb_copy(k).wait_recv()
            for color in (0, 1):
                total = self.u2[k, self.part(color)].astype(f32) + self.zb[k, self.part(color)].astype(f32)
                self.u2[k, self.part(color)] = total.astype(bf16)
            (self.middle_copy(k) if j == self.last else self.climb_copy(k)).start()

    def share_copy(self, k):
        return remote(self.fin.at[k], self.fin.at[k], self.fs.at[k], self.fr.at[k], self.outer)

    def share_wait(self, k):
        return remote(self.fin.at[k], self.fin.at[k], self.fs.at[k], self.fr.at[k], self.inner)

    def out_copies(self, k, i, j):
        p = self.p
        mine, other = self.targets(k, i, j, p.core), self.targets(k, i, j, 1 - p.core)
        sent = [remote(s, d, self.ps.at[k, n], self.pr.at[k, n], (p.partner, p.me)) for n, (s, d) in enumerate(mine)]
        kept = [pltpu.make_async_copy(s, d, self.st.at[k, n]) for n, (s, d) in enumerate(mine)]
        return sent, kept, other

    def done(self, k):
        def go(i, j):
            sent, kept, _ = self.out_copies(k, i, j)
            for c in sent + kept:
                c.start()
        self.source(k, go)

    def retire(self, k):
        p = self.p
        def go(i, j):
            sent, kept, other = self.out_copies(k, i, j)
            for n, c in enumerate(sent):
                c.wait_send()
                s, d = other[n]
                remote(s, d, self.ps.at[k, n], self.pr.at[k, n], (p.partner, p.me)).wait_recv()
            for c in kept:
                c.wait()
        self.source(k, go)

    def middle(self, k):
        @pl.when(self.e == self.last)
        def _():
            self.middle_copy(k).wait_recv()
            for color in (0, 1):
                total = self.u2[k, self.part(color)].astype(f32) + self.mb[k, self.part(color)].astype(f32)
                self.fin[k, self.part(color)] = total.astype(bf16)
            if self.last > 0:
                self.share_copy(k).start()
            self.done(k)

    def descend(self, j, k):
        @pl.when(self.e == j)
        def _():
            self.share_wait(k).wait_recv()
            if j > 0:
                self.share_copy(k).start()
            self.done(k)

    def tick(self, t):
        for s in range(len(self.stages) - 1, 0, -1):
            k = t - self.lags[s]
            @pl.when((k >= 0) & (k < self.total + self.gap) & ((k < self.total - self.gap) | (k >= self.total)))
            def _(s=s, k=k):
                self.stages[s](k - self.gap * (k // self.total))
        @pl.when(t + 1 < self.early)
        def _():
            self.begin(t + 1)
        @pl.when((t >= self.early) & (t < self.total + self.gap) & ((t < self.total - self.gap) | (t >= self.total)))
        def _():
            self.begin(t - self.gap * (t // self.total))

    def drain(self):
        p = self.p
        @pl.loop(0, self.total)
        def _(k):
            self.core_copy(k, self.srcs[0].at[0]).wait_send()
            for color in (0, 1):
                for t in range(p.bits):
                    for mask in subsets(p.orders[color][t + 1:]):
                        self.group_copy(k, color, t, mask).wait_send()
            @pl.when(self.e == self.last)
            def _():
                self.middle_copy(k).wait_send()
            @pl.when(self.e < self.last)
            def _():
                self.climb_copy(k).wait_send()
            @pl.when(self.e > 0)
            def _():
                self.share_copy(k).wait_send()
            self.retire(k)


def wgrad_cols_kernel(a_ref, b_ref, o_ref):
    y = dot(a_ref[...], b_ref[...], TN).astype(bf16)
    _, _, g, _, r, c = o_ref.shape
    for core in (0, 1):
        z = y[:, core * c:(core + 1) * c].reshape(g, 2, 2, r, c)
        for half in (0, 1):
            o_ref[half, core] = z[:, half]


def wgrad_cols(a, b, groups):
    s, m = a.shape
    n = b.shape[1]
    r, c = m // groups // 4, m // 2
    return pl.pallas_call(
        wgrad_cols_kernel, grid=(n // m,),
        in_specs=[pl.BlockSpec((s, m), lambda i: (0, 0)), pl.BlockSpec((s, m), lambda i: (0, i))],
        out_specs=pl.BlockSpec((2, 2, groups, 2, r, c), lambda i: (i, 0, 0, 0, 0, 0)),
        out_shape=jax.ShapeDtypeStruct((2 * n // m, 2, groups, 2, r, c), bf16),
        cost_estimate=pl.CostEstimate(flops=2 * s * m * n, bytes_accessed=2 * (s * (m + n) + m * n),
                                      transcendentals=0), name="wgrad_cols")(a, b)


def wgrad_rows_kernel(a_ref, b_ref, o_ref):
    y = dot(a_ref[...], b_ref[...], TN).astype(bf16)
    q, _, _, _, r, c = o_ref.shape
    for core in (0, 1):
        o_ref[:, core, 0] = y[:, core * c:(core + 1) * c].reshape(q, 2, r, c)


def wgrad_rows(a, b, groups):
    s, m = a.shape
    n = b.shape[1]
    q, r, c = 2 * m // n, n // groups // 4, n // 2
    return pl.pallas_call(
        wgrad_rows_kernel, grid=(groups,),
        in_specs=[pl.BlockSpec((s, m // groups), lambda i: (0, i)), pl.BlockSpec((s, n), lambda i: (0, 0))],
        out_specs=pl.BlockSpec((q, 2, 1, 2, r, c), lambda i: (0, 0, i, 0, 0, 0)),
        out_shape=jax.ShapeDtypeStruct((q, 2, groups, 2, r, c), bf16),
        cost_estimate=pl.CostEstimate(flops=2 * s * m * n, bytes_accessed=2 * (s * (m + n) + m * n),
                                      transcendentals=0), name="wgrad_rows")(a, b)


def pad128(n):
    return -(-n // 128) * 128


def small_row(vectors):
    wide = [jnp.pad(v.astype(f32), (0, pad128(v.shape[0]) - v.shape[0])) for v in vectors]
    return jnp.concatenate([v[None] for v in wide], axis=1)


def unpack(ref, sizes, groups):
    out, base = [], 0
    for size in sizes:
        wide, full = pad128(size), size * groups
        total = None
        for f in range(groups):
            x = ref[f, :, base:base + wide]
            if full > wide:
                x = jnp.concatenate([x, jnp.zeros((1, full - wide), f32)], axis=1)
            if f > 0:
                x = pltpu.roll(jnp.broadcast_to(x, (8, full)), f * size, 1)[0:1]
            total = x if total is None else total + x
        out.append(total)
        base += wide
    return out


def flat(ref, lo, hi):
    groups, _, rows, _ = ref.shape
    if rows % 16 == 0:
        return ref[:, :, :, lo:hi].reshape(groups * 4 * rows, hi - lo)
    parts = [jnp.concatenate([ref[f, i, :, lo:hi].astype(f32) for i in range(4)], axis=0).astype(bf16) for f in range(groups)]
    return jnp.concatenate(parts, axis=0)


def front_kernel(shape, sizes, rows, *refs):
    len_ref, tok_ref, flag_ref, cos_ref, sin_ref, condp_ref, small_ref = refs[:7]
    ins = refs[7:12]
    att_ref, lse_ref, vpre_ref, vmid_ref, b1_ref, n1t_hbm, qkv_hbm = refs[12:19]
    outs = refs[19:24]
    n1, n1t, qkv, wq, ada, smalls, loads, stores = refs[24:32]
    gsems, dsems = refs[32:38], refs[38:40]
    step, steps = pl.program_id(0), pl.num_programs(0)
    s, d = tok_ref.shape
    p = Place(shape)
    g = Gather(p, ins, outs, gsems)
    direct = Direct(p, small_ref, smalls, dsems)
    save = [pltpu.make_async_copy(n1t, n1t_hbm, stores.at[0]), pltpu.make_async_copy(qkv, qkv_hbm, stores.at[1])]

    @pl.when(step == 0)
    def _():
        greet(gather_peers(p, True))
        direct.start()
        g.start(0)
        g.start(1)
        g.after(0, 0)
        g.after(1, 0)
        for w in (2, 3, 4):
            g.start(w)
        for t in range(1, p.bits):
            g.after(0, t)
        g.finish(0)
        direct.finish()
        fetch = pltpu.make_async_copy(outs[0], ada, loads.at[0])
        fetch.start()
        gain1, gain2, b2, emb, b1, bada = unpack(smalls, sizes, p.groups)
        fetch.wait()
        condp = condp_ref[...]
        cond = condp / (1.0 + jnp.exp(-condp))
        stack = jnp.concatenate(list(split3(cond)) + [jnp.zeros((5, cond.shape[1]), f32)], axis=0).astype(bf16)
        mod = colsum(dot(stack, flat(ada, 0, 128), NT)) + bada
        shift_a, scale_a, gate_a, shift_m, scale_m, gate_m = (mod[:, i * d:(i + 1) * d] for i in range(6))
        vpre_ref[...] = jnp.concatenate([emb, gain1, scale_a, shift_a, jnp.zeros((4, d), f32)], axis=0)
        vmid_ref[...] = jnp.concatenate([emb, gain2, scale_m, shift_m, gate_a, gate_m, b2, jnp.zeros((1, d), f32)], axis=0)
        b1_ref[...] = b1
        amp = gain1 * (1.0 + scale_a)

        @pl.loop(0, s // rows)
        def _(i):
            cut = pl.ds(pl.multiple_of(i * rows, rows), rows)
            h0 = jnp.where(flag_ref[cut, :] == 1, emb, tok_ref[cut, :].astype(f32))
            x = norm_parts(h0)[0] * amp + shift_a
            n1[cut, :] = x.astype(bf16)
            n1t[:, cut] = x.T.astype(bf16)

        for t in range(1, p.bits):
            g.after(1, t)
        g.finish(1)
        fetch = pltpu.make_async_copy(outs[1], wq, loads.at[1])
        fetch.start()
        fetch.wait()

        @pl.loop(0, s // rows)
        def _(i):
            cut = pl.ds(pl.multiple_of(i * rows, rows), rows)
            x = n1[cut, :]
            cos, sin = cos_ref[cut, :], sin_ref[cut, :]
            for part in range(3):
                y = dot(x, flat(wq, part * d, (part + 1) * d))
                for c in range(d // 128):
                    lo = part * d + c * 128
                    u = y[:, c * 128:(c + 1) * 128]
                    if part < 2:
                        u = u * cos + swap_halves(u) * sin
                        if part == 0:
                            u = u * QSCALE
                    qkv[cut, lo:lo + 128] = u.astype(bf16)

        for c in save:
            c.start()

    @pl.when(step == 1)
    def _():
        g.after(2, 0)
        g.after(3, 0)

    @pl.when(step == 4)
    def _():
        g.after(4, 0)

    @pl.when(step > 0)
    def _():
        pair = step - 1
        col = lambda base: qkv.at[:, pl.ds(pl.multiple_of(base + pair * 128, 128), 128)]
        attn_fwd_body(len_ref, col(0), col(d), col(2 * d), att_ref, lse_ref, rows, pair)

    @pl.when(step == steps - 1)
    def _():
        for t in range(1, p.bits):
            for w in (2, 3, 4):
                g.after(w, t)
        for w in (2, 3, 4):
            g.finish(w)
        for c in save:
            c.wait()


def front_call(shape, length, tok, flag, cos, sin, condp, small, ws, sizes, rows=256):
    groups = shape["fsdp"]
    s, d = tok.shape
    pairs = d // 128
    sd = jax.ShapeDtypeStruct
    once = pl.Buffered(1)
    whole = lambda dims: pl.BlockSpec(dims, lambda i: (0, 0), pipeline_mode=once)
    sem = pltpu.SemaphoreType.DMA
    gathered = [gather_shape(w, groups) for w in ws]
    ff = sizes[4] * groups
    res = pl.pallas_call(
        functools.partial(front_kernel, shape, sizes, rows), grid=(pairs + 1,),
        in_specs=[pl.BlockSpec(memory_space=pltpu.SMEM), whole((s, d)), whole((s, 1)), whole((s, 128)), whole((s, 128)),
                  whole((1, 128))] + [ANY] * (1 + len(ws)),
        out_specs=[pl.BlockSpec((s, 128), lambda i: (0, jnp.maximum(i - 1, 0))), whole((s, 128)), whole((8, d)),
                   whole((8, d)), whole((1, ff))] + [ANY] * (2 + len(ws)),
        out_shape=[sd((s, d), bf16), sd((s, 128), f32), sd((8, d), f32), sd((8, d), f32), sd((1, ff), f32),
                   sd((d, s), bf16), sd((s, 3 * d), bf16)] + gathered,
        scratch_shapes=[pltpu.VMEM((s, d), bf16), pltpu.VMEM((d, s), bf16), pltpu.VMEM((s, 3 * d), bf16),
                        pltpu.VMEM(gathered[1].shape, bf16), pltpu.VMEM(gathered[0].shape, bf16),
                        pltpu.VMEM((groups,) + small.shape, f32), sem((2,)), sem((2,))]
        + Gather.scratch(len(ws), groups) + Direct.scratch(groups),
        compiler_params=pltpu.CompilerParams(collective_id=1, has_side_effects=True, vmem_limit_bytes=60000 * 1024),
        cost_estimate=pl.CostEstimate(flops=8 * s * s * d + 6 * s * d * d, bytes_accessed=20 * s * d,
                                      transcendentals=s * s * 12),
        name="front")(length, tok, flag, cos, sin, condp, small, *[quarter(w) for w in ws])
    att, lse, vpre, vmid, b1, n1t, qkv = res[:7]
    return att, lse, vpre, vmid, b1, n1t, qkv, [r.reshape(-1, r.shape[-1]) for r in res[7:]]

def f32_rows_dot(row, weights):
    parts = split3(row)
    stack = jnp.concatenate(list(parts) + [jnp.zeros((5, row.shape[1]), f32)], axis=0).astype(bf16)
    return colsum(dot(stack, weights))


class Small:
    def __init__(self, place, scratch):
        self.p = place
        (self.ag, self.rows, self.ab, self.bs, self.bm, self.bb, self.bg, self.s1, self.r1, self.s2, self.r2) = scratch

    @staticmethod
    def widths(shape, d, ff, n_mod):
        groups = shape["fsdp"]
        part = n_mod // groups
        return -(-(d // groups) // 128) * 128, ff // groups, part if part % 128 == 0 else n_mod

    @staticmethod
    def scratch(shape, d, ff, n_mod):
        groups, lines = shape["fsdp"], shape["dp"]
        wide, fpart, gpart = Small.widths(shape, d, ff, n_mod)
        vm = lambda *dims: pltpu.VMEM(dims, f32)
        sem = pltpu.SemaphoreType.DMA
        return [vm(groups, 1, n_mod), vm(groups, 8, d), vm(groups, 1, ff), vm(lines, 8, wide), vm(lines, groups, 384),
                vm(lines, 1, fpart), vm(lines, groups, gpart), sem((groups, 3)), sem((groups, 3)), sem((lines, 4)),
                sem((lines, 4))]

    def peers(self):
        p = self.p
        return [(p.dp, xor(p.me, m)) for m in range(1, p.groups)] + [(xor(p.dp, m), p.me) for m in range(1, p.lines)]

    def copies(self, stage, m, arrived):
        p = self.p
        if stage == 1:
            bufs, ss, rs = (self.ag, self.rows, self.ab), self.s1, self.r1
            where, slot = (p.dp, xor(p.me, m)), xor(p.me, m) if arrived else p.me
        else:
            bufs, ss, rs = (self.bs, self.bm, self.bb, self.bg), self.s2, self.r2
            where, slot = (xor(p.dp, m), p.me), xor(p.dp, m) if arrived else p.dp
        return [remote(b.at[slot], b.at[slot], ss.at[m, i], rs.at[m, i], where) for i, b in enumerate(bufs)]

    def spread(self, stage):
        for m in range(1, self.p.groups if stage == 1 else self.p.lines):
            for c in self.copies(stage, m, False):
                c.start()

    def collect(self, stage):
        for m in range(1, self.p.groups if stage == 1 else self.p.lines):
            for c in self.copies(stage, m, True):
                c.wait_recv()

    def settle(self):
        for stage in (1, 2):
            for m in range(1, self.p.groups if stage == 1 else self.p.lines):
                for c in self.copies(stage, m, False):
                    c.wait_send()

    def first(self, sums, sb1, sums1, vec_pre, vec_mid, condp, meta, ada):
        me = self.p.me
        d = sums.shape[1]
        ggm, gb2, a2, s2, gga, st0, st1, st2 = (sums[i:i + 1] for i in range(8))
        a1, s1, gemb = (sums1[i:i + 1] for i in range(3))
        gain1, scale_a, gain2, scale_m = vec_pre[1:2], vec_pre[2:3], vec_mid[1:2], vec_mid[2:3]
        gm = jnp.concatenate([s1, a1 * gain1, gga, s2, a2 * gain2, ggm], axis=1)
        sig = 1.0 / (1.0 + jnp.exp(-condp))
        gc = f32_rows_dot(gm, ada) * (sig * (1.0 + condp * (1.0 - sig)))
        lane = lax.broadcasted_iota(jnp.int32, (1, 128), 1)
        total = lambda x: jnp.sum(x, axis=1, keepdims=True)
        stat = jnp.where(lane == 0, total(st0), jnp.where(lane == 1, total(st1), jnp.where(lane == 2, total(st2), meta)))
        tail = jnp.concatenate([gc, condp * sig, stat, jnp.zeros((1, d - 384), f32)], axis=1)
        self.ag[me] = gm
        self.ab[me] = sb1
        self.rows[me] = jnp.concatenate([(1.0 + scale_a) * a1, (1.0 + scale_m) * a2, gb2, gemb, tail,
                                         jnp.zeros((3, d), f32)], axis=0)
        self.spread(1)

    def second(self):
        p = self.p
        self.collect(1)
        d = self.rows.shape[2]
        wide, fpart, gpart = self.bs.shape[2], self.bb.shape[2], self.bg.shape[2]
        total = self.rows[0]
        for f in range(1, p.groups):
            total = total + self.rows[f]
        self.bs[p.dp] = pltpu.roll(total, (d - p.me * (d // p.groups)) % d, 1)[:, :wide]
        self.bm[p.dp] = jnp.concatenate([self.rows[f, 4:5, :384] for f in range(p.groups)], axis=0)
        cut = pl.ds(pl.multiple_of(p.me * fpart, 128), fpart)
        part = self.ab[0, :, cut]
        for f in range(1, p.groups):
            part = part + self.ab[f, :, cut]
        self.bb[p.dp] = part
        n_mod = self.ag.shape[2]
        cut = slice(None) if gpart == n_mod else pl.ds(pl.multiple_of(p.me * gpart, 128), gpart)
        self.bg[p.dp] = jnp.concatenate([self.ag[f, :, cut] for f in range(p.groups)], axis=0)
        self.spread(2)

    def third(self, norms_ref, gb1_ref, gada_ref, gbada_ref, table_ref, rms_ref, d):
        p = self.p
        self.collect(2)
        total, part = self.bs[0], self.bb[0]
        for z in range(1, p.lines):
            total = total + self.bs[z]
            part = part + self.bb[z]
        norms_ref[...] = total
        gb1_ref[...] = part
        mods = jnp.concatenate([self.bg[z] for z in range(p.lines)], axis=0)
        info = jnp.concatenate([self.bm[z] for z in range(p.lines)], axis=0)
        gcs, conds, stat = info[:, :128], info[:, 128:256], info[:, 256:384]
        highest = lax.Precision.HIGHEST
        gada_ref[...] = lax.dot_general(mods, conds, TN, precision=highest, preferred_element_type=f32)
        gbada_ref[...] = colsum(mods)
        ids = stat[:, 4:5].astype(jnp.int32)
        hot = (lax.broadcasted_iota(jnp.int32, (ids.shape[0], table_ref.shape[0]), 1) == ids).astype(f32)
        table_ref[...] = lax.dot_general(hot, gcs, TN, precision=highest, preferred_element_type=f32)
        stat = colsum(stat)
        rms_ref[...] = jnp.sqrt(stat / (stat[:, 3:4] * d))


def small_shapes(shape, d, ff, n_mod, table_rows):
    wide, fpart, gpart = Small.widths(shape, d, ff, n_mod)
    sd = lambda *dims: jax.ShapeDtypeStruct(dims, f32)
    return [sd(8, wide), sd(1, fpart), sd(gpart, 128), sd(1, gpart), sd(table_rows, 128), sd(1, 128)]


def small_results(shape, res, sizes):
    norms, gb1, gada, gbada, table, rms = res
    n_ada = sizes[5]
    if gada.shape[0] != n_ada:
        me = lax.axis_index("fsdp")
        gada = lax.dynamic_slice_in_dim(gada, me * n_ada, n_ada, axis=0)
        gbada = lax.dynamic_slice_in_dim(gbada, me * n_ada, n_ada, axis=1)
    g1, g2, gb2, gemb = (norms[i, :sizes[i]] for i in range(4))
    return g1, g2, gb2, gemb, gb1[0], gada, gbada[0], table, rms[0, :3]


def tail_kernel(shape, counts, rows, post, pairs, *refs):
    n = len(counts)
    (len_ref, q_ref, k_ref, v_ref, o_ref, g_ref, lse_ref, cos_ref, sin_ref, n1_ref, w_ref, tok_ref, flag_ref, gh1_ref,
     vpre_ref, vmid_ref, sums_ref, sb1_ref, condp_ref, meta_ref, ada_ref) = refs[:21]
    srcs = refs[21:20 + n]
    outs = refs[20 + n:21 + 2 * n]
    igrad_ref, reduced, small_out = outs[0], outs[1:1 + n], refs[21 + 2 * n:27 + 2 * n]
    dqs, dks, dvs, dqkv, gq, sums1 = refs[27 + 2 * n:33 + 2 * n]
    rscratch, sscratch = refs[33 + 2 * n:54 + 2 * n], refs[54 + 2 * n:]
    step, steps = pl.program_id(0), 2 * pairs + post
    p = Place(shape)
    r = Reduce(p, counts, ["rows"] + ["cols"] * (n - 2) + ["qkv"], list(srcs) + [gq], reduced, rscratch, 2, 2)
    small = Small(p, sscratch)

    @pl.when(step == 0)
    def _():
        r.greet(small.peers())
        r.begin(0)

    r.tick(2 * step)

    @pl.when(step < 2 * pairs)
    def _():
        pair, head = step // 2, step % 2

        def emit(*parts):
            for i, x in enumerate(parts):
                dqkv[i, pair] = x
            y = dot(n1_ref[...], jnp.concatenate(parts, axis=1)).astype(bf16)
            _, _, g, _, rr, c = gq.shape
            y = y.reshape(g, 2, 2, rr, c)
            for half in (0, 1):
                gq[2 * (pair // 2) + half, pair % 2] = y[:, half]

        attn_bwd_body(len_ref, q_ref, k_ref, v_ref, o_ref, g_ref, lse_ref, cos_ref, sin_ref, dqs, dks, dvs, rows,
                      pair, head, emit, lambda: r.tick(2 * step + 1))

    @pl.when(step >= 2 * pairs)
    def _():
        i = step - 2 * pairs
        m = tok_ref.shape[0]
        cut = pl.ds(pl.multiple_of(i * m, m), m)
        grads = [jnp.concatenate([dqkv[a, b, cut, :] for b in range(pairs)], axis=1) for a in range(3)]
        masked = flag_ref[...] == 1
        h0 = jnp.where(masked, vpre_ref[0:1, :], tok_ref[...].astype(f32))
        igrad_ref[...], new = post_rows(grads, h0, masked, gh1_ref[...], vpre_ref[1:2, :], vpre_ref[2:3, :], w_ref)
        sums1[...] = jnp.where(i == 0, new, sums1[...] + new)
        r.tick(2 * step + 1)

    @pl.when(step == steps - 1)
    def _():
        small.first(sums_ref[...], sb1_ref[...], sums1[...], vpre_ref[...], vmid_ref[...], condp_ref[...], meta_ref[...],
                    ada_ref[...])
        last = max(r.ticks, 2 * steps)
        marks = [2 * steps, min(2 * steps + SPLIT[0], last), min(2 * steps + SPLIT[1], last), last]
        for n in range(3):
            @pl.loop(marks[n], marks[n + 1])
            def _(t):
                r.tick(t)
            if n == 0:
                small.second()
            if n == 1:
                small.third(*small_out, sums1.shape[1])
        r.drain()
        small.settle()


SPLIT = (3, 8)


def tail_call(shape, length, qkv, att, gatt, lse, cos, sin, n1t, w, tok, flag, gh1, vpre, vmid, sums, sb1, condp, meta,
              ada, grads, table_rows, rows=256):
    groups = shape["fsdp"]
    s, d3 = qkv.shape
    d = d3 // 3
    pairs = d // 128
    r, c = 2 * grads[0].shape[-2], grads[0].shape[-1]
    post = 256 if r % 32 == 0 else 128
    blocks = s // post
    steps = 2 * pairs + blocks
    ff, n_mod = sb1.shape[1], ada.shape[0]
    counts = [g.shape[0] for g in grads] + [pairs]
    pair = lambda i: jnp.minimum(i // 2, pairs - 1)
    blk = lambda i: jnp.maximum(i - 2 * pairs, 0)
    once = pl.Buffered(1)
    col = lambda base: pl.BlockSpec((s, 128), lambda i: (0, base + pair(i)))
    whole = lambda a: pl.BlockSpec(a.shape, lambda i: (0,) * a.ndim, pipeline_mode=once)
    row = lambda cc: pl.BlockSpec((post, cc), lambda i: (blk(i), 0))
    sd = jax.ShapeDtypeStruct
    shard = d // groups
    red = [sd((shard * (g.shape[0] // 2), d), bf16) if i == 0 else sd((shard, d * (g.shape[0] // 2)), bf16)
           for i, g in enumerate(grads)] + [sd((shard, d3), bf16)]
    smalls = small_shapes(shape, d, ff, n_mod, table_rows)
    const = lambda x: pl.BlockSpec(x.shape, lambda i: (0, 0), pipeline_mode=once)
    res = pl.pallas_call(
        functools.partial(tail_kernel, shape, counts, rows, blocks, pairs), grid=(steps,),
        in_specs=[pl.BlockSpec(memory_space=pltpu.SMEM), col(0), col(pairs), col(2 * pairs), col(0), col(0), whole(lse),
                  whole(cos), whole(sin), whole(n1t), whole(w), row(d), row(1), row(d)]
        + [whole(x) for x in (vpre, vmid, sums, sb1, condp, meta, ada)] + [ANY] * len(grads),
        out_specs=[row(d)] + [ANY] * len(red) + [const(x) for x in smalls],
        out_shape=[sd((s, d), bf16)] + red + smalls,
        scratch_shapes=[pltpu.VMEM((128, s), f32), pltpu.VMEM((s, 128), f32), pltpu.VMEM((s, 128), f32),
                        pltpu.VMEM((3, pairs, s, 128), bf16), pltpu.VMEM((pairs, 2, groups, 2, r // 2, c), bf16),
                        pltpu.VMEM((8, d), f32)]
        + Reduce.scratch(sum(counts), groups, r, c) + Small.scratch(shape, d, ff, n_mod),
        compiler_params=pltpu.CompilerParams(collective_id=3, has_side_effects=True, vmem_limit_bytes=65000 * 1024),
        cost_estimate=pl.CostEstimate(flops=30 * s * s * d, bytes_accessed=40 * s * d, transcendentals=s * s * 12),
        name="tail")(length, qkv, qkv, qkv, att, gatt, lse, cos, sin, n1t, w, tok, flag, gh1, vpre, vmid, sums, sb1, condp,
                     meta, ada, *grads)
    return res[0], res[1:1 + len(red)], res[1 + len(red):]


def widen_kernel(*refs):
    n = len(refs) // 2
    for x, y in zip(refs[:n], refs[n:]):
        y[...] = x[...].astype(f32)


def widen(arrays, pieces):
    specs = [pl.BlockSpec((a.shape[0], a.shape[1] // pieces), lambda i: (0, i)) for a in arrays]
    return pl.pallas_call(
        widen_kernel, grid=(pieces,), in_specs=specs, out_specs=specs,
        out_shape=[jax.ShapeDtypeStruct(a.shape, f32) for a in arrays],
        cost_estimate=pl.CostEstimate(flops=0, bytes_accessed=6 * sum(a.size for a in arrays), transcendentals=0),
        name="widen")(*arrays)
from jax.sharding import PartitionSpec as P

highest = lax.Precision.HIGHEST


def rotary_tables(length):
    half = HD // 2
    rate = 1.0 / 10000.0 ** (jnp.arange(half, dtype=f32) * 2.0 / HD)
    angle = jnp.arange(length, dtype=f32)[:, None] * rate[None, :]
    angle = jnp.concatenate([angle] * (128 // half), axis=-1)
    sign = jnp.where(jnp.arange(128) % HD < half, -1.0, 1.0)
    return jnp.cos(angle), jnp.sin(angle) * sign


def per_device(shape, tokens, hidden_token_indicator, lengths, time_ids, cotangent, gain_one, w_qkv, w_out, gain_two,
               w_fc1, b_fc1, w_fc2, b_fc2, w_ada, b_ada, mask_embed, time_table):
    groups = shape["fsdp"]
    s, d = tokens.shape[1:]
    ff = b_fc1.shape[0] * groups
    tok, cot = tokens[0], cotangent[0]
    flag = hidden_token_indicator.reshape(s, 1)
    sizes = [v.shape[0] for v in (gain_one, gain_two, b_fc2, mask_embed, b_fc1, b_ada)]
    cond_pre = lax.dynamic_slice_in_dim(time_table, time_ids[0], 1, axis=0)
    cos, sin = rotary_tables(s)
    att, lse, vec_pre, vec_mid, b1, n1, qkv, (ada_all, qkv_all, out_all, fc1_all, fc2_all) = front_call(
        shape, lengths, tok, flag, cos, sin, cond_pre, small_row((gain_one, gain_two, b_fc2, mask_embed, b_fc1, b_ada)),
        [w_ada, w_qkv, w_out, w_fc1, w_fc2], sizes)
    out, gh1, gatt, n2, act, gm, gpre, gap, sums, gb1 = mid_call(
        lengths, att, tok, flag, cot, vec_mid, b1, out_all, fc1_all, fc2_all)
    g_fc2 = wgrad_rows(act, gm, groups)
    g_fc1 = wgrad_cols(n2, gpre, groups)
    g_out = wgrad_cols(att, gap, groups)
    meta = jnp.concatenate([jnp.zeros((3,), f32), lengths.astype(f32), time_ids.astype(f32), jnp.zeros((123,), f32)])[None]
    igrad, (r_fc2, r_fc1, r_out, r_qkv), smalls = tail_call(
        shape, lengths, qkv, att, gatt, lse, cos, sin, n1, qkv_all, tok, flag, gh1, vec_pre, vec_mid, sums, gb1, cond_pre,
        meta, ada_all, [g_fc2, g_fc1, g_out], time_table.shape[0])
    g1, g2, gb2, gemb, gb1, g_ada, gbada, table, rms = small_results(shape, smalls, sizes)
    r_fc2, r_fc1, r_out, r_qkv = widen([r_fc2, r_fc1, r_out, r_qkv], d // 256)
    return (out[None], igrad[None], g1, r_qkv, r_out, g2, r_fc1, gb1, r_fc2, gb2, g_ada, gbada, gemb, table, rms)


def solution(mesh):
    both = ("dp", "fsdp")
    f1, f2 = P("fsdp"), P("fsdp", None)
    placed = (P(both, None, None), P(both, None), P(both), P(both), P(both, None, None), f1, f2, f2, f1, f2, f1, f2, f1,
              f2, f1, f1, P())
    outs = (P(both, None, None), P(both, None, None), f1, f2, f2, f1, f2, f1, f2, f1, f2, f1, f1, P(), P())
    return jax.shard_map(functools.partial(per_device, dict(mesh.shape)), mesh=mesh, in_specs=placed, out_specs=outs,
                         check_vma=False)
```

```python
import functools, math
import jax, jax.numpy as jnp
from jax import lax
from jax.experimental import pallas as pl
from jax.experimental.pallas import tpu as pltpu

HD = 64
EPS = 1e-5
LOG2E = math.log2(math.e)
QSCALE = LOG2E * HD ** -0.5
f32, bf16 = jnp.float32, jnp.bfloat16
NT = (((1,), (1,)), ((), ()))
NN = (((1,), (0,)), ((), ()))
TN = (((0,), (0,)), ((), ()))

def dot(a, b, dims=NN):
    return lax.dot_general(a, b, dims, preferred_element_type=f32)

def norm_parts(x):
    mean = jnp.mean(x, axis=-1, keepdims=True)
    cen = x - mean
    rs = lax.rsqrt(jnp.mean(cen * cen, axis=-1, keepdims=True) + EPS)
    return cen * rs, rs

def swap_halves(u):
    lane = lax.broadcasted_iota(jnp.int32, u.shape, 1)
    return jnp.where(lane % HD < HD // 2, pltpu.roll(u, 96, 1), pltpu.roll(u, 32, 1))

def attn_fwd_body(len_ref, q_ref, k_ref, v_ref, o_ref, lse_ref, rows, p):
    s = q_ref.shape[0]
    length = len_ref[0]
    lane = lax.broadcasted_iota(jnp.int32, (s, 128), 1)
    pos = lax.broadcasted_iota(jnp.int32, (s, 128), 0)
    lane_q = lax.broadcasted_iota(jnp.int32, (rows, 128), 1)
    k = k_ref[...].astype(f32)
    v = v_ref[...].astype(f32)
    kx, vx = [], []
    for h in (0, 1):
        extra = HD * (1 - h)
        mine = (lane >= HD) if h else (lane < HD)
        bias = jnp.where(pos >= length, -1e30, 0.0)
        kx.append(jnp.where(mine, k, jnp.where(lane == extra, bias, 0.0)).astype(bf16))
        vx.append(jnp.where(mine, v, jnp.where(lane == extra, 1.0, 0.0)).astype(bf16))
    for b in range(s // rows):
        q = q_ref[b * rows:(b + 1) * rows, :].astype(f32)
        outs, lses = [], []
        for h in (0, 1):
            extra = HD * (1 - h)
            mine = (lane_q >= HD) if h else (lane_q < HD)
            qx = jnp.where(mine, q, jnp.where(lane_q == extra, 1.0, 0.0)).astype(bf16)
            sc = dot(qx, kx[h], NT)
            m = jnp.max(sc, axis=1, keepdims=True)
            pr = jnp.exp2(sc - m).astype(bf16)
            o = dot(pr, vx[h])
            tot = o[:, extra:extra + 1]
            outs.append(o * (1.0 / tot))
            lses.append(m + jnp.log(tot) * LOG2E)
        o_ref[b * rows:(b + 1) * rows, :] = jnp.where(lane_q < HD, outs[0], outs[1]).astype(bf16)
        old = jnp.where(p == 0, 0.0, lse_ref[b * rows:(b + 1) * rows, :])
        lse_ref[b * rows:(b + 1) * rows, :] = jnp.where(
            lane_q == 2 * p, lses[0], jnp.where(lane_q == 2 * p + 1, lses[1], old))

def split3(x):
    hi = x.astype(bf16).astype(f32)
    r = x - hi
    mid = r.astype(bf16).astype(f32)
    return hi, mid, r - mid

def attn_bwd_body(len_ref, q_ref, k_ref, v_ref, o_ref, g_ref, lse_ref, cos_ref, sin_ref,
                  dqs, dks, dvs, rows, p, h, emit, pause):
    s = q_ref.shape[0]
    length = len_ref[0]
    lane = lax.broadcasted_iota(jnp.int32, (s, 128), 1)
    pos = lax.broadcasted_iota(jnp.int32, (s, 128), 0)
    lane_q = lax.broadcasted_iota(jnp.int32, (rows, 128), 1)
    e = HD * (1 - h)
    mine, mine_q = lane // HD == h, lane_q // HD == h
    k = k_ref[...].astype(f32)
    v = v_ref[...].astype(f32)
    ones = jnp.where((lane >= e) & (lane < e + 3), 1.0, 0.0)
    bias = jnp.where(pos >= length, -1e30, 0.0)
    kx = jnp.where(mine, k, jnp.where(lane == e + 3, bias, ones)).astype(bf16)
    vx = jnp.where(mine, v, ones).astype(bf16)
    kt = jnp.where(mine, k, 0.0).T.astype(bf16)
    dk = jnp.zeros((s, 128), f32)
    dv = jnp.zeros((s, 128), f32)
    for b in range(s // rows):
        sl = slice(b * rows, (b + 1) * rows)
        qb = q_ref[sl, :]
        gb = g_ref[sl, :]
        q = qb.astype(f32)
        g = gb.astype(f32)
        lse = jnp.sum(jnp.where(lane_q == 2 * p + h, lse_ref[sl, :], 0.0), axis=1, keepdims=True)
        dd = jnp.sum(jnp.where(mine_q, g * o_ref[sl, :].astype(f32), 0.0), axis=1, keepdims=True)
        l0, l1, l2 = split3(-lse)
        d0, d1, d2 = split3(-dd)
        qx = jnp.where(mine_q, q, jnp.where(lane_q == e, l0, jnp.where(lane_q == e + 1, l1, jnp.where(
            lane_q == e + 2, l2, jnp.where(lane_q == e + 3, 1.0, 0.0))))).astype(bf16)
        gx = jnp.where(mine_q, g, jnp.where(lane_q == e, d0, jnp.where(lane_q == e + 1, d1, jnp.where(
            lane_q == e + 2, d2, 0.0)))).astype(bf16)
        pt = jnp.exp2(dot(kx, qx, NT))
        dst = (pt * dot(vx, gx, NT)).astype(bf16)
        dv = dv + dot(pt.astype(bf16), gb)
        dk = dk + dot(dst, qb)
        dqt = dot(kt, dst)
        dqs[:, sl] = jnp.where(h == 0, dqt, dqs[:, sl] + dqt)
        if b == s // rows // 2 - 1:
            pause()
    @pl.when(h == 0)
    def _():
        dks[...] = dk
        dvs[...] = dv
    @pl.when(h == 1)
    def _():
        cos, sin = cos_ref[...], sin_ref[...]
        dq = dqs[...].T * (HD ** -0.5)
        dkk = jnp.where(lane < HD, dks[...], dk) * (1.0 / LOG2E)
        emit((dq * cos - swap_halves(dq) * sin).astype(bf16), (dkk * cos - swap_halves(dkk) * sin).astype(bf16),
             jnp.where(lane < HD, dvs[...], dv).astype(bf16))


def gelu_both(v):
    a, b = 0.7978845608028654, 0.044715
    v2 = v * v
    t = jnp.tanh(a * v * (1.0 + b * v2))
    half = 0.5 + 0.5 * t
    return v * half, half + (0.5 * a) * v * (1.0 - t * t) * (1.0 + 3.0 * b * v2)

def colsum(x):
    return jnp.sum(x, axis=0, keepdims=True)

def mid_kernel(len_ref, att_ref, tok_ref, flag_ref, cot_ref, vec_ref, b1_ref, wo_ref, w1_ref, w2_ref,
               out_ref, gh1_ref, gatt_ref, n2_ref, act_ref, gm_ref, gpre_ref, gap_ref, sum_ref, sb1_ref,
               gp_s, *, cut):
    i = pl.program_id(0)
    rows, d = att_ref.shape
    ff = w1_ref.shape[1]
    emb, gain, scale, shift, gate_a, gate_m, b2 = (vec_ref[r:r + 1, :] for r in range(7))
    h0 = jnp.where(flag_ref[...] == 1, emb, tok_ref[...].astype(f32))
    ap = dot(att_ref[...], wo_ref[...])
    br_a = gate_a * ap
    h1 = h0 + br_a
    n, rs = norm_parts(h1)
    n2 = (n * gain * (1.0 + scale) + shift).astype(bf16)
    n2_ref[...] = n2
    mp = jnp.zeros((rows, d), f32) + b2
    for j in range(ff // cut):
        sl = slice(j * cut, (j + 1) * cut)
        act, gp = gelu_both(dot(n2, w1_ref[:, sl]) + b1_ref[:, sl])
        act = act.astype(bf16)
        act_ref[:, sl] = act
        gp_s[:, sl] = gp
        mp = mp + dot(act, w2_ref[sl, :])
    br_m = gate_m * mp
    bo = h1 + br_m
    out_ref[...] = bo.astype(bf16)
    pos = lax.broadcasted_iota(jnp.int32, (rows, 1), 0) + i * rows
    valid = jnp.where(pos < len_ref[0], 1.0, 0.0)
    cot = cot_ref[...].astype(f32)
    gm = (gate_m * cot).astype(bf16)
    gm_ref[...] = gm
    gn2 = jnp.zeros((rows, d), f32)
    sb1 = []
    for j in range(ff // cut):
        sl = slice(j * cut, (j + 1) * cut)
        gpre = (dot(gm, w2_ref[sl, :], NT) * gp_s[:, sl]).astype(bf16)
        gpre_ref[:, sl] = gpre
        sb1.append(colsum(gpre.astype(f32)))
        gn2 = gn2 + dot(gpre, w1_ref[:, sl], NT)
    e = gn2 * (gain * (1.0 + scale))
    gh1 = cot + rs * (e - jnp.mean(e, axis=1, keepdims=True) - n * jnp.mean(e * n, axis=1, keepdims=True))
    gh1_ref[...] = gh1
    gap = (gate_a * gh1).astype(bf16)
    gap_ref[...] = gap
    gatt_ref[...] = dot(gap, wo_ref[...], NT).astype(bf16)
    new = jnp.concatenate([
        colsum(cot * mp), colsum(gm.astype(f32)), colsum(gn2 * n), colsum(gn2), colsum(gh1 * ap),
        colsum(valid * bo * bo), colsum(valid * br_a * br_a), colsum(valid * br_m * br_m)], axis=0)
    sb1 = jnp.concatenate(sb1, axis=1)
    @pl.when(i == 0)
    def _():
        sum_ref[...] = new
        sb1_ref[...] = sb1
    @pl.when(i > 0)
    def _():
        sum_ref[...] += new
        sb1_ref[...] += sb1

def mid_call(length, att, tok, flag, cot, vec, b1, wo, w1, w2, rows=256, cut=768):
    s, d = tok.shape
    ff = w1.shape[1]
    row = lambda c: pl.BlockSpec((rows, c), lambda i: (i, 0))
    whole = lambda a: pl.BlockSpec(a.shape, lambda i: (0, 0))
    sd = jax.ShapeDtypeStruct
    return pl.pallas_call(
        functools.partial(mid_kernel, cut=cut), grid=(s // rows,),
        in_specs=[pl.BlockSpec(memory_space=pltpu.SMEM), row(d), row(d), row(1), row(d), whole(vec), whole(b1),
                  whole(wo), whole(w1), whole(w2)],
        out_specs=[row(d), row(d), row(d), row(d), row(ff), row(d), row(ff), row(d),
                   pl.BlockSpec((8, d), lambda i: (0, 0)), pl.BlockSpec((1, ff), lambda i: (0, 0))],
        out_shape=[sd((s, d), bf16), sd((s, d), f32), sd((s, d), bf16), sd((s, d), bf16), sd((s, ff), bf16),
                   sd((s, d), bf16), sd((s, ff), bf16), sd((s, d), bf16), sd((8, d), f32), sd((1, ff), f32)],
        scratch_shapes=[pltpu.VMEM((rows, ff), f32)],
        compiler_params=pltpu.CompilerParams(vmem_limit_bytes=60000 * 1024),
        cost_estimate=pl.CostEstimate(flops=2 * s * d * (2 * d + 4 * ff), bytes_accessed=30 * s * d,
                                      transcendentals=s * ff),
        name="mid")(length, att, tok, flag, cot, vec, b1, wo, w1, w2)

def post_rows(grads, h0, masked, gh1, gain, scale, w_ref):
    d = h0.shape[1]
    n, rs = norm_parts(h0)
    gn1 = sum(dot(g, w_ref[:, i * d:(i + 1) * d], NT) for i, g in enumerate(grads))
    e = gn1 * (gain * (1.0 + scale))
    gh0 = gh1 + rs * (e - jnp.mean(e, axis=1, keepdims=True) - n * jnp.mean(e * n, axis=1, keepdims=True))
    sums = jnp.concatenate([colsum(gn1 * n), colsum(gn1), colsum(jnp.where(masked, gh0, 0.0)),
                            jnp.zeros((5, d), f32)], axis=0)
    return jnp.where(masked, 0.0, gh0).astype(bf16), sums

MESH = pl.DeviceIdType.MESH


def flip(i, b):
    return i + 2 ** b * (1 - 2 * ((i // 2 ** b) % 2))


def xor(i, mask):
    b = 0
    while mask >> b:
        if (mask >> b) & 1:
            i = flip(i, b)
        b += 1
    return i


def subsets(bits):
    masks = [0]
    for b in bits:
        masks = masks + [m | (1 << b) for m in masks]
    return masks


def log2(n):
    return n.bit_length() - 1


class Place:
    def __init__(self, shape):
        self.groups, self.lines = shape["fsdp"], shape["dp"]
        self.bits = log2(self.groups)
        self.orders = [list(range(self.bits)), list(range(self.bits))[::-1]]
        self.me = lax.axis_index("fsdp")
        self.dp = lax.axis_index("dp")
        self.core = self.dp % 2
        self.partner = flip(self.dp, 0)


def remote(src, dst, ssem, rsem, where):
    return pltpu.make_async_remote_copy(src_ref=src, dst_ref=dst, send_sem=ssem, recv_sem=rsem, device_id=where,
                                        device_id_type=MESH)


class Gather:
    def __init__(self, place, ins, outs, sems):
        self.p, self.ins, self.outs = place, ins, outs
        self.ss, self.rs, self.fs, self.fr, self.os, self.orr = sems

    @staticmethod
    def scratch(count, groups):
        a = pltpu.SemaphoreType.DMA((count, 2, groups - 1))
        b = pltpu.SemaphoreType.DMA((count,))
        return [a, a, a, a, b, b]

    def send(self, w, color, t, mask):
        p = self.p
        order = p.orders[color]
        e = 2 ** t - 1 + subsets(order[:t]).index(mask)
        piece = p.core * 2 + color
        blk = xor(p.me, mask)
        src = self.ins[w].at[piece] if mask == 0 else self.outs[w].at[blk, piece]
        return remote(src, self.outs[w].at[blk, piece], self.ss.at[w, color, e], self.rs.at[w, color, e],
                      (p.dp, flip(p.me, order[t])))

    def arrival(self, w, color, t, mask):
        p = self.p
        order = p.orders[color]
        e = 2 ** t - 1 + subsets(order[:t]).index(mask)
        got = self.outs[w].at[xor(p.me, mask | (1 << order[t])), p.core * 2 + color]
        return e, got

    def landed(self, w, color, e, got):
        return remote(got, got, self.ss.at[w, color, e], self.rs.at[w, color, e], (self.p.partner, self.p.me))

    def forward(self, w, color, e, got):
        return remote(got, got, self.fs.at[w, color, e], self.fr.at[w, color, e], (self.p.partner, self.p.me))

    def own(self, w):
        p = self.p
        return remote(self.ins[w], self.outs[w].at[p.me], self.os.at[w], self.orr.at[w], (p.partner, p.me))

    def start(self, w):
        for t in range(self.p.bits):
            for color in (0, 1):
                self.send(w, color, t, 0).start()
        self.own(w).start()

    def after(self, w, t):
        for color in (0, 1):
            order = self.p.orders[color]
            for mask in subsets(order[:t]):
                e, got = self.arrival(w, color, t, mask)
                self.landed(w, color, e, got).wait_recv()
                for later in range(t + 1, self.p.bits):
                    self.send(w, color, later, mask | (1 << order[t])).start()
                self.forward(w, color, e, got).start()

    def finish(self, w):
        p = self.p
        for color in (0, 1):
            order = p.orders[color]
            for t in range(p.bits):
                for mask in subsets(order[:t]):
                    e, got = self.arrival(w, color, t, mask)
                    other = self.outs[w].at[xor(p.me, mask | (1 << order[t])), (1 - p.core) * 2 + color]
                    self.forward(w, color, e, other).wait_recv()
                    self.forward(w, color, e, got).wait_send()
                    self.send(w, color, t, mask).wait_send()
        self.own(w).wait()


class Direct:
    def __init__(self, place, src, out, sems):
        self.p, self.src, self.out = place, src, out
        self.ss, self.rs = sems

    @staticmethod
    def scratch(groups):
        return [pltpu.SemaphoreType.DMA((groups,))] * 2

    def copy(self, m, arrived):
        p = self.p
        where = (p.partner, p.me) if m == 0 else (p.dp, xor(p.me, m))
        slot = xor(p.me, m) if arrived else p.me
        return remote(self.src, self.out.at[slot], self.ss.at[m], self.rs.at[m], where)

    def start(self):
        for m in range(self.p.groups):
            self.copy(m, False).start()

    def finish(self):
        for m in range(self.p.groups):
            self.copy(m, True).wait_recv()
            self.copy(m, False).wait_send()


def greet(devices):
    barrier = pltpu.get_barrier_semaphore()
    for where in devices:
        pl.semaphore_signal(barrier, inc=1, device_id=where, device_id_type=MESH)
    pl.semaphore_wait(barrier, len(devices))


def gather_peers(p, everyone):
    masks = range(1, p.groups) if everyone else [1 << b for b in range(p.bits)]
    return [(p.partner, p.me)] + [(p.dp, xor(p.me, m)) for m in masks]


def quarter(w):
    return w.reshape(4, w.shape[0] // 4, w.shape[1])


def gather_shape(w, groups):
    return jax.ShapeDtypeStruct((groups, 4, w.shape[0] // 4, w.shape[1]), w.dtype)


ANY = pl.BlockSpec(memory_space=pl.ANY)


class Reduce:
    def __init__(self, place, counts, kinds, srcs, outs, scratch, lag, gap):
        self.p, self.counts, self.kinds, self.srcs, self.outs = place, counts, kinds, srcs, outs
        (self.own, self.cb, self.xb, self.zb, self.mb, self.u2, self.fin,
         self.load, self.cs, self.cr, self.xs, self.xr, self.zs, self.zr, self.ms, self.mr, self.fs, self.fr,
         self.ps, self.pr, self.st) = scratch
        p = place
        self.total = sum(counts)
        self.n = p.lines // 2
        self.zi = p.dp // 2
        left = self.zi // (self.n // 2)
        self.e = self.zi * (1 - left) + (self.n - 1 - self.zi) * left
        step = 2 * (1 - 2 * left)
        self.inner = (p.dp + step, p.me)
        self.outer = (p.dp - step, p.me)
        self.last = self.n // 2 - 1
        self.stages = ([self.begin, self.core_add] + [functools.partial(self.group_add, t) for t in range(p.bits)]
                       + [functools.partial(self.climb, j) for j in range(1, self.last + 1)] + [self.middle]
                       + [functools.partial(self.descend, j) for j in range(self.last - 1, -1, -1)])
        self.lags = [0, 1] + [1 + lag * (i + 1) for i in range(len(self.stages) - 2)]
        self.early = self.total - counts[-1]
        self.gap = gap
        self.ticks = self.total + gap + self.lags[-1]

    @staticmethod
    def scratch(total, groups, rows, cols):
        sem = pltpu.SemaphoreType.DMA
        vm = lambda *lead: pltpu.VMEM((total,) + lead + (rows // 2, cols), bf16)
        one = sem((total,))
        line = pltpu.VMEM((total, rows, cols), bf16)
        return [vm(groups, 2), vm(groups, 2), vm(2, groups - 1), line, line, line, line,
                one, one, one, sem((total, 2, groups - 1)), sem((total, 2, groups - 1)),
                one, one, one, one, one, one, sem((total, 3)), sem((total, 3)), sem((total, 3))]

    def greet(self, peers):
        p = self.p
        barrier = pltpu.get_barrier_semaphore()
        for where in peers:
            pl.semaphore_signal(barrier, inc=1, device_id=where, device_id_type=MESH)
        pl.semaphore_wait(barrier, len(peers))

    def source(self, k, fn):
        base = 0
        for i, count in enumerate(self.counts):
            @pl.when((k >= base) & (k < base + count))
            def _(i=i, base=base):
                fn(i, k - base)
            base += count

    def targets(self, k, i, j, core):
        rows, cols = self.fin.shape[1:]
        out, fin = self.outs[i], self.fin.at[k]
        if self.kinds[i] == "rows":
            cut = pl.ds(pl.multiple_of(core * cols, cols), cols)
            return [(fin, out.at[pl.ds(pl.multiple_of(j * rows, rows), rows), cut])]
        down = pl.ds(pl.multiple_of((j % 2) * rows, rows), rows)
        if self.kinds[i] == "cols":
            return [(fin, out.at[down, pl.ds(pl.multiple_of((2 * (j // 2) + core) * cols, cols), cols)])]
        width = out.shape[1] // 3
        pair = 2 * (j // 2) + core
        return [(fin.at[:, part * 128:(part + 1) * 128],
                 out.at[down, pl.ds(pl.multiple_of(part * width + pair * 128, 128), 128)]) for part in range(3)]

    def load_copy(self, k, src):
        return pltpu.make_async_copy(src.at[self.p.core], self.own.at[k], self.load.at[k])

    def core_copy(self, k, src):
        p = self.p
        return remote(src.at[1 - p.core], self.cb.at[k], self.cs.at[k], self.cr.at[k], (p.partner, p.me))

    def begin(self, k):
        def go(i, j):
            self.core_copy(k, self.srcs[i].at[j]).start()
            self.load_copy(k, self.srcs[i].at[j]).start()
        self.source(k, go)

    def slot(self, order, t, mask):
        base = sum(self.p.groups >> (u + 1) for u in range(t))
        return base + subsets(order[t + 1:]).index(mask)

    def group_copy(self, k, color, t, mask):
        p = self.p
        order = p.orders[color]
        i = self.slot(order, t, mask)
        return remote(self.own.at[k, xor(p.me, (1 << order[t]) | mask), color], self.xb.at[k, color, i],
                      self.xs.at[k, color, i], self.xr.at[k, color, i], (p.dp, flip(p.me, order[t])))

    def group_send(self, k, t):
        for color in (0, 1):
            for mask in subsets(self.p.orders[color][t + 1:]):
                self.group_copy(k, color, t, mask).start()

    def core_add(self, k):
        self.load_copy(k, self.srcs[0].at[0]).wait()
        self.core_copy(k, self.srcs[0].at[0]).wait_recv()
        for f in range(self.p.groups):
            for color in (0, 1):
                self.own[k, f, color] = (self.own[k, f, color].astype(f32) + self.cb[k, f, color].astype(f32)).astype(bf16)
        self.group_send(k, 0)

    def group_add(self, t, k):
        p = self.p
        for color in (0, 1):
            order = p.orders[color]
            for mask in subsets(order[t + 1:]):
                self.group_copy(k, color, t, mask).wait_recv()
                blk, i = xor(p.me, mask), self.slot(order, t, mask)
                total = self.own[k, blk, color].astype(f32) + self.xb[k, color, i].astype(f32)
                if t == p.bits - 1:
                    self.u2[k, self.part(color)] = total.astype(bf16)
                else:
                    self.own[k, blk, color] = total.astype(bf16)
        if t < p.bits - 1:
            self.group_send(k, t + 1)
        else:
            @pl.when(self.e == 0)
            def _():
                (self.climb_copy(k) if self.last > 0 else self.middle_copy(k)).start()

    def part(self, color):
        half = self.u2.shape[1] // 2
        return slice(color * half, (color + 1) * half)

    def climb_copy(self, k):
        return remote(self.u2.at[k], self.zb.at[k], self.zs.at[k], self.zr.at[k], self.inner)

    def middle_copy(self, k):
        return remote(self.u2.at[k], self.mb.at[k], self.ms.at[k], self.mr.at[k], self.inner)

    def climb(self, j, k):
        @pl.when(self.e == j)
        def _():
            self.climb_copy(k).wait_recv()
            for color in (0, 1):
                total = self.u2[k, self.part(color)].astype(f32) + self.zb[k, self.part(color)].astype(f32)
                self.u2[k, self.part(color)] = total.astype(bf16)
            (self.middle_copy(k) if j == self.last else self.climb_copy(k)).start()

    def share_copy(self, k):
        return remote(self.fin.at[k], self.fin.at[k], self.fs.at[k], self.fr.at[k], self.outer)

    def share_wait(self, k):
        return remote(self.fin.at[k], self.fin.at[k], self.fs.at[k], self.fr.at[k], self.inner)

    def out_copies(self, k, i, j):
        p = self.p
        mine, other = self.targets(k, i, j, p.core), self.targets(k, i, j, 1 - p.core)
        sent = [remote(s, d, self.ps.at[k, n], self.pr.at[k, n], (p.partner, p.me)) for n, (s, d) in enumerate(mine)]
        kept = [pltpu.make_async_copy(s, d, self.st.at[k, n]) for n, (s, d) in enumerate(mine)]
        return sent, kept, other

    def done(self, k):
        def go(i, j):
            sent, kept, _ = self.out_copies(k, i, j)
            for c in sent + kept:
                c.start()
        self.source(k, go)

    def retire(self, k):
        p = self.p
        def go(i, j):
            sent, kept, other = self.out_copies(k, i, j)
            for n, c in enumerate(sent):
                c.wait_send()
                s, d = other[n]
                remote(s, d, self.ps.at[k, n], self.pr.at[k, n], (p.partner, p.me)).wait_recv()
            for c in kept:
                c.wait()
        self.source(k, go)

    def middle(self, k):
        @pl.when(self.e == self.last)
        def _():
            self.middle_copy(k).wait_recv()
            for color in (0, 1):
                total = self.u2[k, self.part(color)].astype(f32) + self.mb[k, self.part(color)].astype(f32)
                self.fin[k, self.part(color)] = total.astype(bf16)
            if self.last > 0:
                self.share_copy(k).start()
            self.done(k)

    def descend(self, j, k):
        @pl.when(self.e == j)
        def _():
            self.share_wait(k).wait_recv()
            if j > 0:
                self.share_copy(k).start()
            self.done(k)

    def tick(self, t):
        for s in range(len(self.stages) - 1, 0, -1):
            k = t - self.lags[s]
            @pl.when((k >= 0) & (k < self.total + self.gap) & ((k < self.total - self.gap) | (k >= self.total)))
            def _(s=s, k=k):
                self.stages[s](k - self.gap * (k // self.total))
        @pl.when(t + 1 < self.early)
        def _():
            self.begin(t + 1)
        @pl.when((t >= self.early) & (t < self.total + self.gap) & ((t < self.total - self.gap) | (t >= self.total)))
        def _():
            self.begin(t - self.gap * (t // self.total))

    def drain(self):
        p = self.p
        @pl.loop(0, self.total)
        def _(k):
            self.core_copy(k, self.srcs[0].at[0]).wait_send()
            for color in (0, 1):
                for t in range(p.bits):
                    for mask in subsets(p.orders[color][t + 1:]):
                        self.group_copy(k, color, t, mask).wait_send()
            @pl.when(self.e == self.last)
            def _():
                self.middle_copy(k).wait_send()
            @pl.when(self.e < self.last)
            def _():
                self.climb_copy(k).wait_send()
            @pl.when(self.e > 0)
            def _():
                self.share_copy(k).wait_send()
            self.retire(k)


def wgrad_cols_kernel(a_ref, b_ref, o_ref):
    y = dot(a_ref[...], b_ref[...], TN).astype(bf16)
    _, _, g, _, r, c = o_ref.shape
    for core in (0, 1):
        z = y[:, core * c:(core + 1) * c].reshape(g, 2, 2, r, c)
        for half in (0, 1):
            o_ref[half, core] = z[:, half]


def wgrad_cols(a, b, groups):
    s, m = a.shape
    n = b.shape[1]
    r, c = m // groups // 4, m // 2
    return pl.pallas_call(
        wgrad_cols_kernel, grid=(n // m,),
        in_specs=[pl.BlockSpec((s, m), lambda i: (0, 0)), pl.BlockSpec((s, m), lambda i: (0, i))],
        out_specs=pl.BlockSpec((2, 2, groups, 2, r, c), lambda i: (i, 0, 0, 0, 0, 0)),
        out_shape=jax.ShapeDtypeStruct((2 * n // m, 2, groups, 2, r, c), bf16),
        cost_estimate=pl.CostEstimate(flops=2 * s * m * n, bytes_accessed=2 * (s * (m + n) + m * n),
                                      transcendentals=0), name="wgrad_cols")(a, b)


def wgrad_rows_kernel(a_ref, b_ref, o_ref):
    y = dot(a_ref[...], b_ref[...], TN).astype(bf16)
    q, _, _, _, r, c = o_ref.shape
    for core in (0, 1):
        o_ref[:, core, 0] = y[:, core * c:(core + 1) * c].reshape(q, 2, r, c)


def wgrad_rows(a, b, groups):
    s, m = a.shape
    n = b.shape[1]
    q, r, c = 2 * m // n, n // groups // 4, n // 2
    return pl.pallas_call(
        wgrad_rows_kernel, grid=(groups,),
        in_specs=[pl.BlockSpec((s, m // groups), lambda i: (0, i)), pl.BlockSpec((s, n), lambda i: (0, 0))],
        out_specs=pl.BlockSpec((q, 2, 1, 2, r, c), lambda i: (0, 0, i, 0, 0, 0)),
        out_shape=jax.ShapeDtypeStruct((q, 2, groups, 2, r, c), bf16),
        cost_estimate=pl.CostEstimate(flops=2 * s * m * n, bytes_accessed=2 * (s * (m + n) + m * n),
                                      transcendentals=0), name="wgrad_rows")(a, b)


def pad128(n):
    return -(-n // 128) * 128


def small_row(vectors):
    wide = [jnp.pad(v.astype(f32), (0, pad128(v.shape[0]) - v.shape[0])) for v in vectors]
    return jnp.concatenate([v[None] for v in wide], axis=1)


def unpack(ref, sizes, groups):
    out, base = [], 0
    for size in sizes:
        wide, full = pad128(size), size * groups
        total = None
        for f in range(groups):
            x = ref[f, :, base:base + wide]
            if full > wide:
                x = jnp.concatenate([x, jnp.zeros((1, full - wide), f32)], axis=1)
            if f > 0:
                x = pltpu.roll(jnp.broadcast_to(x, (8, full)), f * size, 1)[0:1]
            total = x if total is None else total + x
        out.append(total)
        base += wide
    return out


def flat(ref, lo, hi):
    groups, _, rows, _ = ref.shape
    if rows % 16 == 0:
        return ref[:, :, :, lo:hi].reshape(groups * 4 * rows, hi - lo)
    parts = [jnp.concatenate([ref[f, i, :, lo:hi].astype(f32) for i in range(4)], axis=0).astype(bf16) for f in range(groups)]
    return jnp.concatenate(parts, axis=0)


def front_kernel(shape, sizes, rows, *refs):
    len_ref, tok_ref, flag_ref, cos_ref, sin_ref, condp_ref, small_ref = refs[:7]
    ins = refs[7:12]
    att_ref, lse_ref, vpre_ref, vmid_ref, b1_ref, n1t_hbm, qkv_hbm = refs[12:19]
    outs = refs[19:24]
    n1, n1t, qkv, wq, ada, smalls, loads, stores = refs[24:32]
    gsems, dsems = refs[32:38], refs[38:40]
    step, steps = pl.program_id(0), pl.num_programs(0)
    s, d = tok_ref.shape
    p = Place(shape)
    g = Gather(p, ins, outs, gsems)
    direct = Direct(p, small_ref, smalls, dsems)
    save = [pltpu.make_async_copy(n1t, n1t_hbm, stores.at[0]), pltpu.make_async_copy(qkv, qkv_hbm, stores.at[1])]

    @pl.when(step == 0)
    def _():
        greet(gather_peers(p, True))
        direct.start()
        g.start(0)
        g.start(1)
        g.after(0, 0)
        g.after(1, 0)
        for w in (2, 3, 4):
            g.start(w)
        for t in range(1, p.bits):
            g.after(0, t)
        g.finish(0)
        direct.finish()
        fetch = pltpu.make_async_copy(outs[0], ada, loads.at[0])
        fetch.start()
        gain1, gain2, b2, emb, b1, bada = unpack(smalls, sizes, p.groups)
        fetch.wait()
        condp = condp_ref[...]
        cond = condp / (1.0 + jnp.exp(-condp))
        stack = jnp.concatenate(list(split3(cond)) + [jnp.zeros((5, cond.shape[1]), f32)], axis=0).astype(bf16)
        mod = colsum(dot(stack, flat(ada, 0, 128), NT)) + bada
        shift_a, scale_a, gate_a, shift_m, scale_m, gate_m = (mod[:, i * d:(i + 1) * d] for i in range(6))
        vpre_ref[...] = jnp.concatenate([emb, gain1, scale_a, shift_a, jnp.zeros((4, d), f32)], axis=0)
        vmid_ref[...] = jnp.concatenate([emb, gain2, scale_m, shift_m, gate_a, gate_m, b2, jnp.zeros((1, d), f32)], axis=0)
        b1_ref[...] = b1
        amp = gain1 * (1.0 + scale_a)

        @pl.loop(0, s // rows)
        def _(i):
            cut = pl.ds(pl.multiple_of(i * rows, rows), rows)
            h0 = jnp.where(flag_ref[cut, :] == 1, emb, tok_ref[cut, :].astype(f32))
            x = norm_parts(h0)[0] * amp + shift_a
            n1[cut, :] = x.astype(bf16)
            n1t[:, cut] = x.T.astype(bf16)

        for t in range(1, p.bits):
            g.after(1, t)
        g.finish(1)
        fetch = pltpu.make_async_copy(outs[1], wq, loads.at[1])
        fetch.start()
        fetch.wait()

        @pl.loop(0, s // rows)
        def _(i):
            cut = pl.ds(pl.multiple_of(i * rows, rows), rows)
            x = n1[cut, :]
            cos, sin = cos_ref[cut, :], sin_ref[cut, :]
            for part in range(3):
                y = dot(x, flat(wq, part * d, (part + 1) * d))
                for c in range(d // 128):
                    lo = part * d + c * 128
                    u = y[:, c * 128:(c + 1) * 128]
                    if part < 2:
                        u = u * cos + swap_halves(u) * sin
                        if part == 0:
                            u = u * QSCALE
                    qkv[cut, lo:lo + 128] = u.astype(bf16)

        for c in save:
            c.start()

    @pl.when(step == 1)
    def _():
        g.after(2, 0)
        g.after(3, 0)

    @pl.when(step == 4)
    def _():
        g.after(4, 0)

    @pl.when(step > 0)
    def _():
        pair = step - 1
        col = lambda base: qkv.at[:, pl.ds(pl.multiple_of(base + pair * 128, 128), 128)]
        attn_fwd_body(len_ref, col(0), col(d), col(2 * d), att_ref, lse_ref, rows, pair)

    @pl.when(step == steps - 1)
    def _():
        for t in range(1, p.bits):
            for w in (2, 3, 4):
                g.after(w, t)
        for w in (2, 3, 4):
            g.finish(w)
        for c in save:
            c.wait()


def front_call(shape, length, tok, flag, cos, sin, condp, small, ws, sizes, rows=256):
    groups = shape["fsdp"]
    s, d = tok.shape
    pairs = d // 128
    sd = jax.ShapeDtypeStruct
    once = pl.Buffered(1)
    whole = lambda dims: pl.BlockSpec(dims, lambda i: (0, 0), pipeline_mode=once)
    sem = pltpu.SemaphoreType.DMA
    gathered = [gather_shape(w, groups) for w in ws]
    ff = sizes[4] * groups
    res = pl.pallas_call(
        functools.partial(front_kernel, shape, sizes, rows), grid=(pairs + 1,),
        in_specs=[pl.BlockSpec(memory_space=pltpu.SMEM), whole((s, d)), whole((s, 1)), whole((s, 128)), whole((s, 128)),
                  whole((1, 128))] + [ANY] * (1 + len(ws)),
        out_specs=[pl.BlockSpec((s, 128), lambda i: (0, jnp.maximum(i - 1, 0))), whole((s, 128)), whole((8, d)),
                   whole((8, d)), whole((1, ff))] + [ANY] * (2 + len(ws)),
        out_shape=[sd((s, d), bf16), sd((s, 128), f32), sd((8, d), f32), sd((8, d), f32), sd((1, ff), f32),
                   sd((d, s), bf16), sd((s, 3 * d), bf16)] + gathered,
        scratch_shapes=[pltpu.VMEM((s, d), bf16), pltpu.VMEM((d, s), bf16), pltpu.VMEM((s, 3 * d), bf16),
                        pltpu.VMEM(gathered[1].shape, bf16), pltpu.VMEM(gathered[0].shape, bf16),
                        pltpu.VMEM((groups,) + small.shape, f32), sem((2,)), sem((2,))]
        + Gather.scratch(len(ws), groups) + Direct.scratch(groups),
        compiler_params=pltpu.CompilerParams(collective_id=1, has_side_effects=True, vmem_limit_bytes=60000 * 1024),
        cost_estimate=pl.CostEstimate(flops=8 * s * s * d + 6 * s * d * d, bytes_accessed=20 * s * d,
                                      transcendentals=s * s * 12),
        name="front")(length, tok, flag, cos, sin, condp, small, *[quarter(w) for w in ws])
    att, lse, vpre, vmid, b1, n1t, qkv = res[:7]
    return att, lse, vpre, vmid, b1, n1t, qkv, [r.reshape(-1, r.shape[-1]) for r in res[7:]]

def f32_rows_dot(row, weights):
    parts = split3(row)
    stack = jnp.concatenate(list(parts) + [jnp.zeros((5, row.shape[1]), f32)], axis=0).astype(bf16)
    return colsum(dot(stack, weights))


class Small:
    def __init__(self, place, scratch):
        self.p = place
        (self.ag, self.rows, self.ab, self.bs, self.bm, self.bb, self.bg, self.s1, self.r1, self.s2, self.r2) = scratch

    @staticmethod
    def widths(shape, d, ff, n_mod):
        groups = shape["fsdp"]
        part = n_mod // groups
        return -(-(d // groups) // 128) * 128, ff // groups, part if part % 128 == 0 else n_mod

    @staticmethod
    def scratch(shape, d, ff, n_mod):
        groups, lines = shape["fsdp"], shape["dp"]
        wide, fpart, gpart = Small.widths(shape, d, ff, n_mod)
        vm = lambda *dims: pltpu.VMEM(dims, f32)
        sem = pltpu.SemaphoreType.DMA
        return [vm(groups, 1, n_mod), vm(groups, 8, d), vm(groups, 1, ff), vm(lines, 8, wide), vm(lines, groups, 384),
                vm(lines, 1, fpart), vm(lines, groups, gpart), sem((groups, 3)), sem((groups, 3)), sem((lines, 4)),
                sem((lines, 4))]

    def peers(self):
        p = self.p
        return [(p.dp, xor(p.me, m)) for m in range(1, p.groups)] + [(xor(p.dp, m), p.me) for m in range(1, p.lines)]

    def copies(self, stage, m, arrived):
        p = self.p
        if stage == 1:
            bufs, ss, rs = (self.ag, self.rows, self.ab), self.s1, self.r1
            where, slot = (p.dp, xor(p.me, m)), xor(p.me, m) if arrived else p.me
        else:
            bufs, ss, rs = (self.bs, self.bm, self.bb, self.bg), self.s2, self.r2
            where, slot = (xor(p.dp, m), p.me), xor(p.dp, m) if arrived else p.dp
        return [remote(b.at[slot], b.at[slot], ss.at[m, i], rs.at[m, i], where) for i, b in enumerate(bufs)]

    def spread(self, stage):
        for m in range(1, self.p.groups if stage == 1 else self.p.lines):
            for c in self.copies(stage, m, False):
                c.start()

    def collect(self, stage):
        for m in range(1, self.p.groups if stage == 1 else self.p.lines):
            for c in self.copies(stage, m, True):
                c.wait_recv()

    def settle(self):
        for stage in (1, 2):
            for m in range(1, self.p.groups if stage == 1 else self.p.lines):
                for c in self.copies(stage, m, False):
                    c.wait_send()

    def first(self, sums, sb1, sums1, vec_pre, vec_mid, condp, meta, ada):
        me = self.p.me
        d = sums.shape[1]
        ggm, gb2, a2, s2, gga, st0, st1, st2 = (sums[i:i + 1] for i in range(8))
        a1, s1, gemb = (sums1[i:i + 1] for i in range(3))
        gain1, scale_a, gain2, scale_m = vec_pre[1:2], vec_pre[2:3], vec_mid[1:2], vec_mid[2:3]
        gm = jnp.concatenate([s1, a1 * gain1, gga, s2, a2 * gain2, ggm], axis=1)
        sig = 1.0 / (1.0 + jnp.exp(-condp))
        gc = f32_rows_dot(gm, ada) * (sig * (1.0 + condp * (1.0 - sig)))
        lane = lax.broadcasted_iota(jnp.int32, (1, 128), 1)
        total = lambda x: jnp.sum(x, axis=1, keepdims=True)
        stat = jnp.where(lane == 0, total(st0), jnp.where(lane == 1, total(st1), jnp.where(lane == 2, total(st2), meta)))
        tail = jnp.concatenate([gc, condp * sig, stat, jnp.zeros((1, d - 384), f32)], axis=1)
        self.ag[me] = gm
        self.ab[me] = sb1
        self.rows[me] = jnp.concatenate([(1.0 + scale_a) * a1, (1.0 + scale_m) * a2, gb2, gemb, tail,
                                         jnp.zeros((3, d), f32)], axis=0)
        self.spread(1)

    def second(self):
        p = self.p
        self.collect(1)
        d = self.rows.shape[2]
        wide, fpart, gpart = self.bs.shape[2], self.bb.shape[2], self.bg.shape[2]
        total = self.rows[0]
        for f in range(1, p.groups):
            total = total + self.rows[f]
        self.bs[p.dp] = pltpu.roll(total, (d - p.me * (d // p.groups)) % d, 1)[:, :wide]
        self.bm[p.dp] = jnp.concatenate([self.rows[f, 4:5, :384] for f in range(p.groups)], axis=0)
        cut = pl.ds(pl.multiple_of(p.me * fpart, 128), fpart)
        part = self.ab[0, :, cut]
        for f in range(1, p.groups):
            part = part + self.ab[f, :, cut]
        self.bb[p.dp] = part
        n_mod = self.ag.shape[2]
        cut = slice(None) if gpart == n_mod else pl.ds(pl.multiple_of(p.me * gpart, 128), gpart)
        self.bg[p.dp] = jnp.concatenate([self.ag[f, :, cut] for f in range(p.groups)], axis=0)
        self.spread(2)

    def third(self, norms_ref, gb1_ref, gada_ref, gbada_ref, table_ref, rms_ref, d):
        p = self.p
        self.collect(2)
        total, part = self.bs[0], self.bb[0]
        for z in range(1, p.lines):
            total = total + self.bs[z]
            part = part + self.bb[z]
        norms_ref[...] = total
        gb1_ref[...] = part
        mods = jnp.concatenate([self.bg[z] for z in range(p.lines)], axis=0)
        info = jnp.concatenate([self.bm[z] for z in range(p.lines)], axis=0)
        gcs, conds, stat = info[:, :128], info[:, 128:256], info[:, 256:384]
        highest = lax.Precision.HIGHEST
        gada_ref[...] = lax.dot_general(mods, conds, TN, precision=highest, preferred_element_type=f32)
        gbada_ref[...] = colsum(mods)
        ids = stat[:, 4:5].astype(jnp.int32)
        hot = (lax.broadcasted_iota(jnp.int32, (ids.shape[0], table_ref.shape[0]), 1) == ids).astype(f32)
        table_ref[...] = lax.dot_general(hot, gcs, TN, precision=highest, preferred_element_type=f32)
        stat = colsum(stat)
        rms_ref[...] = jnp.sqrt(stat / (stat[:, 3:4] * d))


def small_shapes(shape, d, ff, n_mod, table_rows):
    wide, fpart, gpart = Small.widths(shape, d, ff, n_mod)
    sd = lambda *dims: jax.ShapeDtypeStruct(dims, f32)
    return [sd(8, wide), sd(1, fpart), sd(gpart, 128), sd(1, gpart), sd(table_rows, 128), sd(1, 128)]


def small_results(shape, res, sizes):
    norms, gb1, gada, gbada, table, rms = res
    n_ada = sizes[5]
    if gada.shape[0] != n_ada:
        me = lax.axis_index("fsdp")
        gada = lax.dynamic_slice_in_dim(gada, me * n_ada, n_ada, axis=0)
        gbada = lax.dynamic_slice_in_dim(gbada, me * n_ada, n_ada, axis=1)
    g1, g2, gb2, gemb = (norms[i, :sizes[i]] for i in range(4))
    return g1, g2, gb2, gemb, gb1[0], gada, gbada[0], table, rms[0, :3]


def tail_kernel(shape, counts, rows, post, pairs, inner, *refs):
    n = len(counts)
    extra, refs = refs[21:21 + 2 * inner], refs[:21] + refs[21 + 2 * inner:]
    m = n - 1 - inner
    (len_ref, q_ref, k_ref, v_ref, o_ref, g_ref, lse_ref, cos_ref, sin_ref, n1_ref, w_ref, tok_ref, flag_ref, gh1_ref,
     vpre_ref, vmid_ref, sums_ref, sb1_ref, condp_ref, meta_ref, ada_ref) = refs[:21]
    srcs, outs, work = refs[21:21 + m], refs[21 + m:28 + m + n], refs[28 + m + n:]
    igrad_ref, reduced, small_out = outs[0], outs[1:1 + n], outs[1 + n:]
    dqs, dks, dvs, dqkv, gq, sums1 = work[:6]
    held, work = work[6:6 + inner], work[6 + inner:]
    rscratch, sscratch = work[:21], work[21:]
    step, steps = pl.program_id(0), 2 * pairs + post
    p = Place(shape)
    r = Reduce(p, counts, ["rows"] + ["cols"] * (n - 2) + ["qkv"], list(srcs) + list(held) + [gq], reduced, rscratch, 2, 2)
    small = Small(p, sscratch)

    @pl.when(step == 0)
    def _():
        r.greet(small.peers())
        r.begin(0)

    r.tick(2 * step)

    if inner:
        n2_ref, gpre_ref = extra
        held_ref = held[0]

        @pl.when(step < held_ref.shape[0] // 2)
        def _():
            y = dot(n2_ref[...], gpre_ref[...], TN).astype(bf16)
            _, _, gr, _, rr, c = held_ref.shape
            for core in (0, 1):
                z = y[:, core * c:(core + 1) * c].reshape(gr, 2, 2, rr, c)
                for half in (0, 1):
                    held_ref[2 * step + half, core] = z[:, half]

    @pl.when(step < 2 * pairs)
    def _():
        pair, head = step // 2, step % 2

        def emit(*parts):
            for i, x in enumerate(parts):
                dqkv[i, pair] = x
            y = dot(n1_ref[...], jnp.concatenate(parts, axis=1)).astype(bf16)
            _, _, g, _, rr, c = gq.shape
            y = y.reshape(g, 2, 2, rr, c)
            for half in (0, 1):
                gq[2 * (pair // 2) + half, pair % 2] = y[:, half]

        attn_bwd_body(len_ref, q_ref, k_ref, v_ref, o_ref, g_ref, lse_ref, cos_ref, sin_ref, dqs, dks, dvs, rows,
                      pair, head, emit, lambda: r.tick(2 * step + 1))

    @pl.when(step >= 2 * pairs)
    def _():
        i = step - 2 * pairs
        m = tok_ref.shape[0]
        cut = pl.ds(pl.multiple_of(i * m, m), m)
        grads = [jnp.concatenate([dqkv[a, b, cut, :] for b in range(pairs)], axis=1) for a in range(3)]
        masked = flag_ref[...] == 1
        h0 = jnp.where(masked, vpre_ref[0:1, :], tok_ref[...].astype(f32))
        igrad_ref[...], new = post_rows(grads, h0, masked, gh1_ref[...], vpre_ref[1:2, :], vpre_ref[2:3, :], w_ref)
        sums1[...] = jnp.where(i == 0, new, sums1[...] + new)
        r.tick(2 * step + 1)

    @pl.when(step == steps - 1)
    def _():
        small.first(sums_ref[...], sb1_ref[...], sums1[...], vpre_ref[...], vmid_ref[...], condp_ref[...], meta_ref[...],
                    ada_ref[...])
        last = max(r.ticks, 2 * steps)
        marks = [2 * steps, min(2 * steps + SPLIT[0], last), min(2 * steps + SPLIT[1], last), last]
        for n in range(3):
            @pl.loop(marks[n], marks[n + 1])
            def _(t):
                r.tick(t)
            if n == 0:
                small.second()
            if n == 1:
                small.third(*small_out, sums1.shape[1])
        r.drain()
        small.settle()


SPLIT = (3, 8)


def tail_call(shape, length, qkv, att, gatt, lse, cos, sin, n1t, w, tok, flag, gh1, vpre, vmid, sums, sb1, condp, meta,
              ada, grads, n2, gpre, table_rows, rows=256):
    groups = shape["fsdp"]
    s, d3 = qkv.shape
    d = d3 // 3
    pairs = d // 128
    r, c = 2 * grads[0].shape[-2], grads[0].shape[-1]
    post = 256 if r % 32 == 0 else 128
    ff, n_mod = sb1.shape[1], ada.shape[0]
    blocks = s // post
    steps = 2 * pairs + blocks
    inner = int(r % 32 == 0)
    if not inner:
        grads = grads + [wgrad_cols(n2, gpre, groups)]
    chunks = [grads[0].shape[0], grads[1].shape[0], 2 * ff // d]
    counts = chunks + [pairs]
    pair = lambda i: jnp.minimum(i // 2, pairs - 1)
    blk = lambda i: jnp.maximum(i - 2 * pairs, 0)
    once = pl.Buffered(1)
    col = lambda base: pl.BlockSpec((s, 128), lambda i: (0, base + pair(i)))
    whole = lambda a: pl.BlockSpec(a.shape, lambda i: (0,) * a.ndim, pipeline_mode=once)
    row = lambda cc: pl.BlockSpec((post, cc), lambda i: (blk(i), 0))
    sd = jax.ShapeDtypeStruct
    shard = d // groups
    red = [sd((shard * (g // 2), d), bf16) if i == 0 else sd((shard, d * (g // 2)), bf16)
           for i, g in enumerate(chunks)] + [sd((shard, d3), bf16)]
    smalls = small_shapes(shape, d, ff, n_mod, table_rows)
    const = lambda x: pl.BlockSpec(x.shape, lambda i: (0, 0), pipeline_mode=once)
    res = pl.pallas_call(
        functools.partial(tail_kernel, shape, counts, rows, blocks, pairs, inner), grid=(steps,),
        in_specs=[pl.BlockSpec(memory_space=pltpu.SMEM), col(0), col(pairs), col(2 * pairs), col(0), col(0), whole(lse),
                  whole(cos), whole(sin), whole(n1t), whole(w), row(d), row(1), row(d)]
        + [whole(x) for x in (vpre, vmid, sums, sb1, condp, meta, ada)]
        + [whole(n2), pl.BlockSpec((s, d), lambda i: (0, jnp.minimum(i, ff // d - 1)))] * inner + [ANY] * len(grads),
        out_specs=[row(d)] + [ANY] * len(red) + [const(x) for x in smalls],
        out_shape=[sd((s, d), bf16)] + red + smalls,
        scratch_shapes=[pltpu.VMEM((128, s), f32), pltpu.VMEM((s, 128), f32), pltpu.VMEM((s, 128), f32),
                        pltpu.VMEM((3, pairs, s, 128), bf16), pltpu.VMEM((pairs, 2, groups, 2, r // 2, c), bf16),
                        pltpu.VMEM((8, d), f32)]
        + [pltpu.VMEM((2 * ff // d, 2, groups, 2, r // 2, c), bf16)] * inner
        + Reduce.scratch(sum(counts), groups, r, c) + Small.scratch(shape, d, ff, n_mod),
        compiler_params=pltpu.CompilerParams(collective_id=3, has_side_effects=True, vmem_limit_bytes=65000 * 1024),
        cost_estimate=pl.CostEstimate(flops=30 * s * s * d, bytes_accessed=40 * s * d, transcendentals=s * s * 12),
        name="tail")(length, qkv, qkv, qkv, att, gatt, lse, cos, sin, n1t, w, tok, flag, gh1, vpre, vmid, sums, sb1, condp,
                     meta, ada, *([n2, gpre] * inner), *grads)
    return res[0], res[1:1 + len(red)], res[1 + len(red):]


def widen_kernel(*refs):
    n = len(refs) // 2
    for x, y in zip(refs[:n], refs[n:]):
        y[...] = x[...].astype(f32)


def widen(arrays, pieces):
    specs = [pl.BlockSpec((a.shape[0], a.shape[1] // pieces), lambda i: (0, i)) for a in arrays]
    return pl.pallas_call(
        widen_kernel, grid=(pieces,), in_specs=specs, out_specs=specs,
        out_shape=[jax.ShapeDtypeStruct(a.shape, f32) for a in arrays],
        cost_estimate=pl.CostEstimate(flops=0, bytes_accessed=6 * sum(a.size for a in arrays), transcendentals=0),
        name="widen")(*arrays)
from jax.sharding import PartitionSpec as P

highest = lax.Precision.HIGHEST


def rotary_tables(length):
    half = HD // 2
    rate = 1.0 / 10000.0 ** (jnp.arange(half, dtype=f32) * 2.0 / HD)
    angle = jnp.arange(length, dtype=f32)[:, None] * rate[None, :]
    angle = jnp.concatenate([angle] * (128 // half), axis=-1)
    sign = jnp.where(jnp.arange(128) % HD < half, -1.0, 1.0)
    return jnp.cos(angle), jnp.sin(angle) * sign


def per_device(shape, tokens, hidden_token_indicator, lengths, time_ids, cotangent, gain_one, w_qkv, w_out, gain_two,
               w_fc1, b_fc1, w_fc2, b_fc2, w_ada, b_ada, mask_embed, time_table):
    groups = shape["fsdp"]
    s, d = tokens.shape[1:]
    ff = b_fc1.shape[0] * groups
    tok, cot = tokens[0], cotangent[0]
    flag = hidden_token_indicator.reshape(s, 1)
    sizes = [v.shape[0] for v in (gain_one, gain_two, b_fc2, mask_embed, b_fc1, b_ada)]
    cond_pre = lax.dynamic_slice_in_dim(time_table, time_ids[0], 1, axis=0)
    cos, sin = rotary_tables(s)
    att, lse, vec_pre, vec_mid, b1, n1, qkv, (ada_all, qkv_all, out_all, fc1_all, fc2_all) = front_call(
        shape, lengths, tok, flag, cos, sin, cond_pre, small_row((gain_one, gain_two, b_fc2, mask_embed, b_fc1, b_ada)),
        [w_ada, w_qkv, w_out, w_fc1, w_fc2], sizes)
    out, gh1, gatt, n2, act, gm, gpre, gap, sums, gb1 = mid_call(
        lengths, att, tok, flag, cot, vec_mid, b1, out_all, fc1_all, fc2_all)
    g_fc2 = wgrad_rows(act, gm, groups)
    g_out = wgrad_cols(att, gap, groups)
    meta = jnp.concatenate([jnp.zeros((3,), f32), lengths.astype(f32), time_ids.astype(f32), jnp.zeros((123,), f32)])[None]
    igrad, (r_fc2, r_out, r_fc1, r_qkv), smalls = tail_call(
        shape, lengths, qkv, att, gatt, lse, cos, sin, n1, qkv_all, tok, flag, gh1, vec_pre, vec_mid, sums, gb1, cond_pre,
        meta, ada_all, [g_fc2, g_out], n2, gpre, time_table.shape[0])
    g1, g2, gb2, gemb, gb1, g_ada, gbada, table, rms = small_results(shape, smalls, sizes)
    r_fc2, r_fc1, r_out, r_qkv = widen([r_fc2, r_fc1, r_out, r_qkv], d // 256)
    return (out[None], igrad[None], g1, r_qkv, r_out, g2, r_fc1, gb1, r_fc2, gb2, g_ada, gbada, gemb, table, rms)


def solution(mesh):
    both = ("dp", "fsdp")
    f1, f2 = P("fsdp"), P("fsdp", None)
    placed = (P(both, None, None), P(both, None), P(both), P(both), P(both, None, None), f1, f2, f2, f1, f2, f1, f2, f1,
              f2, f1, f1, P())
    outs = (P(both, None, None), P(both, None, None), f1, f2, f2, f1, f2, f1, f2, f1, f2, f1, f1, P(), P())
    return jax.shard_map(functools.partial(per_device, dict(mesh.shape)), mesh=mesh, in_specs=placed, out_specs=outs,
                         check_vma=False)
```
